32 devices in a mesh: fsdp: 32 (over z, y, x, core).
Axes of the slice: x: 2, y: 2, z: 4, core: 2. Of those that a mesh axis runs over, the one named last changes fastest.
Arguments:
- hidden_in: bfloat16 [4096, 2048], P('fsdp'), may hold values from -6 to 6
- out_grad: bfloat16 [4096, 2048], P('fsdp'), may hold values from -6 to 6
- seq_lengths: int32 [64], replicated, may hold values from 16 to 112, as said below
- seq_device: int32 [64], replicated, may hold values from 0 to 31, as said below
- attn_gain: bfloat16 [2048], P('fsdp'), may hold values from 0.5 to 1.5
- q_gain: bfloat16 [128], P('fsdp'), may hold values from 0.5 to 2
- k_gain: bfloat16 [128], P('fsdp'), may hold values from 0.5 to 2
- w_query: bfloat16 [2048, 2048], P('fsdp'), may hold values from -0.125 to 0.125
- w_key: bfloat16 [2048, 1024], P('fsdp'), may hold values from -0.125 to 0.125
- w_value: bfloat16 [2048, 1024], P('fsdp'), may hold values from -0.125 to 0.125
- w_out: bfloat16 [2048, 2048], P('fsdp'), may hold values from -0.5 to 0.5
- mlp_gain: bfloat16 [2048], P('fsdp'), may hold values from 0.5 to 1.5
- w_gate: bfloat16 [2048, 6144], P('fsdp'), may hold values from -0.125 to 0.125
- w_up: bfloat16 [2048, 6144], P('fsdp'), may hold values from -0.125 to 0.125
- w_down: bfloat16 [6144, 2048], P('fsdp'), may hold values from -0.078125 to 0.078125
Outputs:
- hidden_out: bfloat16 [4096, 2048], P('fsdp')
- input_grad: float32 [4096, 2048], P('fsdp')
- grad_attn_gain: float32 [2048], P('fsdp')
- grad_q_gain: float32 [128], P('fsdp')
- grad_k_gain: float32 [128], P('fsdp')
- grad_w_query: float32 [2048, 2048], P('fsdp')
- grad_w_key: float32 [2048, 1024], P('fsdp')
- grad_w_value: float32 [2048, 1024], P('fsdp')
- grad_w_out: float32 [2048, 2048], P('fsdp')
- grad_mlp_gain: float32 [2048], P('fsdp')
- grad_w_gate: float32 [2048, 6144], P('fsdp')
- grad_w_up: float32 [2048, 6144], P('fsdp')
- grad_w_down: float32 [6144, 2048], P('fsdp')
The draws below stay inside these ranges and needn't reach their ends.
Inputs may be any that keep to these rules, and one draw needn't show every extreme that they name: `seq_lengths`: each sequence has at least 16 tokens; the two sequences of one device fill together at most 128 slots, and in every draw some device's fill all 128. `seq_device`: every device holds exactly two sequences.
All inputs are finite; a program needn't handle non-finite values.
Results may differ from the reference program's by a relative error of at most 0.017.
Values may be sent and summed in bfloat16 or wider, within the bound.
A program may use at most 384 MiB of HBM per device.

```python
import math
import jax
import jax.numpy as jnp
from jax import lax

D = 2048
H = 16
KVH = 8
HD = 128
FF = 6144
CAP = 128
SEQ_MIN = 16
SEQS = 64
SLOTS = 4096
N_FSDP = 32


def deal_sequences(key):
    base = jax.random.fold_in(key, 4242)
    owners = SEQS // 2
    key_total, key_full, key_first, key_order = jax.random.split(base, 4)
    totals = jax.random.randint(key_total, (owners,), CAP // 2, CAP + 1)
    full = jax.random.randint(key_full, (), 0, owners)
    totals = jnp.where(jnp.arange(owners) == full, CAP, totals)
    first = jax.random.randint(key_first, (owners,), SEQ_MIN, totals - SEQ_MIN + 1)
    order = jax.random.permutation(key_order, SEQS)
    device = order // 2
    lengths = jnp.where(order % 2 == 0, first[device], totals[device] - first[device])
    return (lengths.astype(jnp.int32), device.astype(jnp.int32))


def draw_seq_lengths(key, part):
    return deal_sequences(key)[0]


def draw_seq_device(key, part):
    return deal_sequences(key)[1]


def block_scale(rng, shape, cuts, low, top_value):
    def one(dim, shards_of):
        draws = jax.random.uniform(jax.random.fold_in(jax.random.fold_in(rng, 6), dim), (shards_of,), jnp.float32, low / len(cuts), top_value / len(cuts))
        return jnp.repeat(jnp.exp(draws), shape[dim] // shards_of).reshape((-1,) + (1,) * (len(shape) - dim - 1))

    level = one(*cuts[0])
    for cut in cuts[1:]:
        level = level * one(*cut)
    return level


def centred(key, shape, width, limit, cuts=(), held_as=jnp.bfloat16):
    values = jax.random.normal(key, shape, jnp.float32) * width
    if len(cuts) > 0:
        values = block_scale(key, shape, cuts, -0.22, 0.18) * values
    return jnp.clip(values, min=-limit, max=limit).astype(held_as)


def setup_inputs(seed: int = 0) -> dict:
    key_list = jax.random.split(jax.random.key(seed), 16)
    return {
        "hidden_in": centred(key_list[0], (SLOTS, D), 1.0, 6.0, ((0, 32),)),
        "out_grad": centred(key_list[1], (SLOTS, D), 1.0, 6.0, ((0, 32),)),
        "seq_lengths": draw_seq_lengths(jax.random.fold_in(key_list[15], 71), 0),
        "seq_device": draw_seq_device(jax.random.fold_in(key_list[15], 71), 0),
        "attn_gain": jnp.clip(1.0 + 0.1 * jax.random.normal(key_list[4], (D,), jnp.float32), 0.5, 1.5).astype(jnp.bfloat16),
        "q_gain": jnp.clip(jnp.exp(math.log(2.0) - 1.3862944 * jax.random.uniform(key_list[5], (HD,), jnp.float32) ** block_scale(key_list[5], (HD,), ((0, 32),), -0.2, 0.2)), 0.5, 2.0).astype(jnp.bfloat16),
        "k_gain": jnp.clip(jnp.exp(math.log(2.0) - 1.3862944 * jax.random.uniform(key_list[6], (HD,), jnp.float32) ** block_scale(key_list[6], (HD,), ((0, 32),), -0.2, 0.2)), 0.5, 2.0).astype(jnp.bfloat16),
        "w_query": centred(key_list[7], (D, H * HD), D ** -0.5, 0.125, ((0, 32),)),
        "w_key": centred(key_list[8], (D, KVH * HD), D ** -0.5, 0.125, ((0, 32),)),
        "w_value": centred(key_list[9], (D, KVH * HD), D ** -0.5, 0.125, ((0, 32),)),
        "w_out": centred(key_list[10], (H * HD, D), (H * HD // 16) ** -0.5, 0.5, ((0, 32),)),
        "mlp_gain": jnp.clip(1.0 + 0.1 * jax.random.normal(key_list[11], (D,), jnp.float32), 0.5, 1.5).astype(jnp.bfloat16),
        "w_gate": centred(key_list[12], (D, FF), D ** -0.5, 0.125, ((0, 32),)),
        "w_up": centred(key_list[13], (D, FF), D ** -0.5, 0.125, ((0, 32),)),
        "w_down": centred(key_list[14], (FF, D), FF ** -0.5, 0.078125, ((0, 32),)),
    }


epsilon = 1e-06
rope_base = 1000000.0
masked_score = -1e+30
highest = lax.Precision.HIGHEST

@jax.custom_vjp
def low(v):
    return lax.optimization_barrier(v.astype(jnp.bfloat16)).astype(jnp.float32)

@jax.custom_vjp
def low_back(v):
    return v

def low_keep(v):
    return (low(v), None)

def low_pass(kept, grad):
    return (grad,)

def back_keep(v):
    return (v, None)

def back_low(kept, grad):
    return (low(grad),)
low.defvjp(low_keep, low_pass)
low_back.defvjp(back_keep, back_low)

def layout(seq_lengths, seq_device, owner, slots):
    owned = seq_device == owner
    counts = jnp.where(owned, seq_lengths, 0)
    starts = jnp.cumsum(counts) - counts
    places = jnp.arange(slots, dtype=jnp.int32)
    inside = owned[:, None] & (places[None, :] >= starts[:, None]) & (places[None, :] < (starts + counts)[:, None])
    labels = jnp.arange(seq_lengths.shape[0], dtype=jnp.int32)
    segment = lax.optimization_barrier(jnp.sum(jnp.where(inside, labels[:, None] + 1, 0), axis=0)) - 1
    position = lax.optimization_barrier(jnp.sum(jnp.where(inside, places[None, :] - starts[:, None], 0), axis=0))
    return (segment.astype(jnp.int32), position.astype(jnp.int32))

def allowed_pairs(segment):
    places = jnp.arange(segment.shape[0], dtype=jnp.int32)
    earlier = places[None, :] < places[:, None]
    same_seq = (segment[:, None] == segment[None, :]) & (segment[:, None] >= 0)
    return (places[:, None] == places[None, :]) | earlier & same_seq

def rmsnorm(values, gain):
    return values * lax.rsqrt(lax.optimization_barrier(jnp.mean(values * values, axis=-1, keepdims=True)) + epsilon) * gain

def rotary(values, position):
    half_dim = values.shape[-1] // 2
    freqs = jnp.power(rope_base, -2.0 * jnp.arange(half_dim, dtype=jnp.float32) / values.shape[-1])
    angles = position.astype(jnp.float32)[:, None] * freqs[None, :]
    cosine = jnp.concatenate([jnp.cos(angles), jnp.cos(angles)], axis=-1)[:, None, :]
    sine = jnp.concatenate([jnp.sin(angles), jnp.sin(angles)], axis=-1)[:, None, :]
    rotated = jnp.concatenate([-values[..., half_dim:], values[..., :half_dim]], axis=-1)
    return values * cosine + rotated * sine

def head_path(raw, gain, position, heads):
    shaped = raw.reshape(raw.shape[0], heads, gain.shape[0])
    return rotary(rmsnorm(shaped, gain), position)

def product(left, right):
    return jnp.dot(left, right, precision=highest, preferred_element_type=jnp.float32)

def attend(block):
    queries, keys, values, segment = block
    scores = low_back(jnp.einsum('qgrd,kgd->grqk', queries, keys, precision=highest)) * HD ** (-0.5)
    logits = jnp.where(allowed_pairs(segment)[None, None], scores, masked_score)
    row_top = lax.optimization_barrier(jnp.max(logits, axis=-1, keepdims=True))
    exponent = jnp.exp(logits - row_top)
    weights = low(exponent / lax.optimization_barrier(jnp.sum(exponent, axis=-1, keepdims=True)))
    mixed = jnp.einsum('grqk,kgd->qgrd', weights, values, precision=highest)
    return mixed.reshape(queries.shape[0], H * HD)

def reference(hidden_in, out_grad, seq_lengths, seq_device, attn_gain, q_gain, k_gain, w_query, w_key, w_value, w_out, mlp_gain, w_gate, w_up, w_down):
    owners = jnp.arange(N_FSDP, dtype=jnp.int32)
    segments, positions = jax.vmap(lambda owner: layout(seq_lengths, seq_device, owner, CAP))(owners)
    position = positions.reshape(N_FSDP * CAP)
    groups = H // KVH

    def forward(inputs, gain_attn, gain_query, gain_key, query_w, key_w, value_w, out_w, gain_mlp, gate_w, up_w, down_w):
        normed = low(rmsnorm(inputs, gain_attn))
        query_raw = low_back(product(normed, query_w))
        key_raw = low_back(product(normed, key_w))
        value_raw = low_back(product(normed, value_w))
        queries = low(head_path(query_raw, gain_query, position, H)).reshape(N_FSDP, CAP, KVH, groups, HD)
        keys = low(head_path(key_raw, gain_key, position, KVH)).reshape(N_FSDP, CAP, KVH, HD)
        values = low(value_raw).reshape(N_FSDP, CAP, KVH, HD)
        mixed = lax.map(jax.checkpoint(attend), (queries, keys, values, segments))
        mixed = low(low_back(mixed.reshape(N_FSDP * CAP, H * HD)))
        middle = inputs + low_back(product(mixed, out_w))
        second = low(rmsnorm(middle, gain_mlp))
        gate_out = low_back(product(second, gate_w))
        up_out = low_back(product(second, up_w))
        hidden = low(jax.nn.silu(gate_out) * up_out)
        return middle + product(hidden, down_w)
    floats = tuple((item.astype(jnp.float32) for item in (hidden_in, attn_gain, q_gain, k_gain, w_query, w_key, w_value, w_out, mlp_gain, w_gate, w_up, w_down)))
    result, pull = jax.vjp(forward, *floats)
    grads = pull(out_grad.astype(jnp.float32))
    return (result.astype(jnp.bfloat16), grads[0], grads[1], grads[2], grads[3], grads[4], grads[5], grads[6], grads[7], grads[8], grads[9], grads[10], grads[11])
```

```python
import functools

import jax
import jax.numpy as jnp
from jax import lax
from jax.experimental import pallas as pl
from jax.experimental.pallas import tpu as pltpu
from jax.sharding import PartitionSpec as P

H = 16
KVH = 8
HD = 128
LINE = 4
RING = 8
MESH = pl.DeviceIdType.MESH
ANY = pl.BlockSpec(memory_space=pl.ANY)
VMEM = pl.BlockSpec(memory_space=pltpu.VMEM)
DMA = pltpu.SemaphoreType.DMA
bf16 = jnp.bfloat16
f32 = jnp.float32


def where_am_i():
    me = lax.axis_index("fsdp")
    core = me % 2
    z = me // RING
    f_bit = 2 + 2 * core
    s_bit = 4 - 2 * core
    first = me + f_bit * (1 - 2 * ((me // f_bit) % 2))
    second = me + s_bit * (1 - 2 * ((me // s_bit) % 2))
    sibling = me + 1 - 2 * core
    return me, z, first, second, sibling


def greet(peers):
    barrier = pltpu.get_barrier_semaphore()
    for peer in peers:
        pl.semaphore_signal(barrier, inc=1, device_id=(peer,), device_id_type=MESH)
    pl.semaphore_wait(barrier, len(peers))


def remote(src, dst, send_sem, recv_sem, device):
    return pltpu.make_async_remote_copy(
        src_ref=src,
        dst_ref=dst,
        send_sem=send_sem,
        recv_sem=recv_sem,
        device_id=(device,),
        device_id_type=MESH,
    )


def line_peers(me):
    return [lax.rem(me + RING * k, RING * LINE) for k in range(1, LINE)]


def on_line(z, k, body):
    for step in ((-k, k) if k else (0,)):

        @pl.when((z + step >= 0) & (z + step < LINE))
        def _(step=step):
            body(step)


def fetch_attn_kernel(
    w_ref, gate_ref, up_ref, w_out, p_out,
    w_tmp, p_tmp, local, up_s, down_s, first_s, second_s, sib_s, recv, ex_send, ex_recv,
):
    me, z, first, second, sibling = where_am_i()
    greet(line_peers(me) + [first, second, sibling])
    col, fcol, scol = me % RING, first % RING, second % RING
    sfcol = (second + first - me) % RING
    width = p_tmp.shape[1] // 2

    def send(src, shard, sems, device):
        return remote(src, w_out.at[shard], sems.at[shard], recv.at[shard], device)

    def arrived(shard):
        send(w_out.at[shard], shard, sib_s, sibling).wait_recv()

    def exchange(k, which):
        peer_z = lax.rem(z + k, LINE)
        src = (gate_ref, up_ref)[which].at[:, pl.ds(pl.multiple_of(peer_z * width, width), width)]
        dst = p_out.at[z, :, pl.ds(which * width, width)]
        return remote(src, dst, ex_send.at[k, which], ex_recv.at[k, which], col + RING * peer_z)

    @pl.when(z < LINE - 1)
    def _():
        send(w_ref, me, up_s, me + RING).start()

    @pl.when(z > 0)
    def _():
        send(w_ref, me, down_s, me - RING).start()

    send(w_ref, me, first_s, first).start()
    send(w_ref, me, second_s, second).start()
    send(w_ref, me, sib_s, sibling).start()
    w_in = pltpu.make_async_copy(w_ref, w_tmp, local.at[0])
    w_in.start()
    p_in = [
        pltpu.make_async_copy(
            ref.at[:, pl.ds(pl.multiple_of(z * width, width), width)],
            p_tmp.at[:, pl.ds(which * width, width)],
            local.at[1 + which],
        )
        for which, ref in enumerate((gate_ref, up_ref))
    ]
    for copy in p_in:
        copy.start()
    for k in range(1, LINE):
        for which in range(2):
            exchange(k, which).start()

    def own(k):
        def body(step):
            shard = me + RING * step
            src = w_out.at[shard]
            arrived(shard)
            if step < 0:

                @pl.when(z < LINE - 1)
                def _():
                    send(src, shard, up_s, me + RING).start()
            else:

                @pl.when(z > 0)
                def _():
                    send(src, shard, down_s, me - RING).start()

            send(src, shard, first_s, first).start()
            send(src, shard, second_s, second).start()
            send(src, shard, sib_s, sibling).start()

        on_line(z, k, body)

    def other(base, k, onward):
        def body(step):
            shard = base + RING * (z + step)
            src = w_out.at[shard]
            arrived(shard)
            if onward:
                send(src, shard, second_s, second).start()
            send(src, shard, sib_s, sibling).start()

        on_line(z, k, body)

    own(1)
    other(fcol, 0, True)
    own(2)
    other(fcol, 1, True)
    other(scol, 0, False)
    w_in.wait()
    w_back = pltpu.make_async_copy(w_tmp, w_out.at[me], local.at[3])
    w_back.start()
    for copy in p_in:
        copy.wait()
    p_back = pltpu.make_async_copy(p_tmp, p_out.at[z], local.at[4])
    p_back.start()
    own(3)
    other(fcol, 2, True)
    other(scol, 1, False)
    other(sfcol, 0, False)
    other(fcol, 3, True)
    other(scol, 2, False)
    other(sfcol, 1, False)
    other(scol, 3, False)
    other(sfcol, 2, False)
    other(sfcol, 3, False)

    def from_sibling(i, carry):
        arrived(2 * i + sibling % 2)
        return carry

    lax.fori_loop(0, RING * LINE // 2, from_sibling, 0)
    w_back.wait()
    p_back.wait()
    for k in range(1, LINE):
        for which in range(2):
            exchange(k, which).wait_send()
            src_z = lax.rem(z + LINE - k, LINE)
            landed = p_out.at[src_z, :, pl.ds(which * width, width)]
            remote(
                landed, landed, ex_send.at[k, which], ex_recv.at[k, which], col + RING * src_z
            ).wait_recv()
    for k in range(LINE):

        @pl.when((z < LINE - 1) & (k <= z))
        def _(k=k):
            send(w_ref, col + RING * k, up_s, me + RING).wait_send()

        @pl.when((z > 0) & (k >= z))
        def _(k=k):
            send(w_ref, col + RING * k, down_s, me - RING).wait_send()

        send(w_ref, col + RING * k, first_s, first).wait_send()
        send(w_ref, col + RING * k, second_s, second).wait_send()
        send(w_ref, fcol + RING * k, second_s, second).wait_send()
        for base in (col, fcol, scol, sfcol):
            send(w_ref, base + RING * k, sib_s, sibling).wait_send()


def fetch_attn(w, gate, up):
    rows, cols = w.shape
    width = gate.shape[1] // LINE
    n = RING * LINE
    return pl.pallas_call(
        fetch_attn_kernel,
        out_shape=(
            jax.ShapeDtypeStruct((n, rows, cols), bf16),
            jax.ShapeDtypeStruct((LINE, rows, 2 * width), bf16),
        ),
        in_specs=[ANY] * 3,
        out_specs=(ANY, ANY),
        scratch_shapes=[
            pltpu.VMEM((rows, cols), bf16),
            pltpu.VMEM((rows, 2 * width), bf16),
            DMA((5,)),
            DMA((n,)),
            DMA((n,)),
            DMA((n,)),
            DMA((n,)),
            DMA((n,)),
            DMA((n,)),
            DMA((LINE, 2)),
            DMA((LINE, 2)),
        ],
        compiler_params=pltpu.CompilerParams(collective_id=0, has_side_effects=True),
        name="fetch_attn",
    )(w, gate, up)


def fetch_mlp_kernel(
    p_ref, d_ref, x_ref, g_ref, gu_out, d_out, x_out, g_out,
    p_tmp, d_tmp, x_tmp, g_tmp, local, up_s, down_s, line_r, first_s, second_s, sib_s, recv,
):
    me, z, first, second, sibling = where_am_i()
    greet(line_peers(me) + [first, second, sibling])
    col, fcol, scol = me % RING, first % RING, second % RING
    sfcol = (second + first - me) % RING
    pieces = LINE + 1

    def spot(piece, shard):
        return gu_out.at[piece, shard] if piece < LINE else d_out.at[shard]

    def source(piece):
        return p_ref.at[piece] if piece < LINE else d_ref

    def send(src, piece, shard, sems, device):
        return remote(
            src, spot(piece, shard), sems.at[piece, shard], recv.at[piece, shard], device
        )

    def arrived(piece, shard):
        send(spot(piece, shard), piece, shard, sib_s, sibling).wait_recv()

    tokens = ((x_ref, x_out), (g_ref, g_out))

    def line_send(src, which, shard, sems, device):
        return remote(
            src,
            tokens[which][1].at[shard],
            sems.at[which, shard],
            line_r.at[which, shard],
            device,
        )

    for which in range(2):

        @pl.when(z < LINE - 1)
        def _(which=which):
            line_send(tokens[which][0], which, z, up_s, me + RING).start()

        @pl.when(z > 0)
        def _(which=which):
            line_send(tokens[which][0], which, z, down_s, me - RING).start()

    for piece in range(pieces):
        send(source(piece), piece, col, first_s, first).start()
        send(source(piece), piece, col, second_s, second).start()
        send(source(piece), piece, col, sib_s, sibling).start()
    moves = (
        (p_ref, p_tmp, gu_out.at[:, col]),
        (d_ref, d_tmp, d_out.at[col]),
        (x_ref, x_tmp, x_out.at[z]),
        (g_ref, g_tmp, g_out.at[z]),
    )
    ins = [pltpu.make_async_copy(m[0], m[1], local.at[i]) for i, m in enumerate(moves)]
    outs = [pltpu.make_async_copy(m[1], m[2], local.at[4 + i]) for i, m in enumerate(moves)]
    for copy in ins:
        copy.start()

    def along(k):
        def body(step):
            shard = z + step
            for which in range(2):
                src = tokens[which][1].at[shard]
                line_send(src, which, shard, up_s, second).wait_recv()
                if step < 0:

                    @pl.when(z < LINE - 1)
                    def _(which=which, src=src):
                        line_send(src, which, shard, up_s, me + RING).start()
                else:

                    @pl.when(z > 0)
                    def _(which=which, src=src):
                        line_send(src, which, shard, down_s, me - RING).start()

        on_line(z, k, body)

    def other(piece, shard, onward):
        arrived(piece, shard)
        if onward:
            send(spot(piece, shard), piece, shard, second_s, second).start()
        send(spot(piece, shard), piece, shard, sib_s, sibling).start()

    other(0, fcol, True)
    other(0, scol, False)
    other(1, fcol, True)
    other(1, scol, False)
    for copy, back in zip(ins, outs):
        copy.wait()
        back.start()
    along(1)
    other(2, fcol, True)
    other(2, scol, False)
    other(3, fcol, True)
    other(3, scol, False)
    along(2)
    other(4, fcol, True)
    other(4, scol, False)
    for piece in range(pieces):
        other(piece, sfcol, False)
    along(3)
    for piece in range(pieces):
        for k in range(RING // 2):
            arrived(piece, 2 * k + sibling % 2)
    for back in outs:
        back.wait()
    for which in range(2):
        for k in range(LINE):

            @pl.when((z < LINE - 1) & (k <= z))
            def _(which=which, k=k):
                line_send(tokens[which][0], which, k, up_s, me + RING).wait_send()

            @pl.when((z > 0) & (k >= z))
            def _(which=which, k=k):
                line_send(tokens[which][0], which, k, down_s, me - RING).wait_send()

    for piece in range(pieces):
        src = source(piece)
        send(src, piece, col, first_s, first).wait_send()
        send(src, piece, col, second_s, second).wait_send()
        send(src, piece, fcol, second_s, second).wait_send()
        for base in (col, fcol, scol, sfcol):
            send(src, piece, base, sib_s, sibling).wait_send()


def fetch_mlp(p, down, tokens, cotangent):
    lines, rows, cols = p.shape
    pieces = LINE + 1
    return pl.pallas_call(
        fetch_mlp_kernel,
        out_shape=(
            jax.ShapeDtypeStruct((LINE, RING, rows, cols), bf16),
            jax.ShapeDtypeStruct((RING,) + down.shape, bf16),
            jax.ShapeDtypeStruct((LINE,) + tokens.shape, bf16),
            jax.ShapeDtypeStruct((LINE,) + cotangent.shape, bf16),
        ),
        in_specs=[ANY] * 4,
        out_specs=(ANY,) * 4,
        scratch_shapes=[
            pltpu.VMEM(p.shape, bf16),
            pltpu.VMEM(down.shape, bf16),
            pltpu.VMEM(tokens.shape, bf16),
            pltpu.VMEM(cotangent.shape, bf16),
            DMA((8,)),
            DMA((2, LINE)),
            DMA((2, LINE)),
            DMA((2, LINE)),
            DMA((pieces, RING)),
            DMA((pieces, RING)),
            DMA((pieces, RING)),
            DMA((pieces, RING)),
        ],
        compiler_params=pltpu.CompilerParams(collective_id=1, has_side_effects=True),
        name="fetch_mlp",
    )(p, down, tokens, cotangent)


def add_rows(out, *terms):
    rows = out.shape[0]

    def body(i, carry):
        at = pl.ds(pl.multiple_of(i * 16, 16), 16)
        total = terms[0][at, :].astype(f32)
        for term in terms[1:]:
            total = total + term[at, :].astype(f32)
        out[at, :] = total.astype(out.dtype)
        return carry

    lax.fori_loop(0, rows // 16, body, 0)


def reduce_mlp_kernel(
    gu_ref, d_ref, ds_ref, y_ref, gu_out, d_out, ds_out, y_out,
    gu_own, gu_sib, gu_sec, gu_fst, d_own, d_sib, d_sec, d_fst, t_own, t_down, t_up,
    load, t_load, c_send, c_recv, s_send, s_recv, f_send, f_recv, down_s, down_r, up_s, up_r,
):
    me, z, first, second, sibling = where_am_i()
    greet([lax.rem(me + RING, RING * LINE), lax.rem(me + RING * (LINE - 1), RING * LINE)]
          + [first, second, sibling])
    core = me % 2
    mine, fst, sec = (me % RING) // 2, (first % RING) // 2, (second % RING) // 2
    far = ((second + first - me) % RING) // 2
    half = d_fst.shape[0] // 2
    last = LINE - 1
    groups = ((0, LINE), (LINE, LINE + 2))

    def block(gu, d, piece, group):
        if group == 0:
            return gu.at[piece]
        return d.at[pl.ds(pl.multiple_of((piece - LINE) * half, half), half)]

    def each(body):
        for group, (lo, hi) in enumerate(groups):

            def step(piece, carry, group=group):
                body(piece, group)
                return carry

            lax.fori_loop(lo, hi, step, 0)

    def stored(target, piece, group):
        if group == 0:
            return gu_ref.at[piece, target]
        return block(None, d_ref.at[target], piece, group)

    def to_sibling(quad, piece, group):
        return remote(
            stored(2 * quad + 1 - core, piece, group),
            block(gu_sib.at[quad], d_sib.at[quad], piece, group),
            c_send.at[quad, piece],
            c_recv.at[quad, piece],
            sibling,
        )

    def loading(quad, piece, group):
        return pltpu.make_async_copy(
            stored(2 * quad + core, piece, group),
            block(gu_own.at[quad], d_own.at[quad], piece, group),
            load.at[quad, piece],
        )

    def to_second(quad, slot, piece, group):
        return remote(
            block(gu_own.at[quad], d_own.at[quad], piece, group),
            block(gu_sec.at[slot], d_sec.at[slot], piece, group),
            s_send.at[slot, piece],
            s_recv.at[slot, piece],
            second,
        )

    def to_first(piece, group):
        return remote(
            block(gu_own.at[fst], d_own.at[fst], piece, group),
            block(gu_fst, d_fst, piece, group),
            f_send.at[piece],
            f_recv.at[piece],
            first,
        )

    def send_line(src, which, target, up):
        landing, sends, lands = (t_up, up_s, up_r) if up else (t_down, down_s, down_r)
        return remote(
            src,
            landing.at[which, target],
            sends.at[which, target],
            lands.at[which, target],
            me + RING if up else me - RING,
        )

    tokens = [
        pltpu.make_async_copy(ref, t_own.at[which], t_load.at[which])
        for which, ref in enumerate((ds_ref, y_ref))
    ]
    for copy in tokens:
        copy.start()
    for theirs, own in ((far, far), (fst, sec), (sec, fst), (mine, mine)):

        def begin(piece, group, theirs=theirs, own=own):
            to_sibling(theirs, piece, group).start()
            loading(own, piece, group).start()

        each(begin)
    for copy in tokens:
        copy.wait()
    for k in range(last):
        for which in range(2):

            @pl.when(z == last)
            def _(k=k, which=which):
                send_line(t_own.at[which, k], which, k, False).start()

            @pl.when(z == 0)
            def _(k=k, which=which):
                send_line(t_own.at[which, last - k], which, last - k, True).start()

    def relay(target, which, up):
        @pl.when((target > z) & (z > 0) if up else (target < z) & (z < last))
        def _():
            landing = (t_up if up else t_down).at[which, target]
            send_line(landing, which, target, up).wait_recv()
            add_rows(landing, landing, t_own.at[which, target])
            send_line(landing, which, target, up).start()

    for quad, slot in ((far, 1), (sec, 0)):

        def pass_on(piece, group, quad=quad, slot=slot):
            loading(quad, piece, group).wait()
            to_sibling(quad, piece, group).wait_recv()
            own = block(gu_own.at[quad], d_own.at[quad], piece, group)
            add_rows(own, own, block(gu_sib.at[quad], d_sib.at[quad], piece, group))
            to_second(quad, slot, piece, group).start()

        each(pass_on)
    for which in range(2):
        relay(0, which, False)
        relay(last, which, True)

    def narrow(piece, group):
        loading(fst, piece, group).wait()
        to_sibling(fst, piece, group).wait_recv()
        to_second(far, 1, piece, group).wait_recv()
        own = block(gu_own.at[fst], d_own.at[fst], piece, group)
        add_rows(
            own,
            own,
            block(gu_sib.at[fst], d_sib.at[fst], piece, group),
            block(gu_sec.at[1], d_sec.at[1], piece, group),
        )
        to_first(piece, group).start()

    each(narrow)
    for k in range(1, last):
        for which in range(2):
            relay(k, which, False)
            relay(last - k, which, True)

    def finish(piece, group):
        loading(mine, piece, group).wait()
        to_sibling(mine, piece, group).wait_recv()
        to_second(sec, 0, piece, group).wait_recv()
        to_first(piece, group).wait_recv()
        add_rows(
            block(gu_out, d_out, piece, group),
            block(gu_own.at[mine], d_own.at[mine], piece, group),
            block(gu_sib.at[mine], d_sib.at[mine], piece, group),
            block(gu_sec.at[0], d_sec.at[0], piece, group),
            block(gu_fst, d_fst, piece, group),
        )

    each(finish)
    for which, out in enumerate((ds_out, y_out)):
        own = t_own.at[which, z]
        above, below = t_down.at[which, z], t_up.at[which, z]

        @pl.when(z < last)
        def _(which=which, above=above):
            send_line(above, which, z, False).wait_recv()

        @pl.when(z > 0)
        def _(which=which, below=below):
            send_line(below, which, z, True).wait_recv()

        @pl.when(z == 0)
        def _(out=out, own=own, above=above):
            add_rows(out, own, above)

        @pl.when(z == last)
        def _(out=out, own=own, below=below):
            add_rows(out, own, below)

        @pl.when((z > 0) & (z < last))
        def _(out=out, own=own, above=above, below=below):
            add_rows(out, own, above, below)

    def drain(piece, group):
        for quad in (far, fst, sec, mine):
            to_sibling(quad, piece, group).wait_send()
        to_second(far, 1, piece, group).wait_send()
        to_second(sec, 0, piece, group).wait_send()
        to_first(piece, group).wait_send()

    each(drain)
    for which in range(2):
        for k in range(LINE):

            @pl.when((z > 0) & (k < z))
            def _(which=which, k=k):
                send_line(t_down.at[which, k], which, k, False).wait_send()

            @pl.when((z < last) & (k > z))
            def _(which=which, k=k):
                send_line(t_up.at[which, k], which, k, True).wait_send()


def reduce_mlp(gu, d, ds, y):
    rows, cols = gu.shape[2:]
    drows, dcols = d.shape[1:]
    tok = ds.shape[1:]
    quads = RING // 2
    pieces = LINE + 2
    return pl.pallas_call(
        reduce_mlp_kernel,
        out_shape=(
            jax.ShapeDtypeStruct((LINE, rows, cols), bf16),
            jax.ShapeDtypeStruct((drows, dcols), f32),
            jax.ShapeDtypeStruct(tok, f32),
            jax.ShapeDtypeStruct(tok, f32),
        ),
        in_specs=[ANY] * 4,
        out_specs=(VMEM,) * 4,
        scratch_shapes=[
            pltpu.VMEM((quads, LINE, rows, cols), bf16),
            pltpu.VMEM((quads, LINE, rows, cols), bf16),
            pltpu.VMEM((2, LINE, rows, cols), bf16),
            pltpu.VMEM((LINE, rows, cols), bf16),
            pltpu.VMEM((quads, drows, dcols), bf16),
            pltpu.VMEM((quads, drows, dcols), bf16),
            pltpu.VMEM((2, drows, dcols), bf16),
            pltpu.VMEM((drows, dcols), bf16),
            pltpu.VMEM((2, LINE) + tok, bf16),
            pltpu.VMEM((2, LINE) + tok, bf16),
            pltpu.VMEM((2, LINE) + tok, bf16),
            DMA((quads, pieces)),
            DMA((2,)),
            DMA((quads, pieces)),
            DMA((quads, pieces)),
            DMA((2, pieces)),
            DMA((2, pieces)),
            DMA((pieces,)),
            DMA((pieces,)),
            DMA((2, LINE)),
            DMA((2, LINE)),
            DMA((2, LINE)),
            DMA((2, LINE)),
        ],
        compiler_params=pltpu.CompilerParams(
            collective_id=2, has_side_effects=True, vmem_limit_bytes=64000 * 1024
        ),
        name="reduce_mlp",
    )(gu, d, ds, y)


def reduce_attn_kernel(
    a_ref, o_ref, gu_ref, s_ref, q_out, k_out, v_out, o_out, gate_out, up_out, s_out,
    own, sib, sec, fst, down, up, ex, s_sum, s_got, s_line,
    load, ex_load, c_send, c_recv, s_send, s_recv, f_send, f_recv, down_s, down_r, up_s, up_r,
    ex_s, ex_r, small_s, small_r,
):
    me, z, first, second, sibling = where_am_i()
    greet(line_peers(me) + [first, second, sibling])
    core = me % 2
    q_mine, q_fst, q_sec = (me % RING) // 2, (first % RING) // 2, (second % RING) // 2
    q_far = ((second + first - me) % RING) // 2
    last = LINE - 1
    split = a_ref.shape[2]
    parts = ((a_ref, pl.ds(0, split)), (o_ref, pl.ds(split, o_ref.shape[2])))
    order = (
        last * (1 - z // 2),
        2 - 2 * z + 5 * (z // 2),
        1 + z % 2,
        z,
    )

    def to_sibling(t, quad, part):
        ref, at = parts[part]
        return remote(
            ref.at[RING * t + 2 * quad + 1 - core],
            sib.at[t, quad, :, at],
            c_send.at[t, quad, part],
            c_recv.at[t, quad, part],
            sibling,
        )

    def loading(t, quad, part):
        ref, at = parts[part]
        return pltpu.make_async_copy(
            ref.at[RING * t + 2 * quad + core], own.at[t, quad, :, at], load.at[t, quad, part]
        )

    def ready(t, quad):
        for part in range(2):
            loading(t, quad, part).wait()
            to_sibling(t, quad, part).wait_recv()

    def to_second(t, quad, slot):
        return remote(
            own.at[t, quad], sec.at[slot, t], s_send.at[slot, t], s_recv.at[slot, t], second
        )

    def to_first(t):
        return remote(own.at[t, q_fst], fst.at[t], f_send.at[t], f_recv.at[t], first)

    def send_line(src, t, upward):
        if upward:
            return remote(src, up.at[t], up_s.at[t], up_r.at[t], me + RING)
        return remote(src, down.at[t], down_s.at[t], down_r.at[t], me - RING)

    def exchange(k):
        peer_z = lax.rem(z + k, LINE)
        return remote(
            gu_ref.at[peer_z], ex.at[z], ex_s.at[k], ex_r.at[k], me % RING + RING * peer_z
        )

    def small(step, src, dst, device):
        return remote(src, dst, small_s.at[step], small_r.at[step], device)

    small_c = small(0, s_ref, s_got.at[0], sibling)
    small_c.start()
    for k in range(1, LINE):
        exchange(k).start()
    ex_in = pltpu.make_async_copy(gu_ref.at[z], ex.at[z], ex_load)
    ex_in.start()
    for t in order:
        for theirs, ours in ((q_far, q_far), (q_fst, q_sec), (q_sec, q_fst), (q_mine, q_mine)):
            for part in range(2):
                to_sibling(t, theirs, part).start()
                loading(t, ours, part).start()

    def spread(t):
        for quad, slot in ((q_far, 1), (q_sec, 0)):
            ready(t, quad)
            add_rows(own.at[t, quad], own.at[t, quad], sib.at[t, quad])
            to_second(t, quad, slot).start()

    def narrow(t):
        ready(t, q_fst)
        to_second(t, q_far, 1).wait_recv()
        add_rows(own.at[t, q_fst], own.at[t, q_fst], sib.at[t, q_fst], sec.at[1, t])
        to_first(t).start()

    def collect(t):
        ready(t, q_mine)
        to_second(t, q_sec, 0).wait_recv()
        to_first(t).wait_recv()
        mine = own.at[t, q_mine]
        add_rows(mine, mine, sib.at[t, q_mine], sec.at[0, t], fst.at[t])

        @pl.when((t < z) & (z == last))
        def _():
            send_line(mine, t, False).start()

        @pl.when((t > z) & (z == 0))
        def _():
            send_line(mine, t, True).start()

    def relay(t):
        @pl.when((t < z) & (z < last))
        def _():
            landing = down.at[t]
            send_line(landing, t, False).wait_recv()
            add_rows(landing, landing, own.at[t, q_mine])
            send_line(landing, t, False).start()

        @pl.when((t > z) & (z > 0))
        def _():
            landing = up.at[t]
            send_line(landing, t, True).wait_recv()
            add_rows(landing, landing, own.at[t, q_mine])
            send_line(landing, t, True).start()

    spread(order[0])
    small_c.wait()
    s_sum[0] = s_ref[...] + s_got[0]
    small_f = small(1, s_sum.at[0], s_got.at[1], first)
    small_f.start()
    spread(order[1])
    narrow(order[0])
    small_f.wait()
    s_sum[1] = s_sum[0] + s_got[1]
    small_s2 = small(2, s_sum.at[1], s_got.at[2], second)
    small_s2.start()
    spread(order[2])
    narrow(order[1])
    collect(order[0])
    small_s2.wait()
    s_sum[2] = s_sum[1] + s_got[2]
    small_line = [
        small(
            2 + k, s_sum.at[2], s_line.at[k], me % RING + RING * lax.rem(z + k, LINE)
        )
        for k in range(1, LINE)
    ]
    for copy in small_line:
        copy.start()
    spread(order[3])
    narrow(order[2])
    collect(order[1])
    relay(order[0])
    narrow(order[3])
    collect(order[2])
    relay(order[1])
    collect(order[3])
    relay(order[2])
    ex_in.wait()
    for k in range(1, LINE):
        src_z = lax.rem(z + LINE - k, LINE)
        landed = ex.at[src_z]
        remote(landed, landed, ex_s.at[k], ex_r.at[k], sibling).wait_recv()
    width = gate_out.shape[1] // LINE
    for k in range(LINE):
        add_rows(gate_out.at[:, pl.ds(k * width, width)], ex.at[k, :, pl.ds(0, width)])
        add_rows(up_out.at[:, pl.ds(k * width, width)], ex.at[k, :, pl.ds(width, width)])
    for copy in small_line:
        copy.wait()
    s_out[...] = (s_sum[2] + s_line[2]) + (s_line[1] + s_line[3])
    mine, above, below = own.at[z, q_mine], down.at[z], up.at[z]

    @pl.when(z < last)
    def _():
        send_line(above, z, False).wait_recv()

    @pl.when(z > 0)
    def _():
        send_line(below, z, True).wait_recv()

    def total(*terms):
        lo = 0
        for out in (q_out, k_out, v_out, o_out):
            at = pl.ds(lo, out.shape[1])
            add_rows(out, *[term.at[:, at] for term in terms])
            lo += out.shape[1]

    @pl.when(z == 0)
    def _():
        total(mine, above)

    @pl.when(z == last)
    def _():
        total(mine, below)

    @pl.when((z > 0) & (z < last))
    def _():
        total(mine, above, below)

    for k in range(1, LINE):
        exchange(k).wait_send()
    for t in range(LINE):
        for quad in (q_far, q_fst, q_sec, q_mine):
            for part in range(2):
                to_sibling(t, quad, part).wait_send()
        to_second(t, q_far, 1).wait_send()
        to_second(t, q_sec, 0).wait_send()
        to_first(t).wait_send()

        @pl.when(t < z)
        def _(t=t):
            send_line(down.at[t], t, False).wait_send()

        @pl.when(t > z)
        def _(t=t):
            send_line(up.at[t], t, True).wait_send()


def reduce_attn(a, o, gu, small):
    rows, split = a.shape[1:]
    owide = o.shape[2]
    wide = split + owide
    quads = RING // 2
    width = gu.shape[2] // 2
    kv = KVH * HD
    return pl.pallas_call(
        reduce_attn_kernel,
        out_shape=(
            jax.ShapeDtypeStruct((rows, H * HD), f32),
            jax.ShapeDtypeStruct((rows, kv), f32),
            jax.ShapeDtypeStruct((rows, kv), f32),
            jax.ShapeDtypeStruct((rows, owide), f32),
            jax.ShapeDtypeStruct((rows, LINE * width), f32),
            jax.ShapeDtypeStruct((rows, LINE * width), f32),
            jax.ShapeDtypeStruct(small.shape, f32),
        ),
        in_specs=[ANY, ANY, ANY, VMEM],
        out_specs=(VMEM,) * 7,
        scratch_shapes=[
            pltpu.VMEM((LINE, quads, rows, wide), bf16),
            pltpu.VMEM((LINE, quads, rows, wide), bf16),
            pltpu.VMEM((2, LINE, rows, wide), bf16),
            pltpu.VMEM((LINE, rows, wide), bf16),
            pltpu.VMEM((LINE, rows, wide), bf16),
            pltpu.VMEM((LINE, rows, wide), bf16),
            pltpu.VMEM((LINE, rows, 2 * width), bf16),
            pltpu.VMEM((3,) + small.shape, f32),
            pltpu.VMEM((3,) + small.shape, f32),
            pltpu.VMEM((LINE,) + small.shape, f32),
            DMA((LINE, quads, 2)),
            DMA,
            DMA((LINE, quads, 2)),
            DMA((LINE, quads, 2)),
            DMA((2, LINE)),
            DMA((2, LINE)),
            DMA((LINE,)),
            DMA((LINE,)),
            DMA((LINE,)),
            DMA((LINE,)),
            DMA((LINE,)),
            DMA((LINE,)),
            DMA((LINE,)),
            DMA((LINE,)),
            DMA((2 + LINE,)),
            DMA((2 + LINE,)),
        ],
        compiler_params=pltpu.CompilerParams(
            collective_id=3, has_side_effects=True, vmem_limit_bytes=64000 * 1024
        ),
        name="reduce_attn",
    )(a, o, gu, small)


epsilon = 1e-06
rope_base = 1000000.0
masked_score = -1e30
contract_rows = (((0,), (0,)), ((), ()))
contract_cols = (((1,), (1,)), ((), ()))


def layout(seq_lengths, seq_device, owner, slots):
    owned = seq_device == owner
    counts = jnp.where(owned, seq_lengths, 0)
    starts = jnp.cumsum(counts) - counts
    places = jnp.arange(slots, dtype=jnp.int32)
    inside = (
        owned[:, None]
        & (places[None, :] >= starts[:, None])
        & (places[None, :] < (starts + counts)[:, None])
    )
    labels = jnp.arange(seq_lengths.shape[0], dtype=jnp.int32)
    segment = jnp.sum(jnp.where(inside, labels[:, None] + 1, 0), axis=0) - 1
    position = jnp.sum(jnp.where(inside, places[None, :] - starts[:, None], 0), axis=0)
    return (segment, position)


def allowed_pairs(segment):
    places = jnp.arange(segment.shape[0], dtype=jnp.int32)
    earlier = places[None, :] < places[:, None]
    same_seq = (segment[:, None] == segment[None, :]) & (segment[:, None] >= 0)
    return (places[:, None] == places[None, :]) | earlier & same_seq


def rmsnorm(values, gain):
    return values * lax.rsqrt(jnp.mean(values * values, axis=-1, keepdims=True) + epsilon) * gain


def rotary(values, position):
    half_dim = values.shape[-1] // 2
    freqs = jnp.power(rope_base, -2.0 * jnp.arange(half_dim, dtype=jnp.float32) / values.shape[-1])
    angles = position.astype(jnp.float32)[:, None] * freqs[None, :]
    cosine = jnp.concatenate([jnp.cos(angles), jnp.cos(angles)], axis=-1)[:, None, :]
    sine = jnp.concatenate([jnp.sin(angles), jnp.sin(angles)], axis=-1)[:, None, :]
    rotated = jnp.concatenate([-values[..., half_dim:], values[..., :half_dim]], axis=-1)
    return values * cosine + rotated * sine


def matmul(left, right):
    return jnp.dot(left, right, preferred_element_type=jnp.float32)


def times_rows(left, right):
    return lax.dot_general(left, right, contract_rows, preferred_element_type=jnp.float32)


def times_cols(left, right):
    return lax.dot_general(left, right, contract_cols, preferred_element_type=jnp.float32)


def scatter_sum(partial):
    total = lax.psum_scatter(
        partial.astype(jnp.bfloat16), "fsdp", scatter_dimension=0, tiled=True
    )
    return total.astype(jnp.float32)


def plain(
    hidden_in,
    out_grad,
    seq_lengths,
    seq_device,
    attn_gain,
    q_gain,
    k_gain,
    w_query,
    w_key,
    w_value,
    w_out,
    mlp_gain,
    w_gate,
    w_up,
    w_down,
):
    slots = hidden_in.shape[0]
    groups = H // KVH
    score_scale = HD ** (-0.5)
    segment, position = layout(seq_lengths, seq_device, lax.axis_index("fsdp"), slots)
    allowed = allowed_pairs(segment)[None, None]

    def query_path(raw, gain):
        return rotary(rmsnorm(raw.reshape(slots, H, HD), gain), position)

    def key_path(raw, gain):
        return rotary(rmsnorm(raw.reshape(slots, KVH, HD), gain), position)

    def swiglu(gate_in, up_in):
        return jax.nn.silu(gate_in) * up_in

    attn_set = (
        lax.all_gather(attn_gain, "fsdp", axis=0, tiled=True),
        lax.all_gather(q_gain, "fsdp", axis=0, tiled=True),
        lax.all_gather(k_gain, "fsdp", axis=0, tiled=True),
        lax.all_gather(w_query, "fsdp", axis=0, tiled=True),
        lax.all_gather(w_key, "fsdp", axis=0, tiled=True),
        lax.all_gather(w_value, "fsdp", axis=0, tiled=True),
        lax.all_gather(w_out, "fsdp", axis=0, tiled=True),
    )
    gain_attn, gain_query, gain_key, query_w, key_w, value_w, out_w = attn_set
    inputs = hidden_in.astype(jnp.float32)
    normed = rmsnorm(inputs, gain_attn.astype(jnp.float32)).astype(jnp.bfloat16)
    query_raw = matmul(normed, query_w)
    key_raw = matmul(normed, key_w)
    value_raw = matmul(normed, value_w)
    queries = (
        query_path(query_raw, gain_query.astype(jnp.float32))
        .astype(jnp.bfloat16)
        .reshape(slots, KVH, groups, HD)
    )
    keys = key_path(key_raw, gain_key.astype(jnp.float32)).astype(jnp.bfloat16)
    values = value_raw.astype(jnp.bfloat16).reshape(slots, KVH, HD)

    def masked_logits():
        scores = (
            jnp.einsum("qgrd,kgd->grqk", queries, keys, preferred_element_type=jnp.float32)
            * score_scale
        )
        return jnp.where(allowed, scores, masked_score)

    logits = masked_logits()
    row_top = jnp.max(logits, axis=-1, keepdims=True)
    exponent = jnp.exp(logits - row_top)
    row_total = jnp.sum(exponent, axis=-1, keepdims=True)
    log_total = row_top + jnp.log(row_total)
    weights = (exponent / row_total).astype(jnp.bfloat16)
    mixed = jnp.einsum("grqk,kgd->qgrd", weights, values, preferred_element_type=jnp.float32)
    mixed = mixed.reshape(slots, H * HD).astype(jnp.bfloat16)
    middle = inputs + matmul(mixed, out_w)
    mlp_set = (
        lax.all_gather(mlp_gain, "fsdp", axis=0, tiled=True),
        lax.all_gather(w_gate, "fsdp", axis=0, tiled=True),
        lax.all_gather(w_up, "fsdp", axis=0, tiled=True),
        lax.all_gather(w_down, "fsdp", axis=0, tiled=True),
    )
    gain_mlp, gate_w, up_w, down_w = mlp_set
    second = rmsnorm(middle, gain_mlp.astype(jnp.float32)).astype(jnp.bfloat16)
    gate_out = matmul(second, gate_w)
    up_out = matmul(second, up_w)
    hidden = swiglu(gate_out, up_out).astype(jnp.bfloat16)
    hidden_out = (middle + matmul(hidden, down_w)).astype(jnp.bfloat16)
    gain_mlp, gate_w, up_w, down_w = (
        lax.all_gather(mlp_gain, "fsdp", axis=0, tiled=True),
        lax.all_gather(w_gate, "fsdp", axis=0, tiled=True),
        lax.all_gather(w_up, "fsdp", axis=0, tiled=True),
        lax.all_gather(w_down, "fsdp", axis=0, tiled=True),
    )
    grad_down = scatter_sum(times_rows(hidden, out_grad))
    d_hidden = times_cols(out_grad, down_w)
    unused_out, swiglu_pull = jax.vjp(swiglu, gate_out, up_out)
    d_gate, d_up = swiglu_pull(d_hidden)
    d_gate_up = jnp.concatenate([d_gate.astype(jnp.bfloat16), d_up.astype(jnp.bfloat16)], axis=1)
    grad_gate_up = scatter_sum(times_rows(second, d_gate_up))
    ff_width = gate_w.shape[1]
    d_second = times_cols(d_gate_up, jnp.concatenate([gate_w, up_w], axis=1))
    unused_norm, second_pull = jax.vjp(rmsnorm, middle, gain_mlp.astype(jnp.float32))
    d_middle_norm, grad_gain_mlp = second_pull(d_second)
    d_middle = out_grad.astype(jnp.float32) + d_middle_norm
    gain_attn, gain_query, gain_key, query_w, key_w, value_w, out_w = (
        lax.all_gather(attn_gain, "fsdp", axis=0, tiled=True),
        lax.all_gather(q_gain, "fsdp", axis=0, tiled=True),
        lax.all_gather(k_gain, "fsdp", axis=0, tiled=True),
        lax.all_gather(w_query, "fsdp", axis=0, tiled=True),
        lax.all_gather(w_key, "fsdp", axis=0, tiled=True),
        lax.all_gather(w_value, "fsdp", axis=0, tiled=True),
        lax.all_gather(w_out, "fsdp", axis=0, tiled=True),
    )
    d_branch = d_middle.astype(jnp.bfloat16)
    grad_out_w = scatter_sum(times_rows(mixed, d_branch))
    d_mixed = times_cols(d_branch, out_w).astype(jnp.bfloat16).reshape(slots, KVH, groups, HD)
    probs = jnp.exp(masked_logits() - log_total)
    weights = probs.astype(jnp.bfloat16)
    d_probs = jnp.einsum("qgrd,kgd->grqk", d_mixed, values, preferred_element_type=jnp.float32)
    d_logits = probs * (d_probs - jnp.sum(probs * d_probs, axis=-1, keepdims=True))
    d_scores = (d_logits * score_scale).astype(jnp.bfloat16)
    d_values = jnp.einsum("grqk,qgrd->kgd", weights, d_mixed, preferred_element_type=jnp.float32)
    d_values = d_values.astype(jnp.bfloat16).reshape(slots, KVH * HD)
    d_queries_rot = jnp.einsum(
        "grqk,kgd->qgrd", d_scores, keys, preferred_element_type=jnp.float32
    ).reshape(slots, H, HD)
    d_keys_rot = jnp.einsum("grqk,qgrd->kgd", d_scores, queries, preferred_element_type=jnp.float32)
    unused_query, query_pull = jax.vjp(query_path, query_raw, gain_query.astype(jnp.float32))
    d_query_raw, grad_gain_query = query_pull(d_queries_rot)
    unused_key, key_pull = jax.vjp(key_path, key_raw, gain_key.astype(jnp.float32))
    d_key_raw, grad_gain_key = key_pull(d_keys_rot)
    d_qkv = jnp.concatenate(
        [d_query_raw.astype(jnp.bfloat16), d_key_raw.astype(jnp.bfloat16), d_values], axis=1
    )
    grad_qkv = scatter_sum(times_rows(normed, d_qkv))
    d_normed = times_cols(d_qkv, jnp.concatenate([query_w, key_w, value_w], axis=1))
    unused_first, first_pull = jax.vjp(rmsnorm, inputs, gain_attn.astype(jnp.float32))
    d_input_norm, grad_gain_attn = first_pull(d_normed)
    input_grad = d_middle + d_input_norm
    gain_sums = (
        lax.psum_scatter(grad_gain_attn, "fsdp", scatter_dimension=0, tiled=True),
        lax.psum_scatter(grad_gain_query, "fsdp", scatter_dimension=0, tiled=True),
        lax.psum_scatter(grad_gain_key, "fsdp", scatter_dimension=0, tiled=True),
        lax.psum_scatter(grad_gain_mlp, "fsdp", scatter_dimension=0, tiled=True),
    )
    query_width = H * HD
    key_width = KVH * HD
    grad_query_w = grad_qkv[:, :query_width]
    grad_key_w = grad_qkv[:, query_width : query_width + key_width]
    grad_value_w = grad_qkv[:, query_width + key_width :]
    grad_gate = grad_gate_up[:, :ff_width]
    grad_up = grad_gate_up[:, ff_width:]
    return (
        hidden_out,
        input_grad,
        gain_sums[0],
        gain_sums[1],
        gain_sums[2],
        grad_query_w,
        grad_key_w,
        grad_value_w,
        grad_out_w,
        gain_sums[3],
        grad_gate,
        grad_up,
        grad_down,
    )


def layered(
    hidden_in,
    out_grad,
    seq_lengths,
    seq_device,
    attn_gain,
    q_gain,
    k_gain,
    w_query,
    w_key,
    w_value,
    w_out,
    mlp_gain,
    w_gate,
    w_up,
    w_down,
):
    slots, width = hidden_in.shape
    groups = H // KVH
    score_scale = HD ** (-0.5)
    n = RING * LINE
    rows = w_query.shape[0]
    me = lax.axis_index("fsdp")
    segment, position = layout(seq_lengths, seq_device, me, slots)
    allowed = allowed_pairs(segment)[None, None]
    query_width = H * HD
    qkv_width = query_width + 2 * KVH * HD
    attn_width = qkv_width + w_out.shape[1]

    def query_path(raw, gain):
        return rotary(rmsnorm(raw.reshape(slots, H, HD), gain), position)

    def key_path(raw, gain):
        return rotary(rmsnorm(raw.reshape(slots, KVH, HD), gain), position)

    def swiglu(gate_in, up_in):
        return jax.nn.silu(gate_in) * up_in

    def column(gain):
        return jnp.pad(gain, (0, rows - gain.shape[0]))[:, None]

    gains = jnp.concatenate([column(g) for g in (attn_gain, mlp_gain, q_gain, k_gain)], axis=1)
    gains = jnp.pad(gains, ((0, 0), (0, 128 - gains.shape[1])))
    packed = jnp.concatenate([w_query, w_key, w_value, w_out, gains], axis=1)
    attn_w, mlp_w = fetch_attn(packed, w_gate, w_up)
    gain_cols = attn_w[:, :, attn_width : attn_width + 4].astype(f32)
    gain_attn = gain_cols[:, :, 0].reshape(-1)
    gain_mlp = gain_cols[:, :, 1].reshape(-1)
    gain_query = gain_cols[:, : q_gain.shape[0], 2].reshape(-1)
    gain_key = gain_cols[:, : k_gain.shape[0], 3].reshape(-1)
    attn_w = attn_w.reshape(n * rows, attn_w.shape[2])
    qkv_w = attn_w[:, :qkv_width]
    out_w = attn_w[:, qkv_width:attn_width]

    inputs = hidden_in.astype(f32)
    normed = rmsnorm(inputs, gain_attn).astype(bf16)
    qkv_raw = matmul(normed, qkv_w)
    query_raw = qkv_raw[:, :query_width]
    key_raw = qkv_raw[:, query_width : query_width + KVH * HD]
    value_raw = qkv_raw[:, query_width + KVH * HD :]
    queries = query_path(query_raw, gain_query).astype(bf16).reshape(slots, KVH, groups, HD)
    keys = key_path(key_raw, gain_key).astype(bf16)
    values = value_raw.astype(bf16).reshape(slots, KVH, HD)
    scores = jnp.einsum("qgrd,kgd->grqk", queries, keys, preferred_element_type=f32) * score_scale
    logits = jnp.where(allowed, scores, masked_score)
    exponent = jnp.exp(logits - jnp.max(logits, axis=-1, keepdims=True))
    probs = exponent / jnp.sum(exponent, axis=-1, keepdims=True)
    weights = probs.astype(bf16)
    mixed = jnp.einsum("grqk,kgd->qgrd", weights, values, preferred_element_type=f32)
    mixed = mixed.reshape(slots, query_width).astype(bf16)
    middle = inputs + matmul(mixed, out_w)
    second = rmsnorm(middle, gain_mlp).astype(bf16)

    gate_up_w, down_w, tokens, cotangent = fetch_mlp(mlp_w, w_down, second, out_grad)
    gate_up_w = gate_up_w.reshape(n * rows, gate_up_w.shape[-1])
    down_w = down_w.reshape(-1, down_w.shape[-1])
    tokens = tokens.reshape(-1, width)
    cotangent = cotangent.reshape(-1, width)
    part = gate_up_w.shape[1] // 2
    gate_up = matmul(tokens, gate_up_w)
    gate_out, up_out = gate_up[:, :part], gate_up[:, part:]
    hidden = swiglu(gate_out, up_out).astype(bf16)
    y_part = matmul(hidden, down_w).astype(bf16)
    d_hidden = times_cols(cotangent, down_w)
    unused_out, swiglu_pull = jax.vjp(swiglu, gate_out, up_out)
    d_gate, d_up = swiglu_pull(d_hidden)
    d_gate_up = jnp.concatenate([d_gate.astype(bf16), d_up.astype(bf16)], axis=1)
    ds_part = times_cols(d_gate_up, gate_up_w).astype(bf16)
    g_gate_up = times_rows(tokens, d_gate_up).astype(bf16)
    g_down = times_rows(hidden, cotangent).astype(bf16)
    g_gate_up, grad_down, d_second, y = reduce_mlp(
        g_gate_up.reshape(LINE, RING, rows, 2 * part),
        g_down.reshape(RING, w_down.shape[0], width),
        ds_part.reshape(LINE, slots, width),
        y_part.reshape(LINE, slots, width),
    )
    hidden_out = (middle + y).astype(bf16)

    unused_norm, second_pull = jax.vjp(rmsnorm, middle, gain_mlp)
    d_middle_norm, grad_gain_mlp = second_pull(d_second)
    d_middle = out_grad.astype(f32) + d_middle_norm
    d_branch = d_middle.astype(bf16)
    g_out = times_rows(mixed, d_branch).astype(bf16)
    d_mixed = times_cols(d_branch, out_w).astype(bf16).reshape(slots, KVH, groups, HD)
    d_probs = jnp.einsum("qgrd,kgd->grqk", d_mixed, values, preferred_element_type=f32)
    d_logits = probs * (d_probs - jnp.sum(probs * d_probs, axis=-1, keepdims=True))
    d_scores = (d_logits * score_scale).astype(bf16)
    d_values = jnp.einsum("grqk,qgrd->kgd", weights, d_mixed, preferred_element_type=f32)
    d_values = d_values.astype(bf16).reshape(slots, KVH * HD)
    d_queries_rot = jnp.einsum(
        "grqk,kgd->qgrd", d_scores, keys, preferred_element_type=f32
    ).reshape(slots, H, HD)
    d_keys_rot = jnp.einsum("grqk,qgrd->kgd", d_scores, queries, preferred_element_type=f32)
    unused_query, query_pull = jax.vjp(query_path, query_raw, gain_query)
    d_query_raw, grad_gain_query = query_pull(d_queries_rot)
    unused_key, key_pull = jax.vjp(key_path, key_raw, gain_key)
    d_key_raw, grad_gain_key = key_pull(d_keys_rot)
    d_qkv = jnp.concatenate([d_query_raw.astype(bf16), d_key_raw.astype(bf16), d_values], axis=1)
    g_qkv = times_rows(normed, d_qkv).astype(bf16)
    d_normed = times_cols(d_qkv, qkv_w)
    unused_first, first_pull = jax.vjp(rmsnorm, inputs, gain_attn)
    d_input_norm, grad_gain_attn = first_pull(d_normed)
    input_grad = d_middle + d_input_norm
    gain_grads = (grad_gain_attn, grad_gain_query, grad_gain_key, grad_gain_mlp)
    small = jnp.concatenate(gain_grads)
    small = jnp.pad(small, (0, -small.shape[0] % 1024)).reshape(-1, 128)
    g_query, g_key, g_value, g_out, g_gate, g_up, small = reduce_attn(
        g_qkv.reshape(n, rows, qkv_width), g_out.reshape(n, rows, w_out.shape[1]), g_gate_up, small
    )
    small = small.reshape(-1)
    gain_sums = []
    lo = 0
    for grad in gain_grads:
        share = grad.shape[0] // n
        gain_sums.append(lax.dynamic_slice(small, (lo + me * share,), (share,)))
        lo += grad.shape[0]
    return (
        hidden_out,
        input_grad,
        gain_sums[0],
        gain_sums[1],
        gain_sums[2],
        g_query,
        g_key,
        g_value,
        g_out,
        gain_sums[3],
        g_gate,
        g_up,
        grad_down,
    )


def solution(mesh):
    per_device = layered if mesh.shape["fsdp"] == RING * LINE else plain
    return jax.shard_map(
        per_device,
        mesh=mesh,
        in_specs=(
            P("fsdp", None),
            P("fsdp", None),
            P(),
            P(),
            P("fsdp"),
            P("fsdp"),
            P("fsdp"),
            P("fsdp", None),
            P("fsdp", None),
            P("fsdp", None),
            P("fsdp", None),
            P("fsdp"),
            P("fsdp", None),
            P("fsdp", None),
            P("fsdp", None),
        ),
        out_specs=(
            P("fsdp", None),
            P("fsdp", None),
            P("fsdp"),
            P("fsdp"),
            P("fsdp"),
            P("fsdp", None),
            P("fsdp", None),
            P("fsdp", None),
            P("fsdp", None),
            P("fsdp"),
            P("fsdp", None),
            P("fsdp", None),
            P("fsdp", None),
        ),
        check_vma=False,
    )
```

```python
import functools

import jax
import jax.numpy as jnp
from jax import lax
from jax.experimental import pallas as pl
from jax.experimental.pallas import tpu as pltpu
from jax.sharding import PartitionSpec as P

H = 16
KVH = 8
HD = 128
CAP = 128
LINE = 4
RING = 8
MESH = pl.DeviceIdType.MESH
ANY = pl.BlockSpec(memory_space=pl.ANY)
VMEM = pl.BlockSpec(memory_space=pltpu.VMEM)
DMA = pltpu.SemaphoreType.DMA
bf16 = jnp.bfloat16
f32 = jnp.float32
epsilon = 1e-06
rope_base = 1000000.0
masked_score = -1e30
contract_rows = (((0,), (0,)), ((), ()))
contract_cols = (((1,), (1,)), ((), ()))


def where_am_i():
    me = lax.axis_index("fsdp")
    core = me % 2
    z = me // RING
    f_bit = 2 + 2 * core
    s_bit = 4 - 2 * core
    first = me + f_bit * (1 - 2 * ((me // f_bit) % 2))
    second = me + s_bit * (1 - 2 * ((me // s_bit) % 2))
    sibling = me + 1 - 2 * core
    return me, z, first, second, sibling


def greet(peers):
    barrier = pltpu.get_barrier_semaphore()
    for peer in peers:
        pl.semaphore_signal(barrier, inc=1, device_id=(peer,), device_id_type=MESH)
    pl.semaphore_wait(barrier, len(peers))


def remote(src, dst, send_sem, recv_sem, device):
    return pltpu.make_async_remote_copy(
        src_ref=src,
        dst_ref=dst,
        send_sem=send_sem,
        recv_sem=recv_sem,
        device_id=(device,),
        device_id_type=MESH,
    )


def line_peers(me):
    return [lax.rem(me + RING * k, RING * LINE) for k in range(1, LINE)]


def on_line(z, k, body):
    for step in ((-k, k) if k else (0,)):

        @pl.when((z + step >= 0) & (z + step < LINE))
        def _(step=step):
            body(step)


def lane_sum(x):
    return jnp.sum(x, axis=-1, keepdims=True)


def token_places(len_row, dev_row, len_col, dev_col, me):
    seqs = len_row.shape[1]
    counts_row = jnp.where(dev_row == me, len_row, 0).astype(f32)
    counts_col = jnp.where(dev_col == me, len_col, 0).astype(f32)
    up = lax.broadcasted_iota(jnp.int32, (seqs, seqs), 0)
    across = lax.broadcasted_iota(jnp.int32, (seqs, seqs), 1)
    starts_row = jnp.sum(jnp.where(up < across, counts_col, 0.0), axis=0, keepdims=True)
    starts_col = lane_sum(jnp.where(across < up, counts_row, 0.0))

    def within(places, starts, counts):
        return (places >= starts) & (places < starts + counts)

    places = lax.broadcasted_iota(jnp.int32, (CAP, seqs), 0).astype(f32)
    labels = lax.broadcasted_iota(jnp.int32, (CAP, seqs), 1).astype(f32)
    inside = within(places, starts_row, counts_row)
    segment_col = lane_sum(jnp.where(inside, labels + 1.0, 0.0)) - 1.0
    position = lane_sum(jnp.where(inside, places - starts_row, 0.0))
    places = lax.broadcasted_iota(jnp.int32, (seqs, CAP), 1).astype(f32)
    labels = lax.broadcasted_iota(jnp.int32, (seqs, CAP), 0).astype(f32)
    inside = within(places, starts_col, counts_col)
    segment_row = jnp.sum(jnp.where(inside, labels + 1.0, 0.0), axis=0, keepdims=True) - 1.0
    return segment_col, segment_row, position


def allowed_bias(segment_col, segment_row):
    t = lax.broadcasted_iota(jnp.int32, (CAP, CAP), 0)
    u = lax.broadcasted_iota(jnp.int32, (CAP, CAP), 1)
    same = (segment_col == segment_row) & (segment_col >= 0.0)
    return jnp.where((t == u) | ((u < t) & same), 0.0, masked_score)


def half_turn(v):
    lane = lax.broadcasted_iota(jnp.int32, v.shape, v.ndim - 1)
    turned = pltpu.roll(v, HD // 2, v.ndim - 1)
    return jnp.where(lane < HD // 2, -turned, turned)


def rms_scale(v):
    return lax.rsqrt(jnp.mean(v * v, axis=-1, keepdims=True) + epsilon)


def forward_kernel(
    x_ref, cot_ref, len_row, dev_row, len_col, dev_col, freq_ref, gain_ref,
    wq_ref, wk_ref, wv_ref, wo_ref, gate_ref, up_ref, wd_ref,
    w_out, gu_out, d_out, tok_out, cot_out,
    middle_out, normed_out, raw_out, q_out, k_out, v_out, mixed_out, gains_out,
    w_tmp, p_tmp, d_tmp, cot_tmp, second_tmp, chunk, ow_all, gain_tmp, cos_tmp, sin_tmp, bias_tmp,
    local, up_s, down_s, first_s, second_s, sib_s, recv, ex_send, ex_recv,
    m_first_s, m_second_s, m_sib_s, m_recv, line_up, line_down, line_r, w_load, o_load, g_load,
):
    me, z, first, second, sibling = where_am_i()
    col, fcol, scol = me % RING, first % RING, second % RING
    sfcol = (second + first - me) % RING
    width = p_tmp.shape[2] // 2
    rows = w_tmp.shape[0]
    qkv_width = raw_out.shape[1]
    attn_width = qkv_width + wo_ref.shape[1]
    last = LINE - 1
    pieces = LINE + 1

    w_in = []
    lo = 0
    for i, ref in enumerate((wq_ref, wk_ref, wv_ref, wo_ref, gain_ref)):
        at = pl.ds(lo, ref.shape[1])
        w_in.append(pltpu.make_async_copy(ref, w_tmp.at[:, at], local.at[i]))
        lo += ref.shape[1]
    p_in = [
        pltpu.make_async_copy(
            ref.at[:, pl.ds(pl.multiple_of(z * width, width), width)],
            p_tmp.at[z, :, pl.ds(which * width, width)],
            local.at[5 + which],
        )
        for which, ref in enumerate((gate_ref, up_ref))
    ]
    d_in = pltpu.make_async_copy(wd_ref, d_tmp, local.at[7])
    cot_in = pltpu.make_async_copy(cot_ref, cot_tmp, local.at[8])
    for copy in w_in + p_in + [d_in, cot_in]:
        copy.start()
    greet(line_peers(me) + [first, second, sibling])

    def send(src, shard, sems, device):
        return remote(src, w_out.at[shard], sems.at[shard], recv.at[shard], device)

    def arrived(shard):
        send(w_out.at[shard], shard, sib_s, sibling).wait_recv()

    def exchange(k, which):
        peer_z = lax.rem(z + k, LINE)
        src = (gate_ref, up_ref)[which].at[:, pl.ds(pl.multiple_of(peer_z * width, width), width)]
        dst = p_tmp.at[z, :, pl.ds(which * width, width)]
        return remote(src, dst, ex_send.at[k, which], ex_recv.at[k, which], col + RING * peer_z)

    def line_send(src, which, shard, sems, device):
        landing = (tok_out, cot_out)[which].at[shard]
        return remote(src, landing, sems.at[which, shard], line_r.at[which, shard], device)

    def line_own(which, src):
        @pl.when(z < last)
        def _():
            line_send(src, which, z, line_up, me + RING).start()

        @pl.when(z > 0)
        def _():
            line_send(src, which, z, line_down, me - RING).start()

    def line_relay(which, k):
        def body(step):
            shard = z + step
            src = (tok_out, cot_out)[which].at[shard]
            line_send(src, which, shard, line_up, second).wait_recv()
            if step < 0:

                @pl.when(z < last)
                def _():
                    line_send(src, which, shard, line_up, me + RING).start()
            else:

                @pl.when(z > 0)
                def _():
                    line_send(src, which, shard, line_down, me - RING).start()

        on_line(z, k, body)

    for copy in w_in:
        copy.wait()

    @pl.when(z < last)
    def _():
        send(w_tmp, me, up_s, me + RING).start()

    @pl.when(z > 0)
    def _():
        send(w_tmp, me, down_s, me - RING).start()

    send(w_tmp, me, first_s, first).start()
    send(w_tmp, me, second_s, second).start()
    send(w_tmp, me, sib_s, sibling).start()
    w_back = pltpu.make_async_copy(w_tmp, w_out.at[me], local.at[9])
    w_back.start()

    def own(k):
        def body(step):
            shard = me + RING * step
            src = w_out.at[shard]
            arrived(shard)
            if step < 0:

                @pl.when(z < last)
                def _():
                    send(src, shard, up_s, me + RING).start()
            else:

                @pl.when(z > 0)
                def _():
                    send(src, shard, down_s, me - RING).start()

            send(src, shard, first_s, first).start()
            send(src, shard, second_s, second).start()
            send(src, shard, sib_s, sibling).start()

        on_line(z, k, body)

    def other(base, k, onward):
        def body(step):
            shard = base + RING * (z + step)
            src = w_out.at[shard]
            arrived(shard)
            if onward:
                send(src, shard, second_s, second).start()
            send(src, shard, sib_s, sibling).start()

        on_line(z, k, body)

    segment_col, segment_row, position = token_places(
        len_row[...], dev_row[...], len_col[...], dev_col[...], me
    )
    bias_tmp[...] = allowed_bias(segment_col, segment_row)
    angles = position * freq_ref[...]
    cos_tmp[...] = jnp.cos(angles)
    sin_tmp[...] = jnp.sin(angles)
    x_scale = rms_scale(x_ref[...].astype(f32))
    raw_out[...] = jnp.zeros_like(raw_out)

    def load_group(step):
        zz = z + step
        part = w_out.at[pl.ds(RING * zz, RING)]
        return (
            pltpu.make_async_copy(part.at[:, :, pl.ds(0, qkv_width)], chunk, w_load),
            pltpu.make_async_copy(
                part.at[:, :, pl.ds(qkv_width, attn_width - qkv_width)],
                ow_all.at[pl.ds(RING * zz, RING)],
                o_load.at[zz],
            ),
            pltpu.make_async_copy(
                part.at[:, pl.ds(0, 16), pl.ds(attn_width, 128)], gain_tmp.at[zz], g_load
            ),
        )

    def group(k):
        def body(step):
            zz = z + step
            for i in range(RING // 2):
                arrived(RING * zz + 2 * i + sibling % 2)
            copies = load_group(step)
            for copy in copies:
                copy.start()
            copies[2].wait()
            span = RING * rows
            for pair in range(RING // 2):
                at = pl.ds(pl.multiple_of(zz * span + pair * 128, 128), 128)
                both = gain_tmp[zz, 2 * pair].astype(f32) + gain_tmp[zz, 2 * pair + 1].astype(f32)
                gains_out[0:2, at] = both[0:2]
                piece = x_ref[:, at].astype(f32) * x_scale * both[0:1]
                normed_out[:, at] = piece.astype(bf16)
            copies[0].wait()
            left = normed_out[:, pl.ds(pl.multiple_of(zz * span, span), span)]

            def tile(i, carry):
                at = pl.ds(pl.multiple_of(i * 512, 512), 512)
                right = chunk[:, :, at].reshape(span, 512)
                raw_out[:, at] += jnp.dot(left, right, preferred_element_type=f32)
                return carry

            lax.fori_loop(0, qkv_width // 512, tile, 0)

        on_line(z, k, body)

    own(1)
    other(fcol, 0, True)
    own(2)
    other(fcol, 1, True)
    other(scol, 0, False)
    for k in range(1, LINE):
        for which in range(2):
            exchange(k, which).start()
    cot_in.wait()
    line_own(1, cot_tmp)
    cot_back = pltpu.make_async_copy(cot_tmp, cot_out.at[z], local.at[10])
    cot_back.start()
    own(3)
    other(fcol, 2, True)
    other(scol, 1, False)
    other(sfcol, 0, False)
    w_back.wait()
    group(0)
    other(fcol, 3, True)
    other(scol, 2, False)
    other(sfcol, 1, False)
    group(1)

    for copy in p_in + [d_in]:
        copy.wait()
    for k in range(1, LINE):
        for which in range(2):
            src_z = lax.rem(z + LINE - k, LINE)
            landed = p_tmp.at[src_z, :, pl.ds(which * width, width)]
            remote(landed, landed, ex_send.at[k, which], ex_recv.at[k, which], second).wait_recv()

    def spot(piece, shard):
        return gu_out.at[piece, shard] if piece < LINE else d_out.at[shard]

    def source(piece):
        return p_tmp.at[piece] if piece < LINE else d_tmp

    def m_send(src, piece, shard, sems, device):
        return remote(
            src, spot(piece, shard), sems.at[piece, shard], m_recv.at[piece, shard], device
        )

    def m_arrived(piece, shard):
        m_send(spot(piece, shard), piece, shard, m_sib_s, sibling).wait_recv()

    for piece in range(pieces):
        m_send(source(piece), piece, col, m_first_s, first).start()
        m_send(source(piece), piece, col, m_second_s, second).start()
        m_send(source(piece), piece, col, m_sib_s, sibling).start()
    backs = [
        pltpu.make_async_copy(p_tmp, gu_out.at[:, col], local.at[11]),
        pltpu.make_async_copy(d_tmp, d_out.at[col], local.at[12]),
    ]
    for copy in backs:
        copy.start()
    line_relay(1, 1)
    other(scol, 3, False)
    other(sfcol, 2, False)
    group(2)
    other(sfcol, 3, False)
    group(3)
    line_relay(1, 2)

    small = jnp.zeros((16, 128), f32)
    for zz in range(LINE):
        for i in range(RING):
            small = small + gain_tmp[zz, i].astype(f32)
    q_gain, k_gain = small[2:3], small[3:4]
    gains_out[2:4, 0:128] = small[2:4]
    cosine, sine, bias = cos_tmp[...], sin_tmp[...], bias_tmp[...]

    def turned(v, gain):
        v = v * rms_scale(v) * gain
        return (v * cosine + half_turn(v) * sine).astype(bf16)

    kv0 = H * HD
    v0 = kv0 + KVH * HD

    def head(g, carry):
        at = pl.ds(pl.multiple_of(g * HD, HD), HD)
        qa = pl.ds(pl.multiple_of(g * 2 * HD, 2 * HD), HD)
        qb = pl.ds(pl.multiple_of(g * 2 * HD + HD, HD), HD)
        key = turned(raw_out[:, pl.ds(pl.multiple_of(kv0 + g * HD, HD), HD)], k_gain)
        value = raw_out[:, pl.ds(pl.multiple_of(v0 + g * HD, HD), HD)].astype(bf16)
        k_out[:, at] = key
        v_out[:, at] = value
        query_a = turned(raw_out[:, qa], q_gain)
        query_b = turned(raw_out[:, qb], q_gain)
        q_out[:, qa] = query_a
        q_out[:, qb] = query_b
        for query, where in ((query_a, qa), (query_b, qb)):
            scores = lax.dot_general(query, key, contract_cols, preferred_element_type=f32)
            logits = scores * (HD ** (-0.5)) + bias
            exponent = jnp.exp(logits - jnp.max(logits, axis=-1, keepdims=True))
            weights = (exponent / lane_sum(exponent)).astype(bf16)
            mixed = jnp.dot(weights, value, preferred_element_type=f32)
            mixed_out[:, where] = mixed.astype(bf16)
        return carry

    lax.fori_loop(0, KVH, head, 0)
    for zz in range(LINE):
        pltpu.make_async_copy(
            w_out.at[pl.ds(RING * zz, RING), :, pl.ds(qkv_width, attn_width - qkv_width)],
            ow_all.at[pl.ds(RING * zz, RING)],
            o_load.at[zz],
        ).wait()
    mixed = mixed_out[...]

    def out_tile(i, total):
        at = pl.ds(pl.multiple_of(i * 512, 512), 512)
        right = ow_all[:, :, at].reshape(mixed.shape[1], 512)
        middle = x_ref[:, at].astype(f32) + jnp.dot(mixed, right, preferred_element_type=f32)
        middle_out[:, at] = middle
        return total + lane_sum(middle * middle)

    tiles = middle_out.shape[1] // 512
    total = lax.fori_loop(0, tiles, out_tile, jnp.zeros((CAP, 1), f32))
    scale = lax.rsqrt(total / middle_out.shape[1] + epsilon)

    def norm_tile(i, carry):
        at = pl.ds(pl.multiple_of(i * 512, 512), 512)
        second_tmp[:, at] = (middle_out[:, at] * scale * gains_out[1:2, at]).astype(bf16)
        return carry

    lax.fori_loop(0, tiles, norm_tile, 0)

    def m_other(piece, shard, onward):
        m_arrived(piece, shard)
        if onward:
            m_send(spot(piece, shard), piece, shard, m_second_s, second).start()
        m_send(spot(piece, shard), piece, shard, m_sib_s, sibling).start()

    m_other(0, fcol, True)
    line_own(0, second_tmp)
    tok_back = pltpu.make_async_copy(second_tmp, tok_out.at[z], local.at[13])
    tok_back.start()
    m_other(0, scol, False)
    m_other(1, fcol, True)
    m_other(1, scol, False)
    line_relay(1, 3)
    m_other(2, fcol, True)
    m_other(2, scol, False)
    line_relay(0, 1)
    m_other(3, fcol, True)
    m_other(3, scol, False)
    m_other(4, fcol, True)
    line_relay(0, 2)
    m_other(4, scol, False)
    m_other(0, sfcol, False)
    m_other(1, sfcol, False)
    line_relay(0, 3)
    for piece in range(2, pieces):
        m_other(piece, sfcol, False)
    for piece in range(pieces):
        for k in range(RING // 2):
            m_arrived(piece, 2 * k + sibling % 2)

    cot_back.wait()
    tok_back.wait()
    for copy in backs:
        copy.wait()
    for k in range(1, LINE):
        for which in range(2):
            exchange(k, which).wait_send()
    for k in range(LINE):

        @pl.when((z < last) & (k <= z))
        def _(k=k):
            send(w_tmp, col + RING * k, up_s, me + RING).wait_send()
            for which in range(2):
                line_send(cot_tmp, which, k, line_up, me + RING).wait_send()

        @pl.when((z > 0) & (k >= z))
        def _(k=k):
            send(w_tmp, col + RING * k, down_s, me - RING).wait_send()
            for which in range(2):
                line_send(cot_tmp, which, k, line_down, me - RING).wait_send()

        send(w_tmp, col + RING * k, first_s, first).wait_send()
        send(w_tmp, col + RING * k, second_s, second).wait_send()
        send(w_tmp, fcol + RING * k, second_s, second).wait_send()
        for base in (col, fcol, scol, sfcol):
            send(w_tmp, base + RING * k, sib_s, sibling).wait_send()
    for piece in range(pieces):
        src = source(piece)
        m_send(src, piece, col, m_first_s, first).wait_send()
        m_send(src, piece, col, m_second_s, second).wait_send()
        m_send(src, piece, fcol, m_second_s, second).wait_send()
        for base in (col, fcol, scol, sfcol):
            m_send(src, piece, base, m_sib_s, sibling).wait_send()


def forward(hidden_in, out_grad, seq_lengths, seq_device, gains, wq, wk, wv, wo, gate, up, wd):
    slots, dim = hidden_in.shape
    rows = wq.shape[0]
    n = RING * LINE
    width = gate.shape[1] // LINE
    qkv_width = wq.shape[1] + wk.shape[1] + wv.shape[1]
    wide = qkv_width + wo.shape[1] + gains.shape[1]
    pieces = LINE + 1
    half = jnp.power(rope_base, -2.0 * jnp.arange(HD // 2, dtype=f32) / HD)
    freqs = jnp.concatenate([half, half])[None, :]
    S = jax.ShapeDtypeStruct
    return pl.pallas_call(
        forward_kernel,
        out_shape=(
            S((n, rows, wide), bf16),
            S((LINE, RING, rows, 2 * width), bf16),
            S((RING,) + wd.shape, bf16),
            S((LINE, slots, dim), bf16),
            S((LINE, slots, dim), bf16),
            S((slots, dim), f32),
            S((slots, dim), bf16),
            S((slots, qkv_width), f32),
            S((slots, H * HD), bf16),
            S((slots, KVH * HD), bf16),
            S((slots, KVH * HD), bf16),
            S((slots, H * HD), bf16),
            S((8, dim), f32),
        ),
        in_specs=[VMEM, ANY] + [VMEM] * 5 + [ANY] * 8,
        out_specs=(ANY,) * 5 + (VMEM,) * 8,
        scratch_shapes=[
            pltpu.VMEM((rows, wide), bf16),
            pltpu.VMEM((LINE, rows, 2 * width), bf16),
            pltpu.VMEM(wd.shape, bf16),
            pltpu.VMEM((slots, dim), bf16),
            pltpu.VMEM((slots, dim), bf16),
            pltpu.VMEM((RING, rows, qkv_width), bf16),
            pltpu.VMEM((n, rows, wo.shape[1]), bf16),
            pltpu.VMEM((LINE, RING, 16, 128), bf16),
            pltpu.VMEM((slots, HD), f32),
            pltpu.VMEM((slots, HD), f32),
            pltpu.VMEM((slots, slots), f32),
            DMA((14,)),
            DMA((n,)),
            DMA((n,)),
            DMA((n,)),
            DMA((n,)),
            DMA((n,)),
            DMA((n,)),
            DMA((LINE, 2)),
            DMA((LINE, 2)),
            DMA((pieces, RING)),
            DMA((pieces, RING)),
            DMA((pieces, RING)),
            DMA((pieces, RING)),
            DMA((2, LINE)),
            DMA((2, LINE)),
            DMA((2, LINE)),
            DMA,
            DMA((LINE,)),
            DMA,
        ],
        compiler_params=pltpu.CompilerParams(
            collective_id=0, has_side_effects=True, vmem_limit_bytes=64000 * 1024
        ),
        name="forward",
    )(
        hidden_in, out_grad, seq_lengths[None, :], seq_device[None, :], seq_lengths[:, None],
        seq_device[:, None], freqs, gains, wq, wk, wv, wo, gate, up, wd,
    )


def add_rows(out, *terms):
    rows = out.shape[0]

    def body(i, carry):
        at = pl.ds(pl.multiple_of(i * 16, 16), 16)
        total = terms[0][at, :].astype(f32)
        for term in terms[1:]:
            total = total + term[at, :].astype(f32)
        out[at, :] = total.astype(out.dtype)
        return carry

    lax.fori_loop(0, rows // 16, body, 0)


def reduce_mlp_kernel(
    gu_ref, d_ref, ds_ref, y_ref, gu_out, d_out, ds_out, y_out,
    gu_own, gu_sib, gu_sec, gu_fst, d_own, d_sib, d_sec, d_fst, t_own, t_down, t_up,
    load, t_load, c_send, c_recv, s_send, s_recv, f_send, f_recv, down_s, down_r, up_s, up_r,
):
    me, z, first, second, sibling = where_am_i()
    greet([lax.rem(me + RING, RING * LINE), lax.rem(me + RING * (LINE - 1), RING * LINE)]
          + [first, second, sibling])
    core = me % 2
    mine, fst, sec = (me % RING) // 2, (first % RING) // 2, (second % RING) // 2
    far = ((second + first - me) % RING) // 2
    half = d_fst.shape[0] // 2
    last = LINE - 1
    groups = ((0, LINE), (LINE, LINE + 2))

    def block(gu, d, piece, group):
        if group == 0:
            return gu.at[piece]
        return d.at[pl.ds(pl.multiple_of((piece - LINE) * half, half), half)]

    def each(body):
        for group, (lo, hi) in enumerate(groups):

            def step(piece, carry, group=group):
                body(piece, group)
                return carry

            lax.fori_loop(lo, hi, step, 0)

    def stored(target, piece, group):
        if group == 0:
            return gu_ref.at[piece, target]
        return block(None, d_ref.at[target], piece, group)

    def to_sibling(quad, piece, group):
        return remote(
            stored(2 * quad + 1 - core, piece, group),
            block(gu_sib.at[quad], d_sib.at[quad], piece, group),
            c_send.at[quad, piece],
            c_recv.at[quad, piece],
            sibling,
        )

    def loading(quad, piece, group):
        return pltpu.make_async_copy(
            stored(2 * quad + core, piece, group),
            block(gu_own.at[quad], d_own.at[quad], piece, group),
            load.at[quad, piece],
        )

    def to_second(quad, slot, piece, group):
        return remote(
            block(gu_own.at[quad], d_own.at[quad], piece, group),
            block(gu_sec.at[slot], d_sec.at[slot], piece, group),
            s_send.at[slot, piece],
            s_recv.at[slot, piece],
            second,
        )

    def to_first(piece, group):
        return remote(
            block(gu_own.at[fst], d_own.at[fst], piece, group),
            block(gu_fst, d_fst, piece, group),
            f_send.at[piece],
            f_recv.at[piece],
            first,
        )

    def send_line(src, which, target, up):
        landing, sends, lands = (t_up, up_s, up_r) if up else (t_down, down_s, down_r)
        return remote(
            src,
            landing.at[which, target],
            sends.at[which, target],
            lands.at[which, target],
            me + RING if up else me - RING,
        )

    tokens = [
        pltpu.make_async_copy(ref, t_own.at[which], t_load.at[which])
        for which, ref in enumerate((ds_ref, y_ref))
    ]
    for copy in tokens:
        copy.start()
    for theirs, own in ((far, far), (fst, sec), (sec, fst), (mine, mine)):

        def begin(piece, group, theirs=theirs, own=own):
            to_sibling(theirs, piece, group).start()
            loading(own, piece, group).start()

        each(begin)
    for copy in tokens:
        copy.wait()
    for k in range(last):
        for which in range(2):

            @pl.when(z == last)
            def _(k=k, which=which):
                send_line(t_own.at[which, k], which, k, False).start()

            @pl.when(z == 0)
            def _(k=k, which=which):
                send_line(t_own.at[which, last - k], which, last - k, True).start()

    def relay(target, which, up):
        @pl.when((target > z) & (z > 0) if up else (target < z) & (z < last))
        def _():
            landing = (t_up if up else t_down).at[which, target]
            send_line(landing, which, target, up).wait_recv()
            add_rows(landing, landing, t_own.at[which, target])
            send_line(landing, which, target, up).start()

    for quad, slot in ((far, 1), (sec, 0)):

        def pass_on(piece, group, quad=quad, slot=slot):
            loading(quad, piece, group).wait()
            to_sibling(quad, piece, group).wait_recv()
            own = block(gu_own.at[quad], d_own.at[quad], piece, group)
            add_rows(own, own, block(gu_sib.at[quad], d_sib.at[quad], piece, group))
            to_second(quad, slot, piece, group).start()

        each(pass_on)
    for which in range(2):
        relay(0, which, False)
        relay(last, which, True)

    def narrow(piece, group):
        loading(fst, piece, group).wait()
        to_sibling(fst, piece, group).wait_recv()
        to_second(far, 1, piece, group).wait_recv()
        own = block(gu_own.at[fst], d_own.at[fst], piece, group)
        add_rows(
            own,
            own,
            block(gu_sib.at[fst], d_sib.at[fst], piece, group),
            block(gu_sec.at[1], d_sec.at[1], piece, group),
        )
        to_first(piece, group).start()

    each(narrow)
    for k in range(1, last):
        for which in range(2):
            relay(k, which, False)
            relay(last - k, which, True)

    def finish(piece, group):
        loading(mine, piece, group).wait()
        to_sibling(mine, piece, group).wait_recv()
        to_second(sec, 0, piece, group).wait_recv()
        to_first(piece, group).wait_recv()
        add_rows(
            block(gu_out, d_out, piece, group),
            block(gu_own.at[mine], d_own.at[mine], piece, group),
            block(gu_sib.at[mine], d_sib.at[mine], piece, group),
            block(gu_sec.at[0], d_sec.at[0], piece, group),
            block(gu_fst, d_fst, piece, group),
        )

    each(finish)
    for which, out in enumerate((ds_out, y_out)):
        own = t_own.at[which, z]
        above, below = t_down.at[which, z], t_up.at[which, z]

        @pl.when(z < last)
        def _(which=which, above=above):
            send_line(above, which, z, False).wait_recv()

        @pl.when(z > 0)
        def _(which=which, below=below):
            send_line(below, which, z, True).wait_recv()

        @pl.when(z == 0)
        def _(out=out, own=own, above=above):
            add_rows(out, own, above)

        @pl.when(z == last)
        def _(out=out, own=own, below=below):
            add_rows(out, own, below)

        @pl.when((z > 0) & (z < last))
        def _(out=out, own=own, above=above, below=below):
            add_rows(out, own, above, below)

    def drain(piece, group):
        for quad in (far, fst, sec, mine):
            to_sibling(quad, piece, group).wait_send()
        to_second(far, 1, piece, group).wait_send()
        to_second(sec, 0, piece, group).wait_send()
        to_first(piece, group).wait_send()

    each(drain)
    for which in range(2):
        for k in range(LINE):

            @pl.when((z > 0) & (k < z))
            def _(which=which, k=k):
                send_line(t_down.at[which, k], which, k, False).wait_send()

            @pl.when((z < last) & (k > z))
            def _(which=which, k=k):
                send_line(t_up.at[which, k], which, k, True).wait_send()


def reduce_mlp(gu, d, ds, y):
    rows, cols = gu.shape[2:]
    drows, dcols = d.shape[1:]
    tok = ds.shape[1:]
    quads = RING // 2
    pieces = LINE + 2
    return pl.pallas_call(
        reduce_mlp_kernel,
        out_shape=(
            jax.ShapeDtypeStruct((LINE, rows, cols), bf16),
            jax.ShapeDtypeStruct((drows, dcols), f32),
            jax.ShapeDtypeStruct(tok, f32),
            jax.ShapeDtypeStruct(tok, f32),
        ),
        in_specs=[ANY] * 4,
        out_specs=(VMEM,) * 4,
        scratch_shapes=[
            pltpu.VMEM((quads, LINE, rows, cols), bf16),
            pltpu.VMEM((quads, LINE, rows, cols), bf16),
            pltpu.VMEM((2, LINE, rows, cols), bf16),
            pltpu.VMEM((LINE, rows, cols), bf16),
            pltpu.VMEM((quads, drows, dcols), bf16),
            pltpu.VMEM((quads, drows, dcols), bf16),
            pltpu.VMEM((2, drows, dcols), bf16),
            pltpu.VMEM((drows, dcols), bf16),
            pltpu.VMEM((2, LINE) + tok, bf16),
            pltpu.VMEM((2, LINE) + tok, bf16),
            pltpu.VMEM((2, LINE) + tok, bf16),
            DMA((quads, pieces)),
            DMA((2,)),
            DMA((quads, pieces)),
            DMA((quads, pieces)),
            DMA((2, pieces)),
            DMA((2, pieces)),
            DMA((pieces,)),
            DMA((pieces,)),
            DMA((2, LINE)),
            DMA((2, LINE)),
            DMA((2, LINE)),
            DMA((2, LINE)),
        ],
        compiler_params=pltpu.CompilerParams(
            collective_id=2, has_side_effects=True, vmem_limit_bytes=64000 * 1024
        ),
        name="reduce_mlp",
    )(gu, d, ds, y)


def reduce_attn_kernel(
    a_ref, o_ref, gu_ref, s_ref, q_out, k_out, v_out, o_out, gate_out, up_out, s_out,
    own, sib, sec, fst, down, up, ex, s_sum, s_got, s_line,
    load, ex_load, c_send, c_recv, s_send, s_recv, f_send, f_recv, down_s, down_r, up_s, up_r,
    ex_s, ex_r, small_s, small_r,
):
    me, z, first, second, sibling = where_am_i()
    greet(line_peers(me) + [first, second, sibling])
    core = me % 2
    q_mine, q_fst, q_sec = (me % RING) // 2, (first % RING) // 2, (second % RING) // 2
    q_far = ((second + first - me) % RING) // 2
    last = LINE - 1
    split = a_ref.shape[2]
    parts = ((a_ref, pl.ds(0, split)), (o_ref, pl.ds(split, o_ref.shape[2])))
    order = (
        last * (1 - z // 2),
        2 - 2 * z + 5 * (z // 2),
        1 + z % 2,
        z,
    )

    def to_sibling(t, quad, part):
        ref, at = parts[part]
        return remote(
            ref.at[RING * t + 2 * quad + 1 - core],
            sib.at[t, quad, :, at],
            c_send.at[t, quad, part],
            c_recv.at[t, quad, part],
            sibling,
        )

    def loading(t, quad, part):
        ref, at = parts[part]
        return pltpu.make_async_copy(
            ref.at[RING * t + 2 * quad + core], own.at[t, quad, :, at], load.at[t, quad, part]
        )

    def ready(t, quad):
        for part in range(2):
            loading(t, quad, part).wait()
            to_sibling(t, quad, part).wait_recv()

    def to_second(t, quad, slot):
        return remote(
            own.at[t, quad], sec.at[slot, t], s_send.at[slot, t], s_recv.at[slot, t], second
        )

    def to_first(t):
        return remote(own.at[t, q_fst], fst.at[t], f_send.at[t], f_recv.at[t], first)

    def send_line(src, t, upward):
        if upward:
            return remote(src, up.at[t], up_s.at[t], up_r.at[t], me + RING)
        return remote(src, down.at[t], down_s.at[t], down_r.at[t], me - RING)

    def exchange(k):
        peer_z = lax.rem(z + k, LINE)
        return remote(
            gu_ref.at[peer_z], ex.at[z], ex_s.at[k], ex_r.at[k], me % RING + RING * peer_z
        )

    def small(step, src, dst, device):
        return remote(src, dst, small_s.at[step], small_r.at[step], device)

    small_c = small(0, s_ref, s_got.at[0], sibling)
    small_c.start()
    for k in range(1, LINE):
        exchange(k).start()
    ex_in = pltpu.make_async_copy(gu_ref.at[z], ex.at[z], ex_load)
    ex_in.start()
    for t in order:
        for theirs, ours in ((q_far, q_far), (q_fst, q_sec), (q_sec, q_fst), (q_mine, q_mine)):
            for part in range(2):
                to_sibling(t, theirs, part).start()
                loading(t, ours, part).start()

    def spread(t):
        for quad, slot in ((q_far, 1), (q_sec, 0)):
            ready(t, quad)
            add_rows(own.at[t, quad], own.at[t, quad], sib.at[t, quad])
            to_second(t, quad, slot).start()

    def narrow(t):
        ready(t, q_fst)
        to_second(t, q_far, 1).wait_recv()
        add_rows(own.at[t, q_fst], own.at[t, q_fst], sib.at[t, q_fst], sec.at[1, t])
        to_first(t).start()

    def collect(t):
        ready(t, q_mine)
        to_second(t, q_sec, 0).wait_recv()
        to_first(t).wait_recv()
        mine = own.at[t, q_mine]
        add_rows(mine, mine, sib.at[t, q_mine], sec.at[0, t], fst.at[t])

        @pl.when((t < z) & (z == last))
        def _():
            send_line(mine, t, False).start()

        @pl.when((t > z) & (z == 0))
        def _():
            send_line(mine, t, True).start()

    def relay(t):
        @pl.when((t < z) & (z < last))
        def _():
            landing = down.at[t]
            send_line(landing, t, False).wait_recv()
            add_rows(landing, landing, own.at[t, q_mine])
            send_line(landing, t, False).start()

        @pl.when((t > z) & (z > 0))
        def _():
            landing = up.at[t]
            send_line(landing, t, True).wait_recv()
            add_rows(landing, landing, own.at[t, q_mine])
            send_line(landing, t, True).start()

    spread(order[0])
    small_c.wait()
    s_sum[0] = s_ref[...] + s_got[0]
    small_f = small(1, s_sum.at[0], s_got.at[1], first)
    small_f.start()
    spread(order[1])
    narrow(order[0])
    small_f.wait()
    s_sum[1] = s_sum[0] + s_got[1]
    small_s2 = small(2, s_sum.at[1], s_got.at[2], second)
    small_s2.start()
    spread(order[2])
    narrow(order[1])
    collect(order[0])
    small_s2.wait()
    s_sum[2] = s_sum[1] + s_got[2]
    small_line = [
        small(
            2 + k, s_sum.at[2], s_line.at[k], me % RING + RING * lax.rem(z + k, LINE)
        )
        for k in range(1, LINE)
    ]
    for copy in small_line:
        copy.start()
    spread(order[3])
    narrow(order[2])
    collect(order[1])
    relay(order[0])
    narrow(order[3])
    collect(order[2])
    relay(order[1])
    collect(order[3])
    relay(order[2])
    ex_in.wait()
    for k in range(1, LINE):
        src_z = lax.rem(z + LINE - k, LINE)
        landed = ex.at[src_z]
        remote(landed, landed, ex_s.at[k], ex_r.at[k], sibling).wait_recv()
    width = gate_out.shape[1] // LINE
    for k in range(LINE):
        add_rows(gate_out.at[:, pl.ds(k * width, width)], ex.at[k, :, pl.ds(0, width)])
        add_rows(up_out.at[:, pl.ds(k * width, width)], ex.at[k, :, pl.ds(width, width)])
    for copy in small_line:
        copy.wait()
    s_out[...] = (s_sum[2] + s_line[2]) + (s_line[1] + s_line[3])
    mine, above, below = own.at[z, q_mine], down.at[z], up.at[z]

    @pl.when(z < last)
    def _():
        send_line(above, z, False).wait_recv()

    @pl.when(z > 0)
    def _():
        send_line(below, z, True).wait_recv()

    def total(*terms):
        lo = 0
        for out in (q_out, k_out, v_out, o_out):
            at = pl.ds(lo, out.shape[1])
            add_rows(out, *[term.at[:, at] for term in terms])
            lo += out.shape[1]

    @pl.when(z == 0)
    def _():
        total(mine, above)

    @pl.when(z == last)
    def _():
        total(mine, below)

    @pl.when((z > 0) & (z < last))
    def _():
        total(mine, above, below)

    for k in range(1, LINE):
        exchange(k).wait_send()
    for t in range(LINE):
        for quad in (q_far, q_fst, q_sec, q_mine):
            for part in range(2):
                to_sibling(t, quad, part).wait_send()
        to_second(t, q_far, 1).wait_send()
        to_second(t, q_sec, 0).wait_send()
        to_first(t).wait_send()

        @pl.when(t < z)
        def _(t=t):
            send_line(down.at[t], t, False).wait_send()

        @pl.when(t > z)
        def _(t=t):
            send_line(up.at[t], t, True).wait_send()


def reduce_attn(a, o, gu, small):
    rows, split = a.shape[1:]
    owide = o.shape[2]
    wide = split + owide
    quads = RING // 2
    width = gu.shape[2] // 2
    kv = KVH * HD
    return pl.pallas_call(
        reduce_attn_kernel,
        out_shape=(
            jax.ShapeDtypeStruct((rows, H * HD), f32),
            jax.ShapeDtypeStruct((rows, kv), f32),
            jax.ShapeDtypeStruct((rows, kv), f32),
            jax.ShapeDtypeStruct((rows, owide), f32),
            jax.ShapeDtypeStruct((rows, LINE * width), f32),
            jax.ShapeDtypeStruct((rows, LINE * width), f32),
            jax.ShapeDtypeStruct(small.shape, f32),
        ),
        in_specs=[ANY, ANY, ANY, VMEM],
        out_specs=(VMEM,) * 7,
        scratch_shapes=[
            pltpu.VMEM((LINE, quads, rows, wide), bf16),
            pltpu.VMEM((LINE, quads, rows, wide), bf16),
            pltpu.VMEM((2, LINE, rows, wide), bf16),
            pltpu.VMEM((LINE, rows, wide), bf16),
            pltpu.VMEM((LINE, rows, wide), bf16),
            pltpu.VMEM((LINE, rows, wide), bf16),
            pltpu.VMEM((LINE, rows, 2 * width), bf16),
            pltpu.VMEM((3,) + small.shape, f32),
            pltpu.VMEM((3,) + small.shape, f32),
            pltpu.VMEM((LINE,) + small.shape, f32),
            DMA((LINE, quads, 2)),
            DMA,
            DMA((LINE, quads, 2)),
            DMA((LINE, quads, 2)),
            DMA((2, LINE)),
            DMA((2, LINE)),
            DMA((LINE,)),
            DMA((LINE,)),
            DMA((LINE,)),
            DMA((LINE,)),
            DMA((LINE,)),
            DMA((LINE,)),
            DMA((LINE,)),
            DMA((LINE,)),
            DMA((2 + LINE,)),
            DMA((2 + LINE,)),
        ],
        compiler_params=pltpu.CompilerParams(
            collective_id=3, has_side_effects=True, vmem_limit_bytes=64000 * 1024
        ),
        name="reduce_attn",
    )(a, o, gu, small)


def layout(seq_lengths, seq_device, owner, slots):
    owned = seq_device == owner
    counts = jnp.where(owned, seq_lengths, 0)
    starts = jnp.cumsum(counts) - counts
    places = jnp.arange(slots, dtype=jnp.int32)
    inside = (
        owned[:, None]
        & (places[None, :] >= starts[:, None])
        & (places[None, :] < (starts + counts)[:, None])
    )
    labels = jnp.arange(seq_lengths.shape[0], dtype=jnp.int32)
    segment = jnp.sum(jnp.where(inside, labels[:, None] + 1, 0), axis=0) - 1
    position = jnp.sum(jnp.where(inside, places[None, :] - starts[:, None], 0), axis=0)
    return (segment, position)


def allowed_pairs(segment):
    places = jnp.arange(segment.shape[0], dtype=jnp.int32)
    earlier = places[None, :] < places[:, None]
    same_seq = (segment[:, None] == segment[None, :]) & (segment[:, None] >= 0)
    return (places[:, None] == places[None, :]) | earlier & same_seq


def rmsnorm(values, gain):
    return values * lax.rsqrt(jnp.mean(values * values, axis=-1, keepdims=True) + epsilon) * gain


def rotary(values, position):
    half_dim = values.shape[-1] // 2
    freqs = jnp.power(rope_base, -2.0 * jnp.arange(half_dim, dtype=jnp.float32) / values.shape[-1])
    angles = position.astype(jnp.float32)[:, None] * freqs[None, :]
    cosine = jnp.concatenate([jnp.cos(angles), jnp.cos(angles)], axis=-1)[:, None, :]
    sine = jnp.concatenate([jnp.sin(angles), jnp.sin(angles)], axis=-1)[:, None, :]
    rotated = jnp.concatenate([-values[..., half_dim:], values[..., :half_dim]], axis=-1)
    return values * cosine + rotated * sine


def matmul(left, right):
    return jnp.dot(left, right, preferred_element_type=jnp.float32)


def times_rows(left, right):
    return lax.dot_general(left, right, contract_rows, preferred_element_type=jnp.float32)


def times_cols(left, right):
    return lax.dot_general(left, right, contract_cols, preferred_element_type=jnp.float32)


def scatter_sum(partial):
    total = lax.psum_scatter(
        partial.astype(jnp.bfloat16), "fsdp", scatter_dimension=0, tiled=True
    )
    return total.astype(jnp.float32)


def plain(
    hidden_in,
    out_grad,
    seq_lengths,
    seq_device,
    attn_gain,
    q_gain,
    k_gain,
    w_query,
    w_key,
    w_value,
    w_out,
    mlp_gain,
    w_gate,
    w_up,
    w_down,
):
    slots = hidden_in.shape[0]
    groups = H // KVH
    score_scale = HD ** (-0.5)
    segment, position = layout(seq_lengths, seq_device, lax.axis_index("fsdp"), slots)
    allowed = allowed_pairs(segment)[None, None]

    def query_path(raw, gain):
        return rotary(rmsnorm(raw.reshape(slots, H, HD), gain), position)

    def key_path(raw, gain):
        return rotary(rmsnorm(raw.reshape(slots, KVH, HD), gain), position)

    def swiglu(gate_in, up_in):
        return jax.nn.silu(gate_in) * up_in

    attn_set = (
        lax.all_gather(attn_gain, "fsdp", axis=0, tiled=True),
        lax.all_gather(q_gain, "fsdp", axis=0, tiled=True),
        lax.all_gather(k_gain, "fsdp", axis=0, tiled=True),
        lax.all_gather(w_query, "fsdp", axis=0, tiled=True),
        lax.all_gather(w_key, "fsdp", axis=0, tiled=True),
        lax.all_gather(w_value, "fsdp", axis=0, tiled=True),
        lax.all_gather(w_out, "fsdp", axis=0, tiled=True),
    )
    gain_attn, gain_query, gain_key, query_w, key_w, value_w, out_w = attn_set
    inputs = hidden_in.astype(jnp.float32)
    normed = rmsnorm(inputs, gain_attn.astype(jnp.float32)).astype(jnp.bfloat16)
    query_raw = matmul(normed, query_w)
    key_raw = matmul(normed, key_w)
    value_raw = matmul(normed, value_w)
    queries = (
        query_path(query_raw, gain_query.astype(jnp.float32))
        .astype(jnp.bfloat16)
        .reshape(slots, KVH, groups, HD)
    )
    keys = key_path(key_raw, gain_key.astype(jnp.float32)).astype(jnp.bfloat16)
    values = value_raw.astype(jnp.bfloat16).reshape(slots, KVH, HD)

    def masked_logits():
        scores = (
            jnp.einsum("qgrd,kgd->grqk", queries, keys, preferred_element_type=jnp.float32)
            * score_scale
        )
        return jnp.where(allowed, scores, masked_score)

    logits = masked_logits()
    row_top = jnp.max(logits, axis=-1, keepdims=True)
    exponent = jnp.exp(logits - row_top)
    row_total = jnp.sum(exponent, axis=-1, keepdims=True)
    log_total = row_top + jnp.log(row_total)
    weights = (exponent / row_total).astype(jnp.bfloat16)
    mixed = jnp.einsum("grqk,kgd->qgrd", weights, values, preferred_element_type=jnp.float32)
    mixed = mixed.reshape(slots, H * HD).astype(jnp.bfloat16)
    middle = inputs + matmul(mixed, out_w)
    mlp_set = (
        lax.all_gather(mlp_gain, "fsdp", axis=0, tiled=True),
        lax.all_gather(w_gate, "fsdp", axis=0, tiled=True),
        lax.all_gather(w_up, "fsdp", axis=0, tiled=True),
        lax.all_gather(w_down, "fsdp", axis=0, tiled=True),
    )
    gain_mlp, gate_w, up_w, down_w = mlp_set
    second = rmsnorm(middle, gain_mlp.astype(jnp.float32)).astype(jnp.bfloat16)
    gate_out = matmul(second, gate_w)
    up_out = matmul(second, up_w)
    hidden = swiglu(gate_out, up_out).astype(jnp.bfloat16)
    hidden_out = (middle + matmul(hidden, down_w)).astype(jnp.bfloat16)
    gain_mlp, gate_w, up_w, down_w = (
        lax.all_gather(mlp_gain, "fsdp", axis=0, tiled=True),
        lax.all_gather(w_gate, "fsdp", axis=0, tiled=True),
        lax.all_gather(w_up, "fsdp", axis=0, tiled=True),
        lax.all_gather(w_down, "fsdp", axis=0, tiled=True),
    )
    grad_down = scatter_sum(times_rows(hidden, out_grad))
    d_hidden = times_cols(out_grad, down_w)
    unused_out, swiglu_pull = jax.vjp(swiglu, gate_out, up_out)
    d_gate, d_up = swiglu_pull(d_hidden)
    d_gate_up = jnp.concatenate([d_gate.astype(jnp.bfloat16), d_up.astype(jnp.bfloat16)], axis=1)
    grad_gate_up = scatter_sum(times_rows(second, d_gate_up))
    ff_width = gate_w.shape[1]
    d_second = times_cols(d_gate_up, jnp.concatenate([gate_w, up_w], axis=1))
    unused_norm, second_pull = jax.vjp(rmsnorm, middle, gain_mlp.astype(jnp.float32))
    d_middle_norm, grad_gain_mlp = second_pull(d_second)
    d_middle = out_grad.astype(jnp.float32) + d_middle_norm
    gain_attn, gain_query, gain_key, query_w, key_w, value_w, out_w = (
        lax.all_gather(attn_gain, "fsdp", axis=0, tiled=True),
        lax.all_gather(q_gain, "fsdp", axis=0, tiled=True),
        lax.all_gather(k_gain, "fsdp", axis=0, tiled=True),
        lax.all_gather(w_query, "fsdp", axis=0, tiled=True),
        lax.all_gather(w_key, "fsdp", axis=0, tiled=True),
        lax.all_gather(w_value, "fsdp", axis=0, tiled=True),
        lax.all_gather(w_out, "fsdp", axis=0, tiled=True),
    )
    d_branch = d_middle.astype(jnp.bfloat16)
    grad_out_w = scatter_sum(times_rows(mixed, d_branch))
    d_mixed = times_cols(d_branch, out_w).astype(jnp.bfloat16).reshape(slots, KVH, groups, HD)
    probs = jnp.exp(masked_logits() - log_total)
    weights = probs.astype(jnp.bfloat16)
    d_probs = jnp.einsum("qgrd,kgd->grqk", d_mixed, values, preferred_element_type=jnp.float32)
    d_logits = probs * (d_probs - jnp.sum(probs * d_probs, axis=-1, keepdims=True))
    d_scores = (d_logits * score_scale).astype(jnp.bfloat16)
    d_values = jnp.einsum("grqk,qgrd->kgd", weights, d_mixed, preferred_element_type=jnp.float32)
    d_values = d_values.astype(jnp.bfloat16).reshape(slots, KVH * HD)
    d_queries_rot = jnp.einsum(
        "grqk,kgd->qgrd", d_scores, keys, preferred_element_type=jnp.float32
    ).reshape(slots, H, HD)
    d_keys_rot = jnp.einsum("grqk,qgrd->kgd", d_scores, queries, preferred_element_type=jnp.float32)
    unused_query, query_pull = jax.vjp(query_path, query_raw, gain_query.astype(jnp.float32))
    d_query_raw, grad_gain_query = query_pull(d_queries_rot)
    unused_key, key_pull = jax.vjp(key_path, key_raw, gain_key.astype(jnp.float32))
    d_key_raw, grad_gain_key = key_pull(d_keys_rot)
    d_qkv = jnp.concatenate(
        [d_query_raw.astype(jnp.bfloat16), d_key_raw.astype(jnp.bfloat16), d_values], axis=1
    )
    grad_qkv = scatter_sum(times_rows(normed, d_qkv))
    d_normed = times_cols(d_qkv, jnp.concatenate([query_w, key_w, value_w], axis=1))
    unused_first, first_pull = jax.vjp(rmsnorm, inputs, gain_attn.astype(jnp.float32))
    d_input_norm, grad_gain_attn = first_pull(d_normed)
    input_grad = d_middle + d_input_norm
    gain_sums = (
        lax.psum_scatter(grad_gain_attn, "fsdp", scatter_dimension=0, tiled=True),
        lax.psum_scatter(grad_gain_query, "fsdp", scatter_dimension=0, tiled=True),
        lax.psum_scatter(grad_gain_key, "fsdp", scatter_dimension=0, tiled=True),
        lax.psum_scatter(grad_gain_mlp, "fsdp", scatter_dimension=0, tiled=True),
    )
    query_width = H * HD
    key_width = KVH * HD
    grad_query_w = grad_qkv[:, :query_width]
    grad_key_w = grad_qkv[:, query_width : query_width + key_width]
    grad_value_w = grad_qkv[:, query_width + key_width :]
    grad_gate = grad_gate_up[:, :ff_width]
    grad_up = grad_gate_up[:, ff_width:]
    return (
        hidden_out,
        input_grad,
        gain_sums[0],
        gain_sums[1],
        gain_sums[2],
        grad_query_w,
        grad_key_w,
        grad_value_w,
        grad_out_w,
        gain_sums[3],
        grad_gate,
        grad_up,
        grad_down,
    )


def layered(
    hidden_in,
    out_grad,
    seq_lengths,
    seq_device,
    attn_gain,
    q_gain,
    k_gain,
    w_query,
    w_key,
    w_value,
    w_out,
    mlp_gain,
    w_gate,
    w_up,
    w_down,
):
    slots, width = hidden_in.shape
    groups = H // KVH
    score_scale = HD ** (-0.5)
    n = RING * LINE
    rows = w_query.shape[0]
    me = lax.axis_index("fsdp")
    segment, position = layout(seq_lengths, seq_device, me, slots)
    allowed = allowed_pairs(segment)[None, None]
    query_width = H * HD
    qkv_width = query_width + 2 * KVH * HD
    attn_width = qkv_width + w_out.shape[1]

    def query_path(raw, gain):
        return rotary(rmsnorm(raw.reshape(slots, H, HD), gain), position)

    def key_path(raw, gain):
        return rotary(rmsnorm(raw.reshape(slots, KVH, HD), gain), position)

    def swiglu(gate_in, up_in):
        return jax.nn.silu(gate_in) * up_in

    lane = jnp.arange(128)[None, :]

    def spread(gain, start, share):
        placed = jnp.tile(gain, 128 // share)[None, :]
        return jnp.where((lane >= start) & (lane < start + share), placed, 0)

    pair = rows * (me % 2)
    share = q_gain.shape[0]
    gains = [spread(attn_gain, pair, rows), spread(mlp_gain, pair, rows)]
    gains += [spread(q_gain, me * share, share), spread(k_gain, me * share, share)]
    gains = jnp.pad(jnp.concatenate(gains, axis=0), ((0, rows - 4), (0, 0)))
    (
        attn_w, gate_up_w, down_w, tokens, cotangent,
        middle, normed, qkv_raw, queries, keys, values, mixed, gains,
    ) = forward(
        hidden_in, out_grad, seq_lengths, seq_device, gains,
        w_query, w_key, w_value, w_out, w_gate, w_up, w_down,
    )
    gain_attn, gain_mlp = gains[0], gains[1]
    gain_query, gain_key = gains[2, :HD], gains[3, :HD]
    attn_w = attn_w.reshape(n * rows, attn_w.shape[2])
    qkv_w = attn_w[:, :qkv_width]
    out_w = attn_w[:, qkv_width:attn_width]
    inputs = hidden_in.astype(f32)
    query_raw = qkv_raw[:, :query_width]
    key_raw = qkv_raw[:, query_width : query_width + KVH * HD]
    queries = queries.reshape(slots, KVH, groups, HD)
    keys = keys.reshape(slots, KVH, HD)
    values = values.reshape(slots, KVH, HD)
    scores = jnp.einsum("qgrd,kgd->grqk", queries, keys, preferred_element_type=f32) * score_scale
    logits = jnp.where(allowed, scores, masked_score)
    exponent = jnp.exp(logits - jnp.max(logits, axis=-1, keepdims=True))
    probs = exponent / jnp.sum(exponent, axis=-1, keepdims=True)
    weights = probs.astype(bf16)

    gate_up_w = gate_up_w.reshape(n * rows, gate_up_w.shape[-1])
    down_w = down_w.reshape(-1, down_w.shape[-1])
    tokens = tokens.reshape(-1, width)
    cotangent = cotangent.reshape(-1, width)
    part = gate_up_w.shape[1] // 2
    gate_up = matmul(tokens, gate_up_w)
    gate_out, up_out = gate_up[:, :part], gate_up[:, part:]
    hidden = swiglu(gate_out, up_out).astype(bf16)
    y_part = matmul(hidden, down_w).astype(bf16)
    d_hidden = times_cols(cotangent, down_w)
    unused_out, swiglu_pull = jax.vjp(swiglu, gate_out, up_out)
    d_gate, d_up = swiglu_pull(d_hidden)
    d_gate_up = jnp.concatenate([d_gate.astype(bf16), d_up.astype(bf16)], axis=1)
    ds_part = times_cols(d_gate_up, gate_up_w).astype(bf16)
    g_gate_up = times_rows(tokens, d_gate_up).astype(bf16)
    g_down = times_rows(hidden, cotangent).astype(bf16)
    g_gate_up, grad_down, d_second, y = reduce_mlp(
        g_gate_up.reshape(LINE, RING, rows, 2 * part),
        g_down.reshape(RING, w_down.shape[0], width),
        ds_part.reshape(LINE, slots, width),
        y_part.reshape(LINE, slots, width),
    )
    hidden_out = (middle + y).astype(bf16)

    unused_norm, second_pull = jax.vjp(rmsnorm, middle, gain_mlp)
    d_middle_norm, grad_gain_mlp = second_pull(d_second)
    d_middle = out_grad.astype(f32) + d_middle_norm
    d_branch = d_middle.astype(bf16)
    g_out = times_rows(mixed, d_branch).astype(bf16)
    d_mixed = times_cols(d_branch, out_w).astype(bf16).reshape(slots, KVH, groups, HD)
    d_probs = jnp.einsum("qgrd,kgd->grqk", d_mixed, values, preferred_element_type=f32)
    d_logits = probs * (d_probs - jnp.sum(probs * d_probs, axis=-1, keepdims=True))
    d_scores = (d_logits * score_scale).astype(bf16)
    d_values = jnp.einsum("grqk,qgrd->kgd", weights, d_mixed, preferred_element_type=f32)
    d_values = d_values.astype(bf16).reshape(slots, KVH * HD)
    d_queries_rot = jnp.einsum(
        "grqk,kgd->qgrd", d_scores, keys, preferred_element_type=f32
    ).reshape(slots, H, HD)
    d_keys_rot = jnp.einsum("grqk,qgrd->kgd", d_scores, queries, preferred_element_type=f32)
    unused_query, query_pull = jax.vjp(query_path, query_raw, gain_query)
    d_query_raw, grad_gain_query = query_pull(d_queries_rot)
    unused_key, key_pull = jax.vjp(key_path, key_raw, gain_key)
    d_key_raw, grad_gain_key = key_pull(d_keys_rot)
    d_qkv = jnp.concatenate([d_query_raw.astype(bf16), d_key_raw.astype(bf16), d_values], axis=1)
    g_qkv = times_rows(normed, d_qkv).astype(bf16)
    d_normed = times_cols(d_qkv, qkv_w)
    unused_first, first_pull = jax.vjp(rmsnorm, inputs, gain_attn)
    d_input_norm, grad_gain_attn = first_pull(d_normed)
    input_grad = d_middle + d_input_norm
    gain_grads = (grad_gain_attn, grad_gain_query, grad_gain_key, grad_gain_mlp)
    small = jnp.concatenate(gain_grads)
    small = jnp.pad(small, (0, -small.shape[0] % 1024)).reshape(-1, 128)
    g_query, g_key, g_value, g_out, g_gate, g_up, small = reduce_attn(
        g_qkv.reshape(n, rows, qkv_width), g_out.reshape(n, rows, w_out.shape[1]), g_gate_up, small
    )
    small = small.reshape(-1)
    gain_sums = []
    lo = 0
    for grad in gain_grads:
        share = grad.shape[0] // n
        gain_sums.append(lax.dynamic_slice(small, (lo + me * share,), (share,)))
        lo += grad.shape[0]
    return (
        hidden_out,
        input_grad,
        gain_sums[0],
        gain_sums[1],
        gain_sums[2],
        g_query,
        g_key,
        g_value,
        g_out,
        gain_sums[3],
        g_gate,
        g_up,
        grad_down,
    )


def solution(mesh):
    per_device = layered if mesh.shape["fsdp"] == RING * LINE else plain
    return jax.shard_map(
        per_device,
        mesh=mesh,
        in_specs=(
            P("fsdp", None),
            P("fsdp", None),
            P(),
            P(),
            P("fsdp"),
            P("fsdp"),
            P("fsdp"),
            P("fsdp", None),
            P("fsdp", None),
            P("fsdp", None),
            P("fsdp", None),
            P("fsdp"),
            P("fsdp", None),
            P("fsdp", None),
            P("fsdp", None),
        ),
        out_specs=(
            P("fsdp", None),
            P("fsdp", None),
            P("fsdp"),
            P("fsdp"),
            P("fsdp"),
            P("fsdp", None),
            P("fsdp", None),
            P("fsdp", None),
            P("fsdp", None),
            P("fsdp"),
            P("fsdp", None),
            P("fsdp", None),
            P("fsdp", None),
        ),
        check_vma=False,
    )
```

```python
import math

import jax
import jax.numpy as jnp
from jax import lax
from jax.experimental import pallas as pl
from jax.experimental.pallas import tpu as pltpu
from jax.sharding import PartitionSpec as P

H = 16
KVH = 8
HD = 128
CAP = 128
LINE = 4
RING = 8
MESH = pl.DeviceIdType.MESH
ANY = pl.BlockSpec(memory_space=pl.ANY)
VMEM = pl.BlockSpec(memory_space=pltpu.VMEM)
DMA = pltpu.SemaphoreType.DMA
bf16 = jnp.bfloat16
f32 = jnp.float32
epsilon = 1e-06
rope_base = 1000000.0
masked_score = -1e30
contract_rows = (((0,), (0,)), ((), ()))
contract_cols = (((1,), (1,)), ((), ()))


def where_am_i():
    me = lax.axis_index("fsdp")
    core = me % 2
    z = me // RING
    f_bit = 2 + 2 * core
    s_bit = 4 - 2 * core
    first = me + f_bit * (1 - 2 * ((me // f_bit) % 2))
    second = me + s_bit * (1 - 2 * ((me // s_bit) % 2))
    sibling = me + 1 - 2 * core
    return me, z, first, second, sibling


def greet(peers):
    barrier = pltpu.get_barrier_semaphore()
    for peer in peers:
        pl.semaphore_signal(barrier, inc=1, device_id=(peer,), device_id_type=MESH)
    pl.semaphore_wait(barrier, len(peers))


def remote(src, dst, send_sem, recv_sem, device):
    return pltpu.make_async_remote_copy(
        src_ref=src,
        dst_ref=dst,
        send_sem=send_sem,
        recv_sem=recv_sem,
        device_id=(device,),
        device_id_type=MESH,
    )


def line_peers(me):
    return [lax.rem(me + RING * k, RING * LINE) for k in range(1, LINE)]


def on_line(z, k, body):
    for step in ((-k, k) if k else (0,)):

        @pl.when((z + step >= 0) & (z + step < LINE))
        def _(step=step):
            body(step)


def dot_nt(left, right):
    return lax.dot_general(left, right, contract_cols, preferred_element_type=f32)


def dot_tn(left, right):
    return lax.dot_general(left, right, contract_rows, preferred_element_type=f32)


def streamed(count, fetch, body):
    for copy in fetch(0, 0):
        copy.start()

    def step(i, carry):
        slot = i % 2

        @pl.when(i + 1 < count)
        def _():
            for copy in fetch(i + 1, 1 - slot):
                copy.start()

        for copy in fetch(i, slot):
            copy.wait()
        body(i, slot)
        return carry

    lax.fori_loop(0, count, step, 0)


def tile(i, size):
    return pl.ds(pl.multiple_of(i * size, size), size)


def add_rows(out, *terms):
    rows = out.shape[0]

    def body(i, carry):
        at = pl.ds(pl.multiple_of(i * 16, 16), 16)
        total = terms[0][at, :].astype(f32)
        for term in terms[1:]:
            total = total + term[at, :].astype(f32)
        out[at, :] = total.astype(out.dtype)
        return carry

    lax.fori_loop(0, rows // 16, body, 0)


def lane_sum(x):
    return jnp.sum(x, axis=-1, keepdims=True)


def token_places(lengths, devices, me):
    seqs = lengths.shape[1]
    counts_row = jnp.where(devices == me, lengths, 0).astype(f32)
    up = lax.broadcasted_iota(jnp.int32, (seqs, seqs), 0)
    across = lax.broadcasted_iota(jnp.int32, (seqs, seqs), 1)
    counts_col = lane_sum(jnp.where(up == across, counts_row, 0.0))
    starts_row = jnp.sum(jnp.where(up < across, counts_col, 0.0), axis=0, keepdims=True)
    starts_col = lane_sum(jnp.where(across < up, counts_row, 0.0))

    def within(places, starts, counts):
        return (places >= starts) & (places < starts + counts)

    places = lax.broadcasted_iota(jnp.int32, (CAP, seqs), 0).astype(f32)
    labels = lax.broadcasted_iota(jnp.int32, (CAP, seqs), 1).astype(f32)
    inside = within(places, starts_row, counts_row)
    segment_col = lane_sum(jnp.where(inside, labels + 1.0, 0.0)) - 1.0
    position = lane_sum(jnp.where(inside, places - starts_row, 0.0))
    places = lax.broadcasted_iota(jnp.int32, (seqs, CAP), 1).astype(f32)
    labels = lax.broadcasted_iota(jnp.int32, (seqs, CAP), 0).astype(f32)
    inside = within(places, starts_col, counts_col)
    segment_row = jnp.sum(jnp.where(inside, labels + 1.0, 0.0), axis=0, keepdims=True) - 1.0
    return segment_col, segment_row, position


def allowed_bias(segment_col, segment_row):
    t = lax.broadcasted_iota(jnp.int32, (CAP, CAP), 0)
    u = lax.broadcasted_iota(jnp.int32, (CAP, CAP), 1)
    same = (segment_col == segment_row) & (segment_col >= 0.0)
    return jnp.where((t == u) | ((u < t) & same), 0.0, masked_score)


def half_turn(v):
    lane = lax.broadcasted_iota(jnp.int32, v.shape, v.ndim - 1)
    turned = pltpu.roll(v, HD // 2, v.ndim - 1)
    return jnp.where(lane < HD // 2, -turned, turned)


def rms_scale(v):
    return lax.rsqrt(jnp.mean(v * v, axis=-1, keepdims=True) + epsilon)


def forward_kernel(
    x_ref, len_ref, dev_ref, ga_ref, gm_ref, gq_ref, gk_ref, cot_ref,
    wq_ref, wk_ref, wv_ref, wo_ref, gate_ref, up_ref, wd_ref,
    w_out, gu_out, d_out, tok_out, cot_out,
    hid_out, dgu_out,
    middle_out, normed_out, raw_out, q_out, k_out, v_out, mixed_out, gains_out, rope_out,
    w_tmp, p_tmp, d_tmp, cot_tmp, second_tmp, chunk, ow_all, gain_tmp, gain_own,
    tok_all, cot_all, gate_up, dhid, m_chunk, wd_rows, hid, dgu,
    local, up_s, down_s, first_s, second_s, sib_s, recv, ex_send, ex_recv,
    m_first_s, m_second_s, m_sib_s, m_recv, line_up, line_down, line_r, w_load, o_load, g_load,
    stream, act_out,
):
    me, z, first, second, sibling = where_am_i()
    col, fcol, scol = me % RING, first % RING, second % RING
    sfcol = (second + first - me) % RING
    width = p_tmp.shape[2] // 2
    rows = w_tmp.shape[0]
    qkv_width = raw_out.shape[1]
    attn_width = qkv_width + wo_ref.shape[1]
    last = LINE - 1
    pieces = LINE + 1

    w_in = []
    lo = 0
    for i, ref in enumerate((wq_ref, wk_ref, wv_ref, wo_ref)):
        at = pl.ds(lo, ref.shape[1])
        w_in.append(pltpu.make_async_copy(ref, w_tmp.at[:, at], local.at[i]))
        lo += ref.shape[1]
    p_in = [
        pltpu.make_async_copy(
            ref.at[:, pl.ds(pl.multiple_of(z * width, width), width)],
            p_tmp.at[z, :, pl.ds(which * width, width)],
            local.at[5 + which],
        )
        for which, ref in enumerate((gate_ref, up_ref))
    ]
    d_in = pltpu.make_async_copy(wd_ref, d_tmp, local.at[7])
    cot_in = pltpu.make_async_copy(cot_ref, cot_tmp, local.at[8])
    for copy in w_in + p_in + [d_in, cot_in]:
        copy.start()
    gain_own[...] = jnp.zeros_like(gain_own)
    for i, ref in enumerate((ga_ref, gm_ref, gq_ref, gk_ref)):
        gain_own[i : i + 1, 0 : ref.shape[1]] = ref[...].astype(f32)
    flat = gain_own[...]
    paired = jnp.where(me % 2 == 0, flat, pltpu.roll(flat, rows, 1))
    shared = pltpu.roll(flat, gq_ref.shape[1] * me, 1)
    placed = jnp.where(lax.broadcasted_iota(jnp.int32, flat.shape, 0) < 2, paired, shared)
    w_tmp[0:16, attn_width:] = placed.astype(bf16)
    w_tmp[16:, attn_width:] = jnp.zeros((rows - 16, 128), bf16)
    greet(line_peers(me) + [first, second, sibling])

    def send(src, shard, sems, device):
        return remote(src, w_out.at[shard], sems.at[shard], recv.at[shard], device)

    def arrived(shard):
        send(w_out.at[shard], shard, sib_s, sibling).wait_recv()

    def exchange(k, which):
        peer_z = lax.rem(z + k, LINE)
        src = (gate_ref, up_ref)[which].at[:, pl.ds(pl.multiple_of(peer_z * width, width), width)]
        dst = p_tmp.at[z, :, pl.ds(which * width, width)]
        return remote(src, dst, ex_send.at[k, which], ex_recv.at[k, which], col + RING * peer_z)

    def line_send(src, which, shard, sems, device):
        landing = (tok_out, cot_out)[which].at[shard]
        return remote(src, landing, sems.at[which, shard], line_r.at[which, shard], device)

    def line_own(which, src):
        @pl.when(z < last)
        def _():
            line_send(src, which, z, line_up, me + RING).start()

        @pl.when(z > 0)
        def _():
            line_send(src, which, z, line_down, me - RING).start()

    def line_relay(which, k):
        def body(step):
            shard = z + step
            src = (tok_out, cot_out)[which].at[shard]
            line_send(src, which, shard, line_up, second).wait_recv()
            if step < 0:

                @pl.when(z < last)
                def _():
                    line_send(src, which, shard, line_up, me + RING).start()
            else:

                @pl.when(z > 0)
                def _():
                    line_send(src, which, shard, line_down, me - RING).start()

        on_line(z, k, body)

    for copy in w_in:
        copy.wait()

    @pl.when(z < last)
    def _():
        send(w_tmp, me, up_s, me + RING).start()

    @pl.when(z > 0)
    def _():
        send(w_tmp, me, down_s, me - RING).start()

    send(w_tmp, me, first_s, first).start()
    send(w_tmp, me, second_s, second).start()
    send(w_tmp, me, sib_s, sibling).start()
    w_back = pltpu.make_async_copy(w_tmp, w_out.at[me], local.at[9])
    w_back.start()

    def own(k):
        def body(step):
            shard = me + RING * step
            src = w_out.at[shard]
            arrived(shard)
            if step < 0:

                @pl.when(z < last)
                def _():
                    send(src, shard, up_s, me + RING).start()
            else:

                @pl.when(z > 0)
                def _():
                    send(src, shard, down_s, me - RING).start()

            send(src, shard, first_s, first).start()
            send(src, shard, second_s, second).start()
            send(src, shard, sib_s, sibling).start()

        on_line(z, k, body)

    def other(base, k, onward):
        def body(step):
            shard = base + RING * (z + step)
            src = w_out.at[shard]
            arrived(shard)
            if onward:
                send(src, shard, second_s, second).start()
            send(src, shard, sib_s, sibling).start()

        on_line(z, k, body)

    segment_col, segment_row, position = token_places(len_ref[...], dev_ref[...], me)
    rope_out[2] = allowed_bias(segment_col, segment_row)
    lane = lax.broadcasted_iota(jnp.int32, (1, HD), 1) % (HD // 2)
    angles = position * jnp.exp(lane.astype(f32) * (-2.0 * math.log(rope_base) / HD))
    rope_out[0] = jnp.cos(angles)
    rope_out[1] = jnp.sin(angles)
    x_scale = rms_scale(x_ref[...].astype(f32))
    raw_out[...] = jnp.zeros_like(raw_out)

    def load_group(step):
        zz = z + step
        part = w_out.at[pl.ds(RING * zz, RING)]
        return (
            pltpu.make_async_copy(part.at[:, :, pl.ds(0, qkv_width)], chunk, w_load),
            pltpu.make_async_copy(
                part.at[:, :, pl.ds(qkv_width, attn_width - qkv_width)],
                ow_all.at[pl.ds(RING * zz, RING)],
                o_load.at[zz],
            ),
            pltpu.make_async_copy(
                part.at[:, pl.ds(0, 16), pl.ds(attn_width, 128)], gain_tmp.at[zz], g_load
            ),
        )

    def group(k):
        def body(step):
            zz = z + step
            for i in range(RING // 2):
                arrived(RING * zz + 2 * i + sibling % 2)
            copies = load_group(step)
            for copy in copies:
                copy.start()
            copies[2].wait()
            span = RING * rows
            for pair in range(RING // 2):
                at = pl.ds(pl.multiple_of(zz * span + pair * 128, 128), 128)
                both = gain_tmp[zz, 2 * pair].astype(f32) + gain_tmp[zz, 2 * pair + 1].astype(f32)
                gains_out[0:2, at] = both[0:2]
                piece = x_ref[:, at].astype(f32) * x_scale * both[0:1]
                normed_out[:, at] = piece.astype(bf16)
            copies[0].wait()
            left = normed_out[:, pl.ds(pl.multiple_of(zz * span, span), span)]

            def tile(i, carry):
                at = pl.ds(pl.multiple_of(i * 512, 512), 512)
                right = chunk[:, :, at].reshape(span, 512)
                raw_out[:, at] += jnp.dot(left, right, preferred_element_type=f32)
                return carry

            lax.fori_loop(0, qkv_width // 512, tile, 0)

        on_line(z, k, body)

    own(1)
    other(fcol, 0, True)
    own(2)
    other(fcol, 1, True)
    other(scol, 0, False)
    for k in range(1, LINE):
        for which in range(2):
            exchange(k, which).start()
    cot_in.wait()
    line_own(1, cot_tmp)
    cot_back = pltpu.make_async_copy(cot_tmp, cot_out.at[z], local.at[10])
    cot_back.start()
    own(3)
    other(fcol, 2, True)
    other(scol, 1, False)
    other(sfcol, 0, False)
    w_back.wait()
    group(0)
    other(fcol, 3, True)
    other(scol, 2, False)
    other(sfcol, 1, False)
    group(1)

    for copy in p_in + [d_in]:
        copy.wait()
    for k in range(1, LINE):
        for which in range(2):
            src_z = lax.rem(z + LINE - k, LINE)
            landed = p_tmp.at[src_z, :, pl.ds(which * width, width)]
            remote(landed, landed, ex_send.at[k, which], ex_recv.at[k, which], second).wait_recv()

    def spot(piece, shard):
        return gu_out.at[piece, shard] if piece < LINE else d_out.at[shard]

    def source(piece):
        return p_tmp.at[piece] if piece < LINE else d_tmp

    def m_send(src, piece, shard, sems, device):
        return remote(
            src, spot(piece, shard), sems.at[piece, shard], m_recv.at[piece, shard], device
        )

    def m_arrived(piece, shard):
        m_send(spot(piece, shard), piece, shard, m_sib_s, sibling).wait_recv()

    def m_own(piece):
        m_send(source(piece), piece, col, m_first_s, first).start()
        m_send(source(piece), piece, col, m_second_s, second).start()
        m_send(source(piece), piece, col, m_sib_s, sibling).start()

    m_own(LINE)
    m_own(0)
    backs = [
        pltpu.make_async_copy(p_tmp, gu_out.at[:, col], local.at[11]),
        pltpu.make_async_copy(d_tmp, d_out.at[col], local.at[12]),
    ]
    for copy in backs:
        copy.start()
    line_relay(1, 1)
    other(scol, 3, False)
    other(sfcol, 2, False)
    group(2)
    other(sfcol, 3, False)
    group(3)
    line_relay(1, 2)

    small = jnp.zeros((16, 128), f32)
    for zz in range(LINE):
        for i in range(RING):
            small = small + gain_tmp[zz, i].astype(f32)
    q_gain, k_gain = small[2:3], small[3:4]
    gains_out[2:4, 0:128] = small[2:4]
    cosine, sine, bias = rope_out[0], rope_out[1], rope_out[2]

    def turned(v, gain):
        v = v * rms_scale(v) * gain
        return (v * cosine + half_turn(v) * sine).astype(bf16)

    kv0 = H * HD
    v0 = kv0 + KVH * HD

    def head(g, carry):
        at = pl.ds(pl.multiple_of(g * HD, HD), HD)
        qa = pl.ds(pl.multiple_of(g * 2 * HD, 2 * HD), HD)
        qb = pl.ds(pl.multiple_of(g * 2 * HD + HD, HD), HD)
        key = turned(raw_out[:, pl.ds(pl.multiple_of(kv0 + g * HD, HD), HD)], k_gain)
        value = raw_out[:, pl.ds(pl.multiple_of(v0 + g * HD, HD), HD)].astype(bf16)
        k_out[:, at] = key
        v_out[:, at] = value
        query_a = turned(raw_out[:, qa], q_gain)
        query_b = turned(raw_out[:, qb], q_gain)
        q_out[:, qa] = query_a
        q_out[:, qb] = query_b
        for query, where in ((query_a, qa), (query_b, qb)):
            scores = lax.dot_general(query, key, contract_cols, preferred_element_type=f32)
            logits = scores * (HD ** (-0.5)) + bias
            exponent = jnp.exp(logits - jnp.max(logits, axis=-1, keepdims=True))
            weights = (exponent / lane_sum(exponent)).astype(bf16)
            mixed = jnp.dot(weights, value, preferred_element_type=f32)
            mixed_out[:, where] = mixed.astype(bf16)
        return carry

    lax.fori_loop(0, KVH, head, 0)
    for zz in range(LINE):
        pltpu.make_async_copy(
            w_out.at[pl.ds(RING * zz, RING), :, pl.ds(qkv_width, attn_width - qkv_width)],
            ow_all.at[pl.ds(RING * zz, RING)],
            o_load.at[zz],
        ).wait()
    mixed = mixed_out[...]

    def out_tile(i, total):
        at = pl.ds(pl.multiple_of(i * 512, 512), 512)
        right = ow_all[:, :, at].reshape(mixed.shape[1], 512)
        middle = x_ref[:, at].astype(f32) + jnp.dot(mixed, right, preferred_element_type=f32)
        middle_out[:, at] = middle
        return total + lane_sum(middle * middle)

    tiles = middle_out.shape[1] // 512
    total = lax.fori_loop(0, tiles, out_tile, jnp.zeros((CAP, 1), f32))
    scale = lax.rsqrt(total / middle_out.shape[1] + epsilon)

    def norm_tile(i, carry):
        at = pl.ds(pl.multiple_of(i * 512, 512), 512)
        second_tmp[:, at] = (middle_out[:, at] * scale * gains_out[1:2, at]).astype(bf16)
        return carry

    lax.fori_loop(0, tiles, norm_tile, 0)

    def m_other(piece, shard, onward):
        m_arrived(piece, shard)
        if onward:
            m_send(spot(piece, shard), piece, shard, m_second_s, second).start()
        m_send(spot(piece, shard), piece, shard, m_sib_s, sibling).start()

    def m_whole(piece):
        for k in range(RING // 2):
            m_arrived(piece, 2 * k + sibling % 2)

    part = dhid.shape[1]
    dim = tok_out.shape[2]
    wide = wd_rows.shape[2]

    def down_back(lo, hi):
        def fetch(i, slot):
            j = lo + i
            return (
                pltpu.make_async_copy(
                    d_out.at[tile(j, 2)], wd_rows.at[slot], stream.at[slot]
                ),
            )

        def body(i, slot):
            right = wd_rows[slot].reshape(wide * 2, dim)
            dhid[:, tile(lo + i, 2 * wide)] = dot_nt(cot_all[...].reshape(LINE * CAP, dim), right)

        streamed(hi - lo, fetch, body)

    def gate_up_rows(piece):
        m_whole(piece)
        copy = pltpu.make_async_copy(gu_out.at[piece], m_chunk, stream.at[0])
        copy.start()
        copy.wait()
        span = RING * rows
        left = tok_all[:, :, pl.ds(piece * span, span)].reshape(LINE * CAP, span)

        def columns(n, carry):
            at = tile(n, 512)
            term = jnp.dot(left, m_chunk[:, :, at].reshape(span, 512), preferred_element_type=f32)
            if piece == 0:
                gate_up[:, at] = term
            else:
                gate_up[:, at] += term
            return carry

        lax.fori_loop(0, 2 * part // 512, columns, 0)

    m_other(LINE, fcol, True)
    line_own(0, second_tmp)
    tok_back = pltpu.make_async_copy(second_tmp, tok_out.at[z], local.at[13])
    tok_back.start()
    m_own(1)
    m_other(LINE, scol, False)
    m_other(0, fcol, True)
    m_own(2)
    m_other(0, scol, False)
    line_relay(1, 3)
    cot_back.wait()
    cot_in = pltpu.make_async_copy(cot_out, cot_all, local.at[8])
    cot_in.start()
    m_other(LINE, sfcol, False)
    line_relay(0, 1)
    m_other(1, fcol, True)
    m_own(3)
    m_other(1, scol, False)
    m_whole(LINE)
    for copy in backs:
        copy.wait()
    cot_in.wait()
    down_back(0, RING // 4)
    m_other(0, sfcol, False)
    line_relay(0, 2)
    m_other(2, fcol, True)
    m_other(2, scol, False)
    down_back(RING // 4, RING // 2)
    m_other(1, sfcol, False)
    line_relay(0, 3)
    tok_back.wait()
    tok_in = pltpu.make_async_copy(tok_out, tok_all, local.at[10])
    tok_in.start()
    m_other(3, fcol, True)
    m_other(3, scol, False)
    tok_in.wait()
    gate_up_rows(0)
    m_other(2, sfcol, False)
    gate_up_rows(1)
    m_other(3, sfcol, False)
    gate_up_rows(2)
    gate_up_rows(3)

    def act_copies(n):
        up_at = pl.ds(pl.multiple_of(part + n * 256, 256), 256)
        return (
            pltpu.make_async_copy(hid.at[:, tile(n, 256)], hid_out.at[:, tile(n, 256)], act_out.at[n, 0]),
            pltpu.make_async_copy(dgu.at[:, tile(n, 256)], dgu_out.at[:, tile(n, 256)], act_out.at[n, 1]),
            pltpu.make_async_copy(dgu.at[:, up_at], dgu_out.at[:, up_at], act_out.at[n, 2]),
        )

    def units(n, carry):
        at = tile(n, 256)
        up_at = pl.ds(pl.multiple_of(part + n * 256, 256), 256)

        def act(r, inner):
            some = tile(r, 32)
            gate, up, back = gate_up[some, at], gate_up[some, up_at], dhid[some, at]
            sig = jax.nn.sigmoid(gate)
            silu = gate * sig
            hid[some, at] = (silu * up).astype(bf16)
            dgu[some, at] = (back * up * (sig * (1.0 + gate * (1.0 - sig)))).astype(bf16)
            dgu[some, up_at] = (back * silu).astype(bf16)
            return inner

        lax.fori_loop(0, LINE * CAP // 32, act, 0)
        for copy in act_copies(n):
            copy.start()
        return carry

    lax.fori_loop(0, part // 256, units, 0)

    for n in range(part // 256):
        for copy in act_copies(n):
            copy.wait()
    for k in range(1, LINE):
        for which in range(2):
            exchange(k, which).wait_send()
    for k in range(LINE):

        @pl.when((z < last) & (k <= z))
        def _(k=k):
            send(w_tmp, col + RING * k, up_s, me + RING).wait_send()
            for which in range(2):
                line_send(cot_tmp, which, k, line_up, me + RING).wait_send()

        @pl.when((z > 0) & (k >= z))
        def _(k=k):
            send(w_tmp, col + RING * k, down_s, me - RING).wait_send()
            for which in range(2):
                line_send(cot_tmp, which, k, line_down, me - RING).wait_send()

        send(w_tmp, col + RING * k, first_s, first).wait_send()
        send(w_tmp, col + RING * k, second_s, second).wait_send()
        send(w_tmp, fcol + RING * k, second_s, second).wait_send()
        for base in (col, fcol, scol, sfcol):
            send(w_tmp, base + RING * k, sib_s, sibling).wait_send()
    for piece in range(pieces):
        src = source(piece)
        m_send(src, piece, col, m_first_s, first).wait_send()
        m_send(src, piece, col, m_second_s, second).wait_send()
        m_send(src, piece, fcol, m_second_s, second).wait_send()
        for base in (col, fcol, scol, sfcol):
            m_send(src, piece, base, m_sib_s, sibling).wait_send()


def forward(hidden_in, out_grad, seq_lengths, seq_device, gains, wq, wk, wv, wo, gate, up, wd):
    slots, dim = hidden_in.shape
    rows = wq.shape[0]
    n = RING * LINE
    width = gate.shape[1] // LINE
    qkv_width = wq.shape[1] + wk.shape[1] + wv.shape[1]
    wide = qkv_width + wo.shape[1] + 128
    pieces = LINE + 1
    S = jax.ShapeDtypeStruct
    return pl.pallas_call(
        forward_kernel,
        out_shape=(
            S((n, rows, wide), bf16),
            S((LINE, RING, rows, 2 * width), bf16),
            S((RING,) + wd.shape, bf16),
            S((LINE, slots, dim), bf16),
            S((LINE, slots, dim), bf16),
            S((LINE * slots, width), bf16),
            S((LINE * slots, 2 * width), bf16),
            S((slots, dim), f32),
            S((slots, dim), bf16),
            S((slots, qkv_width), f32),
            S((slots, H * HD), bf16),
            S((slots, KVH * HD), bf16),
            S((slots, KVH * HD), bf16),
            S((slots, H * HD), bf16),
            S((8, dim), f32),
            S((3, slots, HD), f32),
        ),
        in_specs=[VMEM] * 7 + [ANY] * 8,
        out_specs=(ANY,) * 7 + (VMEM,) * 9,
        scratch_shapes=[
            pltpu.VMEM((rows, wide), bf16),
            pltpu.VMEM((LINE, rows, 2 * width), bf16),
            pltpu.VMEM(wd.shape, bf16),
            pltpu.VMEM((slots, dim), bf16),
            pltpu.VMEM((slots, dim), bf16),
            pltpu.VMEM((RING, rows, qkv_width), bf16),
            pltpu.VMEM((n, rows, wo.shape[1]), bf16),
            pltpu.VMEM((LINE, RING, 16, 128), bf16),
            pltpu.VMEM((16, 128), f32),
            pltpu.VMEM((LINE, slots, dim), bf16),
            pltpu.VMEM((LINE, slots, dim), bf16),
            pltpu.VMEM((LINE * slots, 2 * width), f32),
            pltpu.VMEM((LINE * slots, width), f32),
            pltpu.VMEM((RING, rows, 2 * width), bf16),
            pltpu.VMEM((2, 2) + wd.shape, bf16),
            pltpu.VMEM((LINE * slots, width), bf16),
            pltpu.VMEM((LINE * slots, 2 * width), bf16),
            DMA((14,)),
            DMA((n,)),
            DMA((n,)),
            DMA((n,)),
            DMA((n,)),
            DMA((n,)),
            DMA((n,)),
            DMA((LINE, 2)),
            DMA((LINE, 2)),
            DMA((pieces, RING)),
            DMA((pieces, RING)),
            DMA((pieces, RING)),
            DMA((pieces, RING)),
            DMA((2, LINE)),
            DMA((2, LINE)),
            DMA((2, LINE)),
            DMA,
            DMA((LINE,)),
            DMA,
            DMA((2,)),
            DMA((width // 256, 3)),
        ],
        compiler_params=pltpu.CompilerParams(
            collective_id=0, has_side_effects=True, vmem_limit_bytes=64000 * 1024
        ),
        name="forward",
    )(
        hidden_in, seq_lengths[None, :], seq_device[None, :], *[g[None, :] for g in gains],
        out_grad, wq, wk, wv, wo, gate, up, wd,
    )


def turn_kernel(
    gu_ref, wd_ref, tok_ref, cot_ref, hid_ref, dgu_ref, w_ref, middle_ref, normed_ref, raw_ref, q_ref, k_ref, v_ref,
    mixed_ref, gains_ref, rope_ref,
    y_out, dmid_out, dqkv_out, small_out, d_out, gu_out, gq_out, go_out,
    gu_all, gd_all, gu_sib, gd_sib, gu_sec, gd_sec, gu_fst, gd_fst, t_own, t_land,
    c_send, c_recv, s_send, s_recv, f_send, f_recv, down_s, down_r, up_s, up_r, load, stream, back,
):
    me, z, first, second, sibling = where_am_i()
    greet([lax.rem(me + RING, RING * LINE), lax.rem(me + RING * (LINE - 1), RING * LINE)]
          + [first, second, sibling])
    core = me % 2
    mine, fst, sec = (me % RING) // 2, (first % RING) // 2, (second % RING) // 2
    far = ((second + first - me) % RING) // 2
    half = gd_fst.shape[0] // 2
    last = LINE - 1
    tokens, dim = tok_ref.shape
    part = wd_ref.shape[0]
    quad_rows = part // LINE
    MLP_GU, MLP_D = (0, 0, LINE), (1, LINE, LINE + 2)

    def block(gu, d, piece, group):
        if group == 0:
            return gu.at[piece]
        return d.at[tile(piece - LINE, half)]

    def own_block(quad, piece, group, theirs=False):
        shard = 2 * quad + (1 - core if theirs else core)
        if group == 0:
            return gu_all.at[piece, shard]
        return block(None, gd_all.at[shard], piece, group)

    def each(span, body):
        group, lo, hi = span

        def step(piece, carry):
            body(piece, group)
            return carry

        lax.fori_loop(lo, hi, step, 0)

    def to_sibling(quad, piece, group):
        return remote(
            own_block(quad, piece, group, theirs=True),
            block(gu_sib.at[quad], gd_sib.at[quad], piece, group),
            c_send.at[quad, piece],
            c_recv.at[quad, piece],
            sibling,
        )

    def to_second(quad, slot, piece, group):
        return remote(
            own_block(quad, piece, group),
            block(gu_sec.at[slot], gd_sec.at[slot], piece, group),
            s_send.at[slot, piece],
            s_recv.at[slot, piece],
            second,
        )

    def to_first(piece, group):
        return remote(
            own_block(fst, piece, group),
            block(gu_fst, gd_fst, piece, group),
            f_send.at[piece],
            f_recv.at[piece],
            first,
        )

    def pass_on(piece, group):
        for quad, slot in ((far, 1), (sec, 0)):
            to_sibling(quad, piece, group).wait_recv()
            own = own_block(quad, piece, group)
            add_rows(own, own, block(gu_sib.at[quad], gd_sib.at[quad], piece, group))
            to_second(quad, slot, piece, group).start()

    def narrow(piece, group):
        to_sibling(fst, piece, group).wait_recv()
        to_second(far, 1, piece, group).wait_recv()
        own = own_block(fst, piece, group)
        add_rows(
            own,
            own,
            block(gu_sib.at[fst], gd_sib.at[fst], piece, group),
            block(gu_sec.at[1], gd_sec.at[1], piece, group),
        )
        to_first(piece, group).start()

    def finish(piece, group):
        to_sibling(mine, piece, group).wait_recv()
        to_second(sec, 0, piece, group).wait_recv()
        to_first(piece, group).wait_recv()
        own = own_block(mine, piece, group)
        add_rows(
            own if group == 0 else block(None, d_out, piece, group),
            own,
            block(gu_sib.at[mine], gd_sib.at[mine], piece, group),
            block(gu_sec.at[0], gd_sec.at[0], piece, group),
            block(gu_fst, gd_fst, piece, group),
        )

    def send_line(src, which, t, up):
        return remote(
            src,
            t_land.at[which, t + 1 if up else t],
            (up_s if up else down_s).at[which, t],
            (up_r if up else down_r).at[which, t],
            me + RING if up else me - RING,
        )

    def line_own(which):
        for k in range(last):

            @pl.when(z == last)
            def _(k=k):
                send_line(t_own.at[which, k], which, k, False).start()

            @pl.when(z == 0)
            def _(k=k):
                send_line(t_own.at[which, last - k], which, last - k, True).start()

    def relay_at(which, at, t, up):
        @pl.when(z == at)
        def _():
            landing = t_land.at[which, t + 1 if up else t]
            send_line(landing, which, t, up).wait_recv()
            add_rows(landing, landing, t_own.at[which, t])
            send_line(landing, which, t, up).start()

    def relay(which, step):
        if step < 2:
            relay_at(which, 2, step, False)
            relay_at(which, 1, last - step, True)
        else:
            relay_at(which, 1, 0, False)
            relay_at(which, 2, last, True)

    def line_sum(which, out):
        own, above, below = t_own.at[which, z], t_land.at[which, z], t_land.at[which, z + 1]

        @pl.when(z < last)
        def _():
            send_line(above, which, z, False).wait_recv()

        @pl.when(z > 0)
        def _():
            send_line(below, which, z, True).wait_recv()

        @pl.when(z == 0)
        def _():
            add_rows(out, own, above)

        @pl.when(z == last)
        def _():
            add_rows(out, own, below)

        @pl.when((z > 0) & (z < last))
        def _():
            add_rows(out, own, above, below)

    def mlp(tok, cot, hid, dgu):
        ins = [
            pltpu.make_async_copy(hid_ref, hid, load.at[0]),
            pltpu.make_async_copy(cot_ref, cot, load.at[1]),
            pltpu.make_async_copy(dgu_ref, dgu, load.at[2]),
            pltpu.make_async_copy(tok_ref, tok, load.at[3]),
        ]
        for copy in ins:
            copy.start()
        wide = 256
        for copy in ins[:2]:
            copy.wait()

        previous = None
        for quad in (far, sec, fst, mine):

            def columns(n, carry, quad=quad):
                at = tile(n, 512)
                both = dot_tn(hid[:, tile(quad, quad_rows)], cot[:, at]).astype(bf16)
                gd_all[2 * quad, :, at] = both[: quad_rows // 2]
                gd_all[2 * quad + 1, :, at] = both[quad_rows // 2 :]
                return carry

            lax.fori_loop(0, dim // 512, columns, 0)
            if previous is not None:
                each(MLP_D, lambda piece, group, q=previous: to_sibling(q, piece, group).start())
            previous = quad

        def back_through(rows_w):
            def fetch(i, slot):
                return (
                    pltpu.make_async_copy(
                        gu_ref.at[tile(i, wide)], rows_w.at[slot], stream.at[slot, 0]
                    ),
                )

            def body(i, slot):
                out = dot_nt(dgu[...], rows_w[slot]).astype(bf16)
                t_own[0, :, :, tile(i, wide)] = out.reshape(LINE, CAP, wide)

            streamed(dim // wide, fetch, body)

        each(MLP_D, lambda piece, group, q=previous: to_sibling(q, piece, group).start())
        for copy in ins[2:]:
            copy.wait()
        pl.run_scoped(back_through, pltpu.VMEM((2, wide, 2 * part), bf16))
        each(MLP_D, pass_on)
        line_own(0)

        rows = dim // LINE
        for piece in range(LINE):

            def columns(n, carry, piece=piece):
                at = tile(n, 512)
                grad = dot_tn(tok[:, pl.ds(piece * rows, rows)], dgu[:, at]).astype(bf16)
                gu_all[piece, :, :, at] = grad.reshape(RING, rows // RING, 512)
                return carry

            lax.fori_loop(0, 2 * part // 512, columns, 0)
            if piece > 0:
                pass_on(piece - 1, 0)
            for quad in (far, fst, sec, mine):
                to_sibling(quad, piece, 0).start()
        each(MLP_D, narrow)
        relay(0, 0)

        def out_through(cols_w):
            def fetch(i, slot):
                return (
                    pltpu.make_async_copy(
                        wd_ref.at[:, tile(i, wide)], cols_w.at[slot], stream.at[slot, 0]
                    ),
                )

            def body(i, slot):
                out = jnp.dot(hid[...], cols_w[slot], preferred_element_type=f32).astype(bf16)
                t_own[1, :, :, tile(i, wide)] = out.reshape(LINE, CAP, wide)

            streamed(dim // wide, fetch, body)

        pass_on(LINE - 1, 0)
        pl.run_scoped(out_through, pltpu.VMEM((2, part, wide), bf16))

    pl.run_scoped(
        mlp,
        pltpu.VMEM((tokens, dim), bf16),
        pltpu.VMEM((tokens, dim), bf16),
        pltpu.VMEM((tokens, part), bf16),
        pltpu.VMEM((tokens, 2 * part), bf16),
    )

    def attention(middle, raw, q, k, v, mixed, normed, cot, dsec, dbr, dmix, w_rows, o_stage, q_stage):
        kv0 = H * HD
        v0 = kv0 + KVH * HD
        ins = [
            pltpu.make_async_copy(src, dst, load.at[i])
            for i, (src, dst) in enumerate(
                (
                    (middle_ref, middle),
                    (raw_ref.at[:, pl.ds(0, v0)], raw),
                    (q_ref, q),
                    (k_ref, k),
                    (v_ref, v),
                    (mixed_ref, mixed),
                    (normed_ref, normed),
                    (cot_ref.at[tile(z, CAP)], cot),
                )
            )
        ]
        for copy in ins:
            copy.start()
        relay(0, 1)
        narrow(0, 0)
        relay(0, 2)
        line_own(1)
        for copy in ins:
            copy.wait()
        line_sum(0, dsec)

        scale = rms_scale(middle[...])
        wide = 512

        def gather_mean(i, total):
            at = tile(i, wide)
            n = middle[:, at] * scale
            ds = dsec[:, at]
            small_out[0:1, at] = jnp.sum(n * ds, axis=0, keepdims=True)
            return total + lane_sum(n * ds * gains_ref[1:2, at])

        mean = lax.fori_loop(0, dim // wide, gather_mean, jnp.zeros((CAP, 1), f32)) / dim

        def spread_mean(i, carry):
            at = tile(i, wide)
            n = middle[:, at] * scale
            e = dsec[:, at] * gains_ref[1:2, at]
            d_middle = cot[:, at].astype(f32) + scale * (e - n * mean)
            dmid_out[:, at] = d_middle
            dbr[:, at] = d_middle.astype(bf16)
            return carry

        lax.fori_loop(0, dim // wide, spread_mean, 0)
        shards = w_rows.shape[1]
        rows = shards * w_rows.shape[2]

        def w_fetch(i, slot):
            return (
                pltpu.make_async_copy(
                    w_ref.at[tile(i, shards), :, pl.ds(v0 + KVH * HD, dim)],
                    w_rows.at[slot],
                    stream.at[slot, 0],
                ),
            )

        def o_back(i, slot):
            return pltpu.make_async_copy(
                o_stage.at[slot], go_out.at[tile(i, shards)], back.at[slot]
            )

        def through_out(i, slot):
            dmix[:, tile(i, rows)] = dot_nt(dbr[...], w_rows[slot].reshape(rows, dim)).astype(bf16)

            @pl.when(i > 1)
            def _():
                o_back(i - 2, slot).wait()

            def columns(n, carry):
                at = tile(n, 512)
                grad = dot_tn(mixed[:, tile(i, rows)], dbr[:, at]).astype(bf16)
                o_stage[slot, :, :, at] = grad.reshape(shards, rows // shards, 512)
                return carry

            lax.fori_loop(0, dim // 512, columns, 0)
            o_back(i, slot).start()

        count = dim // rows
        streamed(count, w_fetch, through_out)
        narrow(1, 0)
        relay(1, 0)
        for i in (count - 2, count - 1):
            o_back(i, i % 2).wait()

        cosine, sine, bias = rope_ref[0], rope_ref[1], rope_ref[2]
        small_out[1:8] = jnp.zeros((7, dim), f32)

        def unrope(raw_v, d_rot, row):
            d_hat = d_rot * cosine - half_turn(d_rot * sine)
            r = rms_scale(raw_v)
            n = raw_v * r
            small_out[row : row + 1, 0:HD] += jnp.sum(n * d_hat, axis=0, keepdims=True)
            e = d_hat * gains_ref[row + 1 : row + 2, 0:HD]
            return (r * (e - n * jnp.mean(n * e, axis=-1, keepdims=True))).astype(bf16)

        def head(g, carry):
            at = tile(g, HD)
            key, value = k[:, at], v[:, at]
            d_key = jnp.zeros((CAP, HD), f32)
            d_value = jnp.zeros((CAP, HD), f32)
            for i in range(2):
                cols = tile(2 * g + i, HD)
                query, d_mix = q[:, cols], dmix[:, cols]
                logits = dot_nt(query, key) * (HD ** (-0.5)) + bias
                exponent = jnp.exp(logits - jnp.max(logits, axis=-1, keepdims=True))
                probs = exponent / lane_sum(exponent)
                d_probs = dot_nt(d_mix, value)
                d_logits = probs * (d_probs - lane_sum(probs * d_probs))
                d_scores = (d_logits * (HD ** (-0.5))).astype(bf16)
                d_value = d_value + dot_tn(probs.astype(bf16), d_mix)
                d_key = d_key + dot_tn(d_scores, query)
                d_query = jnp.dot(d_scores, key, preferred_element_type=f32)
                dqkv_out[:, cols] = unrope(raw[:, cols], d_query, 1)
            cols = pl.ds(pl.multiple_of(kv0 + g * HD, HD), HD)
            dqkv_out[:, cols] = unrope(raw[:, cols], d_key, 2)
            dqkv_out[:, pl.ds(pl.multiple_of(v0 + g * HD, HD), HD)] = d_value.astype(bf16)
            return carry

        lax.fori_loop(0, KVH // 2, head, 0)
        narrow(2, 0)
        relay(1, 1)
        lax.fori_loop(KVH // 2, KVH, head, 0)
        narrow(3, 0)
        relay(1, 2)
        each(MLP_D, finish)

        q_shards = q_stage.shape[1]
        q_rows = q_shards * q_stage.shape[2]

        def q_back(i, slot):
            return pltpu.make_async_copy(
                q_stage.at[slot], gq_out.at[tile(i, q_shards)], back.at[slot]
            )

        def rows_of(i, carry):
            slot = i % 2

            @pl.when(i > 1)
            def _():
                q_back(i - 2, slot).wait()

            def columns(n, inner):
                at = tile(n, 512)
                grad = dot_tn(normed[:, tile(i, q_rows)], dqkv_out[:, at]).astype(bf16)
                q_stage[slot, :, :, at] = grad.reshape(q_shards, q_rows // q_shards, 512)
                return inner

            lax.fori_loop(0, dqkv_out.shape[1] // 512, columns, 0)
            q_back(i, slot).start()
            return carry

        count = dim // q_rows
        lax.fori_loop(0, count, rows_of, 0)
        for i in (count - 2, count - 1):
            q_back(i, i % 2).wait()
        line_sum(1, dsec)

        def last_add(i, carry):
            at = tile(i, wide)
            y_out[:, at] = (middle[:, at] + dsec[:, at]).astype(bf16)
            return carry

        lax.fori_loop(0, dim // wide, last_add, 0)

    slots = CAP
    kv = KVH * HD
    rows = gu_all.shape[2]
    pl.run_scoped(
        attention,
        pltpu.VMEM((slots, dim), f32),
        pltpu.VMEM((slots, dim + kv), f32),
        pltpu.VMEM((slots, dim), bf16),
        pltpu.VMEM((slots, kv), bf16),
        pltpu.VMEM((slots, kv), bf16),
        pltpu.VMEM((slots, dim), bf16),
        pltpu.VMEM((slots, dim), bf16),
        pltpu.VMEM((slots, dim), bf16),
        pltpu.VMEM((slots, dim), f32),
        pltpu.VMEM((slots, dim), bf16),
        pltpu.VMEM((slots, dim), bf16),
        pltpu.VMEM((2, 4, rows, dim), bf16),
        pltpu.VMEM((2, 4, rows, dim), bf16),
        pltpu.VMEM((2, 2, rows, dim + 2 * kv), bf16),
    )
    each(MLP_GU, finish)
    gu_back = pltpu.make_async_copy(gu_all.at[:, 2 * mine + core], gu_out, back.at[0])
    gu_back.start()

    def drain(piece, group):
        for quad in (far, fst, sec, mine):
            to_sibling(quad, piece, group).wait_send()
        to_second(far, 1, piece, group).wait_send()
        to_second(sec, 0, piece, group).wait_send()
        to_first(piece, group).wait_send()

    each(MLP_GU, drain)
    each(MLP_D, drain)
    for which in range(2):
        for k in range(LINE):

            @pl.when((z > 0) & (k < z))
            def _(which=which, k=k):
                send_line(t_own.at[which, k], which, k, False).wait_send()

            @pl.when((z < last) & (k > z))
            def _(which=which, k=k):
                send_line(t_own.at[which, k], which, k, True).wait_send()

    gu_back.wait()


def turn(gu, wd, tok, cot, hid, dgu, w, middle, normed, raw, q, k, v, mixed, gains, rope):
    dim = tok.shape[1]
    rows = w.shape[1]
    drows = wd.shape[0] // RING
    cols = gu.shape[1]
    quads = RING // 2
    pieces = LINE + 2
    n = RING * LINE
    qkv = raw.shape[1]
    S = jax.ShapeDtypeStruct
    return pl.pallas_call(
        turn_kernel,
        out_shape=(
            S((CAP, dim), bf16),
            S((CAP, dim), f32),
            S((CAP, qkv), bf16),
            S((8, dim), f32),
            S((drows, dim), f32),
            S((LINE, rows, cols), bf16),
            S((n, rows, qkv), bf16),
            S((n, rows, dim), bf16),
        ),
        in_specs=[ANY] * 14 + [VMEM] * 2,
        out_specs=(VMEM,) * 5 + (ANY,) * 3,
        scratch_shapes=[
            pltpu.VMEM((LINE, RING, rows, cols), bf16),
            pltpu.VMEM((RING, drows, dim), bf16),
            pltpu.VMEM((quads, LINE, rows, cols), bf16),
            pltpu.VMEM((quads, drows, dim), bf16),
            pltpu.VMEM((2, LINE, rows, cols), bf16),
            pltpu.VMEM((2, drows, dim), bf16),
            pltpu.VMEM((LINE, rows, cols), bf16),
            pltpu.VMEM((drows, dim), bf16),
            pltpu.VMEM((2, LINE, CAP, dim), bf16),
            pltpu.VMEM((2, LINE + 1, CAP, dim), bf16),
            DMA((quads, pieces)),
            DMA((quads, pieces)),
            DMA((2, pieces)),
            DMA((2, pieces)),
            DMA((pieces,)),
            DMA((pieces,)),
            DMA((2, LINE)),
            DMA((2, LINE)),
            DMA((2, LINE)),
            DMA((2, LINE)),
            DMA((8,)),
            DMA((2, 3)),
            DMA((2,)),
        ],
        compiler_params=pltpu.CompilerParams(
            collective_id=2, has_side_effects=True, vmem_limit_bytes=65400 * 1024
        ),
        name="turn",
    )(gu, wd, tok, cot, hid, dgu, w, middle, normed, raw, q, k, v, mixed, gains, rope)


def close_kernel(
    a_ref, o_ref, gu_ref, w_ref, s_ref, x_ref, dmid_ref, dqkv_ref, gains_ref,
    q_out, k_out, v_out, o_out, gate_out, up_out, s_out, x_out,
    own, sib, sec, fst, down, up, ex, s_sum, s_got, s_line, w_rows,
    load, ex_load, c_send, c_recv, s_send, s_recv, f_send, f_recv, down_s, down_r, up_s, up_r,
    ex_s, ex_r, small_s, small_r, stream,
):
    me, z, first, second, sibling = where_am_i()
    greet(line_peers(me) + [first, second, sibling])
    core = me % 2
    q_mine, q_fst, q_sec = (me % RING) // 2, (first % RING) // 2, (second % RING) // 2
    q_far = ((second + first - me) % RING) // 2
    last = LINE - 1
    split = a_ref.shape[2]
    parts = ((a_ref, pl.ds(0, split)), (o_ref, pl.ds(split, o_ref.shape[2])))
    order = (
        last * (1 - z // 2),
        2 - 2 * z + 5 * (z // 2),
        1 + z % 2,
        z,
    )

    def to_sibling(t, quad, part):
        ref, at = parts[part]
        return remote(
            ref.at[RING * t + 2 * quad + 1 - core],
            sib.at[t, quad, :, at],
            c_send.at[t, quad, part],
            c_recv.at[t, quad, part],
            sibling,
        )

    def loading(t, quad, part):
        ref, at = parts[part]
        return pltpu.make_async_copy(
            ref.at[RING * t + 2 * quad + core], own.at[t, quad, :, at], load.at[t, quad, part]
        )

    def ready(t, quad):
        for part in range(2):
            loading(t, quad, part).wait()
            to_sibling(t, quad, part).wait_recv()

    def to_second(t, quad, slot):
        return remote(
            own.at[t, quad], sec.at[slot, t], s_send.at[slot, t], s_recv.at[slot, t], second
        )

    def to_first(t):
        return remote(own.at[t, q_fst], fst.at[t], f_send.at[t], f_recv.at[t], first)

    def send_line(src, t, upward):
        if upward:
            return remote(src, up.at[t], up_s.at[t], up_r.at[t], me + RING)
        return remote(src, down.at[t], down_s.at[t], down_r.at[t], me - RING)

    def exchange(k):
        peer_z = lax.rem(z + k, LINE)
        return remote(
            gu_ref.at[peer_z], ex.at[z], ex_s.at[k], ex_r.at[k], me % RING + RING * peer_z
        )

    def small(step, src, dst, device):
        return remote(src, dst, small_s.at[step], small_r.at[step], device)

    small_c = small(0, s_sum.at[3], s_got.at[0], sibling)
    for k in range(1, LINE):
        exchange(k).start()
    ex_in = pltpu.make_async_copy(gu_ref.at[z], ex.at[z], ex_load)
    ex_in.start()
    for t in order:
        for theirs, ours in ((q_far, q_far), (q_fst, q_sec), (q_sec, q_fst), (q_mine, q_mine)):
            for part in range(2):
                to_sibling(t, theirs, part).start()
                loading(t, ours, part).start()

    def spread(t):
        for quad, slot in ((q_far, 1), (q_sec, 0)):
            ready(t, quad)
            add_rows(own.at[t, quad], own.at[t, quad], sib.at[t, quad])
            to_second(t, quad, slot).start()

    def narrow(t):
        ready(t, q_fst)
        to_second(t, q_far, 1).wait_recv()
        add_rows(own.at[t, q_fst], own.at[t, q_fst], sib.at[t, q_fst], sec.at[1, t])
        to_first(t).start()

    def collect(t):
        ready(t, q_mine)
        to_second(t, q_sec, 0).wait_recv()
        to_first(t).wait_recv()
        mine = own.at[t, q_mine]
        add_rows(mine, mine, sib.at[t, q_mine], sec.at[0, t], fst.at[t])

        @pl.when((t < z) & (z == last))
        def _():
            send_line(mine, t, False).start()

        @pl.when((t > z) & (z == 0))
        def _():
            send_line(mine, t, True).start()

    def relay(t):
        @pl.when((t < z) & (z < last))
        def _():
            landing = down.at[t]
            send_line(landing, t, False).wait_recv()
            add_rows(landing, landing, own.at[t, q_mine])
            send_line(landing, t, False).start()

        @pl.when((t > z) & (z > 0))
        def _():
            landing = up.at[t]
            send_line(landing, t, True).wait_recv()
            add_rows(landing, landing, own.at[t, q_mine])
            send_line(landing, t, True).start()

    shards = w_rows.shape[1]
    dim = x_ref.shape[1]

    def first_norm():
        wide = 512
        x_scale = rms_scale(x_ref[...].astype(f32))
        w_tile = shards * w_rows.shape[2]

        def w_fetch(i, slot):
            return (
                pltpu.make_async_copy(
                    w_ref.at[tile(i, shards), :, pl.ds(0, split)], w_rows.at[slot], stream.at[slot]
                ),
            )

        def through(i, slot):
            x_out[:, tile(i, w_tile)] = dot_nt(dqkv_ref[...], w_rows[slot].reshape(w_tile, split))

        streamed(dim // w_tile, w_fetch, through)
        s_sum[3] = s_ref[...]

        def gather_mean(i, total):
            at = tile(i, wide)
            n = x_ref[:, at].astype(f32) * x_scale
            s_sum[3, 3:4, at] = jnp.sum(n * x_out[:, at], axis=0, keepdims=True)
            return total + lane_sum(n * x_out[:, at] * gains_ref[0:1, at])

        mean = lax.fori_loop(0, dim // wide, gather_mean, jnp.zeros((CAP, 1), f32)) / dim

        def spread_mean(i, carry):
            at = tile(i, wide)
            n = x_ref[:, at].astype(f32) * x_scale
            e = x_out[:, at] * gains_ref[0:1, at]
            x_out[:, at] = dmid_ref[:, at] + x_scale * (e - n * mean)
            return carry

        lax.fori_loop(0, dim // wide, spread_mean, 0)

    spread(order[0])
    first_norm()
    spread(order[1])
    small_c.start()
    narrow(order[0])
    small_c.wait()
    s_sum[0] = s_sum[3] + s_got[0]
    small_f = small(1, s_sum.at[0], s_got.at[1], first)
    small_f.start()
    spread(order[2])
    small_f.wait()
    s_sum[1] = s_sum[0] + s_got[1]
    small_s2 = small(2, s_sum.at[1], s_got.at[2], second)
    small_s2.start()
    narrow(order[1])
    collect(order[0])
    small_s2.wait()
    s_sum[2] = s_sum[1] + s_got[2]
    small_line = [
        small(
            2 + k, s_sum.at[2], s_line.at[k], me % RING + RING * lax.rem(z + k, LINE)
        )
        for k in range(1, LINE)
    ]
    for copy in small_line:
        copy.start()
    spread(order[3])
    narrow(order[2])
    collect(order[1])
    relay(order[0])
    narrow(order[3])
    collect(order[2])
    relay(order[1])
    relay(order[2])
    collect(order[3])
    ex_in.wait()
    for k in range(1, LINE):
        src_z = lax.rem(z + LINE - k, LINE)
        landed = ex.at[src_z]
        remote(landed, landed, ex_s.at[k], ex_r.at[k], sibling).wait_recv()
    width = gate_out.shape[1] // LINE
    for k in range(LINE):
        add_rows(gate_out.at[:, pl.ds(k * width, width)], ex.at[k, :, pl.ds(0, width)])
        add_rows(up_out.at[:, pl.ds(k * width, width)], ex.at[k, :, pl.ds(width, width)])
    for copy in small_line:
        copy.wait()
    s_out[...] = (s_sum[2] + s_line[2]) + (s_line[1] + s_line[3])
    mine, above, below = own.at[z, q_mine], down.at[z], up.at[z]

    @pl.when(z < last)
    def _():
        send_line(above, z, False).wait_recv()

    @pl.when(z > 0)
    def _():
        send_line(below, z, True).wait_recv()

    def total(*terms):
        lo = 0
        for out in (q_out, k_out, v_out, o_out):
            at = pl.ds(lo, out.shape[1])
            add_rows(out, *[term.at[:, at] for term in terms])
            lo += out.shape[1]

    @pl.when(z == 0)
    def _():
        total(mine, above)

    @pl.when(z == last)
    def _():
        total(mine, below)

    @pl.when((z > 0) & (z < last))
    def _():
        total(mine, above, below)

    for k in range(1, LINE):
        exchange(k).wait_send()
    for t in range(LINE):
        for quad in (q_far, q_fst, q_sec, q_mine):
            for part in range(2):
                to_sibling(t, quad, part).wait_send()
        to_second(t, q_far, 1).wait_send()
        to_second(t, q_sec, 0).wait_send()
        to_first(t).wait_send()

        @pl.when(t < z)
        def _(t=t):
            send_line(down.at[t], t, False).wait_send()

        @pl.when(t > z)
        def _(t=t):
            send_line(up.at[t], t, True).wait_send()


def close(a, o, gu, w, small, x, dmid, dqkv, gains):
    rows, split = a.shape[1:]
    owide = o.shape[2]
    wide = split + owide
    quads = RING // 2
    width = gu.shape[2] // 2
    kv = KVH * HD
    S = jax.ShapeDtypeStruct
    return pl.pallas_call(
        close_kernel,
        out_shape=(
            S((rows, H * HD), f32),
            S((rows, kv), f32),
            S((rows, kv), f32),
            S((rows, owide), f32),
            S((rows, LINE * width), f32),
            S((rows, LINE * width), f32),
            S(small.shape, f32),
            S(x.shape, f32),
        ),
        in_specs=[ANY] * 4 + [VMEM] * 5,
        out_specs=(VMEM,) * 8,
        scratch_shapes=[
            pltpu.VMEM((LINE, quads, rows, wide), bf16),
            pltpu.VMEM((LINE, quads, rows, wide), bf16),
            pltpu.VMEM((2, LINE, rows, wide), bf16),
            pltpu.VMEM((LINE, rows, wide), bf16),
            pltpu.VMEM((LINE, rows, wide), bf16),
            pltpu.VMEM((LINE, rows, wide), bf16),
            pltpu.VMEM((LINE, rows, 2 * width), bf16),
            pltpu.VMEM((4,) + small.shape, f32),
            pltpu.VMEM((3,) + small.shape, f32),
            pltpu.VMEM((LINE,) + small.shape, f32),
            pltpu.VMEM((2, 4, rows, split), bf16),
            DMA((LINE, quads, 2)),
            DMA,
            DMA((LINE, quads, 2)),
            DMA((LINE, quads, 2)),
            DMA((2, LINE)),
            DMA((2, LINE)),
            DMA((LINE,)),
            DMA((LINE,)),
            DMA((LINE,)),
            DMA((LINE,)),
            DMA((LINE,)),
            DMA((LINE,)),
            DMA((LINE,)),
            DMA((LINE,)),
            DMA((2 + LINE,)),
            DMA((2 + LINE,)),
            DMA((2,)),
        ],
        compiler_params=pltpu.CompilerParams(
            collective_id=3, has_side_effects=True, vmem_limit_bytes=65400 * 1024
        ),
        name="close",
    )(a, o, gu, w, small, x, dmid, dqkv, gains)


def layout(seq_lengths, seq_device, owner, slots):
    owned = seq_device == owner
    counts = jnp.where(owned, seq_lengths, 0)
    starts = jnp.cumsum(counts) - counts
    places = jnp.arange(slots, dtype=jnp.int32)
    inside = (
        owned[:, None]
        & (places[None, :] >= starts[:, None])
        & (places[None, :] < (starts + counts)[:, None])
    )
    labels = jnp.arange(seq_lengths.shape[0], dtype=jnp.int32)
    segment = jnp.sum(jnp.where(inside, labels[:, None] + 1, 0), axis=0) - 1
    position = jnp.sum(jnp.where(inside, places[None, :] - starts[:, None], 0), axis=0)
    return (segment, position)


def allowed_pairs(segment):
    places = jnp.arange(segment.shape[0], dtype=jnp.int32)
    earlier = places[None, :] < places[:, None]
    same_seq = (segment[:, None] == segment[None, :]) & (segment[:, None] >= 0)
    return (places[:, None] == places[None, :]) | earlier & same_seq


def rmsnorm(values, gain):
    return values * lax.rsqrt(jnp.mean(values * values, axis=-1, keepdims=True) + epsilon) * gain


def rotary(values, position):
    half_dim = values.shape[-1] // 2
    freqs = jnp.power(rope_base, -2.0 * jnp.arange(half_dim, dtype=jnp.float32) / values.shape[-1])
    angles = position.astype(jnp.float32)[:, None] * freqs[None, :]
    cosine = jnp.concatenate([jnp.cos(angles), jnp.cos(angles)], axis=-1)[:, None, :]
    sine = jnp.concatenate([jnp.sin(angles), jnp.sin(angles)], axis=-1)[:, None, :]
    rotated = jnp.concatenate([-values[..., half_dim:], values[..., :half_dim]], axis=-1)
    return values * cosine + rotated * sine


def matmul(left, right):
    return jnp.dot(left, right, preferred_element_type=jnp.float32)


def times_rows(left, right):
    return lax.dot_general(left, right, contract_rows, preferred_element_type=jnp.float32)


def times_cols(left, right):
    return lax.dot_general(left, right, contract_cols, preferred_element_type=jnp.float32)


def scatter_sum(partial):
    total = lax.psum_scatter(
        partial.astype(jnp.bfloat16), "fsdp", scatter_dimension=0, tiled=True
    )
    return total.astype(jnp.float32)


def plain(
    hidden_in,
    out_grad,
    seq_lengths,
    seq_device,
    attn_gain,
    q_gain,
    k_gain,
    w_query,
    w_key,
    w_value,
    w_out,
    mlp_gain,
    w_gate,
    w_up,
    w_down,
):
    slots = hidden_in.shape[0]
    groups = H // KVH
    score_scale = HD ** (-0.5)
    segment, position = layout(seq_lengths, seq_device, lax.axis_index("fsdp"), slots)
    allowed = allowed_pairs(segment)[None, None]

    def query_path(raw, gain):
        return rotary(rmsnorm(raw.reshape(slots, H, HD), gain), position)

    def key_path(raw, gain):
        return rotary(rmsnorm(raw.reshape(slots, KVH, HD), gain), position)

    def swiglu(gate_in, up_in):
        return jax.nn.silu(gate_in) * up_in

    attn_set = (
        lax.all_gather(attn_gain, "fsdp", axis=0, tiled=True),
        lax.all_gather(q_gain, "fsdp", axis=0, tiled=True),
        lax.all_gather(k_gain, "fsdp", axis=0, tiled=True),
        lax.all_gather(w_query, "fsdp", axis=0, tiled=True),
        lax.all_gather(w_key, "fsdp", axis=0, tiled=True),
        lax.all_gather(w_value, "fsdp", axis=0, tiled=True),
        lax.all_gather(w_out, "fsdp", axis=0, tiled=True),
    )
    gain_attn, gain_query, gain_key, query_w, key_w, value_w, out_w = attn_set
    inputs = hidden_in.astype(jnp.float32)
    normed = rmsnorm(inputs, gain_attn.astype(jnp.float32)).astype(jnp.bfloat16)
    query_raw = matmul(normed, query_w)
    key_raw = matmul(normed, key_w)
    value_raw = matmul(normed, value_w)
    queries = (
        query_path(query_raw, gain_query.astype(jnp.float32))
        .astype(jnp.bfloat16)
        .reshape(slots, KVH, groups, HD)
    )
    keys = key_path(key_raw, gain_key.astype(jnp.float32)).astype(jnp.bfloat16)
    values = value_raw.astype(jnp.bfloat16).reshape(slots, KVH, HD)

    def masked_logits():
        scores = (
            jnp.einsum("qgrd,kgd->grqk", queries, keys, preferred_element_type=jnp.float32)
            * score_scale
        )
        return jnp.where(allowed, scores, masked_score)

    logits = masked_logits()
    row_top = jnp.max(logits, axis=-1, keepdims=True)
    exponent = jnp.exp(logits - row_top)
    row_total = jnp.sum(exponent, axis=-1, keepdims=True)
    log_total = row_top + jnp.log(row_total)
    weights = (exponent / row_total).astype(jnp.bfloat16)
    mixed = jnp.einsum("grqk,kgd->qgrd", weights, values, preferred_element_type=jnp.float32)
    mixed = mixed.reshape(slots, H * HD).astype(jnp.bfloat16)
    middle = inputs + matmul(mixed, out_w)
    mlp_set = (
        lax.all_gather(mlp_gain, "fsdp", axis=0, tiled=True),
        lax.all_gather(w_gate, "fsdp", axis=0, tiled=True),
        lax.all_gather(w_up, "fsdp", axis=0, tiled=True),
        lax.all_gather(w_down, "fsdp", axis=0, tiled=True),
    )
    gain_mlp, gate_w, up_w, down_w = mlp_set
    second = rmsnorm(middle, gain_mlp.astype(jnp.float32)).astype(jnp.bfloat16)
    gate_out = matmul(second, gate_w)
    up_out = matmul(second, up_w)
    hidden = swiglu(gate_out, up_out).astype(jnp.bfloat16)
    hidden_out = (middle + matmul(hidden, down_w)).astype(jnp.bfloat16)
    gain_mlp, gate_w, up_w, down_w = (
        lax.all_gather(mlp_gain, "fsdp", axis=0, tiled=True),
        lax.all_gather(w_gate, "fsdp", axis=0, tiled=True),
        lax.all_gather(w_up, "fsdp", axis=0, tiled=True),
        lax.all_gather(w_down, "fsdp", axis=0, tiled=True),
    )
    grad_down = scatter_sum(times_rows(hidden, out_grad))
    d_hidden = times_cols(out_grad, down_w)
    unused_out, swiglu_pull = jax.vjp(swiglu, gate_out, up_out)
    d_gate, d_up = swiglu_pull(d_hidden)
    d_gate_up = jnp.concatenate([d_gate.astype(jnp.bfloat16), d_up.astype(jnp.bfloat16)], axis=1)
    grad_gate_up = scatter_sum(times_rows(second, d_gate_up))
    ff_width = gate_w.shape[1]
    d_second = times_cols(d_gate_up, jnp.concatenate([gate_w, up_w], axis=1))
    unused_norm, second_pull = jax.vjp(rmsnorm, middle, gain_mlp.astype(jnp.float32))
    d_middle_norm, grad_gain_mlp = second_pull(d_second)
    d_middle = out_grad.astype(jnp.float32) + d_middle_norm
    gain_attn, gain_query, gain_key, query_w, key_w, value_w, out_w = (
        lax.all_gather(attn_gain, "fsdp", axis=0, tiled=True),
        lax.all_gather(q_gain, "fsdp", axis=0, tiled=True),
        lax.all_gather(k_gain, "fsdp", axis=0, tiled=True),
        lax.all_gather(w_query, "fsdp", axis=0, tiled=True),
        lax.all_gather(w_key, "fsdp", axis=0, tiled=True),
        lax.all_gather(w_value, "fsdp", axis=0, tiled=True),
        lax.all_gather(w_out, "fsdp", axis=0, tiled=True),
    )
    d_branch = d_middle.astype(jnp.bfloat16)
    grad_out_w = scatter_sum(times_rows(mixed, d_branch))
    d_mixed = times_cols(d_branch, out_w).astype(jnp.bfloat16).reshape(slots, KVH, groups, HD)
    probs = jnp.exp(masked_logits() - log_total)
    weights = probs.astype(jnp.bfloat16)
    d_probs = jnp.einsum("qgrd,kgd->grqk", d_mixed, values, preferred_element_type=jnp.float32)
    d_logits = probs * (d_probs - jnp.sum(probs * d_probs, axis=-1, keepdims=True))
    d_scores = (d_logits * score_scale).astype(jnp.bfloat16)
    d_values = jnp.einsum("grqk,qgrd->kgd", weights, d_mixed, preferred_element_type=jnp.float32)
    d_values = d_values.astype(jnp.bfloat16).reshape(slots, KVH * HD)
    d_queries_rot = jnp.einsum(
        "grqk,kgd->qgrd", d_scores, keys, preferred_element_type=jnp.float32
    ).reshape(slots, H, HD)
    d_keys_rot = jnp.einsum("grqk,qgrd->kgd", d_scores, queries, preferred_element_type=jnp.float32)
    unused_query, query_pull = jax.vjp(query_path, query_raw, gain_query.astype(jnp.float32))
    d_query_raw, grad_gain_query = query_pull(d_queries_rot)
    unused_key, key_pull = jax.vjp(key_path, key_raw, gain_key.astype(jnp.float32))
    d_key_raw, grad_gain_key = key_pull(d_keys_rot)
    d_qkv = jnp.concatenate(
        [d_query_raw.astype(jnp.bfloat16), d_key_raw.astype(jnp.bfloat16), d_values], axis=1
    )
    grad_qkv = scatter_sum(times_rows(normed, d_qkv))
    d_normed = times_cols(d_qkv, jnp.concatenate([query_w, key_w, value_w], axis=1))
    unused_first, first_pull = jax.vjp(rmsnorm, inputs, gain_attn.astype(jnp.float32))
    d_input_norm, grad_gain_attn = first_pull(d_normed)
    input_grad = d_middle + d_input_norm
    gain_sums = (
        lax.psum_scatter(grad_gain_attn, "fsdp", scatter_dimension=0, tiled=True),
        lax.psum_scatter(grad_gain_query, "fsdp", scatter_dimension=0, tiled=True),
        lax.psum_scatter(grad_gain_key, "fsdp", scatter_dimension=0, tiled=True),
        lax.psum_scatter(grad_gain_mlp, "fsdp", scatter_dimension=0, tiled=True),
    )
    query_width = H * HD
    key_width = KVH * HD
    grad_query_w = grad_qkv[:, :query_width]
    grad_key_w = grad_qkv[:, query_width : query_width + key_width]
    grad_value_w = grad_qkv[:, query_width + key_width :]
    grad_gate = grad_gate_up[:, :ff_width]
    grad_up = grad_gate_up[:, ff_width:]
    return (
        hidden_out,
        input_grad,
        gain_sums[0],
        gain_sums[1],
        gain_sums[2],
        grad_query_w,
        grad_key_w,
        grad_value_w,
        grad_out_w,
        gain_sums[3],
        grad_gate,
        grad_up,
        grad_down,
    )


def layered(
    hidden_in,
    out_grad,
    seq_lengths,
    seq_device,
    attn_gain,
    q_gain,
    k_gain,
    w_query,
    w_key,
    w_value,
    w_out,
    mlp_gain,
    w_gate,
    w_up,
    w_down,
):
    (
        attn_w, gate_up_w, down_w, tokens, cotangent, hidden, d_gate_up,
        middle, normed, qkv_raw, queries, keys, values, mixed, gains, rope,
    ) = forward(
        hidden_in, out_grad, seq_lengths, seq_device, (attn_gain, mlp_gain, q_gain, k_gain),
        w_query, w_key, w_value, w_out, w_gate, w_up, w_down,
    )
    rows, dim = w_query.shape[0], hidden_in.shape[1]
    hidden_out, d_middle, d_qkv, small, grad_down, g_gate_up, g_qkv, g_out = turn(
        gate_up_w.reshape(-1, gate_up_w.shape[-1]),
        down_w.reshape(-1, dim),
        tokens.reshape(-1, dim),
        cotangent.reshape(-1, dim),
        hidden, d_gate_up, attn_w, middle, normed, qkv_raw, queries, keys, values, mixed, gains, rope,
    )
    g_query, g_key, g_value, g_out, g_gate, g_up, small, input_grad = close(
        g_qkv, g_out, g_gate_up, attn_w, small, hidden_in, d_middle, d_qkv, gains
    )
    me = lax.axis_index("fsdp")

    def share(row, grad_of):
        count = grad_of.shape[0]
        return lax.dynamic_slice(small, (row, me * count), (1, count))[0]

    gain_sums = (share(3, attn_gain), share(1, q_gain), share(2, k_gain), share(0, mlp_gain))
    return (
        hidden_out,
        input_grad,
        gain_sums[0],
        gain_sums[1],
        gain_sums[2],
        g_query,
        g_key,
        g_value,
        g_out,
        gain_sums[3],
        g_gate,
        g_up,
        grad_down,
    )


def solution(mesh):
    per_device = layered if mesh.shape["fsdp"] == RING * LINE else plain
    return jax.shard_map(
        per_device,
        mesh=mesh,
        in_specs=(
            P("fsdp", None),
            P("fsdp", None),
            P(),
            P(),
            P("fsdp"),
            P("fsdp"),
            P("fsdp"),
            P("fsdp", None),
            P("fsdp", None),
            P("fsdp", None),
            P("fsdp", None),
            P("fsdp"),
            P("fsdp", None),
            P("fsdp", None),
            P("fsdp", None),
        ),
        out_specs=(
            P("fsdp", None),
            P("fsdp", None),
            P("fsdp"),
            P("fsdp"),
            P("fsdp"),
            P("fsdp", None),
            P("fsdp", None),
            P("fsdp", None),
            P("fsdp", None),
            P("fsdp"),
            P("fsdp", None),
            P("fsdp", None),
            P("fsdp", None),
        ),
        check_vma=False,
    )
```

```python
import math

import jax
import jax.numpy as jnp
from jax import lax
from jax.experimental import pallas as pl
from jax.experimental.pallas import tpu as pltpu
from jax.sharding import PartitionSpec as P

H = 16
KVH = 8
HD = 128
CAP = 128
LINE = 4
RING = 8
MESH = pl.DeviceIdType.MESH
ANY = pl.BlockSpec(memory_space=pl.ANY)
VMEM = pl.BlockSpec(memory_space=pltpu.VMEM)
DMA = pltpu.SemaphoreType.DMA
bf16 = jnp.bfloat16
f32 = jnp.float32
epsilon = 1e-06
rope_base = 1000000.0
masked_score = -1e30
contract_rows = (((0,), (0,)), ((), ()))
contract_cols = (((1,), (1,)), ((), ()))


def where_am_i():
    me = lax.axis_index("fsdp")
    core = me % 2
    z = me // RING
    f_bit = 2 + 2 * core
    s_bit = 4 - 2 * core
    first = me + f_bit * (1 - 2 * ((me // f_bit) % 2))
    second = me + s_bit * (1 - 2 * ((me // s_bit) % 2))
    sibling = me + 1 - 2 * core
    return me, z, first, second, sibling


def greet(peers):
    barrier = pltpu.get_barrier_semaphore()
    for peer in peers:
        pl.semaphore_signal(barrier, inc=1, device_id=(peer,), device_id_type=MESH)
    pl.semaphore_wait(barrier, len(peers))


def remote(src, dst, send_sem, recv_sem, device):
    return pltpu.make_async_remote_copy(
        src_ref=src,
        dst_ref=dst,
        send_sem=send_sem,
        recv_sem=recv_sem,
        device_id=(device,),
        device_id_type=MESH,
    )


def line_peers(me):
    return [lax.rem(me + RING * k, RING * LINE) for k in range(1, LINE)]


def on_line(z, k, body):
    for step in ((-k, k) if k else (0,)):

        @pl.when((z + step >= 0) & (z + step < LINE))
        def _(step=step):
            body(step)


def dot_nt(left, right):
    return lax.dot_general(left, right, contract_cols, preferred_element_type=f32)


def dot_tn(left, right):
    return lax.dot_general(left, right, contract_rows, preferred_element_type=f32)


def streamed(count, fetch, body):
    for copy in fetch(0, 0):
        copy.start()

    def step(i, carry):
        slot = i % 2

        @pl.when(i + 1 < count)
        def _():
            for copy in fetch(i + 1, 1 - slot):
                copy.start()

        for copy in fetch(i, slot):
            copy.wait()
        body(i, slot)
        return carry

    lax.fori_loop(0, count, step, 0)


def tile(i, size):
    return pl.ds(pl.multiple_of(i * size, size), size)


def add_rows(out, *terms):
    rows = out.shape[0]

    def body(i, carry):
        at = pl.ds(pl.multiple_of(i * 16, 16), 16)
        total = terms[0][at, :].astype(f32)
        for term in terms[1:]:
            total = total + term[at, :].astype(f32)
        out[at, :] = total.astype(out.dtype)
        return carry

    lax.fori_loop(0, rows // 16, body, 0)


def lane_sum(x):
    return jnp.sum(x, axis=-1, keepdims=True)


def token_places(lengths, devices, me):
    seqs = lengths.shape[1]
    counts_row = jnp.where(devices == me, lengths, 0).astype(f32)
    up = lax.broadcasted_iota(jnp.int32, (seqs, seqs), 0)
    across = lax.broadcasted_iota(jnp.int32, (seqs, seqs), 1)
    counts_col = lane_sum(jnp.where(up == across, counts_row, 0.0))
    starts_row = jnp.sum(jnp.where(up < across, counts_col, 0.0), axis=0, keepdims=True)
    starts_col = lane_sum(jnp.where(across < up, counts_row, 0.0))

    def within(places, starts, counts):
        return (places >= starts) & (places < starts + counts)

    places = lax.broadcasted_iota(jnp.int32, (CAP, seqs), 0).astype(f32)
    labels = lax.broadcasted_iota(jnp.int32, (CAP, seqs), 1).astype(f32)
    inside = within(places, starts_row, counts_row)
    segment_col = lane_sum(jnp.where(inside, labels + 1.0, 0.0)) - 1.0
    position = lane_sum(jnp.where(inside, places - starts_row, 0.0))
    places = lax.broadcasted_iota(jnp.int32, (seqs, CAP), 1).astype(f32)
    labels = lax.broadcasted_iota(jnp.int32, (seqs, CAP), 0).astype(f32)
    inside = within(places, starts_col, counts_col)
    segment_row = jnp.sum(jnp.where(inside, labels + 1.0, 0.0), axis=0, keepdims=True) - 1.0
    return segment_col, segment_row, position


def allowed_bias(segment_col, segment_row):
    t = lax.broadcasted_iota(jnp.int32, (CAP, CAP), 0)
    u = lax.broadcasted_iota(jnp.int32, (CAP, CAP), 1)
    same = (segment_col == segment_row) & (segment_col >= 0.0)
    return jnp.where((t == u) | ((u < t) & same), 0.0, masked_score)


def half_turn(v):
    lane = lax.broadcasted_iota(jnp.int32, v.shape, v.ndim - 1)
    turned = pltpu.roll(v, HD // 2, v.ndim - 1)
    return jnp.where(lane < HD // 2, -turned, turned)


def rms_scale(v):
    return lax.rsqrt(jnp.mean(v * v, axis=-1, keepdims=True) + epsilon)


def forward_kernel(
    x_ref, len_ref, dev_ref, ga_ref, gm_ref, gq_ref, gk_ref, cot_ref,
    wq_ref, wk_ref, wv_ref, wo_ref, gate_ref, up_ref, wd_ref,
    w_out, gu_out, d_out, tok_out, cot_out,
    hid_out, dgu_out,
    middle_out, normed_out, raw_out, q_out, k_out, v_out, mixed_out, gains_out, rope_out,
    w_tmp, p_tmp, d_tmp, cot_tmp, second_tmp, chunk, ow_all, gain_tmp, gain_own,
    tok_all, cot_all, gate_up, dhid, m_chunk, wd_rows, hid, dgu,
    local, up_s, down_s, first_s, second_s, sib_s, recv, ex_send, ex_recv,
    m_first_s, m_second_s, m_sib_s, m_recv, line_up, line_down, line_r, w_load, o_load, g_load,
    stream, act_out,
):
    me, z, first, second, sibling = where_am_i()
    col, fcol, scol = me % RING, first % RING, second % RING
    sfcol = (second + first - me) % RING
    width = p_tmp.shape[2] // 2
    rows = w_tmp.shape[0]
    qkv_width = raw_out.shape[1]
    attn_width = qkv_width + wo_ref.shape[1]
    last = LINE - 1
    pieces = LINE + 1

    w_in = []
    lo = 0
    for i, ref in enumerate((wq_ref, wk_ref, wv_ref, wo_ref)):
        at = pl.ds(lo, ref.shape[1])
        w_in.append(pltpu.make_async_copy(ref, w_tmp.at[:, at], local.at[i]))
        lo += ref.shape[1]
    p_in = [
        pltpu.make_async_copy(
            ref.at[:, pl.ds(pl.multiple_of(z * width, width), width)],
            p_tmp.at[z, :, pl.ds(which * width, width)],
            local.at[5 + which],
        )
        for which, ref in enumerate((gate_ref, up_ref))
    ]
    d_in = pltpu.make_async_copy(wd_ref, d_tmp, local.at[7])
    cot_in = pltpu.make_async_copy(cot_ref, cot_tmp, local.at[8])
    for copy in w_in + p_in + [d_in, cot_in]:
        copy.start()
    gain_own[...] = jnp.zeros_like(gain_own)
    for i, ref in enumerate((ga_ref, gm_ref, gq_ref, gk_ref)):
        gain_own[i : i + 1, 0 : ref.shape[1]] = ref[...].astype(f32)
    flat = gain_own[...]
    paired = jnp.where(me % 2 == 0, flat, pltpu.roll(flat, rows, 1))
    shared = pltpu.roll(flat, gq_ref.shape[1] * me, 1)
    placed = jnp.where(lax.broadcasted_iota(jnp.int32, flat.shape, 0) < 2, paired, shared)
    w_tmp[0:16, attn_width:] = placed.astype(bf16)
    w_tmp[16:, attn_width:] = jnp.zeros((rows - 16, 128), bf16)
    greet(line_peers(me) + [first, second, sibling])

    def send(src, shard, sems, device):
        return remote(src, w_out.at[shard], sems.at[shard], recv.at[shard], device)

    def arrived(shard):
        send(w_out.at[shard], shard, sib_s, sibling).wait_recv()

    def exchange(k, which):
        peer_z = lax.rem(z + k, LINE)
        src = (gate_ref, up_ref)[which].at[:, pl.ds(pl.multiple_of(peer_z * width, width), width)]
        dst = p_tmp.at[z, :, pl.ds(which * width, width)]
        return remote(src, dst, ex_send.at[k, which], ex_recv.at[k, which], col + RING * peer_z)

    def line_send(src, which, shard, sems, device):
        landing = (tok_out, cot_out)[which].at[shard]
        return remote(src, landing, sems.at[which, shard], line_r.at[which, shard], device)

    def line_own(which, src):
        @pl.when(z < last)
        def _():
            line_send(src, which, z, line_up, me + RING).start()

        @pl.when(z > 0)
        def _():
            line_send(src, which, z, line_down, me - RING).start()

    def line_relay(which, k):
        def body(step):
            shard = z + step
            src = (tok_out, cot_out)[which].at[shard]
            line_send(src, which, shard, line_up, second).wait_recv()
            if step < 0:

                @pl.when(z < last)
                def _():
                    line_send(src, which, shard, line_up, me + RING).start()
            else:

                @pl.when(z > 0)
                def _():
                    line_send(src, which, shard, line_down, me - RING).start()

        on_line(z, k, body)

    for copy in w_in:
        copy.wait()

    @pl.when(z < last)
    def _():
        send(w_tmp, me, up_s, me + RING).start()

    @pl.when(z > 0)
    def _():
        send(w_tmp, me, down_s, me - RING).start()

    send(w_tmp, me, first_s, first).start()
    send(w_tmp, me, second_s, second).start()
    send(w_tmp, me, sib_s, sibling).start()
    w_back = pltpu.make_async_copy(w_tmp, w_out.at[me], local.at[9])
    w_back.start()

    def own(k):
        def body(step):
            shard = me + RING * step
            src = w_out.at[shard]
            arrived(shard)
            if step < 0:

                @pl.when(z < last)
                def _():
                    send(src, shard, up_s, me + RING).start()
            else:

                @pl.when(z > 0)
                def _():
                    send(src, shard, down_s, me - RING).start()

            send(src, shard, first_s, first).start()
            send(src, shard, second_s, second).start()
            send(src, shard, sib_s, sibling).start()

        on_line(z, k, body)

    def other(base, k, onward):
        def body(step):
            shard = base + RING * (z + step)
            src = w_out.at[shard]
            arrived(shard)
            if onward:
                send(src, shard, second_s, second).start()
            send(src, shard, sib_s, sibling).start()

        on_line(z, k, body)

    segment_col, segment_row, position = token_places(len_ref[...], dev_ref[...], me)
    rope_out[2] = allowed_bias(segment_col, segment_row)
    lane = lax.broadcasted_iota(jnp.int32, (1, HD), 1) % (HD // 2)
    angles = position * jnp.exp(lane.astype(f32) * (-2.0 * math.log(rope_base) / HD))
    rope_out[0] = jnp.cos(angles)
    rope_out[1] = jnp.sin(angles)
    x_scale = rms_scale(x_ref[...].astype(f32))
    raw_out[...] = jnp.zeros_like(raw_out)

    def load_group(step):
        zz = z + step
        part = w_out.at[pl.ds(RING * zz, RING)]
        return (
            pltpu.make_async_copy(part.at[:, :, pl.ds(0, qkv_width)], chunk, w_load),
            pltpu.make_async_copy(
                part.at[:, :, pl.ds(qkv_width, attn_width - qkv_width)],
                ow_all.at[pl.ds(RING * zz, RING)],
                o_load.at[zz],
            ),
            pltpu.make_async_copy(
                part.at[:, pl.ds(0, 16), pl.ds(attn_width, 128)], gain_tmp.at[zz], g_load
            ),
        )

    def group(k):
        def body(step):
            zz = z + step
            for i in range(RING // 2):
                arrived(RING * zz + 2 * i + sibling % 2)
            copies = load_group(step)
            for copy in copies:
                copy.start()
            copies[2].wait()
            span = RING * rows
            for pair in range(RING // 2):
                at = pl.ds(pl.multiple_of(zz * span + pair * 128, 128), 128)
                both = gain_tmp[zz, 2 * pair].astype(f32) + gain_tmp[zz, 2 * pair + 1].astype(f32)
                gains_out[0:2, at] = both[0:2]
                piece = x_ref[:, at].astype(f32) * x_scale * both[0:1]
                normed_out[:, at] = piece.astype(bf16)
            copies[0].wait()
            left = normed_out[:, pl.ds(pl.multiple_of(zz * span, span), span)]

            def tile(i, carry):
                at = pl.ds(pl.multiple_of(i * 512, 512), 512)
                right = chunk[:, :, at].reshape(span, 512)
                raw_out[:, at] += jnp.dot(left, right, preferred_element_type=f32)
                return carry

            lax.fori_loop(0, qkv_width // 512, tile, 0)

        on_line(z, k, body)

    own(1)
    other(fcol, 0, True)
    own(2)
    other(fcol, 1, True)
    other(scol, 0, False)
    for k in range(1, LINE):
        for which in range(2):
            exchange(k, which).start()
    cot_in.wait()
    line_own(1, cot_tmp)
    cot_back = pltpu.make_async_copy(cot_tmp, cot_out.at[z], local.at[10])
    cot_back.start()
    own(3)
    other(fcol, 2, True)
    other(scol, 1, False)
    other(sfcol, 0, False)
    w_back.wait()
    group(0)
    other(fcol, 3, True)
    other(scol, 2, False)
    other(sfcol, 1, False)
    group(1)

    for copy in p_in + [d_in]:
        copy.wait()
    for k in range(1, LINE):
        for which in range(2):
            src_z = lax.rem(z + LINE - k, LINE)
            landed = p_tmp.at[src_z, :, pl.ds(which * width, width)]
            remote(landed, landed, ex_send.at[k, which], ex_recv.at[k, which], second).wait_recv()

    def spot(piece, shard):
        return gu_out.at[piece, shard] if piece < LINE else d_out.at[shard]

    def source(piece):
        return p_tmp.at[piece] if piece < LINE else d_tmp

    def m_send(src, piece, shard, sems, device):
        return remote(
            src, spot(piece, shard), sems.at[piece, shard], m_recv.at[piece, shard], device
        )

    def m_arrived(piece, shard):
        m_send(spot(piece, shard), piece, shard, m_sib_s, sibling).wait_recv()

    def m_own(piece):
        m_send(source(piece), piece, col, m_first_s, first).start()
        m_send(source(piece), piece, col, m_second_s, second).start()
        m_send(source(piece), piece, col, m_sib_s, sibling).start()

    m_own(LINE)
    m_own(0)
    backs = [
        pltpu.make_async_copy(p_tmp, gu_out.at[:, col], local.at[11]),
        pltpu.make_async_copy(d_tmp, d_out.at[col], local.at[12]),
    ]
    for copy in backs:
        copy.start()
    line_relay(1, 1)
    other(scol, 3, False)
    other(sfcol, 2, False)
    group(2)
    other(sfcol, 3, False)
    group(3)
    line_relay(1, 2)

    small = jnp.zeros((16, 128), f32)
    for zz in range(LINE):
        for i in range(RING):
            small = small + gain_tmp[zz, i].astype(f32)
    q_gain, k_gain = small[2:3], small[3:4]
    gains_out[2:4, 0:128] = small[2:4]
    cosine, sine, bias = rope_out[0], rope_out[1], rope_out[2]

    def turned(v, gain):
        v = v * rms_scale(v) * gain
        return (v * cosine + half_turn(v) * sine).astype(bf16)

    kv0 = H * HD
    v0 = kv0 + KVH * HD

    def head(g, carry):
        at = pl.ds(pl.multiple_of(g * HD, HD), HD)
        qa = pl.ds(pl.multiple_of(g * 2 * HD, 2 * HD), HD)
        qb = pl.ds(pl.multiple_of(g * 2 * HD + HD, HD), HD)
        key = turned(raw_out[:, pl.ds(pl.multiple_of(kv0 + g * HD, HD), HD)], k_gain)
        value = raw_out[:, pl.ds(pl.multiple_of(v0 + g * HD, HD), HD)].astype(bf16)
        k_out[:, at] = key
        v_out[:, at] = value
        query_a = turned(raw_out[:, qa], q_gain)
        query_b = turned(raw_out[:, qb], q_gain)
        q_out[:, qa] = query_a
        q_out[:, qb] = query_b
        for query, where in ((query_a, qa), (query_b, qb)):
            scores = lax.dot_general(query, key, contract_cols, preferred_element_type=f32)
            logits = scores * (HD ** (-0.5)) + bias
            exponent = jnp.exp(logits - jnp.max(logits, axis=-1, keepdims=True))
            weights = (exponent / lane_sum(exponent)).astype(bf16)
            mixed = jnp.dot(weights, value, preferred_element_type=f32)
            mixed_out[:, where] = mixed.astype(bf16)
        return carry

    lax.fori_loop(0, KVH, head, 0)
    for zz in range(LINE):
        pltpu.make_async_copy(
            w_out.at[pl.ds(RING * zz, RING), :, pl.ds(qkv_width, attn_width - qkv_width)],
            ow_all.at[pl.ds(RING * zz, RING)],
            o_load.at[zz],
        ).wait()
    mixed = mixed_out[...]

    def out_tile(i, total):
        at = pl.ds(pl.multiple_of(i * 512, 512), 512)
        right = ow_all[:, :, at].reshape(mixed.shape[1], 512)
        middle = x_ref[:, at].astype(f32) + jnp.dot(mixed, right, preferred_element_type=f32)
        middle_out[:, at] = middle
        return total + lane_sum(middle * middle)

    tiles = middle_out.shape[1] // 512
    total = lax.fori_loop(0, tiles, out_tile, jnp.zeros((CAP, 1), f32))
    scale = lax.rsqrt(total / middle_out.shape[1] + epsilon)

    def norm_tile(i, carry):
        at = pl.ds(pl.multiple_of(i * 512, 512), 512)
        second_tmp[:, at] = (middle_out[:, at] * scale * gains_out[1:2, at]).astype(bf16)
        return carry

    lax.fori_loop(0, tiles, norm_tile, 0)

    def m_other(piece, shard, onward):
        m_arrived(piece, shard)
        if onward:
            m_send(spot(piece, shard), piece, shard, m_second_s, second).start()
        m_send(spot(piece, shard), piece, shard, m_sib_s, sibling).start()

    def m_whole(piece):
        for k in range(RING // 2):
            m_arrived(piece, 2 * k + sibling % 2)

    part = dhid.shape[1]
    dim = tok_out.shape[2]
    wide = wd_rows.shape[2]

    def down_back(lo, hi):
        def fetch(i, slot):
            j = lo + i
            return (
                pltpu.make_async_copy(
                    d_out.at[tile(j, 2)], wd_rows.at[slot], stream.at[slot]
                ),
            )

        def body(i, slot):
            right = wd_rows[slot].reshape(wide * 2, dim)
            dhid[:, tile(lo + i, 2 * wide)] = dot_nt(cot_all[...].reshape(LINE * CAP, dim), right)

        streamed(hi - lo, fetch, body)

    def gate_up_rows(piece):
        m_whole(piece)
        copy = pltpu.make_async_copy(gu_out.at[piece], m_chunk, stream.at[0])
        copy.start()
        copy.wait()
        span = RING * rows
        left = tok_all[:, :, pl.ds(piece * span, span)].reshape(LINE * CAP, span)

        def columns(n, carry):
            at = tile(n, 512)
            term = jnp.dot(left, m_chunk[:, :, at].reshape(span, 512), preferred_element_type=f32)
            if piece == 0:
                gate_up[:, at] = term
            else:
                gate_up[:, at] += term
            return carry

        lax.fori_loop(0, 2 * part // 512, columns, 0)

    m_other(LINE, fcol, True)
    line_own(0, second_tmp)
    tok_back = pltpu.make_async_copy(second_tmp, tok_out.at[z], local.at[13])
    tok_back.start()
    m_own(1)
    m_other(LINE, scol, False)
    m_other(0, fcol, True)
    m_own(2)
    m_other(0, scol, False)
    line_relay(1, 3)
    cot_back.wait()
    cot_in = pltpu.make_async_copy(cot_out, cot_all, local.at[8])
    cot_in.start()
    m_other(LINE, sfcol, False)
    line_relay(0, 1)
    m_other(1, fcol, True)
    m_own(3)
    m_other(1, scol, False)
    m_whole(LINE)
    for copy in backs:
        copy.wait()
    cot_in.wait()
    down_back(0, RING // 4)
    m_other(0, sfcol, False)
    line_relay(0, 2)
    m_other(2, fcol, True)
    m_other(2, scol, False)
    down_back(RING // 4, RING // 2)
    m_other(1, sfcol, False)
    line_relay(0, 3)
    tok_back.wait()
    tok_in = pltpu.make_async_copy(tok_out, tok_all, local.at[10])
    tok_in.start()
    m_other(3, fcol, True)
    m_other(3, scol, False)
    tok_in.wait()
    gate_up_rows(0)
    m_other(2, sfcol, False)
    gate_up_rows(1)
    m_other(3, sfcol, False)
    gate_up_rows(2)
    gate_up_rows(3)

    def act_copies(n):
        up_at = pl.ds(pl.multiple_of(part + n * 256, 256), 256)
        return (
            pltpu.make_async_copy(hid.at[:, tile(n, 256)], hid_out.at[:, tile(n, 256)], act_out.at[n, 0]),
            pltpu.make_async_copy(dgu.at[:, tile(n, 256)], dgu_out.at[:, tile(n, 256)], act_out.at[n, 1]),
            pltpu.make_async_copy(dgu.at[:, up_at], dgu_out.at[:, up_at], act_out.at[n, 2]),
        )

    def units(n, carry):
        at = tile(n, 256)
        up_at = pl.ds(pl.multiple_of(part + n * 256, 256), 256)

        def act(r, inner):
            some = tile(r, 32)
            gate, up, back = gate_up[some, at], gate_up[some, up_at], dhid[some, at]
            sig = jax.nn.sigmoid(gate)
            silu = gate * sig
            hid[some, at] = (silu * up).astype(bf16)
            dgu[some, at] = (back * up * (sig * (1.0 + gate * (1.0 - sig)))).astype(bf16)
            dgu[some, up_at] = (back * silu).astype(bf16)
            return inner

        lax.fori_loop(0, LINE * CAP // 32, act, 0)
        for copy in act_copies(n):
            copy.start()
        return carry

    lax.fori_loop(0, part // 256, units, 0)

    for n in range(part // 256):
        for copy in act_copies(n):
            copy.wait()
    for k in range(1, LINE):
        for which in range(2):
            exchange(k, which).wait_send()
    for k in range(LINE):

        @pl.when((z < last) & (k <= z))
        def _(k=k):
            send(w_tmp, col + RING * k, up_s, me + RING).wait_send()
            for which in range(2):
                line_send(cot_tmp, which, k, line_up, me + RING).wait_send()

        @pl.when((z > 0) & (k >= z))
        def _(k=k):
            send(w_tmp, col + RING * k, down_s, me - RING).wait_send()
            for which in range(2):
                line_send(cot_tmp, which, k, line_down, me - RING).wait_send()

        send(w_tmp, col + RING * k, first_s, first).wait_send()
        send(w_tmp, col + RING * k, second_s, second).wait_send()
        send(w_tmp, fcol + RING * k, second_s, second).wait_send()
        for base in (col, fcol, scol, sfcol):
            send(w_tmp, base + RING * k, sib_s, sibling).wait_send()
    for piece in range(pieces):
        src = source(piece)
        m_send(src, piece, col, m_first_s, first).wait_send()
        m_send(src, piece, col, m_second_s, second).wait_send()
        m_send(src, piece, fcol, m_second_s, second).wait_send()
        for base in (col, fcol, scol, sfcol):
            m_send(src, piece, base, m_sib_s, sibling).wait_send()


def forward(hidden_in, out_grad, seq_lengths, seq_device, gains, wq, wk, wv, wo, gate, up, wd):
    slots, dim = hidden_in.shape
    rows = wq.shape[0]
    n = RING * LINE
    width = gate.shape[1] // LINE
    qkv_width = wq.shape[1] + wk.shape[1] + wv.shape[1]
    wide = qkv_width + wo.shape[1] + 128
    pieces = LINE + 1
    S = jax.ShapeDtypeStruct
    return pl.pallas_call(
        forward_kernel,
        out_shape=(
            S((n, rows, wide), bf16),
            S((LINE, RING, rows, 2 * width), bf16),
            S((RING,) + wd.shape, bf16),
            S((LINE, slots, dim), bf16),
            S((LINE, slots, dim), bf16),
            S((LINE * slots, width), bf16),
            S((LINE * slots, 2 * width), bf16),
            S((slots, dim), f32),
            S((slots, dim), bf16),
            S((slots, qkv_width), f32),
            S((slots, H * HD), bf16),
            S((slots, KVH * HD), bf16),
            S((slots, KVH * HD), bf16),
            S((slots, H * HD), bf16),
            S((8, dim), f32),
            S((3, slots, HD), f32),
        ),
        in_specs=[VMEM] * 7 + [ANY] * 8,
        out_specs=(ANY,) * 7 + (VMEM,) * 9,
        scratch_shapes=[
            pltpu.VMEM((rows, wide), bf16),
            pltpu.VMEM((LINE, rows, 2 * width), bf16),
            pltpu.VMEM(wd.shape, bf16),
            pltpu.VMEM((slots, dim), bf16),
            pltpu.VMEM((slots, dim), bf16),
            pltpu.VMEM((RING, rows, qkv_width), bf16),
            pltpu.VMEM((n, rows, wo.shape[1]), bf16),
            pltpu.VMEM((LINE, RING, 16, 128), bf16),
            pltpu.VMEM((16, 128), f32),
            pltpu.VMEM((LINE, slots, dim), bf16),
            pltpu.VMEM((LINE, slots, dim), bf16),
            pltpu.VMEM((LINE * slots, 2 * width), f32),
            pltpu.VMEM((LINE * slots, width), f32),
            pltpu.VMEM((RING, rows, 2 * width), bf16),
            pltpu.VMEM((2, 2) + wd.shape, bf16),
            pltpu.VMEM((LINE * slots, width), bf16),
            pltpu.VMEM((LINE * slots, 2 * width), bf16),
            DMA((14,)),
            DMA((n,)),
            DMA((n,)),
            DMA((n,)),
            DMA((n,)),
            DMA((n,)),
            DMA((n,)),
            DMA((LINE, 2)),
            DMA((LINE, 2)),
            DMA((pieces, RING)),
            DMA((pieces, RING)),
            DMA((pieces, RING)),
            DMA((pieces, RING)),
            DMA((2, LINE)),
            DMA((2, LINE)),
            DMA((2, LINE)),
            DMA,
            DMA((LINE,)),
            DMA,
            DMA((2,)),
            DMA((width // 256, 3)),
        ],
        compiler_params=pltpu.CompilerParams(
            collective_id=0, has_side_effects=True, vmem_limit_bytes=64000 * 1024
        ),
        name="forward",
    )(
        hidden_in, seq_lengths[None, :], seq_device[None, :], *[g[None, :] for g in gains],
        out_grad, wq, wk, wv, wo, gate, up, wd,
    )


def backward_kernel(
    gu_ref, wd_ref, tok_ref, cot_ref, hid_ref, dgu_ref, w_ref, middle_ref, normed_ref, raw_ref,
    q_ref, k_ref, v_ref, mixed_ref, x_ref, gains_ref, rope_ref,
    x_out, small_out, y_out, d_out, a_out, ex_land, gu_out, c_land, s_land, f_land, l_land,
    gu_all, gd_all, gu_sib, gd_sib, gu_sec, gd_sec, gu_fst, gd_fst, t_own, t_land,
    dmid, dqkv, s_sum, s_got, s_line,
    c_send, c_recv, s_send, s_recv, f_send, f_recv, down_s, down_r, up_s, up_r, load, stream, back,
    ac_send, ac_recv, as_send, as_recv, af_send, af_recv, ad_send, ad_recv, au_send, au_recv,
    ex_s, ex_r, small_s, small_r,
):
    me, z, first, second, sibling = where_am_i()
    greet(line_peers(me) + [first, second, sibling])
    core = me % 2
    mine, fst, sec = (me % RING) // 2, (first % RING) // 2, (second % RING) // 2
    far = ((second + first - me) % RING) // 2
    half = gd_fst.shape[0] // 2
    last = LINE - 1
    tokens, dim = tok_ref.shape
    part = wd_ref.shape[0]
    quad_rows = part // LINE
    shard_rows = dim // (RING * LINE)
    piece_cols = gu_all.shape[3]
    kv0 = H * HD
    v0 = kv0 + KVH * HD
    qkv_width = v0 + KVH * HD
    MLP_GU, MLP_D = (0, 0, LINE), (1, LINE, LINE + 2)

    def block(gu, d, piece, group):
        if group == 0:
            return gu.at[piece]
        return d.at[tile(piece - LINE, half)]

    def own_block(quad, piece, group, theirs=False):
        shard = 2 * quad + (1 - core if theirs else core)
        if group == 0:
            return gu_all.at[piece, shard]
        return block(None, gd_all.at[shard], piece, group)

    def each(span, body):
        group, lo, hi = span

        def step(piece, carry):
            body(piece, group)
            return carry

        lax.fori_loop(lo, hi, step, 0)

    def to_sibling(quad, piece, group):
        return remote(
            own_block(quad, piece, group, theirs=True),
            block(gu_sib.at[quad], gd_sib.at[quad], piece, group),
            c_send.at[quad, piece],
            c_recv.at[quad, piece],
            sibling,
        )

    def to_second(quad, slot, piece, group):
        return remote(
            own_block(quad, piece, group),
            block(gu_sec.at[slot], gd_sec.at[slot], piece, group),
            s_send.at[slot, piece],
            s_recv.at[slot, piece],
            second,
        )

    def to_first(piece, group):
        return remote(
            own_block(fst, piece, group),
            block(gu_fst, gd_fst, piece, group),
            f_send.at[piece],
            f_recv.at[piece],
            first,
        )

    def pass_on(piece, group):
        for quad, slot in ((far, 1), (sec, 0)):
            to_sibling(quad, piece, group).wait_recv()
            own = own_block(quad, piece, group)
            add_rows(own, own, block(gu_sib.at[quad], gd_sib.at[quad], piece, group))
            to_second(quad, slot, piece, group).start()

    def narrow(piece, group):
        to_sibling(fst, piece, group).wait_recv()
        to_second(far, 1, piece, group).wait_recv()
        own = own_block(fst, piece, group)
        add_rows(
            own,
            own,
            block(gu_sib.at[fst], gd_sib.at[fst], piece, group),
            block(gu_sec.at[1], gd_sec.at[1], piece, group),
        )
        to_first(piece, group).start()

    def finish(piece, group, out=None):
        to_sibling(mine, piece, group).wait_recv()
        to_second(sec, 0, piece, group).wait_recv()
        to_first(piece, group).wait_recv()
        own = own_block(mine, piece, group)
        add_rows(
            own if group == 0 else block(None, out, piece, group),
            own,
            block(gu_sib.at[mine], gd_sib.at[mine], piece, group),
            block(gu_sec.at[0], gd_sec.at[0], piece, group),
            block(gu_fst, gd_fst, piece, group),
        )

    def drain_sibling(piece, group):
        for quad in (far, fst, sec, mine):
            to_sibling(quad, piece, group).wait_send()

    def drain(piece, group):
        to_second(far, 1, piece, group).wait_send()
        to_second(sec, 0, piece, group).wait_send()
        to_first(piece, group).wait_send()

    def send_line(src, which, t, up):
        return remote(
            src,
            t_land.at[which, t + 1 if up else t],
            (up_s if up else down_s).at[which, t],
            (up_r if up else down_r).at[which, t],
            me + RING if up else me - RING,
        )

    def line_own(which):
        for k in range(last):

            @pl.when(z == last)
            def _(k=k):
                send_line(t_own.at[which, k], which, k, False).start()

            @pl.when(z == 0)
            def _(k=k):
                send_line(t_own.at[which, last - k], which, last - k, True).start()

    def relay_at(which, at, t, up):
        @pl.when(z == at)
        def _():
            landing = t_land.at[which, t + 1 if up else t]
            send_line(landing, which, t, up).wait_recv()
            add_rows(landing, landing, t_own.at[which, t])
            send_line(landing, which, t, up).start()

    def relay(which, step):
        if step < 2:
            relay_at(which, 2, step, False)
            relay_at(which, 1, last - step, True)
        else:
            relay_at(which, 1, 0, False)
            relay_at(which, 2, last, True)

    def line_sum(which, out):
        own, above, below = t_own.at[which, z], t_land.at[which, z], t_land.at[which, z + 1]

        @pl.when(z < last)
        def _():
            send_line(above, which, z, False).wait_recv()

        @pl.when(z > 0)
        def _():
            send_line(below, which, z, True).wait_recv()

        @pl.when(z == 0)
        def _():
            add_rows(out, own, above)

        @pl.when(z == last)
        def _():
            add_rows(out, own, below)

        @pl.when((z > 0) & (z < last))
        def _():
            add_rows(out, own, above, below)

    def mlp(tok, cot, hid, dgu):
        ins = [
            pltpu.make_async_copy(hid_ref, hid, load.at[0]),
            pltpu.make_async_copy(cot_ref, cot, load.at[1]),
            pltpu.make_async_copy(dgu_ref, dgu, load.at[2]),
            pltpu.make_async_copy(tok_ref, tok, load.at[3]),
        ]
        for copy in ins:
            copy.start()
        wide = 256
        for copy in ins[:2]:
            copy.wait()

        previous = None
        for quad in (far, sec, fst, mine):

            def columns(n, carry, quad=quad):
                at = tile(n, 512)
                both = dot_tn(hid[:, tile(quad, quad_rows)], cot[:, at]).astype(bf16)
                gd_all[2 * quad, :, at] = both[: quad_rows // 2]
                gd_all[2 * quad + 1, :, at] = both[quad_rows // 2 :]
                return carry

            lax.fori_loop(0, dim // 512, columns, 0)
            if previous is not None:
                each(MLP_D, lambda piece, group, q=previous: to_sibling(q, piece, group).start())
            previous = quad

        def back_through(rows_w):
            def fetch(i, slot):
                return (
                    pltpu.make_async_copy(
                        gu_ref.at[tile(i, wide)], rows_w.at[slot], stream.at[slot]
                    ),
                )

            def body(i, slot):
                out = dot_nt(dgu[...], rows_w[slot]).astype(bf16)
                t_own[0, :, :, tile(i, wide)] = out.reshape(LINE, CAP, wide)

            streamed(dim // wide, fetch, body)

        each(MLP_D, lambda piece, group, q=previous: to_sibling(q, piece, group).start())
        for copy in ins[2:]:
            copy.wait()
        pl.run_scoped(back_through, pltpu.VMEM((2, wide, 2 * part), bf16))
        each(MLP_D, pass_on)
        line_own(0)

        rows = dim // LINE
        for piece in range(LINE):

            def columns(n, carry, piece=piece):
                at = tile(n, 512)
                grad = dot_tn(tok[:, pl.ds(piece * rows, rows)], dgu[:, at]).astype(bf16)
                gu_all[piece, :, :, at] = grad.reshape(RING, rows // RING, 512)
                return carry

            lax.fori_loop(0, 2 * part // 512, columns, 0)
            if piece > 0:
                pass_on(piece - 1, 0)
            for quad in (far, fst, sec, mine):
                to_sibling(quad, piece, 0).start()
        each(MLP_D, narrow)
        relay(0, 0)

        def out_through(cols_w):
            def fetch(i, slot):
                return (
                    pltpu.make_async_copy(
                        wd_ref.at[:, tile(i, wide)], cols_w.at[slot], stream.at[slot]
                    ),
                )

            def body(i, slot):
                out = jnp.dot(hid[...], cols_w[slot], preferred_element_type=f32).astype(bf16)
                t_own[1, :, :, tile(i, wide)] = out.reshape(LINE, CAP, wide)

            streamed(dim // wide, fetch, body)

        pass_on(LINE - 1, 0)
        pl.run_scoped(out_through, pltpu.VMEM((2, part, wide), bf16))

    pl.run_scoped(
        mlp,
        pltpu.VMEM((tokens, dim), bf16),
        pltpu.VMEM((tokens, dim), bf16),
        pltpu.VMEM((tokens, part), bf16),
        pltpu.VMEM((tokens, 2 * part), bf16),
    )

    def attention(dbr, raw, q, k, v, cot, dsec, dmix, middle, w_rows):
        ins = [
            pltpu.make_async_copy(src, dst, load.at[i])
            for i, (src, dst) in enumerate(
                (
                    (middle_ref, middle),
                    (raw_ref.at[:, pl.ds(0, v0)], raw),
                    (q_ref, q),
                    (k_ref, k),
                    (v_ref, v),
                    (cot_ref.at[tile(z, CAP)], cot),
                )
            )
        ]
        for copy in ins:
            copy.start()
        relay(0, 1)
        narrow(0, 0)
        relay(0, 2)
        line_own(1)
        for copy in ins:
            copy.wait()
        line_sum(0, dsec)

        scale = rms_scale(middle[...])
        wide = 512

        def gather_mean(i, total):
            at = tile(i, wide)
            n = middle[:, at] * scale
            ds = dsec[:, at]
            s_sum[3, 0:1, at] = jnp.sum(n * ds, axis=0, keepdims=True)
            return total + lane_sum(n * ds * gains_ref[1:2, at])

        mean = lax.fori_loop(0, dim // wide, gather_mean, jnp.zeros((CAP, 1), f32)) / dim

        def spread_mean(i, carry):
            at = tile(i, wide)
            n = middle[:, at] * scale
            e = dsec[:, at] * gains_ref[1:2, at]
            d_middle = cot[:, at].astype(f32) + scale * (e - n * mean)
            dmid[:, at] = d_middle
            dbr[:, at] = d_middle.astype(bf16)
            return carry

        lax.fori_loop(0, dim // wide, spread_mean, 0)
        shards = w_rows.shape[1]
        rows = shards * w_rows.shape[2]

        def w_fetch(i, slot):
            return (
                pltpu.make_async_copy(
                    w_ref.at[tile(i, shards), :, pl.ds(qkv_width, dim)],
                    w_rows.at[slot],
                    stream.at[slot],
                ),
            )

        def through_out(i, slot):
            dmix[:, tile(i, rows)] = dot_nt(dbr[...], w_rows[slot].reshape(rows, dim)).astype(bf16)

        streamed(dim // rows, w_fetch, through_out)
        narrow(1, 0)
        relay(1, 0)

        cosine, sine, bias = rope_ref[0], rope_ref[1], rope_ref[2]
        s_sum[3, 1:8] = jnp.zeros((7, dim), f32)

        def unrope(raw_v, d_rot, row):
            d_hat = d_rot * cosine - half_turn(d_rot * sine)
            r = rms_scale(raw_v)
            n = raw_v * r
            s_sum[3, row : row + 1, 0:HD] += jnp.sum(n * d_hat, axis=0, keepdims=True)
            e = d_hat * gains_ref[row + 1 : row + 2, 0:HD]
            return (r * (e - n * jnp.mean(n * e, axis=-1, keepdims=True))).astype(bf16)

        def head(g, carry):
            at = tile(g, HD)
            key, value = k[:, at], v[:, at]
            d_key = jnp.zeros((CAP, HD), f32)
            d_value = jnp.zeros((CAP, HD), f32)
            for i in range(2):
                cols = tile(2 * g + i, HD)
                query, d_mix = q[:, cols], dmix[:, cols]
                logits = dot_nt(query, key) * (HD ** (-0.5)) + bias
                exponent = jnp.exp(logits - jnp.max(logits, axis=-1, keepdims=True))
                probs = exponent / lane_sum(exponent)
                d_probs = dot_nt(d_mix, value)
                d_logits = probs * (d_probs - lane_sum(probs * d_probs))
                d_scores = (d_logits * (HD ** (-0.5))).astype(bf16)
                d_value = d_value + dot_tn(probs.astype(bf16), d_mix)
                d_key = d_key + dot_tn(d_scores, query)
                d_query = jnp.dot(d_scores, key, preferred_element_type=f32)
                dqkv[:, cols] = unrope(raw[:, cols], d_query, 1)
            cols = pl.ds(pl.multiple_of(kv0 + g * HD, HD), HD)
            dqkv[:, cols] = unrope(raw[:, cols], d_key, 2)
            dqkv[:, pl.ds(pl.multiple_of(v0 + g * HD, HD), HD)] = d_value.astype(bf16)
            return carry

        lax.fori_loop(0, KVH // 2, head, 0)
        narrow(2, 0)
        lax.fori_loop(KVH // 2, KVH, head, 0)

    order = (
        last * (1 - z // 2),
        2 - 2 * z + 5 * (z // 2),
        1 + z % 2,
        z,
    )

    def a_own(t, quad, h):
        return gu_all.at[t, 2 * quad + (core if h else 1 - core)]

    def sums(dbr, mixed, normed, cbuf, stage, w_rows):
        ins = [
            pltpu.make_async_copy(mixed_ref, mixed, load.at[0]),
            pltpu.make_async_copy(normed_ref, normed, load.at[1]),
        ]
        for copy in ins:
            copy.start()
        for copy in ins:
            copy.wait()
        span = dim // LINE

        def a_sibling(t, quad, h, slot):
            return remote(
                cbuf.at[slot, quad],
                c_land.at[t, h, quad],
                ac_send.at[slot, quad],
                ac_recv.at[t, h, quad],
                sibling,
            )

        def a_second(t, quad, h, slot):
            return remote(
                a_own(t, quad, h),
                s_land.at[slot, t, h],
                as_send.at[slot, t, h],
                as_recv.at[slot, t, h],
                second,
            )

        def a_first(t, h):
            return remote(
                a_own(t, fst, h), f_land.at[t, h], af_send.at[t, h], af_recv.at[t, h], first
            )

        def a_line(t, h, upward):
            src = a_own(t, mine, h)
            if upward:
                return remote(
                    src, l_land.at[1, t, h], au_send.at[t, h], au_recv.at[t, h], me + RING
                )
            return remote(src, l_land.at[0, t, h], ad_send.at[t, h], ad_recv.at[t, h], me - RING)

        def absorb(own, *landed):
            copies = [
                pltpu.make_async_copy(src, stage.at[i], stream.at[i])
                for i, src in enumerate(landed)
            ]
            for copy in copies:
                copy.start()
            for copy in copies:
                copy.wait()
            add_rows(own, own, *[stage.at[i] for i in range(len(landed))])

        def compute(k):
            h, t, slot = k // LINE, order[k % LINE], k % 2
            if k > 1:
                for quad in (far, fst, sec, mine):
                    a_sibling(order[(k - 2) % LINE], quad, (k - 2) // LINE, slot).wait_send()
            col0 = v0 if h else 0
            own_core = core if h else 1 - core

            def columns(n, carry, left, right, at):
                grad = dot_tn(left[:, tile(t, span)], right).astype(bf16)
                grad = grad.reshape(RING // 2, 2, shard_rows, 512)
                ours = jnp.where(core == 0, grad[:, 0], grad[:, 1])
                theirs = jnp.where(core == 0, grad[:, 1], grad[:, 0])
                for quad in range(RING // 2):
                    gu_all[t, 2 * quad + own_core, :, at] = ours[quad]
                cbuf[slot, :, :, at] = theirs
                return carry

            def from_qkv(n, carry):
                at = tile(n, 512)
                right = dqkv[:, pl.ds(pl.multiple_of(col0 + n * 512, 512), 512)]
                return columns(n, carry, normed, right, at)

            def from_out(n, carry):
                at = pl.ds(pl.multiple_of(qkv_width - v0 + n * 512, 512), 512)
                return columns(n, carry, mixed, dbr[:, tile(n, 512)], at)

            if h == 0:
                lax.fori_loop(0, v0 // 512, from_qkv, 0)
            else:
                lax.fori_loop(0, (qkv_width - v0) // 512, from_qkv, 0)
                lax.fori_loop(0, dim // 512, from_out, 0)

        def share(k):
            h, t, slot = k // LINE, order[k % LINE], k % 2
            for quad in (far, fst, sec, mine):
                a_sibling(t, quad, h, slot).start()

        def spread(k):
            h, t, slot = k // LINE, order[k % LINE], k % 2
            for quad, place in ((far, 1), (sec, 0)):
                a_sibling(t, quad, h, slot).wait_recv()
                absorb(a_own(t, quad, h), c_land.at[t, h, quad])
                a_second(t, quad, h, place).start()

        def inward(k):
            h, t, slot = k // LINE, order[k % LINE], k % 2
            a_sibling(t, fst, h, slot).wait_recv()
            a_second(t, far, h, 1).wait_recv()
            absorb(a_own(t, fst, h), c_land.at[t, h, fst], s_land.at[1, t, h])
            a_first(t, h).start()

        def collect(k):
            h, t, slot = k // LINE, order[k % LINE], k % 2
            a_sibling(t, mine, h, slot).wait_recv()
            a_second(t, sec, h, 0).wait_recv()
            a_first(t, h).wait_recv()
            absorb(a_own(t, mine, h), c_land.at[t, h, mine], s_land.at[0, t, h], f_land.at[t, h])

            @pl.when((t < z) & (z == last))
            def _():
                a_line(t, h, False).start()

            @pl.when((t > z) & (z == 0))
            def _():
                a_line(t, h, True).start()

        def onward(k):
            h, t = k // LINE, order[k % LINE]

            @pl.when((t < z) & (z < last))
            def _():
                a_line(t, h, False).wait_recv()
                absorb(a_own(t, mine, h), l_land.at[0, t, h])
                a_line(t, h, False).start()

            @pl.when((t > z) & (z > 0))
            def _():
                a_line(t, h, True).wait_recv()
                absorb(a_own(t, mine, h), l_land.at[1, t, h])
                a_line(t, h, True).start()

        def exchange(k):
            peer_z = lax.rem(z + k, LINE)
            return remote(
                gu_out.at[peer_z], ex_land.at[z], ex_s.at[k], ex_r.at[k], me % RING + RING * peer_z
            )

        def small(step, src, dst, device):
            return remote(src, dst, small_s.at[step], small_r.at[step], device)

        def first_norm():
            shards = w_rows.shape[1]
            wide = 512
            x_scale = rms_scale(x_ref[...].astype(f32))
            w_tile = shards * w_rows.shape[2]

            def w_fetch(i, slot):
                return (
                    pltpu.make_async_copy(
                        w_ref.at[tile(i, shards), :, pl.ds(0, qkv_width)],
                        w_rows.at[slot],
                        stream.at[slot],
                    ),
                )

            def through(i, slot):
                x_out[:, tile(i, w_tile)] = dot_nt(dqkv[...], w_rows[slot].reshape(w_tile, qkv_width))

            streamed(dim // w_tile, w_fetch, through)

            def gather_mean(i, total):
                at = tile(i, wide)
                n = x_ref[:, at].astype(f32) * x_scale
                s_sum[3, 3:4, at] = jnp.sum(n * x_out[:, at], axis=0, keepdims=True)
                return total + lane_sum(n * x_out[:, at] * gains_ref[0:1, at])

            mean = lax.fori_loop(0, dim // wide, gather_mean, jnp.zeros((CAP, 1), f32)) / dim

            def spread_mean(i, carry):
                at = tile(i, wide)
                n = x_ref[:, at].astype(f32) * x_scale
                e = x_out[:, at] * gains_ref[0:1, at]
                x_out[:, at] = dmid[:, at] + x_scale * (e - n * mean)
                return carry

            lax.fori_loop(0, dim // wide, spread_mean, 0)

        small_c = small(0, s_sum.at[3], s_got.at[0], sibling)
        each(MLP_GU, drain_sibling)
        compute(0)
        share(0)
        narrow(3, 0)
        spread(0)
        compute(1)
        share(1)
        spread(1)
        relay(1, 1)
        inward(0)
        compute(2)
        share(2)
        spread(2)
        inward(1)
        relay(1, 2)
        compute(3)
        share(3)
        spread(3)
        each(MLP_GU, finish)
        gu_back = pltpu.make_async_copy(gu_all.at[:, 2 * mine + core], gu_out, back.at[0])
        gu_back.start()
        collect(0)
        inward(2)
        gu_back.wait()
        for k in range(1, LINE):
            exchange(k).start()
        ex_in = pltpu.make_async_copy(gu_all.at[z, 2 * mine + core], ex_land.at[z], back.at[1])
        ex_in.start()
        each(MLP_GU, drain)
        ex_in.wait()
        compute(4)
        share(4)
        spread(4)
        collect(1)
        onward(0)
        first_norm()
        inward(3)
        small_c.start()
        compute(5)
        share(5)
        spread(5)
        collect(2)
        onward(1)
        small_c.wait()
        s_sum[0] = s_sum[3] + s_got[0]
        small_f = small(1, s_sum.at[0], s_got.at[1], first)
        small_f.start()
        inward(4)
        compute(6)
        share(6)
        spread(6)
        collect(3)
        onward(2)
        inward(5)
        small_f.wait()
        s_sum[1] = s_sum[0] + s_got[1]
        small_s2 = small(2, s_sum.at[1], s_got.at[2], second)
        small_s2.start()
        compute(7)
        share(7)
        spread(7)
        collect(4)
        inward(6)
        collect(5)
        onward(4)
        inward(7)
        small_s2.wait()
        s_sum[2] = s_sum[1] + s_got[2]
        small_line = [
            small(2 + k, s_sum.at[2], s_line.at[k], me % RING + RING * lax.rem(z + k, LINE))
            for k in range(1, LINE)
        ]
        for copy in small_line:
            copy.start()
        collect(6)
        onward(5)
        onward(6)
        collect(7)
        for copy in small_line:
            copy.wait()
        small_out[...] = (s_sum[2] + s_line[2]) + (s_line[1] + s_line[3])
        for k in (6, 7):
            for quad in (far, fst, sec, mine):
                a_sibling(order[k % LINE], quad, k // LINE, k % 2).wait_send()
        for k in range(1, LINE):
            exchange(k).wait_send()
            src_z = lax.rem(z + LINE - k, LINE)
            landed = ex_land.at[src_z]
            remote(landed, landed, ex_s.at[k], ex_r.at[k], sibling).wait_recv()
        for t in range(LINE):
            for h in range(2):
                a_second(t, far, h, 1).wait_send()
                a_second(t, sec, h, 0).wait_send()
                a_first(t, h).wait_send()

                @pl.when(t < z)
                def _(t=t, h=h):
                    a_line(t, h, False).wait_send()

                @pl.when(t > z)
                def _(t=t, h=h):
                    a_line(t, h, True).wait_send()

    slots = CAP
    kv = KVH * HD
    rows = gu_all.shape[2]

    def both(dbr):
        pl.run_scoped(
            lambda *refs: attention(dbr, *refs),
            pltpu.VMEM((slots, v0), f32),
            pltpu.VMEM((slots, dim), bf16),
            pltpu.VMEM((slots, kv), bf16),
            pltpu.VMEM((slots, kv), bf16),
            pltpu.VMEM((slots, dim), bf16),
            pltpu.VMEM((slots, dim), f32),
            pltpu.VMEM((slots, dim), bf16),
            pltpu.VMEM((slots, dim), f32),
            pltpu.VMEM((2, 4, rows, dim), bf16),
        )
        pl.run_scoped(
            lambda *refs: sums(dbr, *refs),
            pltpu.VMEM((slots, dim), bf16),
            pltpu.VMEM((slots, dim), bf16),
            pltpu.VMEM((2, RING // 2, rows, piece_cols), bf16),
            pltpu.VMEM((3, rows, piece_cols), bf16),
            pltpu.VMEM((2, 2, rows, qkv_width), bf16),
        )

    pl.run_scoped(both, pltpu.VMEM((slots, dim), bf16))

    def a_landed(t, h, upward):
        landing = l_land.at[1 if upward else 0, t, h]
        sems = (au_send, au_recv) if upward else (ad_send, ad_recv)
        return remote(landing, landing, sems[0].at[t, h], sems[1].at[t, h], sibling)

    def results(middle, y, y_half, d_tmp, a_tmp, stage):
        middle_in = pltpu.make_async_copy(middle_ref, middle, load.at[0])
        middle_in.start()
        each(MLP_D, lambda piece, group: finish(piece, group, d_tmp))
        d_back = pltpu.make_async_copy(d_tmp, d_out, load.at[1])
        d_back.start()
        line_sum(1, y)
        middle_in.wait()

        def last_add(i, carry):
            at = tile(i, 512)
            y_half[:, at] = (middle[:, at] + y[:, at]).astype(bf16)
            return carry

        lax.fori_loop(0, dim // 512, last_add, 0)
        y_back = pltpu.make_async_copy(y_half, y_out, load.at[2])
        y_back.start()
        each(MLP_D, drain_sibling)
        each(MLP_D, drain)

        for h in range(2):

            @pl.when(z < last)
            def _(h=h):
                a_landed(z, h, False).wait_recv()

            @pl.when(z > 0)
            def _(h=h):
                a_landed(z, h, True).wait_recv()

        def total(*sides):
            for h in range(2):
                copies = [
                    pltpu.make_async_copy(l_land.at[side, z, h], stage.at[i], stream.at[i])
                    for i, side in enumerate(sides)
                ]
                for copy in copies:
                    copy.start()
                for copy in copies:
                    copy.wait()
                add_rows(
                    a_tmp.at[:, pl.ds(h * piece_cols, piece_cols)],
                    a_own(z, mine, h),
                    *[stage.at[i] for i in range(len(sides))],
                )

        @pl.when(z == 0)
        def _():
            total(0)

        @pl.when(z == last)
        def _():
            total(1)

        @pl.when((z > 0) & (z < last))
        def _():
            total(0, 1)

        a_back = pltpu.make_async_copy(a_tmp, a_out, load.at[3])
        a_back.start()
        for copy in (d_back, y_back, a_back):
            copy.wait()

    pl.run_scoped(
        results,
        pltpu.VMEM((slots, dim), f32),
        pltpu.VMEM((slots, dim), f32),
        pltpu.VMEM((slots, dim), bf16),
        pltpu.VMEM(gd_fst.shape, f32),
        pltpu.VMEM((rows, 2 * piece_cols), f32),
        pltpu.VMEM((2, rows, piece_cols), bf16),
    )
    for which in range(2):
        for k in range(LINE):

            @pl.when((z > 0) & (k < z))
            def _(which=which, k=k):
                send_line(t_own.at[which, k], which, k, False).wait_send()

            @pl.when((z < last) & (k > z))
            def _(which=which, k=k):
                send_line(t_own.at[which, k], which, k, True).wait_send()


def backward(gu, wd, tok, cot, hid, dgu, w, middle, normed, raw, q, k, v, mixed, x, gains, rope):
    dim = tok.shape[1]
    rows = w.shape[1]
    drows = wd.shape[0] // RING
    cols = gu.shape[1]
    quads = RING // 2
    pieces = LINE + 2
    qkv = raw.shape[1]
    S = jax.ShapeDtypeStruct
    return pl.pallas_call(
        backward_kernel,
        out_shape=(
            S((CAP, dim), f32),
            S((8, dim), f32),
            S((CAP, dim), bf16),
            S((drows, dim), f32),
            S((rows, qkv + dim), f32),
            S((LINE, rows, cols), bf16),
            S((LINE, rows, cols), bf16),
            S((LINE, 2, quads, rows, cols), bf16),
            S((2, LINE, 2, rows, cols), bf16),
            S((LINE, 2, rows, cols), bf16),
            S((2, LINE, 2, rows, cols), bf16),
        ),
        in_specs=[ANY] * 14 + [VMEM] * 3,
        out_specs=(VMEM,) * 2 + (ANY,) * 9,
        scratch_shapes=[
            pltpu.VMEM((LINE, RING, rows, cols), bf16),
            pltpu.VMEM((RING, drows, dim), bf16),
            pltpu.VMEM((quads, LINE, rows, cols), bf16),
            pltpu.VMEM((quads, drows, dim), bf16),
            pltpu.VMEM((2, LINE, rows, cols), bf16),
            pltpu.VMEM((2, drows, dim), bf16),
            pltpu.VMEM((LINE, rows, cols), bf16),
            pltpu.VMEM((drows, dim), bf16),
            pltpu.VMEM((2, LINE, CAP, dim), bf16),
            pltpu.VMEM((2, LINE + 1, CAP, dim), bf16),
            pltpu.VMEM((CAP, dim), f32),
            pltpu.VMEM((CAP, qkv), bf16),
            pltpu.VMEM((4, 8, dim), f32),
            pltpu.VMEM((3, 8, dim), f32),
            pltpu.VMEM((LINE, 8, dim), f32),
            DMA((quads, pieces)),
            DMA((quads, pieces)),
            DMA((2, pieces)),
            DMA((2, pieces)),
            DMA((pieces,)),
            DMA((pieces,)),
            DMA((2, LINE)),
            DMA((2, LINE)),
            DMA((2, LINE)),
            DMA((2, LINE)),
            DMA((6,)),
            DMA((3,)),
            DMA((2,)),
            DMA((2, quads)),
            DMA((LINE, 2, quads)),
            DMA((2, LINE, 2)),
            DMA((2, LINE, 2)),
            DMA((LINE, 2)),
            DMA((LINE, 2)),
            DMA((LINE, 2)),
            DMA((LINE, 2)),
            DMA((LINE, 2)),
            DMA((LINE, 2)),
            DMA((LINE,)),
            DMA((LINE,)),
            DMA((2 + LINE,)),
            DMA((2 + LINE,)),
        ],
        compiler_params=pltpu.CompilerParams(
            collective_id=2, has_side_effects=True, vmem_limit_bytes=65400 * 1024
        ),
        name="backward",
    )(gu, wd, tok, cot, hid, dgu, w, middle, normed, raw, q, k, v, mixed, x, gains, rope)


def results_kernel(
    y_ref, x_ref, small_ref, d_ref, a_ref, ex_ref,
    y_out, x_out, q_out, k_out, v_out, o_out, gate_out, up_out, d_out, ga_out, gq_out, gk_out, gm_out,
    y_tmp, x_tmp, small, d_tmp, a_tmp, ex_tmp, gate_tmp, up_tmp, sem_in, sem_out,
):
    me = lax.axis_index("fsdp")
    width = ex_tmp.shape[2] // 2
    moves = ((small_ref, small), (ex_ref, ex_tmp), (a_ref, a_tmp), (d_ref, d_tmp), (x_ref, x_tmp), (y_ref, y_tmp))
    ins = [pltpu.make_async_copy(src, dst, sem_in.at[i]) for i, (src, dst) in enumerate(moves)]
    for copy in ins:
        copy.start()
    outs = []

    def leave(src, dst):
        copy = pltpu.make_async_copy(src, dst, sem_out.at[len(outs)])
        copy.start()
        outs.append(copy)

    ins[1].wait()
    for k in range(LINE):
        add_rows(gate_tmp.at[:, pl.ds(k * width, width)], ex_tmp.at[k, :, pl.ds(0, width)])
        add_rows(up_tmp.at[:, pl.ds(k * width, width)], ex_tmp.at[k, :, pl.ds(width, width)])
    leave(gate_tmp, gate_out)
    leave(up_tmp, up_out)
    ins[2].wait()
    lo = 0
    for out in (q_out, k_out, v_out, o_out):
        leave(a_tmp.at[:, pl.ds(lo, out.shape[1])], out)
        lo += out.shape[1]
    ins[3].wait()
    leave(d_tmp, d_out)
    ins[4].wait()
    leave(x_tmp, x_out)
    ins[5].wait()
    leave(y_tmp, y_out)
    ins[0].wait()
    for row, out in ((3, ga_out), (1, gq_out), (2, gk_out), (0, gm_out)):
        count = out.shape[1]
        value = jnp.zeros((1, 128), f32)
        for i in range(small.shape[1] // 128):
            held = small[row : row + 1, i * 128 : (i + 1) * 128]
            value = jnp.where((me * count) // 128 == i, held, value)
        value = pltpu.roll(value, (128 - (me * count) % 128) % 128, 1)
        out[...] = value[:, 0:count]
    for copy in outs:
        copy.wait()


def results(y, x, small, d, a, ex, widths, shares):
    rows = a.shape[0]
    wide = LINE * ex.shape[2] // 2
    S = jax.ShapeDtypeStruct
    return pl.pallas_call(
        results_kernel,
        out_shape=(
            S(y.shape, bf16),
            S(x.shape, f32),
            *[S((rows, w), f32) for w in widths],
            S((rows, wide), f32),
            S((rows, wide), f32),
            S(d.shape, f32),
            *[S((1, s), f32) for s in shares],
        ),
        in_specs=[ANY] * 6,
        out_specs=(ANY,) * 9 + (VMEM,) * 4,
        scratch_shapes=[
            pltpu.VMEM(y.shape, bf16),
            pltpu.VMEM(x.shape, f32),
            pltpu.VMEM(small.shape, f32),
            pltpu.VMEM(d.shape, f32),
            pltpu.VMEM(a.shape, f32),
            pltpu.VMEM(ex.shape, bf16),
            pltpu.VMEM((rows, wide), f32),
            pltpu.VMEM((rows, wide), f32),
            DMA((6,)),
            DMA((9,)),
        ],
        name="results",
    )(y, x, small, d, a, ex)


def layout(seq_lengths, seq_device, owner, slots):
    owned = seq_device == owner
    counts = jnp.where(owned, seq_lengths, 0)
    starts = jnp.cumsum(counts) - counts
    places = jnp.arange(slots, dtype=jnp.int32)
    inside = (
        owned[:, None]
        & (places[None, :] >= starts[:, None])
        & (places[None, :] < (starts + counts)[:, None])
    )
    labels = jnp.arange(seq_lengths.shape[0], dtype=jnp.int32)
    segment = jnp.sum(jnp.where(inside, labels[:, None] + 1, 0), axis=0) - 1
    position = jnp.sum(jnp.where(inside, places[None, :] - starts[:, None], 0), axis=0)
    return (segment, position)


def allowed_pairs(segment):
    places = jnp.arange(segment.shape[0], dtype=jnp.int32)
    earlier = places[None, :] < places[:, None]
    same_seq = (segment[:, None] == segment[None, :]) & (segment[:, None] >= 0)
    return (places[:, None] == places[None, :]) | earlier & same_seq


def rmsnorm(values, gain):
    return values * lax.rsqrt(jnp.mean(values * values, axis=-1, keepdims=True) + epsilon) * gain


def rotary(values, position):
    half_dim = values.shape[-1] // 2
    freqs = jnp.power(rope_base, -2.0 * jnp.arange(half_dim, dtype=jnp.float32) / values.shape[-1])
    angles = position.astype(jnp.float32)[:, None] * freqs[None, :]
    cosine = jnp.concatenate([jnp.cos(angles), jnp.cos(angles)], axis=-1)[:, None, :]
    sine = jnp.concatenate([jnp.sin(angles), jnp.sin(angles)], axis=-1)[:, None, :]
    rotated = jnp.concatenate([-values[..., half_dim:], values[..., :half_dim]], axis=-1)
    return values * cosine + rotated * sine


def matmul(left, right):
    return jnp.dot(left, right, preferred_element_type=jnp.float32)


def times_rows(left, right):
    return lax.dot_general(left, right, contract_rows, preferred_element_type=jnp.float32)


def times_cols(left, right):
    return lax.dot_general(left, right, contract_cols, preferred_element_type=jnp.float32)


def scatter_sum(partial):
    total = lax.psum_scatter(
        partial.astype(jnp.bfloat16), "fsdp", scatter_dimension=0, tiled=True
    )
    return total.astype(jnp.float32)


def plain(
    hidden_in,
    out_grad,
    seq_lengths,
    seq_device,
    attn_gain,
    q_gain,
    k_gain,
    w_query,
    w_key,
    w_value,
    w_out,
    mlp_gain,
    w_gate,
    w_up,
    w_down,
):
    slots = hidden_in.shape[0]
    groups = H // KVH
    score_scale = HD ** (-0.5)
    segment, position = layout(seq_lengths, seq_device, lax.axis_index("fsdp"), slots)
    allowed = allowed_pairs(segment)[None, None]

    def query_path(raw, gain):
        return rotary(rmsnorm(raw.reshape(slots, H, HD), gain), position)

    def key_path(raw, gain):
        return rotary(rmsnorm(raw.reshape(slots, KVH, HD), gain), position)

    def swiglu(gate_in, up_in):
        return jax.nn.silu(gate_in) * up_in

    attn_set = (
        lax.all_gather(attn_gain, "fsdp", axis=0, tiled=True),
        lax.all_gather(q_gain, "fsdp", axis=0, tiled=True),
        lax.all_gather(k_gain, "fsdp", axis=0, tiled=True),
        lax.all_gather(w_query, "fsdp", axis=0, tiled=True),
        lax.all_gather(w_key, "fsdp", axis=0, tiled=True),
        lax.all_gather(w_value, "fsdp", axis=0, tiled=True),
        lax.all_gather(w_out, "fsdp", axis=0, tiled=True),
    )
    gain_attn, gain_query, gain_key, query_w, key_w, value_w, out_w = attn_set
    inputs = hidden_in.astype(jnp.float32)
    normed = rmsnorm(inputs, gain_attn.astype(jnp.float32)).astype(jnp.bfloat16)
    query_raw = matmul(normed, query_w)
    key_raw = matmul(normed, key_w)
    value_raw = matmul(normed, value_w)
    queries = (
        query_path(query_raw, gain_query.astype(jnp.float32))
        .astype(jnp.bfloat16)
        .reshape(slots, KVH, groups, HD)
    )
    keys = key_path(key_raw, gain_key.astype(jnp.float32)).astype(jnp.bfloat16)
    values = value_raw.astype(jnp.bfloat16).reshape(slots, KVH, HD)

    def masked_logits():
        scores = (
            jnp.einsum("qgrd,kgd->grqk", queries, keys, preferred_element_type=jnp.float32)
            * score_scale
        )
        return jnp.where(allowed, scores, masked_score)

    logits = masked_logits()
    row_top = jnp.max(logits, axis=-1, keepdims=True)
    exponent = jnp.exp(logits - row_top)
    row_total = jnp.sum(exponent, axis=-1, keepdims=True)
    log_total = row_top + jnp.log(row_total)
    weights = (exponent / row_total).astype(jnp.bfloat16)
    mixed = jnp.einsum("grqk,kgd->qgrd", weights, values, preferred_element_type=jnp.float32)
    mixed = mixed.reshape(slots, H * HD).astype(jnp.bfloat16)
    middle = inputs + matmul(mixed, out_w)
    mlp_set = (
        lax.all_gather(mlp_gain, "fsdp", axis=0, tiled=True),
        lax.all_gather(w_gate, "fsdp", axis=0, tiled=True),
        lax.all_gather(w_up, "fsdp", axis=0, tiled=True),
        lax.all_gather(w_down, "fsdp", axis=0, tiled=True),
    )
    gain_mlp, gate_w, up_w, down_w = mlp_set
    second = rmsnorm(middle, gain_mlp.astype(jnp.float32)).astype(jnp.bfloat16)
    gate_out = matmul(second, gate_w)
    up_out = matmul(second, up_w)
    hidden = swiglu(gate_out, up_out).astype(jnp.bfloat16)
    hidden_out = (middle + matmul(hidden, down_w)).astype(jnp.bfloat16)
    gain_mlp, gate_w, up_w, down_w = (
        lax.all_gather(mlp_gain, "fsdp", axis=0, tiled=True),
        lax.all_gather(w_gate, "fsdp", axis=0, tiled=True),
        lax.all_gather(w_up, "fsdp", axis=0, tiled=True),
        lax.all_gather(w_down, "fsdp", axis=0, tiled=True),
    )
    grad_down = scatter_sum(times_rows(hidden, out_grad))
    d_hidden = times_cols(out_grad, down_w)
    unused_out, swiglu_pull = jax.vjp(swiglu, gate_out, up_out)
    d_gate, d_up = swiglu_pull(d_hidden)
    d_gate_up = jnp.concatenate([d_gate.astype(jnp.bfloat16), d_up.astype(jnp.bfloat16)], axis=1)
    grad_gate_up = scatter_sum(times_rows(second, d_gate_up))
    ff_width = gate_w.shape[1]
    d_second = times_cols(d_gate_up, jnp.concatenate([gate_w, up_w], axis=1))
    unused_norm, second_pull = jax.vjp(rmsnorm, middle, gain_mlp.astype(jnp.float32))
    d_middle_norm, grad_gain_mlp = second_pull(d_second)
    d_middle = out_grad.astype(jnp.float32) + d_middle_norm
    gain_attn, gain_query, gain_key, query_w, key_w, value_w, out_w = (
        lax.all_gather(attn_gain, "fsdp", axis=0, tiled=True),
        lax.all_gather(q_gain, "fsdp", axis=0, tiled=True),
        lax.all_gather(k_gain, "fsdp", axis=0, tiled=True),
        lax.all_gather(w_query, "fsdp", axis=0, tiled=True),
        lax.all_gather(w_key, "fsdp", axis=0, tiled=True),
        lax.all_gather(w_value, "fsdp", axis=0, tiled=True),
        lax.all_gather(w_out, "fsdp", axis=0, tiled=True),
    )
    d_branch = d_middle.astype(jnp.bfloat16)
    grad_out_w = scatter_sum(times_rows(mixed, d_branch))
    d_mixed = times_cols(d_branch, out_w).astype(jnp.bfloat16).reshape(slots, KVH, groups, HD)
    probs = jnp.exp(masked_logits() - log_total)
    weights = probs.astype(jnp.bfloat16)
    d_probs = jnp.einsum("qgrd,kgd->grqk", d_mixed, values, preferred_element_type=jnp.float32)
    d_logits = probs * (d_probs - jnp.sum(probs * d_probs, axis=-1, keepdims=True))
    d_scores = (d_logits * score_scale).astype(jnp.bfloat16)
    d_values = jnp.einsum("grqk,qgrd->kgd", weights, d_mixed, preferred_element_type=jnp.float32)
    d_values = d_values.astype(jnp.bfloat16).reshape(slots, KVH * HD)
    d_queries_rot = jnp.einsum(
        "grqk,kgd->qgrd", d_scores, keys, preferred_element_type=jnp.float32
    ).reshape(slots, H, HD)
    d_keys_rot = jnp.einsum("grqk,qgrd->kgd", d_scores, queries, preferred_element_type=jnp.float32)
    unused_query, query_pull = jax.vjp(query_path, query_raw, gain_query.astype(jnp.float32))
    d_query_raw, grad_gain_query = query_pull(d_queries_rot)
    unused_key, key_pull = jax.vjp(key_path, key_raw, gain_key.astype(jnp.float32))
    d_key_raw, grad_gain_key = key_pull(d_keys_rot)
    d_qkv = jnp.concatenate(
        [d_query_raw.astype(jnp.bfloat16), d_key_raw.astype(jnp.bfloat16), d_values], axis=1
    )
    grad_qkv = scatter_sum(times_rows(normed, d_qkv))
    d_normed = times_cols(d_qkv, jnp.concatenate([query_w, key_w, value_w], axis=1))
    unused_first, first_pull = jax.vjp(rmsnorm, inputs, gain_attn.astype(jnp.float32))
    d_input_norm, grad_gain_attn = first_pull(d_normed)
    input_grad = d_middle + d_input_norm
    gain_sums = (
        lax.psum_scatter(grad_gain_attn, "fsdp", scatter_dimension=0, tiled=True),
        lax.psum_scatter(grad_gain_query, "fsdp", scatter_dimension=0, tiled=True),
        lax.psum_scatter(grad_gain_key, "fsdp", scatter_dimension=0, tiled=True),
        lax.psum_scatter(grad_gain_mlp, "fsdp", scatter_dimension=0, tiled=True),
    )
    query_width = H * HD
    key_width = KVH * HD
    grad_query_w = grad_qkv[:, :query_width]
    grad_key_w = grad_qkv[:, query_width : query_width + key_width]
    grad_value_w = grad_qkv[:, query_width + key_width :]
    grad_gate = grad_gate_up[:, :ff_width]
    grad_up = grad_gate_up[:, ff_width:]
    return (
        hidden_out,
        input_grad,
        gain_sums[0],
        gain_sums[1],
        gain_sums[2],
        grad_query_w,
        grad_key_w,
        grad_value_w,
        grad_out_w,
        gain_sums[3],
        grad_gate,
        grad_up,
        grad_down,
    )


def layered(
    hidden_in,
    out_grad,
    seq_lengths,
    seq_device,
    attn_gain,
    q_gain,
    k_gain,
    w_query,
    w_key,
    w_value,
    w_out,
    mlp_gain,
    w_gate,
    w_up,
    w_down,
):
    (
        attn_w, gate_up_w, down_w, tokens, cotangent, hidden, d_gate_up,
        middle, normed, qkv_raw, queries, keys, values, mixed, gains, rope,
    ) = forward(
        hidden_in, out_grad, seq_lengths, seq_device, (attn_gain, mlp_gain, q_gain, k_gain),
        w_query, w_key, w_value, w_out, w_gate, w_up, w_down,
    )
    dim = hidden_in.shape[1]
    x, small, y, grad_down, attn_sums, exchanged, *unused = backward(
        gate_up_w.reshape(-1, gate_up_w.shape[-1]),
        down_w.reshape(-1, dim),
        tokens.reshape(-1, dim),
        cotangent.reshape(-1, dim),
        hidden, d_gate_up, attn_w, middle, normed, qkv_raw, queries, keys, values, mixed,
        hidden_in, gains, rope,
    )
    (
        hidden_out, input_grad, g_query, g_key, g_value, g_out, g_gate, g_up, g_down,
        g_attn_gain, g_q_gain, g_k_gain, g_mlp_gain,
    ) = results(
        y, x, small, grad_down, attn_sums, exchanged,
        [w.shape[1] for w in (w_query, w_key, w_value, w_out)],
        [g.shape[0] for g in (attn_gain, q_gain, k_gain, mlp_gain)],
    )
    return (
        hidden_out,
        input_grad,
        g_attn_gain[0],
        g_q_gain[0],
        g_k_gain[0],
        g_query,
        g_key,
        g_value,
        g_out,
        g_mlp_gain[0],
        g_gate,
        g_up,
        g_down,
    )


def solution(mesh):
    per_device = layered if mesh.shape["fsdp"] == RING * LINE else plain
    return jax.shard_map(
        per_device,
        mesh=mesh,
        in_specs=(
            P("fsdp", None),
            P("fsdp", None),
            P(),
            P(),
            P("fsdp"),
            P("fsdp"),
            P("fsdp"),
            P("fsdp", None),
            P("fsdp", None),
            P("fsdp", None),
            P("fsdp", None),
            P("fsdp"),
            P("fsdp", None),
            P("fsdp", None),
            P("fsdp", None),
        ),
        out_specs=(
            P("fsdp", None),
            P("fsdp", None),
            P("fsdp"),
            P("fsdp"),
            P("fsdp"),
            P("fsdp", None),
            P("fsdp", None),
            P("fsdp", None),
            P("fsdp", None),
            P("fsdp"),
            P("fsdp", None),
            P("fsdp", None),
            P("fsdp", None),
        ),
        check_vma=False,
    )
```

```python
import math

import jax
import jax.numpy as jnp
from jax import lax
from jax.experimental import pallas as pl
from jax.experimental.pallas import tpu as pltpu
from jax.sharding import PartitionSpec as P

H = 16
KVH = 8
HD = 128
CAP = 128
LINE = 4
RING = 8
MESH = pl.DeviceIdType.MESH
ANY = pl.BlockSpec(memory_space=pl.ANY)
VMEM = pl.BlockSpec(memory_space=pltpu.VMEM)
DMA = pltpu.SemaphoreType.DMA
bf16 = jnp.bfloat16
f32 = jnp.float32
epsilon = 1e-06
rope_base = 1000000.0
masked_score = -1e30
contract_rows = (((0,), (0,)), ((), ()))
contract_cols = (((1,), (1,)), ((), ()))


def where_am_i():
    me = lax.axis_index("fsdp")
    core = me % 2
    z = me // RING
    f_bit = 2 + 2 * core
    s_bit = 4 - 2 * core
    first = me + f_bit * (1 - 2 * ((me // f_bit) % 2))
    second = me + s_bit * (1 - 2 * ((me // s_bit) % 2))
    sibling = me + 1 - 2 * core
    return me, z, first, second, sibling


def greet(peers):
    barrier = pltpu.get_barrier_semaphore()
    for peer in peers:
        pl.semaphore_signal(barrier, inc=1, device_id=(peer,), device_id_type=MESH)
    pl.semaphore_wait(barrier, len(peers))


def remote(src, dst, send_sem, recv_sem, device):
    return pltpu.make_async_remote_copy(
        src_ref=src,
        dst_ref=dst,
        send_sem=send_sem,
        recv_sem=recv_sem,
        device_id=(device,),
        device_id_type=MESH,
    )


def line_peers(me):
    return [lax.rem(me + RING * k, RING * LINE) for k in range(1, LINE)]


def on_line(z, k, body):
    for step in ((-k, k) if k else (0,)):

        @pl.when((z + step >= 0) & (z + step < LINE))
        def _(step=step):
            body(step)


def dot_nt(left, right):
    return lax.dot_general(left, right, contract_cols, preferred_element_type=f32)


def dot_tn(left, right):
    return lax.dot_general(left, right, contract_rows, preferred_element_type=f32)


def streamed(count, fetch, body):
    for copy in fetch(0, 0):
        copy.start()

    def step(i, carry):
        slot = i % 2

        @pl.when(i + 1 < count)
        def _():
            for copy in fetch(i + 1, 1 - slot):
                copy.start()

        for copy in fetch(i, slot):
            copy.wait()
        body(i, slot)
        return carry

    lax.fori_loop(0, count, step, 0)


def tile(i, size):
    return pl.ds(pl.multiple_of(i * size, size), size)


def add_rows(out, *terms):
    rows = out.shape[0]

    def body(i, carry):
        at = pl.ds(pl.multiple_of(i * 16, 16), 16)
        total = terms[0][at, :].astype(f32)
        for term in terms[1:]:
            total = total + term[at, :].astype(f32)
        out[at, :] = total.astype(out.dtype)
        return carry

    lax.fori_loop(0, rows // 16, body, 0)


def lane_sum(x):
    return jnp.sum(x, axis=-1, keepdims=True)


def token_places(lengths, devices, me):
    seqs = lengths.shape[1]
    counts_row = jnp.where(devices == me, lengths, 0).astype(f32)
    up = lax.broadcasted_iota(jnp.int32, (seqs, seqs), 0)
    across = lax.broadcasted_iota(jnp.int32, (seqs, seqs), 1)
    counts_col = lane_sum(jnp.where(up == across, counts_row, 0.0))
    starts_row = jnp.sum(jnp.where(up < across, counts_col, 0.0), axis=0, keepdims=True)
    starts_col = lane_sum(jnp.where(across < up, counts_row, 0.0))

    def within(places, starts, counts):
        return (places >= starts) & (places < starts + counts)

    places = lax.broadcasted_iota(jnp.int32, (CAP, seqs), 0).astype(f32)
    labels = lax.broadcasted_iota(jnp.int32, (CAP, seqs), 1).astype(f32)
    inside = within(places, starts_row, counts_row)
    segment_col = lane_sum(jnp.where(inside, labels + 1.0, 0.0)) - 1.0
    position = lane_sum(jnp.where(inside, places - starts_row, 0.0))
    places = lax.broadcasted_iota(jnp.int32, (seqs, CAP), 1).astype(f32)
    labels = lax.broadcasted_iota(jnp.int32, (seqs, CAP), 0).astype(f32)
    inside = within(places, starts_col, counts_col)
    segment_row = jnp.sum(jnp.where(inside, labels + 1.0, 0.0), axis=0, keepdims=True) - 1.0
    return segment_col, segment_row, position


def allowed_bias(segment_col, segment_row):
    t = lax.broadcasted_iota(jnp.int32, (CAP, CAP), 0)
    u = lax.broadcasted_iota(jnp.int32, (CAP, CAP), 1)
    same = (segment_col == segment_row) & (segment_col >= 0.0)
    return jnp.where((t == u) | ((u < t) & same), 0.0, masked_score)


def half_turn(v):
    lane = lax.broadcasted_iota(jnp.int32, v.shape, v.ndim - 1)
    turned = pltpu.roll(v, HD // 2, v.ndim - 1)
    return jnp.where(lane < HD // 2, -turned, turned)


def rms_scale(v):
    return lax.rsqrt(jnp.mean(v * v, axis=-1, keepdims=True) + epsilon)


def forward_kernel(
    x_ref, len_ref, dev_ref, ga_ref, gm_ref, gq_ref, gk_ref, cot_ref,
    wq_ref, wk_ref, wv_ref, wo_ref, gate_ref, up_ref,
    w_out, gu_out, tok_out, cot_out, hid_out, pre_out,
    middle_out, normed_out, raw_out, q_out, k_out, v_out, mixed_out, gains_out, rope_out,
    w_tmp, p_tmp, cot_tmp, second_tmp, chunk, ow_all, gain_tmp, gain_own,
    tok_all, gate_up, m_chunk, hid,
    local, up_s, down_s, first_s, second_s, sib_s, recv, ex_send, ex_recv,
    m_first_s, m_second_s, m_sib_s, m_recv, line_up, line_down, line_r, w_load, o_load, g_load,
    act_out,
):
    me, z, first, second, sibling = where_am_i()
    col, fcol, scol = me % RING, first % RING, second % RING
    sfcol = (second + first - me) % RING
    width = p_tmp.shape[2] // 2
    rows = w_tmp.shape[0]
    qkv_width = raw_out.shape[1]
    attn_width = qkv_width + wo_ref.shape[1]
    last = LINE - 1
    pieces = LINE

    w_in = []
    lo = 0
    for i, ref in enumerate((wq_ref, wk_ref, wv_ref, wo_ref)):
        at = pl.ds(lo, ref.shape[1])
        w_in.append(pltpu.make_async_copy(ref, w_tmp.at[:, at], local.at[i]))
        lo += ref.shape[1]
    p_in = [
        pltpu.make_async_copy(
            ref.at[:, pl.ds(pl.multiple_of(z * width, width), width)],
            p_tmp.at[z, :, pl.ds(which * width, width)],
            local.at[5 + which],
        )
        for which, ref in enumerate((gate_ref, up_ref))
    ]
    cot_in = pltpu.make_async_copy(cot_ref, cot_tmp, local.at[8])
    for copy in w_in + p_in + [cot_in]:
        copy.start()
    gain_own[...] = jnp.zeros_like(gain_own)
    for i, ref in enumerate((ga_ref, gm_ref, gq_ref, gk_ref)):
        gain_own[i : i + 1, 0 : ref.shape[1]] = ref[...].astype(f32)
    flat = gain_own[...]
    paired = jnp.where(me % 2 == 0, flat, pltpu.roll(flat, rows, 1))
    shared = pltpu.roll(flat, gq_ref.shape[1] * me, 1)
    placed = jnp.where(lax.broadcasted_iota(jnp.int32, flat.shape, 0) < 2, paired, shared)
    w_tmp[0:16, attn_width:] = placed.astype(bf16)
    w_tmp[16:, attn_width:] = jnp.zeros((rows - 16, 128), bf16)
    greet(line_peers(me) + [first, second, sibling])

    def send(src, shard, sems, device):
        return remote(src, w_out.at[shard], sems.at[shard], recv.at[shard], device)

    def arrived(shard):
        send(w_out.at[shard], shard, sib_s, sibling).wait_recv()

    def exchange(k, which):
        peer_z = lax.rem(z + k, LINE)
        src = (gate_ref, up_ref)[which].at[:, pl.ds(pl.multiple_of(peer_z * width, width), width)]
        dst = p_tmp.at[z, :, pl.ds(which * width, width)]
        return remote(src, dst, ex_send.at[k, which], ex_recv.at[k, which], col + RING * peer_z)

    token_half = second_tmp.shape[1] // 2

    def line_spot(which, shard):
        if which == 1:
            return cot_out.at[shard]
        return tok_out.at[shard, :, pl.ds(token_half * (which // 2), token_half)]

    def line_send(src, which, shard, sems, device):
        landing = line_spot(which, shard)
        return remote(src, landing, sems.at[which, shard], line_r.at[which, shard], device)

    def line_own(which, src):
        @pl.when(z < last)
        def _():
            line_send(src, which, z, line_up, me + RING).start()

        @pl.when(z > 0)
        def _():
            line_send(src, which, z, line_down, me - RING).start()

    def line_relay(which, k):
        def body(step):
            shard = z + step
            src = line_spot(which, shard)
            line_send(src, which, shard, line_up, second).wait_recv()
            if step < 0:

                @pl.when(z < last)
                def _():
                    line_send(src, which, shard, line_up, me + RING).start()
            else:

                @pl.when(z > 0)
                def _():
                    line_send(src, which, shard, line_down, me - RING).start()

        on_line(z, k, body)

    for copy in w_in:
        copy.wait()

    @pl.when(z < last)
    def _():
        send(w_tmp, me, up_s, me + RING).start()

    @pl.when(z > 0)
    def _():
        send(w_tmp, me, down_s, me - RING).start()

    send(w_tmp, me, first_s, first).start()
    send(w_tmp, me, second_s, second).start()
    send(w_tmp, me, sib_s, sibling).start()
    w_back = pltpu.make_async_copy(w_tmp, w_out.at[me], local.at[9])
    w_back.start()

    def own(k):
        def body(step):
            shard = me + RING * step
            src = w_out.at[shard]
            arrived(shard)
            if step < 0:

                @pl.when(z < last)
                def _():
                    send(src, shard, up_s, me + RING).start()
            else:

                @pl.when(z > 0)
                def _():
                    send(src, shard, down_s, me - RING).start()

            send(src, shard, first_s, first).start()
            send(src, shard, second_s, second).start()
            send(src, shard, sib_s, sibling).start()

        on_line(z, k, body)

    def other(base, k, onward):
        def body(step):
            shard = base + RING * (z + step)
            src = w_out.at[shard]
            arrived(shard)
            if onward:
                send(src, shard, second_s, second).start()
            send(src, shard, sib_s, sibling).start()

        on_line(z, k, body)

    segment_col, segment_row, position = token_places(len_ref[...], dev_ref[...], me)
    rope_out[2] = allowed_bias(segment_col, segment_row)
    lane = lax.broadcasted_iota(jnp.int32, (1, HD), 1) % (HD // 2)
    angles = position * jnp.exp(lane.astype(f32) * (-2.0 * math.log(rope_base) / HD))
    rope_out[0] = jnp.cos(angles)
    rope_out[1] = jnp.sin(angles)
    x_scale = rms_scale(x_ref[...].astype(f32))
    raw_out[...] = jnp.zeros_like(raw_out)

    def load_group(step):
        zz = z + step
        part = w_out.at[pl.ds(RING * zz, RING)]
        return (
            pltpu.make_async_copy(part.at[:, :, pl.ds(0, qkv_width)], chunk, w_load),
            pltpu.make_async_copy(
                part.at[:, :, pl.ds(qkv_width, attn_width - qkv_width)],
                ow_all.at[pl.ds(RING * zz, RING)],
                o_load.at[zz],
            ),
            pltpu.make_async_copy(
                part.at[:, pl.ds(0, 16), pl.ds(attn_width, 128)], gain_tmp.at[zz], g_load
            ),
        )

    def group(k):
        def body(step):
            zz = z + step
            for i in range(RING // 2):
                arrived(RING * zz + 2 * i + sibling % 2)
            copies = load_group(step)
            for copy in copies:
                copy.start()
            copies[2].wait()
            span = RING * rows
            for pair in range(RING // 2):
                at = pl.ds(pl.multiple_of(zz * span + pair * 128, 128), 128)
                both = gain_tmp[zz, 2 * pair].astype(f32) + gain_tmp[zz, 2 * pair + 1].astype(f32)
                gains_out[0:2, at] = both[0:2]
                piece = x_ref[:, at].astype(f32) * x_scale * both[0:1]
                normed_out[:, at] = piece.astype(bf16)
            copies[0].wait()
            left = normed_out[:, pl.ds(pl.multiple_of(zz * span, span), span)]

            def tile(i, carry):
                at = pl.ds(pl.multiple_of(i * 512, 512), 512)
                right = chunk[:, :, at].reshape(span, 512)
                raw_out[:, at] += jnp.dot(left, right, preferred_element_type=f32)
                return carry

            lax.fori_loop(0, qkv_width // 512, tile, 0)

        on_line(z, k, body)

    own(1)
    other(fcol, 0, True)
    own(2)
    other(fcol, 1, True)
    other(scol, 0, False)
    for k in range(1, LINE):
        for which in range(2):
            exchange(k, which).start()
    cot_in.wait()
    line_own(1, cot_tmp)
    cot_back = pltpu.make_async_copy(cot_tmp, cot_out.at[z], local.at[10])
    cot_back.start()
    own(3)
    other(fcol, 2, True)
    other(scol, 1, False)
    other(sfcol, 0, False)
    w_back.wait()
    group(0)
    other(fcol, 3, True)
    other(scol, 2, False)
    other(sfcol, 1, False)
    group(1)

    for copy in p_in:
        copy.wait()
    for k in range(1, LINE):
        for which in range(2):
            src_z = lax.rem(z + LINE - k, LINE)
            landed = p_tmp.at[src_z, :, pl.ds(which * width, width)]
            remote(landed, landed, ex_send.at[k, which], ex_recv.at[k, which], second).wait_recv()

    def spot(piece, shard):
        return gu_out.at[piece, shard]

    def source(piece):
        return p_tmp.at[piece]

    def m_send(src, piece, shard, sems, device):
        return remote(
            src, spot(piece, shard), sems.at[piece, shard], m_recv.at[piece, shard], device
        )

    def m_arrived(piece, shard):
        m_send(spot(piece, shard), piece, shard, m_sib_s, sibling).wait_recv()

    def m_own_second(piece):
        m_send(source(piece), piece, col, m_second_s, second).start()

    def m_own_first(piece):
        m_send(source(piece), piece, col, m_first_s, first).start()
        m_send(source(piece), piece, col, m_sib_s, sibling).start()

    def m_own(piece):
        m_own_second(piece)
        m_own_first(piece)

    m_own_second(0)
    m_own_second(1)
    p_back = pltpu.make_async_copy(p_tmp, gu_out.at[:, col], local.at[11])
    p_back.start()
    line_relay(1, 1)
    other(scol, 3, False)
    other(sfcol, 2, False)
    group(2)
    other(sfcol, 3, False)
    m_own_first(0)
    m_own_first(1)
    group(3)

    small = jnp.zeros((16, 128), f32)
    for zz in range(LINE):
        for i in range(RING):
            small = small + gain_tmp[zz, i].astype(f32)
    q_gain, k_gain = small[2:3], small[3:4]
    gains_out[2:4, 0:128] = small[2:4]
    cosine, sine, bias = rope_out[0], rope_out[1], rope_out[2]

    def turned(v, gain):
        v = v * rms_scale(v) * gain
        return (v * cosine + half_turn(v) * sine).astype(bf16)

    kv0 = H * HD
    v0 = kv0 + KVH * HD

    def head(g, carry):
        at = pl.ds(pl.multiple_of(g * HD, HD), HD)
        qa = pl.ds(pl.multiple_of(g * 2 * HD, 2 * HD), HD)
        qb = pl.ds(pl.multiple_of(g * 2 * HD + HD, HD), HD)
        key = turned(raw_out[:, pl.ds(pl.multiple_of(kv0 + g * HD, HD), HD)], k_gain)
        value = raw_out[:, pl.ds(pl.multiple_of(v0 + g * HD, HD), HD)].astype(bf16)
        k_out[:, at] = key
        v_out[:, at] = value
        query_a = turned(raw_out[:, qa], q_gain)
        query_b = turned(raw_out[:, qb], q_gain)
        q_out[:, qa] = query_a
        q_out[:, qb] = query_b
        for query, where in ((query_a, qa), (query_b, qb)):
            scores = lax.dot_general(query, key, contract_cols, preferred_element_type=f32)
            logits = scores * (HD ** (-0.5)) + bias
            exponent = jnp.exp(logits - jnp.max(logits, axis=-1, keepdims=True))
            weights = (exponent / lane_sum(exponent)).astype(bf16)
            mixed = jnp.dot(weights, value, preferred_element_type=f32)
            mixed_out[:, where] = mixed.astype(bf16)
        return carry

    lax.fori_loop(0, KVH, head, 0, unroll=2)
    for zz in range(LINE):
        pltpu.make_async_copy(
            w_out.at[pl.ds(RING * zz, RING), :, pl.ds(qkv_width, attn_width - qkv_width)],
            ow_all.at[pl.ds(RING * zz, RING)],
            o_load.at[zz],
        ).wait()
    mixed = mixed_out[...]

    def out_tile(i, total):
        at = pl.ds(pl.multiple_of(i * 512, 512), 512)
        right = ow_all[:, :, at].reshape(mixed.shape[1], 512)
        middle = x_ref[:, at].astype(f32) + jnp.dot(mixed, right, preferred_element_type=f32)
        middle_out[:, at] = middle
        return total + lane_sum(middle * middle)

    tiles = middle_out.shape[1] // 512
    total = lax.fori_loop(0, tiles, out_tile, jnp.zeros((CAP, 1), f32))
    scale = lax.rsqrt(total / middle_out.shape[1] + epsilon)

    def norm_tile(i, carry):
        at = pl.ds(pl.multiple_of(i * 512, 512), 512)
        second_tmp[:, at] = (middle_out[:, at] * scale * gains_out[1:2, at]).astype(bf16)
        return carry

    lax.fori_loop(0, tiles, norm_tile, 0)

    def m_other(piece, shard, onward):
        m_arrived(piece, shard)
        if onward:
            m_send(spot(piece, shard), piece, shard, m_second_s, second).start()
        m_send(spot(piece, shard), piece, shard, m_sib_s, sibling).start()

    def m_whole(piece):
        for k in range(RING // 2):
            m_arrived(piece, 2 * k + sibling % 2)

    part = width

    def gate_up_copy(piece):
        return pltpu.make_async_copy(
            gu_out.at[piece], m_chunk.at[piece % 2], act_out.at[piece % 2, 0]
        )

    def gate_up_load(piece):
        m_whole(piece)
        gate_up_copy(piece).start()

    def gate_up_rows(piece):
        gate_up_copy(piece).wait()
        span = RING * rows
        left = tok_all[:, :, pl.ds(piece * span, span)].reshape(LINE * CAP, span)

        def columns(n, carry):
            at = tile(n, 512)
            right = m_chunk[piece % 2, :, :, at].reshape(span, 512)
            term = jnp.dot(left, right, preferred_element_type=f32)
            if piece == 0:
                gate_up[:, at] = term
            else:
                gate_up[:, at] += term
            return carry

        lax.fori_loop(0, 2 * part // 512, columns, 0)

    m_own(2)
    line_own(0, second_tmp.at[:, pl.ds(0, token_half)])
    line_own(2, second_tmp.at[:, pl.ds(token_half, token_half)])
    tok_back = pltpu.make_async_copy(second_tmp, tok_out.at[z], local.at[13])
    tok_back.start()
    line_relay(1, 2)
    m_other(0, fcol, True)
    m_other(0, scol, False)
    m_own(3)
    line_relay(0, 1)
    line_relay(2, 1)
    m_other(1, fcol, True)
    line_relay(1, 3)
    m_other(1, scol, False)
    m_other(0, sfcol, False)
    line_relay(0, 2)
    line_relay(2, 2)
    m_other(2, fcol, True)
    m_other(2, scol, False)
    m_other(1, sfcol, False)
    p_back.wait()
    gate_up_load(0)
    m_other(3, fcol, True)
    m_other(3, scol, False)
    line_relay(0, 3)
    tok_back.wait()
    cot_back.wait()
    tok_in = []
    for half in range(2):
        at = pl.ds(half * token_half, token_half)
        tok_in.append(
            pltpu.make_async_copy(
                tok_out.at[:, :, at], tok_all.at[:, :, at], local.at[10 if half else 12]
            )
        )
    tok_in[0].start()
    gate_up_load(1)
    tok_in[0].wait()
    gate_up_rows(0)
    m_other(2, sfcol, False)
    gate_up_load(2)
    gate_up_rows(1)
    line_relay(2, 3)
    tok_in[1].start()
    tok_in[1].wait()
    m_other(3, sfcol, False)
    gate_up_load(3)
    gate_up_rows(2)
    gate_up_rows(3)

    def hid_copy(n):
        at = tile(n, 256)
        return pltpu.make_async_copy(hid.at[:, at], hid_out.at[:, at], act_out.at[n, 0])

    def pre_copies(n):
        up_at = pl.ds(pl.multiple_of(part + n * 256, 256), 256)
        return [
            pltpu.make_async_copy(gate_up.at[:, at], pre_out.at[:, at], act_out.at[n, i])
            for i, at in ((1, tile(n, 256)), (2, up_at))
        ]

    def units(n, carry):
        at = tile(n, 256)
        up_at = pl.ds(pl.multiple_of(part + n * 256, 256), 256)
        for copy in pre_copies(n):
            copy.start()

        def act(r, inner):
            some = tile(r, 32)
            gate, up = gate_up[some, at], gate_up[some, up_at]
            hid[some, at] = (gate * jax.nn.sigmoid(gate) * up).astype(bf16)
            return inner

        lax.fori_loop(0, LINE * CAP // 32, act, 0)
        hid_copy(n).start()
        return carry

    lax.fori_loop(0, part // 256, units, 0)

    for n in range(part // 256):
        for copy in [hid_copy(n)] + pre_copies(n):
            copy.wait()
    for k in range(1, LINE):
        for which in range(2):
            exchange(k, which).wait_send()
    for k in range(LINE):

        @pl.when((z < last) & (k <= z))
        def _(k=k):
            send(w_tmp, col + RING * k, up_s, me + RING).wait_send()
            for which in range(3):
                line_send(line_spot(which, k), which, k, line_up, me + RING).wait_send()

        @pl.when((z > 0) & (k >= z))
        def _(k=k):
            send(w_tmp, col + RING * k, down_s, me - RING).wait_send()
            for which in range(3):
                line_send(line_spot(which, k), which, k, line_down, me - RING).wait_send()

        send(w_tmp, col + RING * k, first_s, first).wait_send()
        send(w_tmp, col + RING * k, second_s, second).wait_send()
        send(w_tmp, fcol + RING * k, second_s, second).wait_send()
        for base in (col, fcol, scol, sfcol):
            send(w_tmp, base + RING * k, sib_s, sibling).wait_send()
    for piece in range(pieces):
        src = source(piece)
        m_send(src, piece, col, m_first_s, first).wait_send()
        m_send(src, piece, col, m_second_s, second).wait_send()
        m_send(src, piece, fcol, m_second_s, second).wait_send()
        for base in (col, fcol, scol, sfcol):
            m_send(src, piece, base, m_sib_s, sibling).wait_send()


def forward(hidden_in, out_grad, seq_lengths, seq_device, gains, wq, wk, wv, wo, gate, up):
    slots, dim = hidden_in.shape
    rows = wq.shape[0]
    n = RING * LINE
    width = gate.shape[1] // LINE
    qkv_width = wq.shape[1] + wk.shape[1] + wv.shape[1]
    wide = qkv_width + wo.shape[1] + 128
    pieces = LINE
    S = jax.ShapeDtypeStruct
    return pl.pallas_call(
        forward_kernel,
        out_shape=(
            S((n, rows, wide), bf16),
            S((LINE, RING, rows, 2 * width), bf16),
            S((LINE, slots, dim), bf16),
            S((LINE, slots, dim), bf16),
            S((LINE * slots, width), bf16),
            S((LINE * slots, 2 * width), f32),
            S((slots, dim), f32),
            S((slots, dim), bf16),
            S((slots, qkv_width), f32),
            S((slots, H * HD), bf16),
            S((slots, KVH * HD), bf16),
            S((slots, KVH * HD), bf16),
            S((slots, H * HD), bf16),
            S((8, dim), f32),
            S((3, slots, HD), f32),
        ),
        in_specs=[VMEM] * 7 + [ANY] * 7,
        out_specs=(ANY,) * 6 + (VMEM,) * 9,
        scratch_shapes=[
            pltpu.VMEM((rows, wide), bf16),
            pltpu.VMEM((LINE, rows, 2 * width), bf16),
            pltpu.VMEM((slots, dim), bf16),
            pltpu.VMEM((slots, dim), bf16),
            pltpu.VMEM((RING, rows, qkv_width), bf16),
            pltpu.VMEM((n, rows, wo.shape[1]), bf16),
            pltpu.VMEM((LINE, RING, 16, 128), bf16),
            pltpu.VMEM((16, 128), f32),
            pltpu.VMEM((LINE, slots, dim), bf16),
            pltpu.VMEM((LINE * slots, 2 * width), f32),
            pltpu.VMEM((2, RING, rows, 2 * width), bf16),
            pltpu.VMEM((LINE * slots, width), bf16),
            DMA((14,)),
            DMA((n,)),
            DMA((n,)),
            DMA((n,)),
            DMA((n,)),
            DMA((n,)),
            DMA((n,)),
            DMA((LINE, 2)),
            DMA((LINE, 2)),
            DMA((pieces, RING)),
            DMA((pieces, RING)),
            DMA((pieces, RING)),
            DMA((pieces, RING)),
            DMA((3, LINE)),
            DMA((3, LINE)),
            DMA((3, LINE)),
            DMA,
            DMA((LINE,)),
            DMA,
            DMA((width // 256, 3)),
        ],
        compiler_params=pltpu.CompilerParams(
            collective_id=0, has_side_effects=True, vmem_limit_bytes=64000 * 1024
        ),
        name="forward",
    )(
        hidden_in, seq_lengths[None, :], seq_device[None, :], *[g[None, :] for g in gains],
        out_grad, wq, wk, wv, wo, gate, up,
    )


def backward_kernel(
    gu_ref, down_ref, tok_ref, cot_ref, hid_ref, pre_ref, w_ref, middle_ref, normed_ref, raw_ref,
    q_ref, k_ref, v_ref, mixed_ref, x_ref, gains_ref, rope_ref,
    x_out, small_out, y_out, d_out, a_out, ex_land, gu_out, c_land, s_land, f_land, l_land, wd_ref,
    gu_all, gd_all, gu_sib, gd_sib, gu_sec, gd_sec, gu_fst, gd_fst, t_own, t_land,
    dmid, dqkv, s_sum, s_got, s_line,
    c_send, c_recv, s_send, s_recv, f_send, f_recv, down_s, down_r, up_s, up_r, load, stream, back,
    ac_send, ac_recv, as_send, as_recv, af_send, af_recv, ad_send, ad_recv, au_send, au_recv,
    ex_s, ex_r, small_s, small_r, w_first, w_second, w_sib, w_recv, units_in,
    a_load,
):
    me, z, first, second, sibling = where_am_i()
    greet(line_peers(me) + [first, second, sibling])
    core = me % 2
    col, fcol, scol = me % RING, first % RING, second % RING
    sfcol = (second + first - me) % RING
    mine, fst, sec = (me % RING) // 2, (first % RING) // 2, (second % RING) // 2
    far = ((second + first - me) % RING) // 2
    half = gd_fst.shape[0] // 2
    last = LINE - 1
    tokens, dim = tok_ref.shape
    part = hid_ref.shape[1]
    quad_rows = part // LINE
    shard_rows = dim // (RING * LINE)
    piece_cols = gu_all.shape[3]
    kv0 = H * HD
    v0 = kv0 + KVH * HD
    qkv_width = v0 + KVH * HD
    MLP_GU, MLP_D = (0, 0, LINE), (1, LINE, LINE + 2)

    def block(gu, d, piece, group):
        if group == 0:
            return gu.at[piece]
        return d.at[tile(piece - LINE, half)]

    def own_block(quad, piece, group, theirs=False):
        shard = 2 * quad + (1 - core if theirs else core)
        if group == 0:
            return gu_all.at[piece, shard]
        return block(None, gd_all.at[shard], piece, group)

    def each(span, body):
        group, lo, hi = span

        def step(piece, carry):
            body(piece, group)
            return carry

        lax.fori_loop(lo, hi, step, 0)

    def to_sibling(quad, piece, group):
        return remote(
            own_block(quad, piece, group, theirs=True),
            block(gu_sib.at[quad], gd_sib.at[quad], piece, group),
            c_send.at[quad, piece],
            c_recv.at[quad, piece],
            sibling,
        )

    def to_second(quad, slot, piece, group):
        return remote(
            own_block(quad, piece, group),
            block(gu_sec.at[slot], gd_sec.at[slot], piece, group),
            s_send.at[slot, piece],
            s_recv.at[slot, piece],
            second,
        )

    def to_first(piece, group):
        return remote(
            own_block(fst, piece, group),
            block(gu_fst, gd_fst, piece, group),
            f_send.at[piece],
            f_recv.at[piece],
            first,
        )

    def pass_on(piece, group):
        for quad, slot in ((far, 1), (sec, 0)):
            to_sibling(quad, piece, group).wait_recv()
            own = own_block(quad, piece, group)
            add_rows(own, own, block(gu_sib.at[quad], gd_sib.at[quad], piece, group))
            to_second(quad, slot, piece, group).start()

    def narrow(piece, group):
        to_sibling(fst, piece, group).wait_recv()
        to_second(far, 1, piece, group).wait_recv()
        own = own_block(fst, piece, group)
        add_rows(
            own,
            own,
            block(gu_sib.at[fst], gd_sib.at[fst], piece, group),
            block(gu_sec.at[1], gd_sec.at[1], piece, group),
        )
        to_first(piece, group).start()

    def finish(piece, group, out=None):
        to_sibling(mine, piece, group).wait_recv()
        to_second(sec, 0, piece, group).wait_recv()
        to_first(piece, group).wait_recv()
        own = own_block(mine, piece, group)
        add_rows(
            own if group == 0 else block(None, out, piece, group),
            own,
            block(gu_sib.at[mine], gd_sib.at[mine], piece, group),
            block(gu_sec.at[0], gd_sec.at[0], piece, group),
            block(gu_fst, gd_fst, piece, group),
        )

    def drain_sibling(piece, group):
        for quad in (far, fst, sec, mine):
            to_sibling(quad, piece, group).wait_send()

    def drain(piece, group):
        to_second(far, 1, piece, group).wait_send()
        to_second(sec, 0, piece, group).wait_send()
        to_first(piece, group).wait_send()

    def send_line(src, which, t, up):
        return remote(
            src,
            t_land.at[which, t + 1 if up else t],
            (up_s if up else down_s).at[which, t],
            (up_r if up else down_r).at[which, t],
            me + RING if up else me - RING,
        )

    def line_own(which):
        for k in range(last):

            @pl.when(z == last)
            def _(k=k):
                send_line(t_own.at[which, k], which, k, False).start()

            @pl.when(z == 0)
            def _(k=k):
                send_line(t_own.at[which, last - k], which, last - k, True).start()

    def relay_at(which, at, t, up):
        @pl.when(z == at)
        def _():
            landing = t_land.at[which, t + 1 if up else t]
            send_line(landing, which, t, up).wait_recv()
            add_rows(landing, landing, t_own.at[which, t])
            send_line(landing, which, t, up).start()

    def relay(which, step):
        if step < 2:
            relay_at(which, 2, step, False)
            relay_at(which, 1, last - step, True)
        else:
            relay_at(which, 1, 0, False)
            relay_at(which, 2, last, True)

    def line_sum(which, out):
        own, above, below = t_own.at[which, z], t_land.at[which, z], t_land.at[which, z + 1]

        @pl.when(z < last)
        def _():
            send_line(above, which, z, False).wait_recv()

        @pl.when(z > 0)
        def _():
            send_line(below, which, z, True).wait_recv()

        @pl.when(z == 0)
        def _():
            add_rows(out, own, above)

        @pl.when(z == last)
        def _():
            add_rows(out, own, below)

        @pl.when((z > 0) & (z < last))
        def _():
            add_rows(out, own, above, below)

    def w_spot(shard, piece):
        return wd_ref.at[pl.ds(pl.multiple_of(shard * 2 * half + piece * half, half), half)]

    def w_send(src, shard, piece, sems, device):
        return remote(
            src, w_spot(shard, piece), sems.at[shard, piece], w_recv.at[shard, piece], device
        )

    def w_arrived(shard, piece):
        w_send(w_spot(shard, piece), shard, piece, w_sib, sibling).wait_recv()

    def w_other(shard, onward):
        for piece in range(2):
            w_arrived(shard, piece)
            src = w_spot(shard, piece)
            if onward:
                w_send(src, shard, piece, w_second, second).start()
            w_send(src, shard, piece, w_sib, sibling).start()

    for piece in range(2):
        src = down_ref.at[pl.ds(piece * half, half)]
        w_send(src, col, piece, w_first, first).start()
        w_send(src, col, piece, w_second, second).start()
        w_send(src, col, piece, w_sib, sibling).start()

    def mlp(tok, cot, hid, dgu, down_own):
        ins = [
            pltpu.make_async_copy(hid_ref, hid, load.at[0]),
            pltpu.make_async_copy(cot_ref, cot, load.at[1]),
            pltpu.make_async_copy(down_ref, down_own, load.at[2]),
            pltpu.make_async_copy(tok_ref, tok, load.at[3]),
        ]
        for copy in ins:
            copy.start()
        wide = 256
        for copy in ins[:2]:
            copy.wait()

        previous = None
        for quad in (far, sec, fst, mine):

            def columns(n, carry, quad=quad):
                at = tile(n, 512)
                both = dot_tn(hid[:, tile(quad, quad_rows)], cot[:, at]).astype(bf16)
                gd_all[2 * quad, :, at] = both[: quad_rows // 2]
                gd_all[2 * quad + 1, :, at] = both[quad_rows // 2 :]
                return carry

            lax.fori_loop(0, dim // 512, columns, 0)
            if previous is not None:
                each(MLP_D, lambda piece, group, q=previous: to_sibling(q, piece, group).start())
            previous = quad
        ins[2].wait()
        down_back = pltpu.make_async_copy(
            down_own, wd_ref.at[tile(col, 2 * half)], load.at[4]
        )
        down_back.start()
        each(MLP_D, lambda piece, group, q=previous: to_sibling(q, piece, group).start())
        w_other(fcol, True)
        w_other(scol, False)
        each(MLP_D, pass_on)
        w_other(sfcol, False)
        for piece in range(2):
            for k in range(RING // 2):
                w_arrived(2 * k + sibling % 2, piece)
        down_back.wait()

        def units(gate_t, up_t, down_w, dhid_t):
            def fetch(i, slot):
                up_at = pl.ds(pl.multiple_of(part + i * wide, wide), wide)
                return (
                    pltpu.make_async_copy(
                        pre_ref.at[:, tile(i, wide)], gate_t.at[slot], units_in.at[slot, 0]
                    ),
                    pltpu.make_async_copy(pre_ref.at[:, up_at], up_t.at[slot], units_in.at[slot, 1]),
                    pltpu.make_async_copy(
                        wd_ref.at[tile(i, wide)], down_w.at[slot], units_in.at[slot, 2]
                    ),
                )

            def body(i, slot):
                dhid_t[...] = dot_nt(cot[...], down_w[slot])

                def act(r, carry):
                    at = tile(r, 32)
                    gate, up, dhid = gate_t[slot, at], up_t[slot, at], dhid_t[at]
                    sig = jax.nn.sigmoid(gate)
                    dgate = dhid * up * (sig * (1.0 + gate * (1.0 - sig)))
                    dgu[at, tile(i, wide)] = dgate.astype(bf16)
                    up_at = pl.ds(pl.multiple_of(part + i * wide, wide), wide)
                    dgu[at, up_at] = (dhid * (gate * sig)).astype(bf16)
                    return carry

                lax.fori_loop(0, tokens // 32, act, 0)

            streamed(part // wide, fetch, body)

        pl.run_scoped(
            units,
            pltpu.VMEM((2, tokens, wide), f32),
            pltpu.VMEM((2, tokens, wide), f32),
            pltpu.VMEM((2, wide, dim), bf16),
            pltpu.VMEM((tokens, wide), f32),
        )

        def back_through(rows_w):
            def fetch(i, slot):
                return (
                    pltpu.make_async_copy(
                        gu_ref.at[tile(i, wide)], rows_w.at[slot], stream.at[slot]
                    ),
                )

            def body(i, slot):
                out = dot_nt(dgu[...], rows_w[slot]).astype(bf16)
                t_own[0, :, :, tile(i, wide)] = out.reshape(LINE, CAP, wide)

            streamed(dim // wide, fetch, body)

        ins[3].wait()
        pl.run_scoped(back_through, pltpu.VMEM((2, wide, 2 * part), bf16))

        rows = dim // LINE
        for piece in range(LINE):

            def columns(n, carry, piece=piece):
                at = tile(n, 512)
                grad = dot_tn(tok[:, pl.ds(piece * rows, rows)], dgu[:, at]).astype(bf16)
                gu_all[piece, :, :, at] = grad.reshape(RING, rows // RING, 512)
                return carry

            lax.fori_loop(0, 2 * part // 512, columns, 0)
            if piece == 0:
                line_own(0)
            else:
                pass_on(piece - 1, 0)
            for quad in (far, fst, sec, mine):
                to_sibling(quad, piece, 0).start()
        each(MLP_D, narrow)
        relay(0, 0)

        def out_through(cols_w):
            def fetch(i, slot):
                return (
                    pltpu.make_async_copy(
                        wd_ref.at[:, tile(i, wide)], cols_w.at[slot], stream.at[slot]
                    ),
                )

            def body(i, slot):
                out = jnp.dot(hid[...], cols_w[slot], preferred_element_type=f32).astype(bf16)
                t_own[1, :, :, tile(i, wide)] = out.reshape(LINE, CAP, wide)

            streamed(dim // wide, fetch, body)

        pass_on(LINE - 1, 0)
        pl.run_scoped(out_through, pltpu.VMEM((2, part, wide), bf16))

    pl.run_scoped(
        mlp,
        pltpu.VMEM((tokens, dim), bf16),
        pltpu.VMEM((tokens, dim), bf16),
        pltpu.VMEM((tokens, part), bf16),
        pltpu.VMEM((tokens, 2 * part), bf16),
        pltpu.VMEM((2 * half, dim), bf16),
    )
    for piece in range(2):
        src = down_ref.at[pl.ds(piece * half, half)]
        w_send(src, col, piece, w_first, first).wait_send()
        w_send(src, col, piece, w_second, second).wait_send()
        w_send(src, fcol, piece, w_second, second).wait_send()
        for base in (col, fcol, scol, sfcol):
            w_send(src, base, piece, w_sib, sibling).wait_send()

    def attention(dbr, mixed, normed, raw, q, k, v, cot, dsec, dmix, middle, w_rows):
        ins = [
            pltpu.make_async_copy(src, dst, load.at[i])
            for i, (src, dst) in enumerate(
                (
                    (middle_ref, middle),
                    (raw_ref.at[:, pl.ds(0, v0)], raw),
                    (q_ref, q),
                    (k_ref, k),
                    (v_ref, v),
                    (cot_ref.at[tile(z, CAP)], cot),
                    (mixed_ref, mixed),
                    (normed_ref, normed),
                )
            )
        ]
        for copy in ins:
            copy.start()
        relay(0, 1)
        narrow(0, 0)
        relay(0, 2)
        line_own(1)
        for copy in ins:
            copy.wait()
        line_sum(0, dsec)

        scale = rms_scale(middle[...])
        wide = 512

        def gather_mean(i, total):
            at = tile(i, wide)
            n = middle[:, at] * scale
            ds = dsec[:, at]
            s_sum[3, 0:1, at] = jnp.sum(n * ds, axis=0, keepdims=True)
            return total + lane_sum(n * ds * gains_ref[1:2, at])

        mean = lax.fori_loop(0, dim // wide, gather_mean, jnp.zeros((CAP, 1), f32)) / dim

        def spread_mean(i, carry):
            at = tile(i, wide)
            n = middle[:, at] * scale
            e = dsec[:, at] * gains_ref[1:2, at]
            d_middle = cot[:, at].astype(f32) + scale * (e - n * mean)
            dmid[:, at] = d_middle
            dbr[:, at] = d_middle.astype(bf16)
            return carry

        lax.fori_loop(0, dim // wide, spread_mean, 0)
        shards = w_rows.shape[1]
        rows = shards * w_rows.shape[2]

        def w_fetch(i, slot):
            return (
                pltpu.make_async_copy(
                    w_ref.at[tile(i, shards), :, pl.ds(qkv_width, dim)],
                    w_rows.at[slot],
                    stream.at[slot],
                ),
            )

        def through_out(i, slot):
            dmix[:, tile(i, rows)] = dot_nt(dbr[...], w_rows[slot].reshape(rows, dim)).astype(bf16)

        streamed(dim // rows, w_fetch, through_out)
        narrow(1, 0)
        relay(1, 0)

        cosine, sine, bias = rope_ref[0], rope_ref[1], rope_ref[2]
        s_sum[3, 1:8] = jnp.zeros((7, dim), f32)

        def unrope(raw_v, d_rot, row):
            d_hat = d_rot * cosine - half_turn(d_rot * sine)
            r = rms_scale(raw_v)
            n = raw_v * r
            s_sum[3, row : row + 1, 0:HD] += jnp.sum(n * d_hat, axis=0, keepdims=True)
            e = d_hat * gains_ref[row + 1 : row + 2, 0:HD]
            return (r * (e - n * jnp.mean(n * e, axis=-1, keepdims=True))).astype(bf16)

        def head(g, carry):
            at = tile(g, HD)
            key, value = k[:, at], v[:, at]
            d_key = jnp.zeros((CAP, HD), f32)
            d_value = jnp.zeros((CAP, HD), f32)
            for i in range(2):
                cols = tile(2 * g + i, HD)
                query, d_mix = q[:, cols], dmix[:, cols]
                logits = dot_nt(query, key) * (HD ** (-0.5)) + bias
                exponent = jnp.exp(logits - jnp.max(logits, axis=-1, keepdims=True))
                probs = exponent / lane_sum(exponent)
                d_probs = dot_nt(d_mix, value)
                d_logits = probs * (d_probs - lane_sum(probs * d_probs))
                d_scores = (d_logits * (HD ** (-0.5))).astype(bf16)
                d_value = d_value + dot_tn(probs.astype(bf16), d_mix)
                d_key = d_key + dot_tn(d_scores, query)
                d_query = jnp.dot(d_scores, key, preferred_element_type=f32)
                dqkv[:, cols] = unrope(raw[:, cols], d_query, 1)
            cols = pl.ds(pl.multiple_of(kv0 + g * HD, HD), HD)
            dqkv[:, cols] = unrope(raw[:, cols], d_key, 2)
            dqkv[:, pl.ds(pl.multiple_of(v0 + g * HD, HD), HD)] = d_value.astype(bf16)
            return carry

        lax.fori_loop(0, KVH // 2, head, 0, unroll=2)
        narrow(2, 0)
        lax.fori_loop(KVH // 2, KVH, head, 0, unroll=2)

    order = (
        last * (1 - z // 2),
        2 - 2 * z + 5 * (z // 2),
        1 + z % 2,
        z,
    )

    def a_own(t, quad, h):
        return gu_all.at[t, 2 * quad + (core if h else 1 - core)]

    def sums(dbr, mixed, normed, cbuf, stage):
        span = dim // LINE

        def a_sibling(t, quad, h, slot):
            return remote(
                cbuf.at[slot, quad],
                c_land.at[t, h, quad],
                ac_send.at[slot, quad],
                ac_recv.at[t, h, quad],
                sibling,
            )

        def a_second(t, quad, h, slot):
            return remote(
                a_own(t, quad, h),
                s_land.at[slot, t, h],
                as_send.at[slot, t, h],
                as_recv.at[slot, t, h],
                second,
            )

        def a_first(t, h):
            return remote(
                a_own(t, fst, h), f_land.at[t, h], af_send.at[t, h], af_recv.at[t, h], first
            )

        def a_line(t, h, upward):
            src = a_own(t, mine, h)
            if upward:
                return remote(
                    src, l_land.at[1, t, h], au_send.at[t, h], au_recv.at[t, h], me + RING
                )
            return remote(src, l_land.at[0, t, h], ad_send.at[t, h], ad_recv.at[t, h], me - RING)

        def staged(lo, *landed):
            return [
                pltpu.make_async_copy(src, stage.at[lo + i], a_load.at[lo + i])
                for i, src in enumerate(landed)
            ]

        def begin(copies):
            for copy in copies:
                copy.start()

        def add_staged(own, copies, lo):
            for copy in copies:
                copy.wait()
            add_rows(own, own, *[stage.at[lo + i] for i in range(len(copies))])

        def compute(k):
            h, t, slot = k // LINE, order[k % LINE], k % 2
            if k > 1:
                for quad in (far, fst, sec, mine):
                    a_sibling(order[(k - 2) % LINE], quad, (k - 2) // LINE, slot).wait_send()
            col0 = v0 if h else 0
            own_core = core if h else 1 - core

            def columns(n, carry, left, right, at):
                grad = dot_tn(left[:, tile(t, span)], right).astype(bf16)
                grad = grad.reshape(RING // 2, 2, shard_rows, 512)
                ours = jnp.where(core == 0, grad[:, 0], grad[:, 1])
                theirs = jnp.where(core == 0, grad[:, 1], grad[:, 0])
                for quad in range(RING // 2):
                    gu_all[t, 2 * quad + own_core, :, at] = ours[quad]
                cbuf[slot, :, :, at] = theirs
                return carry

            def from_qkv(n, carry):
                at = tile(n, 512)
                right = dqkv[:, pl.ds(pl.multiple_of(col0 + n * 512, 512), 512)]
                return columns(n, carry, normed, right, at)

            def from_out(n, carry):
                at = pl.ds(pl.multiple_of(qkv_width - v0 + n * 512, 512), 512)
                return columns(n, carry, mixed, dbr[:, tile(n, 512)], at)

            if h == 0:
                lax.fori_loop(0, v0 // 512, from_qkv, 0)
            else:
                lax.fori_loop(0, (qkv_width - v0) // 512, from_qkv, 0)
                lax.fori_loop(0, dim // 512, from_out, 0)

        def share(k):
            h, t, slot = k // LINE, order[k % LINE], k % 2
            for quad in (far, fst, sec, mine):
                a_sibling(t, quad, h, slot).start()

        def spread_in(k):
            t, h = order[k % LINE], k // LINE
            return staged(0, c_land.at[t, h, far], c_land.at[t, h, sec])

        def spread_begin(k):
            h, t, slot = k // LINE, order[k % LINE], k % 2
            for quad in (far, sec):
                a_sibling(t, quad, h, slot).wait_recv()
            begin(spread_in(k))

        def spread(k):
            h, t = k // LINE, order[k % LINE]
            copies = spread_in(k)
            for i, (quad, place) in enumerate(((far, 1), (sec, 0))):
                add_staged(a_own(t, quad, h), copies[i : i + 1], i)
                a_second(t, quad, h, place).start()

        def inward_in(k):
            t, h = order[k % LINE], k // LINE
            return staged(2, c_land.at[t, h, fst], s_land.at[1, t, h])

        def inward_begin(k):
            h, t, slot = k // LINE, order[k % LINE], k % 2
            a_sibling(t, fst, h, slot).wait_recv()
            a_second(t, far, h, 1).wait_recv()
            begin(inward_in(k))

        def inward(k):
            h, t = k // LINE, order[k % LINE]
            add_staged(a_own(t, fst, h), inward_in(k), 2)
            a_first(t, h).start()

        def collect_in(k):
            t, h = order[k % LINE], k // LINE
            return staged(4, c_land.at[t, h, mine], s_land.at[0, t, h], f_land.at[t, h])

        def collect_begin(k):
            h, t, slot = k // LINE, order[k % LINE], k % 2
            a_sibling(t, mine, h, slot).wait_recv()
            a_second(t, sec, h, 0).wait_recv()
            a_first(t, h).wait_recv()
            begin(collect_in(k))

        def collect(k):
            h, t = k // LINE, order[k % LINE]
            add_staged(a_own(t, mine, h), collect_in(k), 4)

            @pl.when((t < z) & (z == last))
            def _():
                a_line(t, h, False).start()

            @pl.when((t > z) & (z == 0))
            def _():
                a_line(t, h, True).start()

        def onward(k):
            h, t = k // LINE, order[k % LINE]

            @pl.when((t < z) & (z < last))
            def _():
                a_line(t, h, False).wait_recv()
                copies = staged(7, l_land.at[0, t, h])
                begin(copies)
                add_staged(a_own(t, mine, h), copies, 7)
                a_line(t, h, False).start()

            @pl.when((t > z) & (z > 0))
            def _():
                a_line(t, h, True).wait_recv()
                copies = staged(7, l_land.at[1, t, h])
                begin(copies)
                add_staged(a_own(t, mine, h), copies, 7)
                a_line(t, h, True).start()

        def exchange(k):
            peer_z = lax.rem(z + k, LINE)
            return remote(
                gu_out.at[peer_z], ex_land.at[z], ex_s.at[k], ex_r.at[k], me % RING + RING * peer_z
            )

        def small(step, src, dst, device):
            return remote(src, dst, small_s.at[step], small_r.at[step], device)

        def first_norm(w_rows):
            shards = w_rows.shape[1]
            wide = 512
            x_scale = rms_scale(x_ref[...].astype(f32))
            w_tile = shards * w_rows.shape[2]

            def w_fetch(i, slot):
                return (
                    pltpu.make_async_copy(
                        w_ref.at[tile(i, shards), :, pl.ds(0, qkv_width)],
                        w_rows.at[slot],
                        stream.at[slot],
                    ),
                )

            def through(i, slot):
                x_out[:, tile(i, w_tile)] = dot_nt(dqkv[...], w_rows[slot].reshape(w_tile, qkv_width))

            streamed(dim // w_tile, w_fetch, through)

            def gather_mean(i, total):
                at = tile(i, wide)
                n = x_ref[:, at].astype(f32) * x_scale
                s_sum[3, 3:4, at] = jnp.sum(n * x_out[:, at], axis=0, keepdims=True)
                return total + lane_sum(n * x_out[:, at] * gains_ref[0:1, at])

            mean = lax.fori_loop(0, dim // wide, gather_mean, jnp.zeros((CAP, 1), f32)) / dim

            def spread_mean(i, carry):
                at = tile(i, wide)
                n = x_ref[:, at].astype(f32) * x_scale
                e = x_out[:, at] * gains_ref[0:1, at]
                x_out[:, at] = dmid[:, at] + x_scale * (e - n * mean)
                return carry

            lax.fori_loop(0, dim // wide, spread_mean, 0)

        def mlp_results(d_tmp, middle, y, y_half):
            middle_in = pltpu.make_async_copy(middle_ref, middle, load.at[0])
            middle_in.start()
            each(MLP_D, lambda piece, group: finish(piece, group, d_tmp))
            d_back = pltpu.make_async_copy(d_tmp, d_out, load.at[1])
            d_back.start()
            line_sum(1, y)
            middle_in.wait()

            def last_add(i, carry):
                at = tile(i, 512)
                y_half[:, at] = (middle[:, at] + y[:, at]).astype(bf16)
                return carry

            lax.fori_loop(0, dim // 512, last_add, 0)
            y_back = pltpu.make_async_copy(y_half, y_out, load.at[2])
            y_back.start()
            each(MLP_D, drain_sibling)
            each(MLP_D, drain)
            d_back.wait()
            y_back.wait()

        small_c = small(0, s_sum.at[3], s_got.at[0], sibling)
        each(MLP_GU, drain_sibling)
        compute(0)
        share(0)
        narrow(3, 0)
        compute(1)
        share(1)
        spread_begin(0)
        compute(2)
        share(2)
        spread(0)
        spread_begin(1)
        relay(1, 1)
        compute(3)
        share(3)
        spread(1)
        spread_begin(2)
        inward_begin(0)
        spread(2)
        spread_begin(3)
        inward(0)
        each(MLP_GU, finish)
        gu_back = pltpu.make_async_copy(gu_all.at[:, 2 * mine + core], gu_out, back.at[0])
        gu_back.start()
        ex_in = pltpu.make_async_copy(gu_all.at[z, 2 * mine + core], ex_land.at[z], back.at[1])
        ex_in.start()
        spread(3)
        each(MLP_GU, drain)
        gu_back.wait()
        exchange(2).start()
        exchange(1).start()
        ex_in.wait()
        compute(4)
        share(4)
        pl.run_scoped(first_norm, pltpu.VMEM((2, 4, shard_rows, qkv_width), bf16))
        small_c.start()
        inward_begin(1)
        compute(5)
        share(5)
        inward(1)
        small_c.wait()
        s_sum[0] = s_sum[3] + s_got[0]
        small_f = small(1, s_sum.at[0], s_got.at[1], first)
        small_f.start()
        spread_begin(4)
        relay(1, 2)
        compute(6)
        share(6)
        spread(4)
        spread_begin(5)
        inward_begin(2)
        compute(7)
        share(7)
        inward(2)
        spread(5)
        spread_begin(6)
        small_f.wait()
        s_sum[1] = s_sum[0] + s_got[1]
        small_s2 = small(2, s_sum.at[1], s_got.at[2], second)
        small_s2.start()
        spread(6)
        spread_begin(7)
        collect_begin(0)
        spread(7)
        collect(0)
        collect_begin(1)
        inward_begin(3)
        collect(1)
        inward(3)
        collect_begin(2)
        collect(2)
        onward(0)
        onward(2)
        collect_begin(3)
        inward_begin(4)
        collect(3)
        inward(4)
        exchange(3).start()
        onward(1)
        pl.run_scoped(
            mlp_results,
            pltpu.VMEM(gd_fst.shape, f32),
            pltpu.VMEM((CAP, dim), f32),
            pltpu.VMEM((CAP, dim), f32),
            pltpu.VMEM((CAP, dim), bf16),
        )
        inward_begin(5)
        collect_begin(4)
        inward(5)
        collect(4)
        inward_begin(6)
        collect_begin(5)
        inward(6)
        collect(5)
        onward(4)
        small_s2.wait()
        s_sum[2] = s_sum[1] + s_got[2]
        small_line = [
            small(2 + k, s_sum.at[2], s_line.at[k], me % RING + RING * lax.rem(z + k, LINE))
            for k in range(1, LINE)
        ]
        for copy in small_line:
            copy.start()
        onward(5)
        inward_begin(7)
        collect_begin(6)
        inward(7)
        collect(6)
        onward(6)
        collect_begin(7)
        collect(7)
        for copy in small_line:
            copy.wait()
        small_out[...] = (s_sum[2] + s_line[2]) + (s_line[1] + s_line[3])
        for k in (6, 7):
            for quad in (far, fst, sec, mine):
                a_sibling(order[k % LINE], quad, k // LINE, k % 2).wait_send()
        for k in range(1, LINE):
            exchange(k).wait_send()
            src_z = lax.rem(z + LINE - k, LINE)
            landed = ex_land.at[src_z]
            remote(landed, landed, ex_s.at[k], ex_r.at[k], sibling).wait_recv()
        for t in range(LINE):
            for h in range(2):
                a_second(t, far, h, 1).wait_send()
                a_second(t, sec, h, 0).wait_send()
                a_first(t, h).wait_send()

                @pl.when(t < z)
                def _(t=t, h=h):
                    a_line(t, h, False).wait_send()

                @pl.when(t > z)
                def _(t=t, h=h):
                    a_line(t, h, True).wait_send()

    slots = CAP
    kv = KVH * HD
    rows = gu_all.shape[2]

    def both(dbr, mixed, normed):
        pl.run_scoped(
            lambda *refs: attention(dbr, mixed, normed, *refs),
            pltpu.VMEM((slots, v0), f32),
            pltpu.VMEM((slots, dim), bf16),
            pltpu.VMEM((slots, kv), bf16),
            pltpu.VMEM((slots, kv), bf16),
            pltpu.VMEM((slots, dim), bf16),
            pltpu.VMEM((slots, dim), f32),
            pltpu.VMEM((slots, dim), bf16),
            pltpu.VMEM((slots, dim), f32),
            pltpu.VMEM((2, 4, rows, dim), bf16),
        )
        pl.run_scoped(
            lambda *refs: sums(dbr, mixed, normed, *refs),
            pltpu.VMEM((2, RING // 2, rows, piece_cols), bf16),
            pltpu.VMEM((8, rows, piece_cols), bf16),
        )

    pl.run_scoped(
        both,
        pltpu.VMEM((slots, dim), bf16),
        pltpu.VMEM((slots, dim), bf16),
        pltpu.VMEM((slots, dim), bf16),
    )

    def a_landed(t, h, upward):
        landing = l_land.at[1 if upward else 0, t, h]
        sems = (au_send, au_recv) if upward else (ad_send, ad_recv)
        return remote(landing, landing, sems[0].at[t, h], sems[1].at[t, h], sibling)

    def results(a_tmp, stage):
        for h in range(2):

            @pl.when(z < last)
            def _(h=h):
                a_landed(z, h, False).wait_recv()

            @pl.when(z > 0)
            def _(h=h):
                a_landed(z, h, True).wait_recv()

        def total(*sides):
            for h in range(2):
                copies = [
                    pltpu.make_async_copy(l_land.at[side, z, h], stage.at[i], stream.at[i])
                    for i, side in enumerate(sides)
                ]
                for copy in copies:
                    copy.start()
                for copy in copies:
                    copy.wait()
                add_rows(
                    a_tmp.at[:, pl.ds(h * piece_cols, piece_cols)],
                    a_own(z, mine, h),
                    *[stage.at[i] for i in range(len(sides))],
                )

        @pl.when(z == 0)
        def _():
            total(0)

        @pl.when(z == last)
        def _():
            total(1)

        @pl.when((z > 0) & (z < last))
        def _():
            total(0, 1)

        a_back = pltpu.make_async_copy(a_tmp, a_out, load.at[3])
        a_back.start()
        a_back.wait()

    pl.run_scoped(
        results,
        pltpu.VMEM((rows, 2 * piece_cols), f32),
        pltpu.VMEM((2, rows, piece_cols), bf16),
    )
    for which in range(2):
        for k in range(LINE):

            @pl.when((z > 0) & (k < z))
            def _(which=which, k=k):
                send_line(t_own.at[which, k], which, k, False).wait_send()

            @pl.when((z < last) & (k > z))
            def _(which=which, k=k):
                send_line(t_own.at[which, k], which, k, True).wait_send()


def backward(gu, down, tok, cot, hid, pre, w, middle, normed, raw, q, k, v, mixed, x, gains, rope):
    dim = tok.shape[1]
    rows = w.shape[1]
    drows = down.shape[0]
    cols = gu.shape[1]
    quads = RING // 2
    pieces = LINE + 2
    qkv = raw.shape[1]
    S = jax.ShapeDtypeStruct
    return pl.pallas_call(
        backward_kernel,
        out_shape=(
            S((CAP, dim), f32),
            S((8, dim), f32),
            S((CAP, dim), bf16),
            S((drows, dim), f32),
            S((rows, qkv + dim), f32),
            S((LINE, rows, cols), bf16),
            S((LINE, rows, cols), bf16),
            S((LINE, 2, quads, rows, cols), bf16),
            S((2, LINE, 2, rows, cols), bf16),
            S((LINE, 2, rows, cols), bf16),
            S((2, LINE, 2, rows, cols), bf16),
            S((RING * drows, dim), bf16),
        ),
        in_specs=[ANY] * 14 + [VMEM] * 3,
        out_specs=(VMEM,) * 2 + (ANY,) * 10,
        scratch_shapes=[
            pltpu.VMEM((LINE, RING, rows, cols), bf16),
            pltpu.VMEM((RING, drows, dim), bf16),
            pltpu.VMEM((quads, LINE, rows, cols), bf16),
            pltpu.VMEM((quads, drows, dim), bf16),
            pltpu.VMEM((2, LINE, rows, cols), bf16),
            pltpu.VMEM((2, drows, dim), bf16),
            pltpu.VMEM((LINE, rows, cols), bf16),
            pltpu.VMEM((drows, dim), bf16),
            pltpu.VMEM((2, LINE, CAP, dim), bf16),
            pltpu.VMEM((2, LINE + 1, CAP, dim), bf16),
            pltpu.VMEM((CAP, dim), f32),
            pltpu.VMEM((CAP, qkv), bf16),
            pltpu.VMEM((4, 8, dim), f32),
            pltpu.VMEM((3, 8, dim), f32),
            pltpu.VMEM((LINE, 8, dim), f32),
            DMA((quads, pieces)),
            DMA((quads, pieces)),
            DMA((2, pieces)),
            DMA((2, pieces)),
            DMA((pieces,)),
            DMA((pieces,)),
            DMA((2, LINE)),
            DMA((2, LINE)),
            DMA((2, LINE)),
            DMA((2, LINE)),
            DMA((8,)),
            DMA((3,)),
            DMA((2,)),
            DMA((2, quads)),
            DMA((LINE, 2, quads)),
            DMA((2, LINE, 2)),
            DMA((2, LINE, 2)),
            DMA((LINE, 2)),
            DMA((LINE, 2)),
            DMA((LINE, 2)),
            DMA((LINE, 2)),
            DMA((LINE, 2)),
            DMA((LINE, 2)),
            DMA((LINE,)),
            DMA((LINE,)),
            DMA((2 + LINE,)),
            DMA((2 + LINE,)),
            DMA((RING, 2)),
            DMA((RING, 2)),
            DMA((RING, 2)),
            DMA((RING, 2)),
            DMA((2, 3)),
            DMA((8,)),
        ],
        compiler_params=pltpu.CompilerParams(
            collective_id=2, has_side_effects=True, vmem_limit_bytes=65400 * 1024
        ),
        name="backward",
    )(gu, down, tok, cot, hid, pre, w, middle, normed, raw, q, k, v, mixed, x, gains, rope)


def results_kernel(
    y_ref, x_ref, small_ref, d_ref, a_ref, ex_ref,
    y_out, x_out, q_out, k_out, v_out, o_out, gate_out, up_out, d_out, ga_out, gq_out, gk_out, gm_out,
    y_tmp, x_tmp, small, d_tmp, a_tmp, ex_tmp, gate_tmp, up_tmp, sem_in, sem_out,
):
    me = lax.axis_index("fsdp")
    width = ex_tmp.shape[2] // 2
    moves = ((small_ref, small), (ex_ref, ex_tmp), (a_ref, a_tmp), (d_ref, d_tmp), (x_ref, x_tmp), (y_ref, y_tmp))
    ins = [pltpu.make_async_copy(src, dst, sem_in.at[i]) for i, (src, dst) in enumerate(moves)]
    for copy in ins:
        copy.start()
    outs = []

    def leave(src, dst):
        copy = pltpu.make_async_copy(src, dst, sem_out.at[len(outs)])
        copy.start()
        outs.append(copy)

    ins[1].wait()
    for k in range(LINE):
        add_rows(gate_tmp.at[:, pl.ds(k * width, width)], ex_tmp.at[k, :, pl.ds(0, width)])
        add_rows(up_tmp.at[:, pl.ds(k * width, width)], ex_tmp.at[k, :, pl.ds(width, width)])
    leave(gate_tmp, gate_out)
    leave(up_tmp, up_out)
    ins[2].wait()
    lo = 0
    for out in (q_out, k_out, v_out, o_out):
        leave(a_tmp.at[:, pl.ds(lo, out.shape[1])], out)
        lo += out.shape[1]
    ins[3].wait()
    leave(d_tmp, d_out)
    ins[4].wait()
    leave(x_tmp, x_out)
    ins[5].wait()
    leave(y_tmp, y_out)
    ins[0].wait()
    for row, out in ((3, ga_out), (1, gq_out), (2, gk_out), (0, gm_out)):
        count = out.shape[1]
        value = jnp.zeros((1, 128), f32)
        for i in range(small.shape[1] // 128):
            held = small[row : row + 1, i * 128 : (i + 1) * 128]
            value = jnp.where((me * count) // 128 == i, held, value)
        value = pltpu.roll(value, (128 - (me * count) % 128) % 128, 1)
        out[...] = value[:, 0:count]
    for copy in outs:
        copy.wait()


def results(y, x, small, d, a, ex, widths, shares):
    rows = a.shape[0]
    wide = LINE * ex.shape[2] // 2
    S = jax.ShapeDtypeStruct
    return pl.pallas_call(
        results_kernel,
        out_shape=(
            S(y.shape, bf16),
            S(x.shape, f32),
            *[S((rows, w), f32) for w in widths],
            S((rows, wide), f32),
            S((rows, wide), f32),
            S(d.shape, f32),
            *[S((1, s), f32) for s in shares],
        ),
        in_specs=[ANY] * 6,
        out_specs=(ANY,) * 9 + (VMEM,) * 4,
        scratch_shapes=[
            pltpu.VMEM(y.shape, bf16),
            pltpu.VMEM(x.shape, f32),
            pltpu.VMEM(small.shape, f32),
            pltpu.VMEM(d.shape, f32),
            pltpu.VMEM(a.shape, f32),
            pltpu.VMEM(ex.shape, bf16),
            pltpu.VMEM((rows, wide), f32),
            pltpu.VMEM((rows, wide), f32),
            DMA((6,)),
            DMA((9,)),
        ],
        name="results",
    )(y, x, small, d, a, ex)


def layout(seq_lengths, seq_device, owner, slots):
    owned = seq_device == owner
    counts = jnp.where(owned, seq_lengths, 0)
    starts = jnp.cumsum(counts) - counts
    places = jnp.arange(slots, dtype=jnp.int32)
    inside = (
        owned[:, None]
        & (places[None, :] >= starts[:, None])
        & (places[None, :] < (starts + counts)[:, None])
    )
    labels = jnp.arange(seq_lengths.shape[0], dtype=jnp.int32)
    segment = jnp.sum(jnp.where(inside, labels[:, None] + 1, 0), axis=0) - 1
    position = jnp.sum(jnp.where(inside, places[None, :] - starts[:, None], 0), axis=0)
    return (segment, position)


def allowed_pairs(segment):
    places = jnp.arange(segment.shape[0], dtype=jnp.int32)
    earlier = places[None, :] < places[:, None]
    same_seq = (segment[:, None] == segment[None, :]) & (segment[:, None] >= 0)
    return (places[:, None] == places[None, :]) | earlier & same_seq


def rmsnorm(values, gain):
    return values * lax.rsqrt(jnp.mean(values * values, axis=-1, keepdims=True) + epsilon) * gain


def rotary(values, position):
    half_dim = values.shape[-1] // 2
    freqs = jnp.power(rope_base, -2.0 * jnp.arange(half_dim, dtype=jnp.float32) / values.shape[-1])
    angles = position.astype(jnp.float32)[:, None] * freqs[None, :]
    cosine = jnp.concatenate([jnp.cos(angles), jnp.cos(angles)], axis=-1)[:, None, :]
    sine = jnp.concatenate([jnp.sin(angles), jnp.sin(angles)], axis=-1)[:, None, :]
    rotated = jnp.concatenate([-values[..., half_dim:], values[..., :half_dim]], axis=-1)
    return values * cosine + rotated * sine


def matmul(left, right):
    return jnp.dot(left, right, preferred_element_type=jnp.float32)


def times_rows(left, right):
    return lax.dot_general(left, right, contract_rows, preferred_element_type=jnp.float32)


def times_cols(left, right):
    return lax.dot_general(left, right, contract_cols, preferred_element_type=jnp.float32)


def scatter_sum(partial):
    total = lax.psum_scatter(
        partial.astype(jnp.bfloat16), "fsdp", scatter_dimension=0, tiled=True
    )
    return total.astype(jnp.float32)


def plain(
    hidden_in,
    out_grad,
    seq_lengths,
    seq_device,
    attn_gain,
    q_gain,
    k_gain,
    w_query,
    w_key,
    w_value,
    w_out,
    mlp_gain,
    w_gate,
    w_up,
    w_down,
):
    slots = hidden_in.shape[0]
    groups = H // KVH
    score_scale = HD ** (-0.5)
    segment, position = layout(seq_lengths, seq_device, lax.axis_index("fsdp"), slots)
    allowed = allowed_pairs(segment)[None, None]

    def query_path(raw, gain):
        return rotary(rmsnorm(raw.reshape(slots, H, HD), gain), position)

    def key_path(raw, gain):
        return rotary(rmsnorm(raw.reshape(slots, KVH, HD), gain), position)

    def swiglu(gate_in, up_in):
        return jax.nn.silu(gate_in) * up_in

    attn_set = (
        lax.all_gather(attn_gain, "fsdp", axis=0, tiled=True),
        lax.all_gather(q_gain, "fsdp", axis=0, tiled=True),
        lax.all_gather(k_gain, "fsdp", axis=0, tiled=True),
        lax.all_gather(w_query, "fsdp", axis=0, tiled=True),
        lax.all_gather(w_key, "fsdp", axis=0, tiled=True),
        lax.all_gather(w_value, "fsdp", axis=0, tiled=True),
        lax.all_gather(w_out, "fsdp", axis=0, tiled=True),
    )
    gain_attn, gain_query, gain_key, query_w, key_w, value_w, out_w = attn_set
    inputs = hidden_in.astype(jnp.float32)
    normed = rmsnorm(inputs, gain_attn.astype(jnp.float32)).astype(jnp.bfloat16)
    query_raw = matmul(normed, query_w)
    key_raw = matmul(normed, key_w)
    value_raw = matmul(normed, value_w)
    queries = (
        query_path(query_raw, gain_query.astype(jnp.float32))
        .astype(jnp.bfloat16)
        .reshape(slots, KVH, groups, HD)
    )
    keys = key_path(key_raw, gain_key.astype(jnp.float32)).astype(jnp.bfloat16)
    values = value_raw.astype(jnp.bfloat16).reshape(slots, KVH, HD)

    def masked_logits():
        scores = (
            jnp.einsum("qgrd,kgd->grqk", queries, keys, preferred_element_type=jnp.float32)
            * score_scale
        )
        return jnp.where(allowed, scores, masked_score)

    logits = masked_logits()
    row_top = jnp.max(logits, axis=-1, keepdims=True)
    exponent = jnp.exp(logits - row_top)
    row_total = jnp.sum(exponent, axis=-1, keepdims=True)
    log_total = row_top + jnp.log(row_total)
    weights = (exponent / row_total).astype(jnp.bfloat16)
    mixed = jnp.einsum("grqk,kgd->qgrd", weights, values, preferred_element_type=jnp.float32)
    mixed = mixed.reshape(slots, H * HD).astype(jnp.bfloat16)
    middle = inputs + matmul(mixed, out_w)
    mlp_set = (
        lax.all_gather(mlp_gain, "fsdp", axis=0, tiled=True),
        lax.all_gather(w_gate, "fsdp", axis=0, tiled=True),
        lax.all_gather(w_up, "fsdp", axis=0, tiled=True),
        lax.all_gather(w_down, "fsdp", axis=0, tiled=True),
    )
    gain_mlp, gate_w, up_w, down_w = mlp_set
    second = rmsnorm(middle, gain_mlp.astype(jnp.float32)).astype(jnp.bfloat16)
    gate_out = matmul(second, gate_w)
    up_out = matmul(second, up_w)
    hidden = swiglu(gate_out, up_out).astype(jnp.bfloat16)
    hidden_out = (middle + matmul(hidden, down_w)).astype(jnp.bfloat16)
    gain_mlp, gate_w, up_w, down_w = (
        lax.all_gather(mlp_gain, "fsdp", axis=0, tiled=True),
        lax.all_gather(w_gate, "fsdp", axis=0, tiled=True),
        lax.all_gather(w_up, "fsdp", axis=0, tiled=True),
        lax.all_gather(w_down, "fsdp", axis=0, tiled=True),
    )
    grad_down = scatter_sum(times_rows(hidden, out_grad))
    d_hidden = times_cols(out_grad, down_w)
    unused_out, swiglu_pull = jax.vjp(swiglu, gate_out, up_out)
    d_gate, d_up = swiglu_pull(d_hidden)
    d_gate_up = jnp.concatenate([d_gate.astype(jnp.bfloat16), d_up.astype(jnp.bfloat16)], axis=1)
    grad_gate_up = scatter_sum(times_rows(second, d_gate_up))
    ff_width = gate_w.shape[1]
    d_second = times_cols(d_gate_up, jnp.concatenate([gate_w, up_w], axis=1))
    unused_norm, second_pull = jax.vjp(rmsnorm, middle, gain_mlp.astype(jnp.float32))
    d_middle_norm, grad_gain_mlp = second_pull(d_second)
    d_middle = out_grad.astype(jnp.float32) + d_middle_norm
    gain_attn, gain_query, gain_key, query_w, key_w, value_w, out_w = (
        lax.all_gather(attn_gain, "fsdp", axis=0, tiled=True),
        lax.all_gather(q_gain, "fsdp", axis=0, tiled=True),
        lax.all_gather(k_gain, "fsdp", axis=0, tiled=True),
        lax.all_gather(w_query, "fsdp", axis=0, tiled=True),
        lax.all_gather(w_key, "fsdp", axis=0, tiled=True),
        lax.all_gather(w_value, "fsdp", axis=0, tiled=True),
        lax.all_gather(w_out, "fsdp", axis=0, tiled=True),
    )
    d_branch = d_middle.astype(jnp.bfloat16)
    grad_out_w = scatter_sum(times_rows(mixed, d_branch))
    d_mixed = times_cols(d_branch, out_w).astype(jnp.bfloat16).reshape(slots, KVH, groups, HD)
    probs = jnp.exp(masked_logits() - log_total)
    weights = probs.astype(jnp.bfloat16)
    d_probs = jnp.einsum("qgrd,kgd->grqk", d_mixed, values, preferred_element_type=jnp.float32)
    d_logits = probs * (d_probs - jnp.sum(probs * d_probs, axis=-1, keepdims=True))
    d_scores = (d_logits * score_scale).astype(jnp.bfloat16)
    d_values = jnp.einsum("grqk,qgrd->kgd", weights, d_mixed, preferred_element_type=jnp.float32)
    d_values = d_values.astype(jnp.bfloat16).reshape(slots, KVH * HD)
    d_queries_rot = jnp.einsum(
        "grqk,kgd->qgrd", d_scores, keys, preferred_element_type=jnp.float32
    ).reshape(slots, H, HD)
    d_keys_rot = jnp.einsum("grqk,qgrd->kgd", d_scores, queries, preferred_element_type=jnp.float32)
    unused_query, query_pull = jax.vjp(query_path, query_raw, gain_query.astype(jnp.float32))
    d_query_raw, grad_gain_query = query_pull(d_queries_rot)
    unused_key, key_pull = jax.vjp(key_path, key_raw, gain_key.astype(jnp.float32))
    d_key_raw, grad_gain_key = key_pull(d_keys_rot)
    d_qkv = jnp.concatenate(
        [d_query_raw.astype(jnp.bfloat16), d_key_raw.astype(jnp.bfloat16), d_values], axis=1
    )
    grad_qkv = scatter_sum(times_rows(normed, d_qkv))
    d_normed = times_cols(d_qkv, jnp.concatenate([query_w, key_w, value_w], axis=1))
    unused_first, first_pull = jax.vjp(rmsnorm, inputs, gain_attn.astype(jnp.float32))
    d_input_norm, grad_gain_attn = first_pull(d_normed)
    input_grad = d_middle + d_input_norm
    gain_sums = (
        lax.psum_scatter(grad_gain_attn, "fsdp", scatter_dimension=0, tiled=True),
        lax.psum_scatter(grad_gain_query, "fsdp", scatter_dimension=0, tiled=True),
        lax.psum_scatter(grad_gain_key, "fsdp", scatter_dimension=0, tiled=True),
        lax.psum_scatter(grad_gain_mlp, "fsdp", scatter_dimension=0, tiled=True),
    )
    query_width = H * HD
    key_width = KVH * HD
    grad_query_w = grad_qkv[:, :query_width]
    grad_key_w = grad_qkv[:, query_width : query_width + key_width]
    grad_value_w = grad_qkv[:, query_width + key_width :]
    grad_gate = grad_gate_up[:, :ff_width]
    grad_up = grad_gate_up[:, ff_width:]
    return (
        hidden_out,
        input_grad,
        gain_sums[0],
        gain_sums[1],
        gain_sums[2],
        grad_query_w,
        grad_key_w,
        grad_value_w,
        grad_out_w,
        gain_sums[3],
        grad_gate,
        grad_up,
        grad_down,
    )


def layered(
    hidden_in,
    out_grad,
    seq_lengths,
    seq_device,
    attn_gain,
    q_gain,
    k_gain,
    w_query,
    w_key,
    w_value,
    w_out,
    mlp_gain,
    w_gate,
    w_up,
    w_down,
):
    (
        attn_w, gate_up_w, tokens, cotangent, hidden, gate_up,
        middle, normed, qkv_raw, queries, keys, values, mixed, gains, rope,
    ) = forward(
        hidden_in, out_grad, seq_lengths, seq_device, (attn_gain, mlp_gain, q_gain, k_gain),
        w_query, w_key, w_value, w_out, w_gate, w_up,
    )
    dim = hidden_in.shape[1]
    x, small, y, grad_down, attn_sums, exchanged, *unused = backward(
        gate_up_w.reshape(-1, gate_up_w.shape[-1]),
        w_down,
        tokens.reshape(-1, dim),
        cotangent.reshape(-1, dim),
        hidden, gate_up, attn_w, middle, normed, qkv_raw, queries, keys, values, mixed,
        hidden_in, gains, rope,
    )
    (
        hidden_out, input_grad, g_query, g_key, g_value, g_out, g_gate, g_up, g_down,
        g_attn_gain, g_q_gain, g_k_gain, g_mlp_gain,
    ) = results(
        y, x, small, grad_down, attn_sums, exchanged,
        [w.shape[1] for w in (w_query, w_key, w_value, w_out)],
        [g.shape[0] for g in (attn_gain, q_gain, k_gain, mlp_gain)],
    )
    return (
        hidden_out,
        input_grad,
        g_attn_gain[0],
        g_q_gain[0],
        g_k_gain[0],
        g_query,
        g_key,
        g_value,
        g_out,
        g_mlp_gain[0],
        g_gate,
        g_up,
        g_down,
    )


def solution(mesh):
    per_device = layered if mesh.shape["fsdp"] == RING * LINE else plain
    return jax.shard_map(
        per_device,
        mesh=mesh,
        in_specs=(
            P("fsdp", None),
            P("fsdp", None),
            P(),
            P(),
            P("fsdp"),
            P("fsdp"),
            P("fsdp"),
            P("fsdp", None),
            P("fsdp", None),
            P("fsdp", None),
            P("fsdp", None),
            P("fsdp"),
            P("fsdp", None),
            P("fsdp", None),
            P("fsdp", None),
        ),
        out_specs=(
            P("fsdp", None),
            P("fsdp", None),
            P("fsdp"),
            P("fsdp"),
            P("fsdp"),
            P("fsdp", None),
            P("fsdp", None),
            P("fsdp", None),
            P("fsdp", None),
            P("fsdp"),
            P("fsdp", None),
            P("fsdp", None),
            P("fsdp", None),
        ),
        check_vma=False,
    )
```

```python
import math

import jax
import jax.numpy as jnp
from jax import lax
from jax.experimental import pallas as pl
from jax.experimental.pallas import tpu as pltpu
from jax.sharding import PartitionSpec as P

H = 16
KVH = 8
HD = 128
CAP = 128
LINE = 4
RING = 8
MESH = pl.DeviceIdType.MESH
ANY = pl.BlockSpec(memory_space=pl.ANY)
VMEM = pl.BlockSpec(memory_space=pltpu.VMEM)
DMA = pltpu.SemaphoreType.DMA
bf16 = jnp.bfloat16
f32 = jnp.float32
epsilon = 1e-06
rope_base = 1000000.0
masked_score = -1e30
contract_rows = (((0,), (0,)), ((), ()))
contract_cols = (((1,), (1,)), ((), ()))


def where_am_i():
    me = lax.axis_index("fsdp")
    core = me % 2
    z = me // RING
    f_bit = 2 + 2 * core
    s_bit = 4 - 2 * core
    first = me + f_bit * (1 - 2 * ((me // f_bit) % 2))
    second = me + s_bit * (1 - 2 * ((me // s_bit) % 2))
    sibling = me + 1 - 2 * core
    return me, z, first, second, sibling


def greet(peers):
    barrier = pltpu.get_barrier_semaphore()
    for peer in peers:
        pl.semaphore_signal(barrier, inc=1, device_id=(peer,), device_id_type=MESH)
    pl.semaphore_wait(barrier, len(peers))


def remote(src, dst, send_sem, recv_sem, device):
    return pltpu.make_async_remote_copy(
        src_ref=src,
        dst_ref=dst,
        send_sem=send_sem,
        recv_sem=recv_sem,
        device_id=(device,),
        device_id_type=MESH,
    )


def line_peers(me):
    return [lax.rem(me + RING * k, RING * LINE) for k in range(1, LINE)]


def on_line(z, k, body):
    for step in ((-k, k) if k else (0,)):

        @pl.when((z + step >= 0) & (z + step < LINE))
        def _(step=step):
            body(step)


def dot_nt(left, right):
    return lax.dot_general(left, right, contract_cols, preferred_element_type=f32)


def dot_tn(left, right):
    return lax.dot_general(left, right, contract_rows, preferred_element_type=f32)


def streamed(count, fetch, body):
    for copy in fetch(0, 0):
        copy.start()

    def step(i, carry):
        slot = i % 2

        @pl.when(i + 1 < count)
        def _():
            for copy in fetch(i + 1, 1 - slot):
                copy.start()

        for copy in fetch(i, slot):
            copy.wait()
        body(i, slot)
        return carry

    lax.fori_loop(0, count, step, 0)


def tile(i, size):
    return pl.ds(pl.multiple_of(i * size, size), size)


def add_rows(out, *terms):
    rows = out.shape[0]

    def body(i, carry):
        at = pl.ds(pl.multiple_of(i * 16, 16), 16)
        total = terms[0][at, :].astype(f32)
        for term in terms[1:]:
            total = total + term[at, :].astype(f32)
        out[at, :] = total.astype(out.dtype)
        return carry

    lax.fori_loop(0, rows // 16, body, 0)


def lane_sum(x):
    return jnp.sum(x, axis=-1, keepdims=True)


def token_places(lengths, devices, me):
    seqs = lengths.shape[1]
    counts_row = jnp.where(devices == me, lengths, 0).astype(f32)
    up = lax.broadcasted_iota(jnp.int32, (seqs, seqs), 0)
    across = lax.broadcasted_iota(jnp.int32, (seqs, seqs), 1)
    counts_col = lane_sum(jnp.where(up == across, counts_row, 0.0))
    starts_row = jnp.sum(jnp.where(up < across, counts_col, 0.0), axis=0, keepdims=True)
    starts_col = lane_sum(jnp.where(across < up, counts_row, 0.0))

    def within(places, starts, counts):
        return (places >= starts) & (places < starts + counts)

    places = lax.broadcasted_iota(jnp.int32, (CAP, seqs), 0).astype(f32)
    labels = lax.broadcasted_iota(jnp.int32, (CAP, seqs), 1).astype(f32)
    inside = within(places, starts_row, counts_row)
    segment_col = lane_sum(jnp.where(inside, labels + 1.0, 0.0)) - 1.0
    position = lane_sum(jnp.where(inside, places - starts_row, 0.0))
    places = lax.broadcasted_iota(jnp.int32, (seqs, CAP), 1).astype(f32)
    labels = lax.broadcasted_iota(jnp.int32, (seqs, CAP), 0).astype(f32)
    inside = within(places, starts_col, counts_col)
    segment_row = jnp.sum(jnp.where(inside, labels + 1.0, 0.0), axis=0, keepdims=True) - 1.0
    return segment_col, segment_row, position


def allowed_bias(segment_col, segment_row):
    t = lax.broadcasted_iota(jnp.int32, (CAP, CAP), 0)
    u = lax.broadcasted_iota(jnp.int32, (CAP, CAP), 1)
    same = (segment_col == segment_row) & (segment_col >= 0.0)
    return jnp.where((t == u) | ((u < t) & same), 0.0, masked_score)


def half_turn(v):
    lane = lax.broadcasted_iota(jnp.int32, v.shape, v.ndim - 1)
    turned = pltpu.roll(v, HD // 2, v.ndim - 1)
    return jnp.where(lane < HD // 2, -turned, turned)


def rms_scale(v):
    return lax.rsqrt(jnp.mean(v * v, axis=-1, keepdims=True) + epsilon)


def forward_kernel(
    x_ref, len_ref, dev_ref, ga_ref, gm_ref, gq_ref, gk_ref, cot_ref,
    wq_ref, wk_ref, wv_ref, wo_ref, gate_ref, up_ref, wd_ref,
    w_out, gu_out, d_out, tok_out, cot_out, hid_out, pre_out,
    middle_out, normed_out, raw_out, q_out, k_out, v_out, mixed_out, gains_out, rope_out,
    w_tmp, p_tmp, d_tmp, cot_tmp, second_tmp, chunk, ow_all, gain_tmp, gain_own,
    tok_all, gate_up, m_chunk, hid,
    local, up_s, down_s, first_s, second_s, sib_s, recv, ex_send, ex_recv,
    m_first_s, m_second_s, m_sib_s, m_recv, line_up, line_down, line_r, w_load, o_load, g_load,
    act_out,
):
    me, z, first, second, sibling = where_am_i()
    col, fcol, scol = me % RING, first % RING, second % RING
    sfcol = (second + first - me) % RING
    width = p_tmp.shape[2] // 2
    rows = w_tmp.shape[0]
    qkv_width = raw_out.shape[1]
    attn_width = qkv_width + wo_ref.shape[1]
    last = LINE - 1
    pieces = LINE + 1

    w_in = []
    lo = 0
    for i, ref in enumerate((wq_ref, wk_ref, wv_ref, wo_ref)):
        at = pl.ds(lo, ref.shape[1])
        w_in.append(pltpu.make_async_copy(ref, w_tmp.at[:, at], local.at[i]))
        lo += ref.shape[1]
    p_in = [
        pltpu.make_async_copy(
            ref.at[:, pl.ds(pl.multiple_of(z * width, width), width)],
            p_tmp.at[z, :, pl.ds(which * width, width)],
            local.at[5 + which],
        )
        for which, ref in enumerate((gate_ref, up_ref))
    ]
    cot_in = pltpu.make_async_copy(cot_ref, cot_tmp, local.at[8])
    d_in = pltpu.make_async_copy(wd_ref, d_tmp, local.at[7])
    for copy in w_in + p_in + [d_in, cot_in]:
        copy.start()
    gain_own[...] = jnp.zeros_like(gain_own)
    for i, ref in enumerate((ga_ref, gm_ref, gq_ref, gk_ref)):
        gain_own[i : i + 1, 0 : ref.shape[1]] = ref[...].astype(f32)
    flat = gain_own[...]
    paired = jnp.where(me % 2 == 0, flat, pltpu.roll(flat, rows, 1))
    shared = pltpu.roll(flat, gq_ref.shape[1] * me, 1)
    placed = jnp.where(lax.broadcasted_iota(jnp.int32, flat.shape, 0) < 2, paired, shared)
    w_tmp[0:16, attn_width:] = placed.astype(bf16)
    w_tmp[16:, attn_width:] = jnp.zeros((rows - 16, 128), bf16)
    greet(line_peers(me) + [first, second, sibling])

    def send(src, shard, sems, device):
        return remote(src, w_out.at[shard], sems.at[shard], recv.at[shard], device)

    def arrived(shard):
        send(w_out.at[shard], shard, sib_s, sibling).wait_recv()

    def exchange(k, which):
        peer_z = lax.rem(z + k, LINE)
        src = (gate_ref, up_ref)[which].at[:, pl.ds(pl.multiple_of(peer_z * width, width), width)]
        dst = p_tmp.at[z, :, pl.ds(which * width, width)]
        return remote(src, dst, ex_send.at[k, which], ex_recv.at[k, which], col + RING * peer_z)

    token_half = second_tmp.shape[1] // 2

    def line_spot(which, shard):
        if which == 1:
            return cot_out.at[shard]
        return tok_out.at[shard, :, pl.ds(token_half * (which // 2), token_half)]

    def line_send(src, which, shard, sems, device):
        landing = line_spot(which, shard)
        return remote(src, landing, sems.at[which, shard], line_r.at[which, shard], device)

    def line_own(which, src):
        @pl.when(z < last)
        def _():
            line_send(src, which, z, line_up, me + RING).start()

        @pl.when(z > 0)
        def _():
            line_send(src, which, z, line_down, me - RING).start()

    def line_relay(which, k):
        def body(step):
            shard = z + step
            src = line_spot(which, shard)
            line_send(src, which, shard, line_up, second).wait_recv()
            if step < 0:

                @pl.when(z < last)
                def _():
                    line_send(src, which, shard, line_up, me + RING).start()
            else:

                @pl.when(z > 0)
                def _():
                    line_send(src, which, shard, line_down, me - RING).start()

        on_line(z, k, body)

    for copy in w_in:
        copy.wait()

    @pl.when(z < last)
    def _():
        send(w_tmp, me, up_s, me + RING).start()

    @pl.when(z > 0)
    def _():
        send(w_tmp, me, down_s, me - RING).start()

    send(w_tmp, me, first_s, first).start()
    send(w_tmp, me, second_s, second).start()
    send(w_tmp, me, sib_s, sibling).start()
    w_back = pltpu.make_async_copy(w_tmp, w_out.at[me], local.at[9])
    w_back.start()

    def own(k):
        def body(step):
            shard = me + RING * step
            src = w_out.at[shard]
            arrived(shard)
            if step < 0:

                @pl.when(z < last)
                def _():
                    send(src, shard, up_s, me + RING).start()
            else:

                @pl.when(z > 0)
                def _():
                    send(src, shard, down_s, me - RING).start()

            send(src, shard, first_s, first).start()
            send(src, shard, second_s, second).start()
            send(src, shard, sib_s, sibling).start()

        on_line(z, k, body)

    def other(base, k, onward):
        def body(step):
            shard = base + RING * (z + step)
            src = w_out.at[shard]
            arrived(shard)
            if onward:
                send(src, shard, second_s, second).start()
            send(src, shard, sib_s, sibling).start()

        on_line(z, k, body)

    segment_col, segment_row, position = token_places(len_ref[...], dev_ref[...], me)
    rope_out[2] = allowed_bias(segment_col, segment_row)
    lane = lax.broadcasted_iota(jnp.int32, (1, HD), 1) % (HD // 2)
    angles = position * jnp.exp(lane.astype(f32) * (-2.0 * math.log(rope_base) / HD))
    rope_out[0] = jnp.cos(angles)
    rope_out[1] = jnp.sin(angles)
    x_scale = rms_scale(x_ref[...].astype(f32))
    raw_out[...] = jnp.zeros_like(raw_out)

    def load_group(step):
        zz = z + step
        part = w_out.at[pl.ds(RING * zz, RING)]
        return (
            pltpu.make_async_copy(part.at[:, :, pl.ds(0, qkv_width)], chunk, w_load),
            pltpu.make_async_copy(
                part.at[:, :, pl.ds(qkv_width, attn_width - qkv_width)],
                ow_all.at[pl.ds(RING * zz, RING)],
                o_load.at[zz],
            ),
            pltpu.make_async_copy(
                part.at[:, pl.ds(0, 16), pl.ds(attn_width, 128)], gain_tmp.at[zz], g_load
            ),
        )

    def group(k):
        def body(step):
            zz = z + step
            for i in range(RING // 2):
                arrived(RING * zz + 2 * i + sibling % 2)
            copies = load_group(step)
            for copy in copies:
                copy.start()
            copies[2].wait()
            span = RING * rows
            for pair in range(RING // 2):
                at = pl.ds(pl.multiple_of(zz * span + pair * 128, 128), 128)
                both = gain_tmp[zz, 2 * pair].astype(f32) + gain_tmp[zz, 2 * pair + 1].astype(f32)
                gains_out[0:2, at] = both[0:2]
                piece = x_ref[:, at].astype(f32) * x_scale * both[0:1]
                normed_out[:, at] = piece.astype(bf16)
            copies[0].wait()
            left = normed_out[:, pl.ds(pl.multiple_of(zz * span, span), span)]

            def tile(i, carry):
                at = pl.ds(pl.multiple_of(i * 512, 512), 512)
                right = chunk[:, :, at].reshape(span, 512)
                raw_out[:, at] += jnp.dot(left, right, preferred_element_type=f32)
                return carry

            lax.fori_loop(0, qkv_width // 512, tile, 0)

        on_line(z, k, body)

    own(1)
    other(fcol, 0, True)
    own(2)
    other(fcol, 1, True)
    other(scol, 0, False)
    for k in range(1, LINE):
        for which in range(2):
            exchange(k, which).start()
    cot_in.wait()
    line_own(1, cot_tmp)
    cot_back = pltpu.make_async_copy(cot_tmp, cot_out.at[z], local.at[10])
    cot_back.start()
    own(3)
    other(fcol, 2, True)
    other(scol, 1, False)
    other(sfcol, 0, False)
    w_back.wait()
    line_relay(1, 1)
    group(0)
    other(fcol, 3, True)
    other(scol, 2, False)
    other(sfcol, 1, False)
    for copy in p_in + [d_in]:
        copy.wait()
    for k in range(1, LINE):
        for which in range(2):
            src_z = lax.rem(z + LINE - k, LINE)
            landed = p_tmp.at[src_z, :, pl.ds(which * width, width)]
            remote(landed, landed, ex_send.at[k, which], ex_recv.at[k, which], second).wait_recv()

    def spot(piece, shard):
        return gu_out.at[piece, shard] if piece < LINE else d_out.at[shard]

    def source(piece):
        return p_tmp.at[piece] if piece < LINE else d_tmp

    def m_send(src, piece, shard, sems, device):
        return remote(
            src, spot(piece, shard), sems.at[piece, shard], m_recv.at[piece, shard], device
        )

    def m_arrived(piece, shard):
        m_send(spot(piece, shard), piece, shard, m_sib_s, sibling).wait_recv()

    def m_own_second(piece):
        m_send(source(piece), piece, col, m_second_s, second).start()

    def m_own_first(piece):
        m_send(source(piece), piece, col, m_first_s, first).start()
        m_send(source(piece), piece, col, m_sib_s, sibling).start()

    def m_own(piece):
        m_own_second(piece)
        m_own_first(piece)

    m_own_second(0)
    m_own_second(1)
    m_own_second(LINE)
    p_back = pltpu.make_async_copy(p_tmp, gu_out.at[:, col], local.at[11])
    p_back.start()
    d_back = pltpu.make_async_copy(d_tmp, d_out.at[col], local.at[4])
    d_back.start()
    line_relay(1, 2)
    group(1)

    other(scol, 3, False)
    other(sfcol, 2, False)
    group(2)
    other(sfcol, 3, False)
    m_own_first(0)
    m_own_first(1)
    m_own_first(LINE)
    line_relay(1, 3)
    group(3)

    small = jnp.zeros((16, 128), f32)
    for zz in range(LINE):
        for i in range(RING):
            small = small + gain_tmp[zz, i].astype(f32)
    q_gain, k_gain = small[2:3], small[3:4]
    gains_out[2:4, 0:128] = small[2:4]
    cosine, sine, bias = rope_out[0], rope_out[1], rope_out[2]

    def turned(v, gain):
        v = v * rms_scale(v) * gain
        return (v * cosine + half_turn(v) * sine).astype(bf16)

    kv0 = H * HD
    v0 = kv0 + KVH * HD

    def head(g, carry):
        at = pl.ds(pl.multiple_of(g * HD, HD), HD)
        qa = pl.ds(pl.multiple_of(g * 2 * HD, 2 * HD), HD)
        qb = pl.ds(pl.multiple_of(g * 2 * HD + HD, HD), HD)
        key = turned(raw_out[:, pl.ds(pl.multiple_of(kv0 + g * HD, HD), HD)], k_gain)
        value = raw_out[:, pl.ds(pl.multiple_of(v0 + g * HD, HD), HD)].astype(bf16)
        k_out[:, at] = key
        v_out[:, at] = value
        query_a = turned(raw_out[:, qa], q_gain)
        query_b = turned(raw_out[:, qb], q_gain)
        q_out[:, qa] = query_a
        q_out[:, qb] = query_b
        for query, where in ((query_a, qa), (query_b, qb)):
            scores = lax.dot_general(query, key, contract_cols, preferred_element_type=f32)
            logits = scores * (HD ** (-0.5)) + bias
            exponent = jnp.exp(logits - jnp.max(logits, axis=-1, keepdims=True))
            weights = (exponent / lane_sum(exponent)).astype(bf16)
            mixed = jnp.dot(weights, value, preferred_element_type=f32)
            mixed_out[:, where] = mixed.astype(bf16)
        return carry

    lax.fori_loop(0, KVH, head, 0, unroll=2)
    for zz in range(LINE):
        pltpu.make_async_copy(
            w_out.at[pl.ds(RING * zz, RING), :, pl.ds(qkv_width, attn_width - qkv_width)],
            ow_all.at[pl.ds(RING * zz, RING)],
            o_load.at[zz],
        ).wait()
    mixed = mixed_out[...]

    def out_tile(i, total):
        at = pl.ds(pl.multiple_of(i * 512, 512), 512)
        right = ow_all[:, :, at].reshape(mixed.shape[1], 512)
        middle = x_ref[:, at].astype(f32) + jnp.dot(mixed, right, preferred_element_type=f32)
        middle_out[:, at] = middle
        return total + lane_sum(middle * middle)

    tiles = middle_out.shape[1] // 512
    total = lax.fori_loop(0, tiles, out_tile, jnp.zeros((CAP, 1), f32))
    scale = lax.rsqrt(total / middle_out.shape[1] + epsilon)

    def norm_tile(i, carry):
        at = pl.ds(pl.multiple_of(i * 512, 512), 512)
        second_tmp[:, at] = (middle_out[:, at] * scale * gains_out[1:2, at]).astype(bf16)
        return carry

    lax.fori_loop(0, tiles, norm_tile, 0)

    def m_other(piece, shard, onward):
        m_arrived(piece, shard)
        if onward:
            m_send(spot(piece, shard), piece, shard, m_second_s, second).start()
        m_send(spot(piece, shard), piece, shard, m_sib_s, sibling).start()

    def m_whole(piece):
        for k in range(RING // 2):
            m_arrived(piece, 2 * k + sibling % 2)

    part = width

    def gate_up_copy(piece):
        return pltpu.make_async_copy(
            gu_out.at[piece], m_chunk.at[piece % 2], act_out.at[piece % 2, 0]
        )

    def gate_up_load(piece):
        m_whole(piece)
        gate_up_copy(piece).start()

    def gate_up_rows(piece):
        gate_up_copy(piece).wait()
        span = RING * rows
        left = tok_all[:, :, pl.ds(piece * span, span)].reshape(LINE * CAP, span)

        def columns(n, carry):
            at = tile(n, 512)
            right = m_chunk[piece % 2, :, :, at].reshape(span, 512)
            term = jnp.dot(left, right, preferred_element_type=f32)
            if piece == 0:
                gate_up[:, at] = term
            else:
                gate_up[:, at] += term
            return carry

        lax.fori_loop(0, 2 * part // 512, columns, 0)

    m_own(2)
    line_own(0, second_tmp.at[:, pl.ds(0, token_half)])
    line_own(2, second_tmp.at[:, pl.ds(token_half, token_half)])
    tok_back = pltpu.make_async_copy(second_tmp, tok_out.at[z], local.at[13])
    tok_back.start()
    m_other(0, fcol, True)
    m_other(0, scol, False)
    m_own(3)
    line_relay(0, 1)
    line_relay(2, 1)
    m_other(1, fcol, True)
    m_other(1, scol, False)
    m_other(0, sfcol, False)
    line_relay(0, 2)
    line_relay(2, 2)
    m_other(2, fcol, True)
    m_other(2, scol, False)
    m_other(1, sfcol, False)
    p_back.wait()
    gate_up_load(0)
    m_other(3, fcol, True)
    m_other(3, scol, False)
    m_other(LINE, fcol, True)
    m_other(LINE, scol, False)
    line_relay(0, 3)
    tok_back.wait()
    cot_back.wait()
    tok_in = []
    for half in range(2):
        at = pl.ds(half * token_half, token_half)
        tok_in.append(
            pltpu.make_async_copy(
                tok_out.at[:, :, at], tok_all.at[:, :, at], local.at[10 if half else 12]
            )
        )
    tok_in[0].start()
    gate_up_load(1)
    tok_in[0].wait()
    gate_up_rows(0)
    m_other(2, sfcol, False)
    gate_up_load(2)
    gate_up_rows(1)
    line_relay(2, 3)
    tok_in[1].start()
    tok_in[1].wait()
    m_other(3, sfcol, False)
    gate_up_load(3)
    gate_up_rows(2)
    gate_up_rows(3)

    def hid_copy(n):
        at = tile(n, 256)
        return pltpu.make_async_copy(hid.at[:, at], hid_out.at[:, at], act_out.at[n, 0])

    def pre_copies(n):
        up_at = pl.ds(pl.multiple_of(part + n * 256, 256), 256)
        return [
            pltpu.make_async_copy(gate_up.at[:, at], pre_out.at[:, at], act_out.at[n, i])
            for i, at in ((1, tile(n, 256)), (2, up_at))
        ]

    def units(n, carry):
        at = tile(n, 256)
        up_at = pl.ds(pl.multiple_of(part + n * 256, 256), 256)
        for copy in pre_copies(n):
            copy.start()

        def act(r, inner):
            some = tile(r, 32)
            gate, up = gate_up[some, at], gate_up[some, up_at]
            hid[some, at] = (gate * jax.nn.sigmoid(gate) * up).astype(bf16)
            return inner

        lax.fori_loop(0, LINE * CAP // 32, act, 0)
        hid_copy(n).start()
        return carry

    lax.fori_loop(0, part // 256, units, 0)
    m_other(LINE, sfcol, False)
    d_back.wait()
    m_whole(LINE)

    for n in range(part // 256):
        for copy in [hid_copy(n)] + pre_copies(n):
            copy.wait()
    for k in range(1, LINE):
        for which in range(2):
            exchange(k, which).wait_send()
    for k in range(LINE):

        @pl.when((z < last) & (k <= z))
        def _(k=k):
            send(w_tmp, col + RING * k, up_s, me + RING).wait_send()
            for which in range(3):
                line_send(line_spot(which, k), which, k, line_up, me + RING).wait_send()

        @pl.when((z > 0) & (k >= z))
        def _(k=k):
            send(w_tmp, col + RING * k, down_s, me - RING).wait_send()
            for which in range(3):
                line_send(line_spot(which, k), which, k, line_down, me - RING).wait_send()

        send(w_tmp, col + RING * k, first_s, first).wait_send()
        send(w_tmp, col + RING * k, second_s, second).wait_send()
        send(w_tmp, fcol + RING * k, second_s, second).wait_send()
        for base in (col, fcol, scol, sfcol):
            send(w_tmp, base + RING * k, sib_s, sibling).wait_send()
    for piece in range(pieces):
        src = source(piece)
        m_send(src, piece, col, m_first_s, first).wait_send()
        m_send(src, piece, col, m_second_s, second).wait_send()
        m_send(src, piece, fcol, m_second_s, second).wait_send()
        for base in (col, fcol, scol, sfcol):
            m_send(src, piece, base, m_sib_s, sibling).wait_send()


def forward(hidden_in, out_grad, seq_lengths, seq_device, gains, wq, wk, wv, wo, gate, up, wd):
    slots, dim = hidden_in.shape
    rows = wq.shape[0]
    n = RING * LINE
    width = gate.shape[1] // LINE
    qkv_width = wq.shape[1] + wk.shape[1] + wv.shape[1]
    wide = qkv_width + wo.shape[1] + 128
    pieces = LINE + 1
    S = jax.ShapeDtypeStruct
    return pl.pallas_call(
        forward_kernel,
        out_shape=(
            S((n, rows, wide), bf16),
            S((LINE, RING, rows, 2 * width), bf16),
            S((RING,) + wd.shape, bf16),
            S((LINE, slots, dim), bf16),
            S((LINE, slots, dim), bf16),
            S((LINE * slots, width), bf16),
            S((LINE * slots, 2 * width), f32),
            S((slots, dim), f32),
            S((slots, dim), bf16),
            S((slots, qkv_width), f32),
            S((slots, H * HD), bf16),
            S((slots, KVH * HD), bf16),
            S((slots, KVH * HD), bf16),
            S((slots, H * HD), bf16),
            S((8, dim), f32),
            S((3, slots, HD), f32),
        ),
        in_specs=[VMEM] * 7 + [ANY] * 8,
        out_specs=(ANY,) * 7 + (VMEM,) * 9,
        scratch_shapes=[
            pltpu.VMEM((rows, wide), bf16),
            pltpu.VMEM((LINE, rows, 2 * width), bf16),
            pltpu.VMEM(wd.shape, bf16),
            pltpu.VMEM((slots, dim), bf16),
            pltpu.VMEM((slots, dim), bf16),
            pltpu.VMEM((RING, rows, qkv_width), bf16),
            pltpu.VMEM((n, rows, wo.shape[1]), bf16),
            pltpu.VMEM((LINE, RING, 16, 128), bf16),
            pltpu.VMEM((16, 128), f32),
            pltpu.VMEM((LINE, slots, dim), bf16),
            pltpu.VMEM((LINE * slots, 2 * width), f32),
            pltpu.VMEM((2, RING, rows, 2 * width), bf16),
            pltpu.VMEM((LINE * slots, width), bf16),
            DMA((14,)),
            DMA((n,)),
            DMA((n,)),
            DMA((n,)),
            DMA((n,)),
            DMA((n,)),
            DMA((n,)),
            DMA((LINE, 2)),
            DMA((LINE, 2)),
            DMA((pieces, RING)),
            DMA((pieces, RING)),
            DMA((pieces, RING)),
            DMA((pieces, RING)),
            DMA((3, LINE)),
            DMA((3, LINE)),
            DMA((3, LINE)),
            DMA,
            DMA((LINE,)),
            DMA,
            DMA((width // 256, 3)),
        ],
        compiler_params=pltpu.CompilerParams(
            collective_id=0, has_side_effects=True, vmem_limit_bytes=64000 * 1024
        ),
        name="forward",
    )(
        hidden_in, seq_lengths[None, :], seq_device[None, :], *[g[None, :] for g in gains],
        out_grad, wq, wk, wv, wo, gate, up, wd,
    )


def backward_kernel(
    gu_ref, wd_ref, tok_ref, cot_ref, hid_ref, pre_ref, w_ref, middle_ref, normed_ref, raw_ref,
    q_ref, k_ref, v_ref, mixed_ref, x_ref, gains_ref, rope_ref,
    x_out, small_out, y_out, d_out, a_out, ex_land, gu_out, c_land, s_land, f_land, l_land,
    gu_all, gd_all, gu_sib, gd_sib, gu_sec, gd_sec, gu_fst, gd_fst, t_own, t_land,
    dmid, dqkv, s_sum, s_got, s_line,
    c_send, c_recv, s_send, s_recv, f_send, f_recv, down_s, down_r, up_s, up_r, load, stream, back,
    ac_send, ac_recv, as_send, as_recv, af_send, af_recv, ad_send, ad_recv, au_send, au_recv,
    ex_s, ex_r, small_s, small_r, units_in,
    a_load,
):
    me, z, first, second, sibling = where_am_i()
    greet(line_peers(me) + [first, second, sibling])
    core = me % 2
    mine, fst, sec = (me % RING) // 2, (first % RING) // 2, (second % RING) // 2
    far = ((second + first - me) % RING) // 2
    half = gd_fst.shape[0] // 2
    last = LINE - 1
    tokens, dim = tok_ref.shape
    part = hid_ref.shape[1]
    quad_rows = part // LINE
    shard_rows = dim // (RING * LINE)
    piece_cols = gu_all.shape[3]
    kv0 = H * HD
    v0 = kv0 + KVH * HD
    qkv_width = v0 + KVH * HD
    MLP_GU, MLP_D = (0, 0, LINE), (1, LINE, LINE + 2)

    def block(gu, d, piece, group):
        if group == 0:
            return gu.at[piece]
        return d.at[tile(piece - LINE, half)]

    def own_block(quad, piece, group, theirs=False):
        shard = 2 * quad + (1 - core if theirs else core)
        if group == 0:
            return gu_all.at[piece, shard]
        return block(None, gd_all.at[shard], piece, group)

    def each(span, body):
        group, lo, hi = span

        def step(piece, carry):
            body(piece, group)
            return carry

        lax.fori_loop(lo, hi, step, 0)

    def to_sibling(quad, piece, group):
        return remote(
            own_block(quad, piece, group, theirs=True),
            block(gu_sib.at[quad], gd_sib.at[quad], piece, group),
            c_send.at[quad, piece],
            c_recv.at[quad, piece],
            sibling,
        )

    def to_second(quad, slot, piece, group):
        return remote(
            own_block(quad, piece, group),
            block(gu_sec.at[slot], gd_sec.at[slot], piece, group),
            s_send.at[slot, piece],
            s_recv.at[slot, piece],
            second,
        )

    def to_first(piece, group):
        return remote(
            own_block(fst, piece, group),
            block(gu_fst, gd_fst, piece, group),
            f_send.at[piece],
            f_recv.at[piece],
            first,
        )

    def pass_on(piece, group):
        for quad, slot in ((far, 1), (sec, 0)):
            to_sibling(quad, piece, group).wait_recv()
            own = own_block(quad, piece, group)
            add_rows(own, own, block(gu_sib.at[quad], gd_sib.at[quad], piece, group))
            to_second(quad, slot, piece, group).start()

    def narrow(piece, group):
        to_sibling(fst, piece, group).wait_recv()
        to_second(far, 1, piece, group).wait_recv()
        own = own_block(fst, piece, group)
        add_rows(
            own,
            own,
            block(gu_sib.at[fst], gd_sib.at[fst], piece, group),
            block(gu_sec.at[1], gd_sec.at[1], piece, group),
        )
        to_first(piece, group).start()

    def finish(piece, group, out=None):
        to_sibling(mine, piece, group).wait_recv()
        to_second(sec, 0, piece, group).wait_recv()
        to_first(piece, group).wait_recv()
        own = own_block(mine, piece, group)
        add_rows(
            own if group == 0 else block(None, out, piece, group),
            own,
            block(gu_sib.at[mine], gd_sib.at[mine], piece, group),
            block(gu_sec.at[0], gd_sec.at[0], piece, group),
            block(gu_fst, gd_fst, piece, group),
        )

    def drain_sibling(piece, group):
        for quad in (far, fst, sec, mine):
            to_sibling(quad, piece, group).wait_send()

    def drain(piece, group):
        to_second(far, 1, piece, group).wait_send()
        to_second(sec, 0, piece, group).wait_send()
        to_first(piece, group).wait_send()

    def send_line(src, which, t, up):
        return remote(
            src,
            t_land.at[which, t + 1 if up else t],
            (up_s if up else down_s).at[which, t],
            (up_r if up else down_r).at[which, t],
            me + RING if up else me - RING,
        )

    def line_own(which):
        for k in range(last):

            @pl.when(z == last)
            def _(k=k):
                send_line(t_own.at[which, k], which, k, False).start()

            @pl.when(z == 0)
            def _(k=k):
                send_line(t_own.at[which, last - k], which, last - k, True).start()

    def relay_at(which, at, t, up):
        @pl.when(z == at)
        def _():
            landing = t_land.at[which, t + 1 if up else t]
            send_line(landing, which, t, up).wait_recv()
            add_rows(landing, landing, t_own.at[which, t])
            send_line(landing, which, t, up).start()

    def relay(which, step):
        if step < 2:
            relay_at(which, 2, step, False)
            relay_at(which, 1, last - step, True)
        else:
            relay_at(which, 1, 0, False)
            relay_at(which, 2, last, True)

    def line_sum(which, out):
        own, above, below = t_own.at[which, z], t_land.at[which, z], t_land.at[which, z + 1]

        @pl.when(z < last)
        def _():
            send_line(above, which, z, False).wait_recv()

        @pl.when(z > 0)
        def _():
            send_line(below, which, z, True).wait_recv()

        @pl.when(z == 0)
        def _():
            add_rows(out, own, above)

        @pl.when(z == last)
        def _():
            add_rows(out, own, below)

        @pl.when((z > 0) & (z < last))
        def _():
            add_rows(out, own, above, below)

    def mlp(tok, cot, hid, dgu):
        ins = [
            pltpu.make_async_copy(hid_ref, hid, load.at[0]),
            pltpu.make_async_copy(cot_ref, cot, load.at[1]),
            pltpu.make_async_copy(tok_ref, tok, load.at[3]),
        ]
        for copy in ins:
            copy.start()
        wide = 256
        for copy in ins[:2]:
            copy.wait()

        previous = None
        for quad in (far, sec, fst, mine):

            def columns(n, carry, quad=quad):
                at = tile(n, 512)
                both = dot_tn(hid[:, tile(quad, quad_rows)], cot[:, at]).astype(bf16)
                gd_all[2 * quad, :, at] = both[: quad_rows // 2]
                gd_all[2 * quad + 1, :, at] = both[quad_rows // 2 :]
                return carry

            lax.fori_loop(0, dim // 512, columns, 0)
            if previous is not None:
                each(MLP_D, lambda piece, group, q=previous: to_sibling(q, piece, group).start())
            previous = quad
        each(MLP_D, lambda piece, group, q=previous: to_sibling(q, piece, group).start())
        each(MLP_D, pass_on)

        def units(gate_t, up_t, down_w, dhid_t):
            def fetch(i, slot):
                up_at = pl.ds(pl.multiple_of(part + i * wide, wide), wide)
                return (
                    pltpu.make_async_copy(
                        pre_ref.at[:, tile(i, wide)], gate_t.at[slot], units_in.at[slot, 0]
                    ),
                    pltpu.make_async_copy(pre_ref.at[:, up_at], up_t.at[slot], units_in.at[slot, 1]),
                    pltpu.make_async_copy(
                        wd_ref.at[tile(i, wide)], down_w.at[slot], units_in.at[slot, 2]
                    ),
                )

            def body(i, slot):
                dhid_t[...] = dot_nt(cot[...], down_w[slot])

                def act(r, carry):
                    at = tile(r, 32)
                    gate, up, dhid = gate_t[slot, at], up_t[slot, at], dhid_t[at]
                    sig = jax.nn.sigmoid(gate)
                    dgate = dhid * up * (sig * (1.0 + gate * (1.0 - sig)))
                    dgu[at, tile(i, wide)] = dgate.astype(bf16)
                    up_at = pl.ds(pl.multiple_of(part + i * wide, wide), wide)
                    dgu[at, up_at] = (dhid * (gate * sig)).astype(bf16)
                    return carry

                lax.fori_loop(0, tokens // 32, act, 0)

            streamed(part // wide, fetch, body)

        pl.run_scoped(
            units,
            pltpu.VMEM((2, tokens, wide), f32),
            pltpu.VMEM((2, tokens, wide), f32),
            pltpu.VMEM((2, wide, dim), bf16),
            pltpu.VMEM((tokens, wide), f32),
        )

        def back_through(rows_w):
            def fetch(i, slot):
                return (
                    pltpu.make_async_copy(
                        gu_ref.at[tile(i, wide)], rows_w.at[slot], stream.at[slot]
                    ),
                )

            def body(i, slot):
                out = dot_nt(dgu[...], rows_w[slot]).astype(bf16)
                t_own[0, :, :, tile(i, wide)] = out.reshape(LINE, CAP, wide)

            streamed(dim // wide, fetch, body)

        pl.run_scoped(back_through, pltpu.VMEM((2, wide, 2 * part), bf16))
        ins[2].wait()
        line_own(0)

        rows = dim // LINE
        for piece in range(LINE):

            def columns(n, carry, piece=piece):
                at = tile(n, 512)
                grad = dot_tn(tok[:, pl.ds(piece * rows, rows)], dgu[:, at]).astype(bf16)
                gu_all[piece, :, :, at] = grad.reshape(RING, rows // RING, 512)
                return carry

            lax.fori_loop(0, 2 * part // 512, columns, 0)
            if piece > 0:
                pass_on(piece - 1, 0)
            for quad in (far, fst, sec, mine):
                to_sibling(quad, piece, 0).start()
            if piece == 2:
                relay(0, 0)
        pass_on(LINE - 1, 0)
        each(MLP_D, narrow)

        def out_through(cols_w):
            def fetch(i, slot):
                return (
                    pltpu.make_async_copy(
                        wd_ref.at[:, tile(i, wide)], cols_w.at[slot], stream.at[slot]
                    ),
                )

            def body(i, slot):
                out = jnp.dot(hid[...], cols_w[slot], preferred_element_type=f32).astype(bf16)
                t_own[1, :, :, tile(i, wide)] = out.reshape(LINE, CAP, wide)

                @pl.when(i == 3)
                def _():
                    relay(0, 1)

                @pl.when(i == 5)
                def _():
                    relay(0, 2)

            streamed(dim // wide, fetch, body)

        pl.run_scoped(out_through, pltpu.VMEM((2, part, wide), bf16))

    pl.run_scoped(
        mlp,
        pltpu.VMEM((tokens, dim), bf16),
        pltpu.VMEM((tokens, dim), bf16),
        pltpu.VMEM((tokens, part), bf16),
        pltpu.VMEM((tokens, 2 * part), bf16),
    )
    def attention(dbr, mixed, normed, raw, q, k, v, cot, dsec, dmix, middle, w_rows):
        ins = [
            pltpu.make_async_copy(src, dst, load.at[i])
            for i, (src, dst) in enumerate(
                (
                    (middle_ref, middle),
                    (raw_ref.at[:, pl.ds(0, v0)], raw),
                    (q_ref, q),
                    (k_ref, k),
                    (v_ref, v),
                    (cot_ref.at[tile(z, CAP)], cot),
                    (mixed_ref, mixed),
                    (normed_ref, normed),
                )
            )
        ]
        for copy in ins:
            copy.start()
        narrow(0, 0)
        line_own(1)
        for copy in ins:
            copy.wait()
        line_sum(0, dsec)

        scale = rms_scale(middle[...])
        wide = 512

        def gather_mean(i, total):
            at = tile(i, wide)
            n = middle[:, at] * scale
            ds = dsec[:, at]
            s_sum[3, 0:1, at] = jnp.sum(n * ds, axis=0, keepdims=True)
            return total + lane_sum(n * ds * gains_ref[1:2, at])

        mean = lax.fori_loop(0, dim // wide, gather_mean, jnp.zeros((CAP, 1), f32)) / dim

        def spread_mean(i, carry):
            at = tile(i, wide)
            n = middle[:, at] * scale
            e = dsec[:, at] * gains_ref[1:2, at]
            d_middle = cot[:, at].astype(f32) + scale * (e - n * mean)
            dmid[:, at] = d_middle
            dbr[:, at] = d_middle.astype(bf16)
            return carry

        lax.fori_loop(0, dim // wide, spread_mean, 0)
        shards = w_rows.shape[1]
        rows = shards * w_rows.shape[2]

        def w_fetch(i, slot):
            return (
                pltpu.make_async_copy(
                    w_ref.at[tile(i, shards), :, pl.ds(qkv_width, dim)],
                    w_rows.at[slot],
                    stream.at[slot],
                ),
            )

        def through_out(i, slot):
            dmix[:, tile(i, rows)] = dot_nt(dbr[...], w_rows[slot].reshape(rows, dim)).astype(bf16)

        streamed(dim // rows, w_fetch, through_out)
        narrow(1, 0)
        relay(1, 0)

        cosine, sine, bias = rope_ref[0], rope_ref[1], rope_ref[2]
        s_sum[3, 1:8] = jnp.zeros((7, dim), f32)

        def unrope(raw_v, d_rot, row):
            d_hat = d_rot * cosine - half_turn(d_rot * sine)
            r = rms_scale(raw_v)
            n = raw_v * r
            s_sum[3, row : row + 1, 0:HD] += jnp.sum(n * d_hat, axis=0, keepdims=True)
            e = d_hat * gains_ref[row + 1 : row + 2, 0:HD]
            return (r * (e - n * jnp.mean(n * e, axis=-1, keepdims=True))).astype(bf16)

        def head(g, carry):
            at = tile(g, HD)
            key, value = k[:, at], v[:, at]
            d_key = jnp.zeros((CAP, HD), f32)
            d_value = jnp.zeros((CAP, HD), f32)
            for i in range(2):
                cols = tile(2 * g + i, HD)
                query, d_mix = q[:, cols], dmix[:, cols]
                logits = dot_nt(query, key) * (HD ** (-0.5)) + bias
                exponent = jnp.exp(logits - jnp.max(logits, axis=-1, keepdims=True))
                probs = exponent / lane_sum(exponent)
                d_probs = dot_nt(d_mix, value)
                d_logits = probs * (d_probs - lane_sum(probs * d_probs))
                d_scores = (d_logits * (HD ** (-0.5))).astype(bf16)
                d_value = d_value + dot_tn(probs.astype(bf16), d_mix)
                d_key = d_key + dot_tn(d_scores, query)
                d_query = jnp.dot(d_scores, key, preferred_element_type=f32)
                dqkv[:, cols] = unrope(raw[:, cols], d_query, 1)
            cols = pl.ds(pl.multiple_of(kv0 + g * HD, HD), HD)
            dqkv[:, cols] = unrope(raw[:, cols], d_key, 2)
            dqkv[:, pl.ds(pl.multiple_of(v0 + g * HD, HD), HD)] = d_value.astype(bf16)
            return carry

        lax.fori_loop(0, KVH // 2, head, 0, unroll=2)
        narrow(2, 0)
        lax.fori_loop(KVH // 2, KVH, head, 0, unroll=2)

    order = (
        last * (1 - z // 2),
        2 - 2 * z + 5 * (z // 2),
        1 + z % 2,
        z,
    )

    def a_own(t, quad, h):
        return gu_all.at[t, 2 * quad + (core if h else 1 - core)]

    def sums(dbr, mixed, normed, cbuf, stage):
        span = dim // LINE

        def a_sibling(t, quad, h, slot):
            return remote(
                cbuf.at[slot, quad],
                c_land.at[t, h, quad],
                ac_send.at[slot, quad],
                ac_recv.at[t, h, quad],
                sibling,
            )

        def a_second(t, quad, h, slot):
            return remote(
                a_own(t, quad, h),
                s_land.at[slot, t, h],
                as_send.at[slot, t, h],
                as_recv.at[slot, t, h],
                second,
            )

        def a_first(t, h):
            return remote(
                a_own(t, fst, h), f_land.at[t, h], af_send.at[t, h], af_recv.at[t, h], first
            )

        def a_line(t, h, upward):
            src = a_own(t, mine, h)
            if upward:
                return remote(
                    src, l_land.at[1, t, h], au_send.at[t, h], au_recv.at[t, h], me + RING
                )
            return remote(src, l_land.at[0, t, h], ad_send.at[t, h], ad_recv.at[t, h], me - RING)

        def staged(lo, *landed):
            return [
                pltpu.make_async_copy(src, stage.at[lo + i], a_load.at[lo + i])
                for i, src in enumerate(landed)
            ]

        def begin(copies):
            for copy in copies:
                copy.start()

        def add_staged(own, copies, lo):
            for copy in copies:
                copy.wait()
            add_rows(own, own, *[stage.at[lo + i] for i in range(len(copies))])

        def compute(k):
            h, t, slot = k // LINE, order[k % LINE], k % 2
            if k > 1:
                for quad in (far, fst, sec, mine):
                    a_sibling(order[(k - 2) % LINE], quad, (k - 2) // LINE, slot).wait_send()
            col0 = v0 if h else 0
            own_core = core if h else 1 - core

            def columns(n, carry, left, right, at):
                grad = dot_tn(left[:, tile(t, span)], right).astype(bf16)
                grad = grad.reshape(RING // 2, 2, shard_rows, 512)
                ours = jnp.where(core == 0, grad[:, 0], grad[:, 1])
                theirs = jnp.where(core == 0, grad[:, 1], grad[:, 0])
                for quad in range(RING // 2):
                    gu_all[t, 2 * quad + own_core, :, at] = ours[quad]
                cbuf[slot, :, :, at] = theirs
                return carry

            def from_qkv(n, carry):
                at = tile(n, 512)
                right = dqkv[:, pl.ds(pl.multiple_of(col0 + n * 512, 512), 512)]
                return columns(n, carry, normed, right, at)

            def from_out(n, carry):
                at = pl.ds(pl.multiple_of(qkv_width - v0 + n * 512, 512), 512)
                return columns(n, carry, mixed, dbr[:, tile(n, 512)], at)

            if h == 0:
                lax.fori_loop(0, v0 // 512, from_qkv, 0)
            else:
                lax.fori_loop(0, (qkv_width - v0) // 512, from_qkv, 0)
                lax.fori_loop(0, dim // 512, from_out, 0)

        def share(k):
            h, t, slot = k // LINE, order[k % LINE], k % 2
            for quad in (far, fst, sec, mine):
                a_sibling(t, quad, h, slot).start()

        def spread_in(k):
            t, h = order[k % LINE], k // LINE
            return staged(0, c_land.at[t, h, far], c_land.at[t, h, sec])

        def spread_begin(k):
            h, t, slot = k // LINE, order[k % LINE], k % 2
            for quad in (far, sec):
                a_sibling(t, quad, h, slot).wait_recv()
            begin(spread_in(k))

        def spread(k):
            h, t = k // LINE, order[k % LINE]
            copies = spread_in(k)
            for i, (quad, place) in enumerate(((far, 1), (sec, 0))):
                add_staged(a_own(t, quad, h), copies[i : i + 1], i)
                a_second(t, quad, h, place).start()

        def inward_in(k):
            t, h = order[k % LINE], k // LINE
            return staged(2, c_land.at[t, h, fst], s_land.at[1, t, h])

        def inward_begin(k):
            h, t, slot = k // LINE, order[k % LINE], k % 2
            a_sibling(t, fst, h, slot).wait_recv()
            a_second(t, far, h, 1).wait_recv()
            begin(inward_in(k))

        def inward(k):
            h, t = k // LINE, order[k % LINE]
            add_staged(a_own(t, fst, h), inward_in(k), 2)
            a_first(t, h).start()

        def collect_in(k):
            t, h = order[k % LINE], k // LINE
            return staged(4, c_land.at[t, h, mine], s_land.at[0, t, h], f_land.at[t, h])

        def collect_begin(k):
            h, t, slot = k // LINE, order[k % LINE], k % 2
            a_sibling(t, mine, h, slot).wait_recv()
            a_second(t, sec, h, 0).wait_recv()
            a_first(t, h).wait_recv()
            begin(collect_in(k))

        def collect(k):
            h, t = k // LINE, order[k % LINE]
            add_staged(a_own(t, mine, h), collect_in(k), 4)

            @pl.when((t < z) & (z == last))
            def _():
                a_line(t, h, False).start()

            @pl.when((t > z) & (z == 0))
            def _():
                a_line(t, h, True).start()

        def onward(k):
            h, t = k // LINE, order[k % LINE]

            @pl.when((t < z) & (z < last))
            def _():
                a_line(t, h, False).wait_recv()
                copies = staged(7, l_land.at[0, t, h])
                begin(copies)
                add_staged(a_own(t, mine, h), copies, 7)
                a_line(t, h, False).start()

            @pl.when((t > z) & (z > 0))
            def _():
                a_line(t, h, True).wait_recv()
                copies = staged(7, l_land.at[1, t, h])
                begin(copies)
                add_staged(a_own(t, mine, h), copies, 7)
                a_line(t, h, True).start()

        def exchange(k):
            peer_z = lax.rem(z + k, LINE)
            return remote(
                gu_out.at[peer_z], ex_land.at[z], ex_s.at[k], ex_r.at[k], me % RING + RING * peer_z
            )

        def small(step, src, dst, device):
            return remote(src, dst, small_s.at[step], small_r.at[step], device)

        def first_norm(w_rows):
            shards = w_rows.shape[1]
            wide = 512
            x_scale = rms_scale(x_ref[...].astype(f32))
            w_tile = shards * w_rows.shape[2]

            def w_fetch(i, slot):
                return (
                    pltpu.make_async_copy(
                        w_ref.at[tile(i, shards), :, pl.ds(0, qkv_width)],
                        w_rows.at[slot],
                        stream.at[slot],
                    ),
                )

            def through(i, slot):
                x_out[:, tile(i, w_tile)] = dot_nt(dqkv[...], w_rows[slot].reshape(w_tile, qkv_width))

            streamed(dim // w_tile, w_fetch, through)

            def gather_mean(i, total):
                at = tile(i, wide)
                n = x_ref[:, at].astype(f32) * x_scale
                s_sum[3, 3:4, at] = jnp.sum(n * x_out[:, at], axis=0, keepdims=True)
                return total + lane_sum(n * x_out[:, at] * gains_ref[0:1, at])

            mean = lax.fori_loop(0, dim // wide, gather_mean, jnp.zeros((CAP, 1), f32)) / dim

            def spread_mean(i, carry):
                at = tile(i, wide)
                n = x_ref[:, at].astype(f32) * x_scale
                e = x_out[:, at] * gains_ref[0:1, at]
                x_out[:, at] = dmid[:, at] + x_scale * (e - n * mean)
                return carry

            lax.fori_loop(0, dim // wide, spread_mean, 0)

        def mlp_results(d_tmp, middle, y, y_half):
            middle_in = pltpu.make_async_copy(middle_ref, middle, load.at[0])
            middle_in.start()
            each(MLP_D, lambda piece, group: finish(piece, group, d_tmp))
            d_back = pltpu.make_async_copy(d_tmp, d_out, load.at[1])
            d_back.start()
            line_sum(1, y)
            middle_in.wait()

            def last_add(i, carry):
                at = tile(i, 512)
                y_half[:, at] = (middle[:, at] + y[:, at]).astype(bf16)
                return carry

            lax.fori_loop(0, dim // 512, last_add, 0)
            y_back = pltpu.make_async_copy(y_half, y_out, load.at[2])
            y_back.start()
            each(MLP_D, drain_sibling)
            each(MLP_D, drain)
            d_back.wait()
            y_back.wait()

        small_c = small(0, s_sum.at[3], s_got.at[0], sibling)
        each(MLP_GU, drain_sibling)
        compute(0)
        share(0)
        narrow(3, 0)
        compute(1)
        share(1)
        spread_begin(0)
        compute(2)
        share(2)
        spread(0)
        spread_begin(1)
        relay(1, 1)
        compute(3)
        share(3)
        spread(1)
        spread_begin(2)
        inward_begin(0)
        spread(2)
        spread_begin(3)
        inward(0)
        each(MLP_GU, finish)
        gu_back = pltpu.make_async_copy(gu_all.at[:, 2 * mine + core], gu_out, back.at[0])
        gu_back.start()
        ex_in = pltpu.make_async_copy(gu_all.at[z, 2 * mine + core], ex_land.at[z], back.at[1])
        ex_in.start()
        spread(3)
        each(MLP_GU, drain)
        gu_back.wait()
        exchange(2).start()
        exchange(1).start()
        ex_in.wait()
        compute(4)
        share(4)
        pl.run_scoped(first_norm, pltpu.VMEM((2, 4, shard_rows, qkv_width), bf16))
        small_c.start()
        inward_begin(1)
        compute(5)
        share(5)
        inward(1)
        small_c.wait()
        s_sum[0] = s_sum[3] + s_got[0]
        small_f = small(1, s_sum.at[0], s_got.at[1], first)
        small_f.start()
        spread_begin(4)
        relay(1, 2)
        compute(6)
        share(6)
        spread(4)
        spread_begin(5)
        inward_begin(2)
        compute(7)
        share(7)
        inward(2)
        spread(5)
        spread_begin(6)
        small_f.wait()
        s_sum[1] = s_sum[0] + s_got[1]
        small_s2 = small(2, s_sum.at[1], s_got.at[2], second)
        small_s2.start()
        spread(6)
        spread_begin(7)
        collect_begin(0)
        spread(7)
        collect(0)
        collect_begin(1)
        inward_begin(3)
        collect(1)
        inward(3)
        collect_begin(2)
        collect(2)
        onward(0)
        onward(2)
        collect_begin(3)
        inward_begin(4)
        collect(3)
        inward(4)
        exchange(3).start()
        onward(1)
        pl.run_scoped(
            mlp_results,
            pltpu.VMEM(gd_fst.shape, f32),
            pltpu.VMEM((CAP, dim), f32),
            pltpu.VMEM((CAP, dim), f32),
            pltpu.VMEM((CAP, dim), bf16),
        )
        inward_begin(5)
        collect_begin(4)
        inward(5)
        collect(4)
        inward_begin(6)
        collect_begin(5)
        inward(6)
        collect(5)
        onward(4)
        small_s2.wait()
        s_sum[2] = s_sum[1] + s_got[2]
        small_line = [
            small(2 + k, s_sum.at[2], s_line.at[k], me % RING + RING * lax.rem(z + k, LINE))
            for k in range(1, LINE)
        ]
        for copy in small_line:
            copy.start()
        onward(5)
        inward_begin(7)
        collect_begin(6)
        inward(7)
        collect(6)
        onward(6)
        collect_begin(7)
        collect(7)
        for copy in small_line:
            copy.wait()
        small_out[...] = (s_sum[2] + s_line[2]) + (s_line[1] + s_line[3])
        for k in (6, 7):
            for quad in (far, fst, sec, mine):
                a_sibling(order[k % LINE], quad, k // LINE, k % 2).wait_send()
        for k in range(1, LINE):
            exchange(k).wait_send()
            src_z = lax.rem(z + LINE - k, LINE)
            landed = ex_land.at[src_z]
            remote(landed, landed, ex_s.at[k], ex_r.at[k], sibling).wait_recv()
        for t in range(LINE):
            for h in range(2):
                a_second(t, far, h, 1).wait_send()
                a_second(t, sec, h, 0).wait_send()
                a_first(t, h).wait_send()

                @pl.when(t < z)
                def _(t=t, h=h):
                    a_line(t, h, False).wait_send()

                @pl.when(t > z)
                def _(t=t, h=h):
                    a_line(t, h, True).wait_send()

    slots = CAP
    kv = KVH * HD
    rows = gu_all.shape[2]

    def both(dbr, mixed, normed):
        pl.run_scoped(
            lambda *refs: attention(dbr, mixed, normed, *refs),
            pltpu.VMEM((slots, v0), f32),
            pltpu.VMEM((slots, dim), bf16),
            pltpu.VMEM((slots, kv), bf16),
            pltpu.VMEM((slots, kv), bf16),
            pltpu.VMEM((slots, dim), bf16),
            pltpu.VMEM((slots, dim), f32),
            pltpu.VMEM((slots, dim), bf16),
            pltpu.VMEM((slots, dim), f32),
            pltpu.VMEM((2, 4, rows, dim), bf16),
        )
        pl.run_scoped(
            lambda *refs: sums(dbr, mixed, normed, *refs),
            pltpu.VMEM((2, RING // 2, rows, piece_cols), bf16),
            pltpu.VMEM((8, rows, piece_cols), bf16),
        )

    pl.run_scoped(
        both,
        pltpu.VMEM((slots, dim), bf16),
        pltpu.VMEM((slots, dim), bf16),
        pltpu.VMEM((slots, dim), bf16),
    )

    def a_landed(t, h, upward):
        landing = l_land.at[1 if upward else 0, t, h]
        sems = (au_send, au_recv) if upward else (ad_send, ad_recv)
        return remote(landing, landing, sems[0].at[t, h], sems[1].at[t, h], sibling)

    def results(a_tmp, stage):
        for h in range(2):

            @pl.when(z < last)
            def _(h=h):
                a_landed(z, h, False).wait_recv()

            @pl.when(z > 0)
            def _(h=h):
                a_landed(z, h, True).wait_recv()

        def total(*sides):
            for h in range(2):
                copies = [
                    pltpu.make_async_copy(l_land.at[side, z, h], stage.at[i], stream.at[i])
                    for i, side in enumerate(sides)
                ]
                for copy in copies:
                    copy.start()
                for copy in copies:
                    copy.wait()
                add_rows(
                    a_tmp.at[:, pl.ds(h * piece_cols, piece_cols)],
                    a_own(z, mine, h),
                    *[stage.at[i] for i in range(len(sides))],
                )

        @pl.when(z == 0)
        def _():
            total(0)

        @pl.when(z == last)
        def _():
            total(1)

        @pl.when((z > 0) & (z < last))
        def _():
            total(0, 1)

        a_back = pltpu.make_async_copy(a_tmp, a_out, load.at[3])
        a_back.start()
        a_back.wait()

    pl.run_scoped(
        results,
        pltpu.VMEM((rows, 2 * piece_cols), f32),
        pltpu.VMEM((2, rows, piece_cols), bf16),
    )
    for which in range(2):
        for k in range(LINE):

            @pl.when((z > 0) & (k < z))
            def _(which=which, k=k):
                send_line(t_own.at[which, k], which, k, False).wait_send()

            @pl.when((z < last) & (k > z))
            def _(which=which, k=k):
                send_line(t_own.at[which, k], which, k, True).wait_send()


def backward(gu, wd, tok, cot, hid, pre, w, middle, normed, raw, q, k, v, mixed, x, gains, rope):
    dim = tok.shape[1]
    rows = w.shape[1]
    drows = wd.shape[0] // RING
    cols = gu.shape[1]
    quads = RING // 2
    pieces = LINE + 2
    qkv = raw.shape[1]
    S = jax.ShapeDtypeStruct
    return pl.pallas_call(
        backward_kernel,
        out_shape=(
            S((CAP, dim), f32),
            S((8, dim), f32),
            S((CAP, dim), bf16),
            S((drows, dim), f32),
            S((rows, qkv + dim), f32),
            S((LINE, rows, cols), bf16),
            S((LINE, rows, cols), bf16),
            S((LINE, 2, quads, rows, cols), bf16),
            S((2, LINE, 2, rows, cols), bf16),
            S((LINE, 2, rows, cols), bf16),
            S((2, LINE, 2, rows, cols), bf16),
        ),
        in_specs=[ANY] * 14 + [VMEM] * 3,
        out_specs=(VMEM,) * 2 + (ANY,) * 9,
        scratch_shapes=[
            pltpu.VMEM((LINE, RING, rows, cols), bf16),
            pltpu.VMEM((RING, drows, dim), bf16),
            pltpu.VMEM((quads, LINE, rows, cols), bf16),
            pltpu.VMEM((quads, drows, dim), bf16),
            pltpu.VMEM((2, LINE, rows, cols), bf16),
            pltpu.VMEM((2, drows, dim), bf16),
            pltpu.VMEM((LINE, rows, cols), bf16),
            pltpu.VMEM((drows, dim), bf16),
            pltpu.VMEM((2, LINE, CAP, dim), bf16),
            pltpu.VMEM((2, LINE + 1, CAP, dim), bf16),
            pltpu.VMEM((CAP, dim), f32),
            pltpu.VMEM((CAP, qkv), bf16),
            pltpu.VMEM((4, 8, dim), f32),
            pltpu.VMEM((3, 8, dim), f32),
            pltpu.VMEM((LINE, 8, dim), f32),
            DMA((quads, pieces)),
            DMA((quads, pieces)),
            DMA((2, pieces)),
            DMA((2, pieces)),
            DMA((pieces,)),
            DMA((pieces,)),
            DMA((2, LINE)),
            DMA((2, LINE)),
            DMA((2, LINE)),
            DMA((2, LINE)),
            DMA((8,)),
            DMA((3,)),
            DMA((2,)),
            DMA((2, quads)),
            DMA((LINE, 2, quads)),
            DMA((2, LINE, 2)),
            DMA((2, LINE, 2)),
            DMA((LINE, 2)),
            DMA((LINE, 2)),
            DMA((LINE, 2)),
            DMA((LINE, 2)),
            DMA((LINE, 2)),
            DMA((LINE, 2)),
            DMA((LINE,)),
            DMA((LINE,)),
            DMA((2 + LINE,)),
            DMA((2 + LINE,)),
            DMA((2, 3)),
            DMA((8,)),
        ],
        compiler_params=pltpu.CompilerParams(
            collective_id=2, has_side_effects=True, vmem_limit_bytes=65400 * 1024
        ),
        name="backward",
    )(gu, wd, tok, cot, hid, pre, w, middle, normed, raw, q, k, v, mixed, x, gains, rope)


def results_kernel(
    y_ref, x_ref, small_ref, d_ref, a_ref, ex_ref,
    y_out, x_out, q_out, k_out, v_out, o_out, gate_out, up_out, d_out, ga_out, gq_out, gk_out, gm_out,
    y_tmp, x_tmp, small, d_tmp, a_tmp, ex_tmp, gate_tmp, up_tmp, sem_in, sem_out,
):
    me = lax.axis_index("fsdp")
    width = ex_tmp.shape[2] // 2
    moves = ((small_ref, small), (ex_ref, ex_tmp), (a_ref, a_tmp), (d_ref, d_tmp), (x_ref, x_tmp), (y_ref, y_tmp))
    ins = [pltpu.make_async_copy(src, dst, sem_in.at[i]) for i, (src, dst) in enumerate(moves)]
    for copy in ins:
        copy.start()
    outs = []

    def leave(src, dst):
        copy = pltpu.make_async_copy(src, dst, sem_out.at[len(outs)])
        copy.start()
        outs.append(copy)

    ins[1].wait()
    for k in range(LINE):
        add_rows(gate_tmp.at[:, pl.ds(k * width, width)], ex_tmp.at[k, :, pl.ds(0, width)])
        add_rows(up_tmp.at[:, pl.ds(k * width, width)], ex_tmp.at[k, :, pl.ds(width, width)])
    leave(gate_tmp, gate_out)
    leave(up_tmp, up_out)
    ins[2].wait()
    lo = 0
    for out in (q_out, k_out, v_out, o_out):
        leave(a_tmp.at[:, pl.ds(lo, out.shape[1])], out)
        lo += out.shape[1]
    ins[3].wait()
    leave(d_tmp, d_out)
    ins[4].wait()
    leave(x_tmp, x_out)
    ins[5].wait()
    leave(y_tmp, y_out)
    ins[0].wait()
    for row, out in ((3, ga_out), (1, gq_out), (2, gk_out), (0, gm_out)):
        count = out.shape[1]
        value = jnp.zeros((1, 128), f32)
        for i in range(small.shape[1] // 128):
            held = small[row : row + 1, i * 128 : (i + 1) * 128]
            value = jnp.where((me * count) // 128 == i, held, value)
        value = pltpu.roll(value, (128 - (me * count) % 128) % 128, 1)
        out[...] = value[:, 0:count]
    for copy in outs:
        copy.wait()


def results(y, x, small, d, a, ex, widths, shares):
    rows = a.shape[0]
    wide = LINE * ex.shape[2] // 2
    S = jax.ShapeDtypeStruct
    return pl.pallas_call(
        results_kernel,
        out_shape=(
            S(y.shape, bf16),
            S(x.shape, f32),
            *[S((rows, w), f32) for w in widths],
            S((rows, wide), f32),
            S((rows, wide), f32),
            S(d.shape, f32),
            *[S((1, s), f32) for s in shares],
        ),
        in_specs=[ANY] * 6,
        out_specs=(ANY,) * 9 + (VMEM,) * 4,
        scratch_shapes=[
            pltpu.VMEM(y.shape, bf16),
            pltpu.VMEM(x.shape, f32),
            pltpu.VMEM(small.shape, f32),
            pltpu.VMEM(d.shape, f32),
            pltpu.VMEM(a.shape, f32),
            pltpu.VMEM(ex.shape, bf16),
            pltpu.VMEM((rows, wide), f32),
            pltpu.VMEM((rows, wide), f32),
            DMA((6,)),
            DMA((9,)),
        ],
        name="results",
    )(y, x, small, d, a, ex)


def layout(seq_lengths, seq_device, owner, slots):
    owned = seq_device == owner
    counts = jnp.where(owned, seq_lengths, 0)
    starts = jnp.cumsum(counts) - counts
    places = jnp.arange(slots, dtype=jnp.int32)
    inside = (
        owned[:, None]
        & (places[None, :] >= starts[:, None])
        & (places[None, :] < (starts + counts)[:, None])
    )
    labels = jnp.arange(seq_lengths.shape[0], dtype=jnp.int32)
    segment = jnp.sum(jnp.where(inside, labels[:, None] + 1, 0), axis=0) - 1
    position = jnp.sum(jnp.where(inside, places[None, :] - starts[:, None], 0), axis=0)
    return (segment, position)


def allowed_pairs(segment):
    places = jnp.arange(segment.shape[0], dtype=jnp.int32)
    earlier = places[None, :] < places[:, None]
    same_seq = (segment[:, None] == segment[None, :]) & (segment[:, None] >= 0)
    return (places[:, None] == places[None, :]) | earlier & same_seq


def rmsnorm(values, gain):
    return values * lax.rsqrt(jnp.mean(values * values, axis=-1, keepdims=True) + epsilon) * gain


def rotary(values, position):
    half_dim = values.shape[-1] // 2
    freqs = jnp.power(rope_base, -2.0 * jnp.arange(half_dim, dtype=jnp.float32) / values.shape[-1])
    angles = position.astype(jnp.float32)[:, None] * freqs[None, :]
    cosine = jnp.concatenate([jnp.cos(angles), jnp.cos(angles)], axis=-1)[:, None, :]
    sine = jnp.concatenate([jnp.sin(angles), jnp.sin(angles)], axis=-1)[:, None, :]
    rotated = jnp.concatenate([-values[..., half_dim:], values[..., :half_dim]], axis=-1)
    return values * cosine + rotated * sine


def matmul(left, right):
    return jnp.dot(left, right, preferred_element_type=jnp.float32)


def times_rows(left, right):
    return lax.dot_general(left, right, contract_rows, preferred_element_type=jnp.float32)


def times_cols(left, right):
    return lax.dot_general(left, right, contract_cols, preferred_element_type=jnp.float32)


def scatter_sum(partial):
    total = lax.psum_scatter(
        partial.astype(jnp.bfloat16), "fsdp", scatter_dimension=0, tiled=True
    )
    return total.astype(jnp.float32)


def plain(
    hidden_in,
    out_grad,
    seq_lengths,
    seq_device,
    attn_gain,
    q_gain,
    k_gain,
    w_query,
    w_key,
    w_value,
    w_out,
    mlp_gain,
    w_gate,
    w_up,
    w_down,
):
    slots = hidden_in.shape[0]
    groups = H // KVH
    score_scale = HD ** (-0.5)
    segment, position = layout(seq_lengths, seq_device, lax.axis_index("fsdp"), slots)
    allowed = allowed_pairs(segment)[None, None]

    def query_path(raw, gain):
        return rotary(rmsnorm(raw.reshape(slots, H, HD), gain), position)

    def key_path(raw, gain):
        return rotary(rmsnorm(raw.reshape(slots, KVH, HD), gain), position)

    def swiglu(gate_in, up_in):
        return jax.nn.silu(gate_in) * up_in

    attn_set = (
        lax.all_gather(attn_gain, "fsdp", axis=0, tiled=True),
        lax.all_gather(q_gain, "fsdp", axis=0, tiled=True),
        lax.all_gather(k_gain, "fsdp", axis=0, tiled=True),
        lax.all_gather(w_query, "fsdp", axis=0, tiled=True),
        lax.all_gather(w_key, "fsdp", axis=0, tiled=True),
        lax.all_gather(w_value, "fsdp", axis=0, tiled=True),
        lax.all_gather(w_out, "fsdp", axis=0, tiled=True),
    )
    gain_attn, gain_query, gain_key, query_w, key_w, value_w, out_w = attn_set
    inputs = hidden_in.astype(jnp.float32)
    normed = rmsnorm(inputs, gain_attn.astype(jnp.float32)).astype(jnp.bfloat16)
    query_raw = matmul(normed, query_w)
    key_raw = matmul(normed, key_w)
    value_raw = matmul(normed, value_w)
    queries = (
        query_path(query_raw, gain_query.astype(jnp.float32))
        .astype(jnp.bfloat16)
        .reshape(slots, KVH, groups, HD)
    )
    keys = key_path(key_raw, gain_key.astype(jnp.float32)).astype(jnp.bfloat16)
    values = value_raw.astype(jnp.bfloat16).reshape(slots, KVH, HD)

    def masked_logits():
        scores = (
            jnp.einsum("qgrd,kgd->grqk", queries, keys, preferred_element_type=jnp.float32)
            * score_scale
        )
        return jnp.where(allowed, scores, masked_score)

    logits = masked_logits()
    row_top = jnp.max(logits, axis=-1, keepdims=True)
    exponent = jnp.exp(logits - row_top)
    row_total = jnp.sum(exponent, axis=-1, keepdims=True)
    log_total = row_top + jnp.log(row_total)
    weights = (exponent / row_total).astype(jnp.bfloat16)
    mixed = jnp.einsum("grqk,kgd->qgrd", weights, values, preferred_element_type=jnp.float32)
    mixed = mixed.reshape(slots, H * HD).astype(jnp.bfloat16)
    middle = inputs + matmul(mixed, out_w)
    mlp_set = (
        lax.all_gather(mlp_gain, "fsdp", axis=0, tiled=True),
        lax.all_gather(w_gate, "fsdp", axis=0, tiled=True),
        lax.all_gather(w_up, "fsdp", axis=0, tiled=True),
        lax.all_gather(w_down, "fsdp", axis=0, tiled=True),
    )
    gain_mlp, gate_w, up_w, down_w = mlp_set
    second = rmsnorm(middle, gain_mlp.astype(jnp.float32)).astype(jnp.bfloat16)
    gate_out = matmul(second, gate_w)
    up_out = matmul(second, up_w)
    hidden = swiglu(gate_out, up_out).astype(jnp.bfloat16)
    hidden_out = (middle + matmul(hidden, down_w)).astype(jnp.bfloat16)
    gain_mlp, gate_w, up_w, down_w = (
        lax.all_gather(mlp_gain, "fsdp", axis=0, tiled=True),
        lax.all_gather(w_gate, "fsdp", axis=0, tiled=True),
        lax.all_gather(w_up, "fsdp", axis=0, tiled=True),
        lax.all_gather(w_down, "fsdp", axis=0, tiled=True),
    )
    grad_down = scatter_sum(times_rows(hidden, out_grad))
    d_hidden = times_cols(out_grad, down_w)
    unused_out, swiglu_pull = jax.vjp(swiglu, gate_out, up_out)
    d_gate, d_up = swiglu_pull(d_hidden)
    d_gate_up = jnp.concatenate([d_gate.astype(jnp.bfloat16), d_up.astype(jnp.bfloat16)], axis=1)
    grad_gate_up = scatter_sum(times_rows(second, d_gate_up))
    ff_width = gate_w.shape[1]
    d_second = times_cols(d_gate_up, jnp.concatenate([gate_w, up_w], axis=1))
    unused_norm, second_pull = jax.vjp(rmsnorm, middle, gain_mlp.astype(jnp.float32))
    d_middle_norm, grad_gain_mlp = second_pull(d_second)
    d_middle = out_grad.astype(jnp.float32) + d_middle_norm
    gain_attn, gain_query, gain_key, query_w, key_w, value_w, out_w = (
        lax.all_gather(attn_gain, "fsdp", axis=0, tiled=True),
        lax.all_gather(q_gain, "fsdp", axis=0, tiled=True),
        lax.all_gather(k_gain, "fsdp", axis=0, tiled=True),
        lax.all_gather(w_query, "fsdp", axis=0, tiled=True),
        lax.all_gather(w_key, "fsdp", axis=0, tiled=True),
        lax.all_gather(w_value, "fsdp", axis=0, tiled=True),
        lax.all_gather(w_out, "fsdp", axis=0, tiled=True),
    )
    d_branch = d_middle.astype(jnp.bfloat16)
    grad_out_w = scatter_sum(times_rows(mixed, d_branch))
    d_mixed = times_cols(d_branch, out_w).astype(jnp.bfloat16).reshape(slots, KVH, groups, HD)
    probs = jnp.exp(masked_logits() - log_total)
    weights = probs.astype(jnp.bfloat16)
    d_probs = jnp.einsum("qgrd,kgd->grqk", d_mixed, values, preferred_element_type=jnp.float32)
    d_logits = probs * (d_probs - jnp.sum(probs * d_probs, axis=-1, keepdims=True))
    d_scores = (d_logits * score_scale).astype(jnp.bfloat16)
    d_values = jnp.einsum("grqk,qgrd->kgd", weights, d_mixed, preferred_element_type=jnp.float32)
    d_values = d_values.astype(jnp.bfloat16).reshape(slots, KVH * HD)
    d_queries_rot = jnp.einsum(
        "grqk,kgd->qgrd", d_scores, keys, preferred_element_type=jnp.float32
    ).reshape(slots, H, HD)
    d_keys_rot = jnp.einsum("grqk,qgrd->kgd", d_scores, queries, preferred_element_type=jnp.float32)
    unused_query, query_pull = jax.vjp(query_path, query_raw, gain_query.astype(jnp.float32))
    d_query_raw, grad_gain_query = query_pull(d_queries_rot)
    unused_key, key_pull = jax.vjp(key_path, key_raw, gain_key.astype(jnp.float32))
    d_key_raw, grad_gain_key = key_pull(d_keys_rot)
    d_qkv = jnp.concatenate(
        [d_query_raw.astype(jnp.bfloat16), d_key_raw.astype(jnp.bfloat16), d_values], axis=1
    )
    grad_qkv = scatter_sum(times_rows(normed, d_qkv))
    d_normed = times_cols(d_qkv, jnp.concatenate([query_w, key_w, value_w], axis=1))
    unused_first, first_pull = jax.vjp(rmsnorm, inputs, gain_attn.astype(jnp.float32))
    d_input_norm, grad_gain_attn = first_pull(d_normed)
    input_grad = d_middle + d_input_norm
    gain_sums = (
        lax.psum_scatter(grad_gain_attn, "fsdp", scatter_dimension=0, tiled=True),
        lax.psum_scatter(grad_gain_query, "fsdp", scatter_dimension=0, tiled=True),
        lax.psum_scatter(grad_gain_key, "fsdp", scatter_dimension=0, tiled=True),
        lax.psum_scatter(grad_gain_mlp, "fsdp", scatter_dimension=0, tiled=True),
    )
    query_width = H * HD
    key_width = KVH * HD
    grad_query_w = grad_qkv[:, :query_width]
    grad_key_w = grad_qkv[:, query_width : query_width + key_width]
    grad_value_w = grad_qkv[:, query_width + key_width :]
    grad_gate = grad_gate_up[:, :ff_width]
    grad_up = grad_gate_up[:, ff_width:]
    return (
        hidden_out,
        input_grad,
        gain_sums[0],
        gain_sums[1],
        gain_sums[2],
        grad_query_w,
        grad_key_w,
        grad_value_w,
        grad_out_w,
        gain_sums[3],
        grad_gate,
        grad_up,
        grad_down,
    )


def layered(
    hidden_in,
    out_grad,
    seq_lengths,
    seq_device,
    attn_gain,
    q_gain,
    k_gain,
    w_query,
    w_key,
    w_value,
    w_out,
    mlp_gain,
    w_gate,
    w_up,
    w_down,
):
    (
        attn_w, gate_up_w, down_w, tokens, cotangent, hidden, gate_up,
        middle, normed, qkv_raw, queries, keys, values, mixed, gains, rope,
    ) = forward(
        hidden_in, out_grad, seq_lengths, seq_device, (attn_gain, mlp_gain, q_gain, k_gain),
        w_query, w_key, w_value, w_out, w_gate, w_up, w_down,
    )
    dim = hidden_in.shape[1]
    x, small, y, grad_down, attn_sums, exchanged, *unused = backward(
        gate_up_w.reshape(-1, gate_up_w.shape[-1]),
        down_w.reshape(-1, dim),
        tokens.reshape(-1, dim),
        cotangent.reshape(-1, dim),
        hidden, gate_up, attn_w, middle, normed, qkv_raw, queries, keys, values, mixed,
        hidden_in, gains, rope,
    )
    (
        hidden_out, input_grad, g_query, g_key, g_value, g_out, g_gate, g_up, g_down,
        g_attn_gain, g_q_gain, g_k_gain, g_mlp_gain,
    ) = results(
        y, x, small, grad_down, attn_sums, exchanged,
        [w.shape[1] for w in (w_query, w_key, w_value, w_out)],
        [g.shape[0] for g in (attn_gain, q_gain, k_gain, mlp_gain)],
    )
    return (
        hidden_out,
        input_grad,
        g_attn_gain[0],
        g_q_gain[0],
        g_k_gain[0],
        g_query,
        g_key,
        g_value,
        g_out,
        g_mlp_gain[0],
        g_gate,
        g_up,
        g_down,
    )


def solution(mesh):
    per_device = layered if mesh.shape["fsdp"] == RING * LINE else plain
    return jax.shard_map(
        per_device,
        mesh=mesh,
        in_specs=(
            P("fsdp", None),
            P("fsdp", None),
            P(),
            P(),
            P("fsdp"),
            P("fsdp"),
            P("fsdp"),
            P("fsdp", None),
            P("fsdp", None),
            P("fsdp", None),
            P("fsdp", None),
            P("fsdp"),
            P("fsdp", None),
            P("fsdp", None),
            P("fsdp", None),
        ),
        out_specs=(
            P("fsdp", None),
            P("fsdp", None),
            P("fsdp"),
            P("fsdp"),
            P("fsdp"),
            P("fsdp", None),
            P("fsdp", None),
            P("fsdp", None),
            P("fsdp", None),
            P("fsdp"),
            P("fsdp", None),
            P("fsdp", None),
            P("fsdp", None),
        ),
        check_vma=False,
    )
```

```python
import math

import jax
import jax.numpy as jnp
from jax import lax
from jax.experimental import pallas as pl
from jax.experimental.pallas import tpu as pltpu
from jax.sharding import PartitionSpec as P

H = 16
KVH = 8
HD = 128
CAP = 128
LINE = 4
RING = 8
MESH = pl.DeviceIdType.MESH
ANY = pl.BlockSpec(memory_space=pl.ANY)
VMEM = pl.BlockSpec(memory_space=pltpu.VMEM)
DMA = pltpu.SemaphoreType.DMA
bf16 = jnp.bfloat16
f32 = jnp.float32
epsilon = 1e-06
rope_base = 1000000.0
masked_score = -1e30
contract_rows = (((0,), (0,)), ((), ()))
contract_cols = (((1,), (1,)), ((), ()))


def where_am_i():
    me = lax.axis_index("fsdp")
    core = me % 2
    z = me // RING
    f_bit = 2 + 2 * core
    s_bit = 4 - 2 * core
    first = me + f_bit * (1 - 2 * ((me // f_bit) % 2))
    second = me + s_bit * (1 - 2 * ((me // s_bit) % 2))
    sibling = me + 1 - 2 * core
    return me, z, first, second, sibling


def greet(peers):
    barrier = pltpu.get_barrier_semaphore()
    for peer in peers:
        pl.semaphore_signal(barrier, inc=1, device_id=(peer,), device_id_type=MESH)
    pl.semaphore_wait(barrier, len(peers))


def remote(src, dst, send_sem, recv_sem, device):
    return pltpu.make_async_remote_copy(
        src_ref=src,
        dst_ref=dst,
        send_sem=send_sem,
        recv_sem=recv_sem,
        device_id=(device,),
        device_id_type=MESH,
    )


def line_peers(me):
    return [lax.rem(me + RING * k, RING * LINE) for k in range(1, LINE)]


def on_line(z, k, body):
    for step in ((-k, k) if k else (0,)):

        @pl.when((z + step >= 0) & (z + step < LINE))
        def _(step=step):
            body(step)


def dot_nt(left, right):
    return lax.dot_general(left, right, contract_cols, preferred_element_type=f32)


def dot_tn(left, right):
    return lax.dot_general(left, right, contract_rows, preferred_element_type=f32)


def streamed(count, fetch, body):
    for copy in fetch(0, 0):
        copy.start()

    def step(i, carry):
        slot = i % 2

        @pl.when(i + 1 < count)
        def _():
            for copy in fetch(i + 1, 1 - slot):
                copy.start()

        for copy in fetch(i, slot):
            copy.wait()
        body(i, slot)
        return carry

    lax.fori_loop(0, count, step, 0)


def tile(i, size):
    return pl.ds(pl.multiple_of(i * size, size), size)


def add_rows(out, *terms):
    rows = out.shape[0]

    def body(i, carry):
        at = pl.ds(pl.multiple_of(i * 16, 16), 16)
        total = terms[0][at, :].astype(f32)
        for term in terms[1:]:
            total = total + term[at, :].astype(f32)
        out[at, :] = total.astype(out.dtype)
        return carry

    lax.fori_loop(0, rows // 16, body, 0)


def lane_sum(x):
    return jnp.sum(x, axis=-1, keepdims=True)


def token_places(lengths, devices, me):
    seqs = lengths.shape[1]
    counts_row = jnp.where(devices == me, lengths, 0).astype(f32)
    up = lax.broadcasted_iota(jnp.int32, (seqs, seqs), 0)
    across = lax.broadcasted_iota(jnp.int32, (seqs, seqs), 1)
    counts_col = lane_sum(jnp.where(up == across, counts_row, 0.0))
    starts_row = jnp.sum(jnp.where(up < across, counts_col, 0.0), axis=0, keepdims=True)
    starts_col = lane_sum(jnp.where(across < up, counts_row, 0.0))

    def within(places, starts, counts):
        return (places >= starts) & (places < starts + counts)

    places = lax.broadcasted_iota(jnp.int32, (CAP, seqs), 0).astype(f32)
    labels = lax.broadcasted_iota(jnp.int32, (CAP, seqs), 1).astype(f32)
    inside = within(places, starts_row, counts_row)
    segment_col = lane_sum(jnp.where(inside, labels + 1.0, 0.0)) - 1.0
    position = lane_sum(jnp.where(inside, places - starts_row, 0.0))
    places = lax.broadcasted_iota(jnp.int32, (seqs, CAP), 1).astype(f32)
    labels = lax.broadcasted_iota(jnp.int32, (seqs, CAP), 0).astype(f32)
    inside = within(places, starts_col, counts_col)
    segment_row = jnp.sum(jnp.where(inside, labels + 1.0, 0.0), axis=0, keepdims=True) - 1.0
    return segment_col, segment_row, position


def allowed_bias(segment_col, segment_row):
    t = lax.broadcasted_iota(jnp.int32, (CAP, CAP), 0)
    u = lax.broadcasted_iota(jnp.int32, (CAP, CAP), 1)
    same = (segment_col == segment_row) & (segment_col >= 0.0)
    return jnp.where((t == u) | ((u < t) & same), 0.0, masked_score)


def half_turn(v):
    lane = lax.broadcasted_iota(jnp.int32, v.shape, v.ndim - 1)
    turned = pltpu.roll(v, HD // 2, v.ndim - 1)
    return jnp.where(lane < HD // 2, -turned, turned)


def rms_scale(v):
    return lax.rsqrt(jnp.mean(v * v, axis=-1, keepdims=True) + epsilon)


def forward_kernel(
    x_ref, len_ref, dev_ref, ga_ref, gm_ref, gq_ref, gk_ref, cot_ref,
    wq_ref, wk_ref, wv_ref, wo_ref, gate_ref, up_ref, wd_ref,
    w_out, gu_out, d_out, tok_out, cot_out, hid_out, pre_out,
    middle_out, normed_out, raw_out, q_out, k_out, v_out, mixed_out, gains_out, rope_out,
    w_tmp, p_tmp, d_tmp, cot_tmp, second_tmp, chunk, ow_all, gain_tmp, gain_own,
    tok_all, gate_up, m_chunk, hid,
    local, up_s, down_s, first_s, second_s, sib_s, recv, ex_send, ex_recv,
    m_first_s, m_second_s, m_sib_s, m_recv, line_up, line_down, line_r, w_load, o_load, g_load,
    act_out,
):
    me, z, first, second, sibling = where_am_i()
    col, fcol, scol = me % RING, first % RING, second % RING
    sfcol = (second + first - me) % RING
    width = p_tmp.shape[2] // 2
    rows = w_tmp.shape[0]
    qkv_width = raw_out.shape[1]
    attn_width = qkv_width + wo_ref.shape[1]
    last = LINE - 1
    pieces = LINE + 1

    w_in = []
    lo = 0
    for i, ref in enumerate((wq_ref, wk_ref, wv_ref, wo_ref)):
        at = pl.ds(lo, ref.shape[1])
        w_in.append(pltpu.make_async_copy(ref, w_tmp.at[:, at], local.at[i]))
        lo += ref.shape[1]
    p_in = [
        pltpu.make_async_copy(
            ref.at[:, pl.ds(pl.multiple_of(z * width, width), width)],
            p_tmp.at[z, :, pl.ds(which * width, width)],
            local.at[5 + which],
        )
        for which, ref in enumerate((gate_ref, up_ref))
    ]
    cot_in = pltpu.make_async_copy(cot_ref, cot_tmp, local.at[8])
    d_in = pltpu.make_async_copy(wd_ref, d_tmp, local.at[7])
    for copy in w_in + p_in + [d_in, cot_in]:
        copy.start()
    gain_own[...] = jnp.zeros_like(gain_own)
    for i, ref in enumerate((ga_ref, gm_ref, gq_ref, gk_ref)):
        gain_own[i : i + 1, 0 : ref.shape[1]] = ref[...].astype(f32)
    flat = gain_own[...]
    paired = jnp.where(me % 2 == 0, flat, pltpu.roll(flat, rows, 1))
    shared = pltpu.roll(flat, gq_ref.shape[1] * me, 1)
    placed = jnp.where(lax.broadcasted_iota(jnp.int32, flat.shape, 0) < 2, paired, shared)
    w_tmp[0:16, attn_width:] = placed.astype(bf16)
    w_tmp[16:, attn_width:] = jnp.zeros((rows - 16, 128), bf16)
    greet(line_peers(me) + [first, second, sibling])

    def send(src, shard, sems, device):
        return remote(src, w_out.at[shard], sems.at[shard], recv.at[shard], device)

    def arrived(shard):
        send(w_out.at[shard], shard, sib_s, sibling).wait_recv()

    def exchange(k, which):
        peer_z = lax.rem(z + k, LINE)
        src = (gate_ref, up_ref)[which].at[:, pl.ds(pl.multiple_of(peer_z * width, width), width)]
        dst = p_tmp.at[z, :, pl.ds(which * width, width)]
        return remote(src, dst, ex_send.at[k, which], ex_recv.at[k, which], col + RING * peer_z)

    token_half = second_tmp.shape[1] // 2

    def line_spot(which, shard):
        if which == 1:
            return cot_out.at[shard]
        return tok_out.at[shard, :, pl.ds(token_half * (which // 2), token_half)]

    def line_send(src, which, shard, sems, device):
        landing = line_spot(which, shard)
        return remote(src, landing, sems.at[which, shard], line_r.at[which, shard], device)

    def line_own(which, src):
        @pl.when(z < last)
        def _():
            line_send(src, which, z, line_up, me + RING).start()

        @pl.when(z > 0)
        def _():
            line_send(src, which, z, line_down, me - RING).start()

    def line_relay(which, k):
        def body(step):
            shard = z + step
            src = line_spot(which, shard)
            line_send(src, which, shard, line_up, second).wait_recv()
            if step < 0:

                @pl.when(z < last)
                def _():
                    line_send(src, which, shard, line_up, me + RING).start()
            else:

                @pl.when(z > 0)
                def _():
                    line_send(src, which, shard, line_down, me - RING).start()

        on_line(z, k, body)

    for copy in w_in:
        copy.wait()

    @pl.when(z < last)
    def _():
        send(w_tmp, me, up_s, me + RING).start()

    @pl.when(z > 0)
    def _():
        send(w_tmp, me, down_s, me - RING).start()

    send(w_tmp, me, first_s, first).start()
    send(w_tmp, me, second_s, second).start()
    send(w_tmp, me, sib_s, sibling).start()
    w_back = pltpu.make_async_copy(w_tmp, w_out.at[me], local.at[9])
    w_back.start()

    def own(k):
        def body(step):
            shard = me + RING * step
            src = w_out.at[shard]
            arrived(shard)
            if step < 0:

                @pl.when(z < last)
                def _():
                    send(src, shard, up_s, me + RING).start()
            else:

                @pl.when(z > 0)
                def _():
                    send(src, shard, down_s, me - RING).start()

            send(src, shard, first_s, first).start()
            send(src, shard, second_s, second).start()
            send(src, shard, sib_s, sibling).start()

        on_line(z, k, body)

    def other(base, k, onward):
        def body(step):
            shard = base + RING * (z + step)
            src = w_out.at[shard]
            arrived(shard)
            if onward:
                send(src, shard, second_s, second).start()
            send(src, shard, sib_s, sibling).start()

        on_line(z, k, body)

    segment_col, segment_row, position = token_places(len_ref[...], dev_ref[...], me)
    rope_out[2] = allowed_bias(segment_col, segment_row)
    lane = lax.broadcasted_iota(jnp.int32, (1, HD), 1) % (HD // 2)
    angles = position * jnp.exp(lane.astype(f32) * (-2.0 * math.log(rope_base) / HD))
    rope_out[0] = jnp.cos(angles)
    rope_out[1] = jnp.sin(angles)
    x_scale = rms_scale(x_ref[...].astype(f32))
    raw_out[...] = jnp.zeros_like(raw_out)

    def load_group(step):
        zz = z + step
        part = w_out.at[pl.ds(RING * zz, RING)]
        return (
            pltpu.make_async_copy(part.at[:, :, pl.ds(0, qkv_width)], chunk, w_load),
            pltpu.make_async_copy(
                part.at[:, :, pl.ds(qkv_width, attn_width - qkv_width)],
                ow_all.at[pl.ds(RING * zz, RING)],
                o_load.at[zz],
            ),
            pltpu.make_async_copy(
                part.at[:, pl.ds(0, 16), pl.ds(attn_width, 128)], gain_tmp.at[zz], g_load
            ),
        )

    def group(k):
        def body(step):
            zz = z + step
            for i in range(RING // 2):
                arrived(RING * zz + 2 * i + sibling % 2)
            copies = load_group(step)
            for copy in copies:
                copy.start()
            copies[2].wait()
            span = RING * rows
            for pair in range(RING // 2):
                at = pl.ds(pl.multiple_of(zz * span + pair * 128, 128), 128)
                both = gain_tmp[zz, 2 * pair].astype(f32) + gain_tmp[zz, 2 * pair + 1].astype(f32)
                gains_out[0:2, at] = both[0:2]
                piece = x_ref[:, at].astype(f32) * x_scale * both[0:1]
                normed_out[:, at] = piece.astype(bf16)
            copies[0].wait()
            left = normed_out[:, pl.ds(pl.multiple_of(zz * span, span), span)]

            def tile(i, carry):
                at = pl.ds(pl.multiple_of(i * 512, 512), 512)
                right = chunk[:, :, at].reshape(span, 512)
                raw_out[:, at] += jnp.dot(left, right, preferred_element_type=f32)
                return carry

            lax.fori_loop(0, qkv_width // 512, tile, 0)

        on_line(z, k, body)

    own(1)
    other(fcol, 0, True)
    own(2)
    other(fcol, 1, True)
    other(scol, 0, False)
    for k in range(1, LINE):
        for which in range(2):
            exchange(k, which).start()
    cot_in.wait()
    line_own(1, cot_tmp)
    cot_back = pltpu.make_async_copy(cot_tmp, cot_out.at[z], local.at[10])
    cot_back.start()
    own(3)
    other(fcol, 2, True)
    other(scol, 1, False)
    other(sfcol, 0, False)
    w_back.wait()
    line_relay(1, 1)
    group(0)
    other(fcol, 3, True)
    other(scol, 2, False)
    other(sfcol, 1, False)
    for copy in p_in + [d_in]:
        copy.wait()
    for k in range(1, LINE):
        for which in range(2):
            src_z = lax.rem(z + LINE - k, LINE)
            landed = p_tmp.at[src_z, :, pl.ds(which * width, width)]
            remote(landed, landed, ex_send.at[k, which], ex_recv.at[k, which], second).wait_recv()

    def spot(piece, shard):
        return gu_out.at[piece, shard] if piece < LINE else d_out.at[shard]

    def source(piece):
        return p_tmp.at[piece] if piece < LINE else d_tmp

    def m_send(src, piece, shard, sems, device):
        return remote(
            src, spot(piece, shard), sems.at[piece, shard], m_recv.at[piece, shard], device
        )

    def m_arrived(piece, shard):
        m_send(spot(piece, shard), piece, shard, m_sib_s, sibling).wait_recv()

    def m_own_second(piece):
        m_send(source(piece), piece, col, m_second_s, second).start()

    def m_own_first(piece):
        m_send(source(piece), piece, col, m_first_s, first).start()
        m_send(source(piece), piece, col, m_sib_s, sibling).start()

    def m_own(piece):
        m_own_second(piece)
        m_own_first(piece)

    m_own_second(0)
    m_own_second(1)
    m_own_second(LINE)
    p_back = pltpu.make_async_copy(p_tmp, gu_out.at[:, col], local.at[11])
    p_back.start()
    d_back = pltpu.make_async_copy(d_tmp, d_out.at[col], local.at[4])
    d_back.start()
    line_relay(1, 2)
    group(1)

    other(scol, 3, False)
    other(sfcol, 2, False)
    group(2)
    other(sfcol, 3, False)
    m_own_first(0)
    m_own_first(1)
    m_own_first(LINE)
    line_relay(1, 3)
    group(3)

    small = jnp.zeros((16, 128), f32)
    for zz in range(LINE):
        for i in range(RING):
            small = small + gain_tmp[zz, i].astype(f32)
    q_gain, k_gain = small[2:3], small[3:4]
    gains_out[2:4, 0:128] = small[2:4]
    cosine, sine, bias = rope_out[0], rope_out[1], rope_out[2]

    def turned(v, gain):
        v = v * rms_scale(v) * gain
        return (v * cosine + half_turn(v) * sine).astype(bf16)

    kv0 = H * HD
    v0 = kv0 + KVH * HD

    def head(g, carry):
        at = pl.ds(pl.multiple_of(g * HD, HD), HD)
        qa = pl.ds(pl.multiple_of(g * 2 * HD, 2 * HD), HD)
        qb = pl.ds(pl.multiple_of(g * 2 * HD + HD, HD), HD)
        key = turned(raw_out[:, pl.ds(pl.multiple_of(kv0 + g * HD, HD), HD)], k_gain)
        value = raw_out[:, pl.ds(pl.multiple_of(v0 + g * HD, HD), HD)].astype(bf16)
        k_out[:, at] = key
        v_out[:, at] = value
        query_a = turned(raw_out[:, qa], q_gain)
        query_b = turned(raw_out[:, qb], q_gain)
        q_out[:, qa] = query_a
        q_out[:, qb] = query_b
        for query, where in ((query_a, qa), (query_b, qb)):
            scores = lax.dot_general(query, key, contract_cols, preferred_element_type=f32)
            logits = scores * (HD ** (-0.5)) + bias
            exponent = jnp.exp(logits - jnp.max(logits, axis=-1, keepdims=True))
            weights = (exponent / lane_sum(exponent)).astype(bf16)
            mixed = jnp.dot(weights, value, preferred_element_type=f32)
            mixed_out[:, where] = mixed.astype(bf16)
        return carry

    lax.fori_loop(0, KVH, head, 0, unroll=2)
    for zz in range(LINE):
        pltpu.make_async_copy(
            w_out.at[pl.ds(RING * zz, RING), :, pl.ds(qkv_width, attn_width - qkv_width)],
            ow_all.at[pl.ds(RING * zz, RING)],
            o_load.at[zz],
        ).wait()
    mixed = mixed_out[...]

    def out_tile(i, total):
        at = pl.ds(pl.multiple_of(i * 512, 512), 512)
        right = ow_all[:, :, at].reshape(mixed.shape[1], 512)
        middle = x_ref[:, at].astype(f32) + jnp.dot(mixed, right, preferred_element_type=f32)
        middle_out[:, at] = middle
        return total + lane_sum(middle * middle)

    tiles = middle_out.shape[1] // 512
    total = lax.fori_loop(0, tiles, out_tile, jnp.zeros((CAP, 1), f32))
    scale = lax.rsqrt(total / middle_out.shape[1] + epsilon)

    def norm_tile(i, carry):
        at = pl.ds(pl.multiple_of(i * 512, 512), 512)
        second_tmp[:, at] = (middle_out[:, at] * scale * gains_out[1:2, at]).astype(bf16)
        return carry

    lax.fori_loop(0, tiles, norm_tile, 0)

    def m_other(piece, shard, onward):
        m_arrived(piece, shard)
        if onward:
            m_send(spot(piece, shard), piece, shard, m_second_s, second).start()
        m_send(spot(piece, shard), piece, shard, m_sib_s, sibling).start()

    def m_whole(piece):
        for k in range(RING // 2):
            m_arrived(piece, 2 * k + sibling % 2)

    part = width

    def gate_up_copy(piece):
        return pltpu.make_async_copy(
            gu_out.at[piece], m_chunk.at[piece % 2], act_out.at[piece % 2, 0]
        )

    def gate_up_load(piece):
        m_whole(piece)
        gate_up_copy(piece).start()

    def gate_up_rows(piece):
        gate_up_copy(piece).wait()
        span = RING * rows
        left = tok_all[:, :, pl.ds(piece * span, span)].reshape(LINE * CAP, span)

        def columns(n, carry):
            at = tile(n, 512)
            right = m_chunk[piece % 2, :, :, at].reshape(span, 512)
            term = jnp.dot(left, right, preferred_element_type=f32)
            if piece == 0:
                gate_up[:, at] = term
            else:
                gate_up[:, at] += term
            return carry

        lax.fori_loop(0, 2 * part // 512, columns, 0)

    m_own(2)
    line_own(0, second_tmp.at[:, pl.ds(0, token_half)])
    line_own(2, second_tmp.at[:, pl.ds(token_half, token_half)])
    tok_back = pltpu.make_async_copy(second_tmp, tok_out.at[z], local.at[13])
    tok_back.start()
    m_other(0, fcol, True)
    m_other(0, scol, False)
    m_own(3)
    line_relay(0, 1)
    line_relay(2, 1)
    m_other(1, fcol, True)
    m_other(1, scol, False)
    m_other(0, sfcol, False)
    line_relay(0, 2)
    line_relay(2, 2)
    m_other(2, fcol, True)
    m_other(2, scol, False)
    m_other(1, sfcol, False)
    p_back.wait()
    gate_up_load(0)
    m_other(3, fcol, True)
    m_other(3, scol, False)
    m_other(LINE, fcol, True)
    m_other(LINE, scol, False)
    line_relay(0, 3)
    tok_back.wait()
    cot_back.wait()
    tok_in = []
    for half in range(2):
        at = pl.ds(half * token_half, token_half)
        tok_in.append(
            pltpu.make_async_copy(
                tok_out.at[:, :, at], tok_all.at[:, :, at], local.at[10 if half else 12]
            )
        )
    tok_in[0].start()
    gate_up_load(1)
    tok_in[0].wait()
    gate_up_rows(0)
    m_other(2, sfcol, False)
    gate_up_load(2)
    gate_up_rows(1)
    line_relay(2, 3)
    tok_in[1].start()
    tok_in[1].wait()
    m_other(3, sfcol, False)
    gate_up_load(3)
    gate_up_rows(2)
    gate_up_rows(3)

    def hid_copy(n):
        at = tile(n, 256)
        return pltpu.make_async_copy(hid.at[:, at], hid_out.at[:, at], act_out.at[n, 0])

    def pre_copies(n):
        up_at = pl.ds(pl.multiple_of(part + n * 256, 256), 256)
        return [
            pltpu.make_async_copy(gate_up.at[:, at], pre_out.at[:, at], act_out.at[n, i])
            for i, at in ((1, tile(n, 256)), (2, up_at))
        ]

    def units(n, carry):
        at = tile(n, 256)
        up_at = pl.ds(pl.multiple_of(part + n * 256, 256), 256)
        for copy in pre_copies(n):
            copy.start()

        def act(r, inner):
            some = tile(r, 32)
            gate, up = gate_up[some, at], gate_up[some, up_at]
            hid[some, at] = (gate * jax.nn.sigmoid(gate) * up).astype(bf16)
            return inner

        lax.fori_loop(0, LINE * CAP // 32, act, 0, unroll=4)
        hid_copy(n).start()
        return carry

    lax.fori_loop(0, part // 256, units, 0)
    m_other(LINE, sfcol, False)
    d_back.wait()
    m_whole(LINE)

    for n in range(part // 256):
        for copy in [hid_copy(n)] + pre_copies(n):
            copy.wait()
    for k in range(1, LINE):
        for which in range(2):
            exchange(k, which).wait_send()
    for k in range(LINE):

        @pl.when((z < last) & (k <= z))
        def _(k=k):
            send(w_tmp, col + RING * k, up_s, me + RING).wait_send()
            for which in range(3):
                line_send(line_spot(which, k), which, k, line_up, me + RING).wait_send()

        @pl.when((z > 0) & (k >= z))
        def _(k=k):
            send(w_tmp, col + RING * k, down_s, me - RING).wait_send()
            for which in range(3):
                line_send(line_spot(which, k), which, k, line_down, me - RING).wait_send()

        send(w_tmp, col + RING * k, first_s, first).wait_send()
        send(w_tmp, col + RING * k, second_s, second).wait_send()
        send(w_tmp, fcol + RING * k, second_s, second).wait_send()
        for base in (col, fcol, scol, sfcol):
            send(w_tmp, base + RING * k, sib_s, sibling).wait_send()
    for piece in range(pieces):
        src = source(piece)
        m_send(src, piece, col, m_first_s, first).wait_send()
        m_send(src, piece, col, m_second_s, second).wait_send()
        m_send(src, piece, fcol, m_second_s, second).wait_send()
        for base in (col, fcol, scol, sfcol):
            m_send(src, piece, base, m_sib_s, sibling).wait_send()


def forward(hidden_in, out_grad, seq_lengths, seq_device, gains, wq, wk, wv, wo, gate, up, wd):
    slots, dim = hidden_in.shape
    rows = wq.shape[0]
    n = RING * LINE
    width = gate.shape[1] // LINE
    qkv_width = wq.shape[1] + wk.shape[1] + wv.shape[1]
    wide = qkv_width + wo.shape[1] + 128
    pieces = LINE + 1
    S = jax.ShapeDtypeStruct
    return pl.pallas_call(
        forward_kernel,
        out_shape=(
            S((n, rows, wide), bf16),
            S((LINE, RING, rows, 2 * width), bf16),
            S((RING,) + wd.shape, bf16),
            S((LINE, slots, dim), bf16),
            S((LINE, slots, dim), bf16),
            S((LINE * slots, width), bf16),
            S((LINE * slots, 2 * width), f32),
            S((slots, dim), f32),
            S((slots, dim), bf16),
            S((slots, qkv_width), f32),
            S((slots, H * HD), bf16),
            S((slots, KVH * HD), bf16),
            S((slots, KVH * HD), bf16),
            S((slots, H * HD), bf16),
            S((8, dim), f32),
            S((3, slots, HD), f32),
        ),
        in_specs=[VMEM] * 7 + [ANY] * 8,
        out_specs=(ANY,) * 7 + (VMEM,) * 9,
        scratch_shapes=[
            pltpu.VMEM((rows, wide), bf16),
            pltpu.VMEM((LINE, rows, 2 * width), bf16),
            pltpu.VMEM(wd.shape, bf16),
            pltpu.VMEM((slots, dim), bf16),
            pltpu.VMEM((slots, dim), bf16),
            pltpu.VMEM((RING, rows, qkv_width), bf16),
            pltpu.VMEM((n, rows, wo.shape[1]), bf16),
            pltpu.VMEM((LINE, RING, 16, 128), bf16),
            pltpu.VMEM((16, 128), f32),
            pltpu.VMEM((LINE, slots, dim), bf16),
            pltpu.VMEM((LINE * slots, 2 * width), f32),
            pltpu.VMEM((2, RING, rows, 2 * width), bf16),
            pltpu.VMEM((LINE * slots, width), bf16),
            DMA((14,)),
            DMA((n,)),
            DMA((n,)),
            DMA((n,)),
            DMA((n,)),
            DMA((n,)),
            DMA((n,)),
            DMA((LINE, 2)),
            DMA((LINE, 2)),
            DMA((pieces, RING)),
            DMA((pieces, RING)),
            DMA((pieces, RING)),
            DMA((pieces, RING)),
            DMA((3, LINE)),
            DMA((3, LINE)),
            DMA((3, LINE)),
            DMA,
            DMA((LINE,)),
            DMA,
            DMA((width // 256, 3)),
        ],
        compiler_params=pltpu.CompilerParams(
            collective_id=0, has_side_effects=True, vmem_limit_bytes=64000 * 1024
        ),
        name="forward",
    )(
        hidden_in, seq_lengths[None, :], seq_device[None, :], *[g[None, :] for g in gains],
        out_grad, wq, wk, wv, wo, gate, up, wd,
    )


def backward_kernel(
    gu_ref, wd_ref, tok_ref, cot_ref, hid_ref, pre_ref, w_ref, middle_ref, normed_ref, raw_ref,
    q_ref, k_ref, v_ref, mixed_ref, x_ref, gains_ref, rope_ref,
    x_out, small_out, y_out, d_out, a_out, ex_land, gu_out, c_land, s_land, f_land, l_land,
    gu_all, gd_all, gu_sib, gd_sib, gu_sec, gd_sec, gu_fst, gd_fst, t_own, t_land,
    dmid, dqkv, s_sum, s_got, s_line,
    c_send, c_recv, s_send, s_recv, f_send, f_recv, down_s, down_r, up_s, up_r, load, stream, back,
    ac_send, ac_recv, as_send, as_recv, af_send, af_recv, ad_send, ad_recv, au_send, au_recv,
    ex_s, ex_r, small_s, small_r, units_in,
    a_load,
):
    me, z, first, second, sibling = where_am_i()
    greet(line_peers(me) + [first, second, sibling])
    core = me % 2
    mine, fst, sec = (me % RING) // 2, (first % RING) // 2, (second % RING) // 2
    far = ((second + first - me) % RING) // 2
    half = gd_fst.shape[0] // 2
    last = LINE - 1
    tokens, dim = tok_ref.shape
    part = hid_ref.shape[1]
    quad_rows = part // LINE
    shard_rows = dim // (RING * LINE)
    piece_cols = gu_all.shape[3]
    kv0 = H * HD
    v0 = kv0 + KVH * HD
    qkv_width = v0 + KVH * HD
    MLP_GU, MLP_D = (0, 0, LINE), (1, LINE, LINE + 2)

    def block(gu, d, piece, group):
        if group == 0:
            return gu.at[piece]
        return d.at[tile(piece - LINE, half)]

    def own_block(quad, piece, group, theirs=False):
        shard = 2 * quad + (1 - core if theirs else core)
        if group == 0:
            return gu_all.at[piece, shard]
        return block(None, gd_all.at[shard], piece, group)

    def each(span, body):
        group, lo, hi = span

        def step(piece, carry):
            body(piece, group)
            return carry

        lax.fori_loop(lo, hi, step, 0)

    def to_sibling(quad, piece, group):
        return remote(
            own_block(quad, piece, group, theirs=True),
            block(gu_sib.at[quad], gd_sib.at[quad], piece, group),
            c_send.at[quad, piece],
            c_recv.at[quad, piece],
            sibling,
        )

    def to_second(quad, slot, piece, group):
        return remote(
            own_block(quad, piece, group),
            block(gu_sec.at[slot], gd_sec.at[slot], piece, group),
            s_send.at[slot, piece],
            s_recv.at[slot, piece],
            second,
        )

    def to_first(piece, group):
        return remote(
            own_block(fst, piece, group),
            block(gu_fst, gd_fst, piece, group),
            f_send.at[piece],
            f_recv.at[piece],
            first,
        )

    def pass_on(piece, group):
        for quad, slot in ((far, 1), (sec, 0)):
            to_sibling(quad, piece, group).wait_recv()
            own = own_block(quad, piece, group)
            add_rows(own, own, block(gu_sib.at[quad], gd_sib.at[quad], piece, group))
            to_second(quad, slot, piece, group).start()

    def narrow(piece, group):
        to_sibling(fst, piece, group).wait_recv()
        to_second(far, 1, piece, group).wait_recv()
        own = own_block(fst, piece, group)
        add_rows(
            own,
            own,
            block(gu_sib.at[fst], gd_sib.at[fst], piece, group),
            block(gu_sec.at[1], gd_sec.at[1], piece, group),
        )
        to_first(piece, group).start()

    def finish(piece, group, out=None):
        to_sibling(mine, piece, group).wait_recv()
        to_second(sec, 0, piece, group).wait_recv()
        to_first(piece, group).wait_recv()
        own = own_block(mine, piece, group)
        add_rows(
            own if group == 0 else block(None, out, piece, group),
            own,
            block(gu_sib.at[mine], gd_sib.at[mine], piece, group),
            block(gu_sec.at[0], gd_sec.at[0], piece, group),
            block(gu_fst, gd_fst, piece, group),
        )

    def drain_sibling(piece, group):
        for quad in (far, fst, sec, mine):
            to_sibling(quad, piece, group).wait_send()

    def drain(piece, group):
        to_second(far, 1, piece, group).wait_send()
        to_second(sec, 0, piece, group).wait_send()
        to_first(piece, group).wait_send()

    def send_line(src, which, t, up):
        return remote(
            src,
            t_land.at[which, t + 1 if up else t],
            (up_s if up else down_s).at[which, t],
            (up_r if up else down_r).at[which, t],
            me + RING if up else me - RING,
        )

    def line_own(which):
        for k in range(last):

            @pl.when(z == last)
            def _(k=k):
                send_line(t_own.at[which, k], which, k, False).start()

            @pl.when(z == 0)
            def _(k=k):
                send_line(t_own.at[which, last - k], which, last - k, True).start()

    def relay_at(which, at, t, up):
        @pl.when(z == at)
        def _():
            landing = t_land.at[which, t + 1 if up else t]
            send_line(landing, which, t, up).wait_recv()
            add_rows(landing, landing, t_own.at[which, t])
            send_line(landing, which, t, up).start()

    def relay(which, step):
        if step < 2:
            relay_at(which, 2, step, False)
            relay_at(which, 1, last - step, True)
        else:
            relay_at(which, 1, 0, False)
            relay_at(which, 2, last, True)

    def line_sum(which, out):
        own, above, below = t_own.at[which, z], t_land.at[which, z], t_land.at[which, z + 1]

        @pl.when(z < last)
        def _():
            send_line(above, which, z, False).wait_recv()

        @pl.when(z > 0)
        def _():
            send_line(below, which, z, True).wait_recv()

        @pl.when(z == 0)
        def _():
            add_rows(out, own, above)

        @pl.when(z == last)
        def _():
            add_rows(out, own, below)

        @pl.when((z > 0) & (z < last))
        def _():
            add_rows(out, own, above, below)

    def mlp(tok, cot, hid, dgu):
        ins = [
            pltpu.make_async_copy(hid_ref, hid, load.at[0]),
            pltpu.make_async_copy(cot_ref, cot, load.at[1]),
            pltpu.make_async_copy(tok_ref, tok, load.at[3]),
        ]
        for copy in ins:
            copy.start()
        wide = 256
        for copy in ins[:2]:
            copy.wait()

        previous = None
        for quad in (far, sec, fst, mine):

            def columns(n, carry, quad=quad):
                at = tile(n, 512)
                both = dot_tn(hid[:, tile(quad, quad_rows)], cot[:, at]).astype(bf16)
                gd_all[2 * quad, :, at] = both[: quad_rows // 2]
                gd_all[2 * quad + 1, :, at] = both[quad_rows // 2 :]
                return carry

            lax.fori_loop(0, dim // 512, columns, 0)
            if previous is not None:
                each(MLP_D, lambda piece, group, q=previous: to_sibling(q, piece, group).start())
            previous = quad
        each(MLP_D, lambda piece, group, q=previous: to_sibling(q, piece, group).start())
        each(MLP_D, pass_on)

        def units(gate_t, up_t, down_w, dhid_t):
            def fetch(i, slot):
                up_at = pl.ds(pl.multiple_of(part + i * wide, wide), wide)
                return (
                    pltpu.make_async_copy(
                        pre_ref.at[:, tile(i, wide)], gate_t.at[slot], units_in.at[slot, 0]
                    ),
                    pltpu.make_async_copy(pre_ref.at[:, up_at], up_t.at[slot], units_in.at[slot, 1]),
                    pltpu.make_async_copy(
                        wd_ref.at[tile(i, wide)], down_w.at[slot], units_in.at[slot, 2]
                    ),
                )

            def body(i, slot):
                dhid_t[...] = dot_nt(cot[...], down_w[slot])

                def act(r, carry):
                    at = tile(r, 32)
                    gate, up, dhid = gate_t[slot, at], up_t[slot, at], dhid_t[at]
                    sig = jax.nn.sigmoid(gate)
                    dgate = dhid * up * (sig * (1.0 + gate * (1.0 - sig)))
                    dgu[at, tile(i, wide)] = dgate.astype(bf16)
                    up_at = pl.ds(pl.multiple_of(part + i * wide, wide), wide)
                    dgu[at, up_at] = (dhid * (gate * sig)).astype(bf16)
                    return carry

                lax.fori_loop(0, tokens // 32, act, 0, unroll=4)

            streamed(part // wide, fetch, body)

        pl.run_scoped(
            units,
            pltpu.VMEM((2, tokens, wide), f32),
            pltpu.VMEM((2, tokens, wide), f32),
            pltpu.VMEM((2, wide, dim), bf16),
            pltpu.VMEM((tokens, wide), f32),
        )

        def back_through(rows_w):
            def fetch(i, slot):
                return (
                    pltpu.make_async_copy(
                        gu_ref.at[tile(i, wide)], rows_w.at[slot], stream.at[slot]
                    ),
                )

            def body(i, slot):
                out = dot_nt(dgu[...], rows_w[slot]).astype(bf16)
                t_own[0, :, :, tile(i, wide)] = out.reshape(LINE, CAP, wide)

            streamed(dim // wide, fetch, body)

        pl.run_scoped(back_through, pltpu.VMEM((2, wide, 2 * part), bf16))
        ins[2].wait()
        line_own(0)

        rows = dim // LINE
        for piece in range(LINE):

            def columns(n, carry, piece=piece):
                at = tile(n, 512)
                grad = dot_tn(tok[:, pl.ds(piece * rows, rows)], dgu[:, at]).astype(bf16)
                gu_all[piece, :, :, at] = grad.reshape(RING, rows // RING, 512)
                return carry

            lax.fori_loop(0, 2 * part // 512, columns, 0)
            if piece > 0:
                pass_on(piece - 1, 0)
            for quad in (far, fst, sec, mine):
                to_sibling(quad, piece, 0).start()
            if piece == 2:
                relay(0, 0)
        pass_on(LINE - 1, 0)
        each(MLP_D, narrow)

        def out_through(cols_w):
            def fetch(i, slot):
                return (
                    pltpu.make_async_copy(
                        wd_ref.at[:, tile(i, wide)], cols_w.at[slot], stream.at[slot]
                    ),
                )

            def body(i, slot):
                out = jnp.dot(hid[...], cols_w[slot], preferred_element_type=f32).astype(bf16)
                t_own[1, :, :, tile(i, wide)] = out.reshape(LINE, CAP, wide)

                @pl.when(i == 3)
                def _():
                    relay(0, 1)

                @pl.when(i == 5)
                def _():
                    relay(0, 2)

            streamed(dim // wide, fetch, body)

        pl.run_scoped(out_through, pltpu.VMEM((2, part, wide), bf16))

    pl.run_scoped(
        mlp,
        pltpu.VMEM((tokens, dim), bf16),
        pltpu.VMEM((tokens, dim), bf16),
        pltpu.VMEM((tokens, part), bf16),
        pltpu.VMEM((tokens, 2 * part), bf16),
    )
    def attention(dbr, mixed, normed, raw, q, k, v, cot, dsec, dmix, middle, w_rows):
        ins = [
            pltpu.make_async_copy(src, dst, load.at[i])
            for i, (src, dst) in enumerate(
                (
                    (middle_ref, middle),
                    (raw_ref.at[:, pl.ds(0, v0)], raw),
                    (q_ref, q),
                    (k_ref, k),
                    (v_ref, v),
                    (cot_ref.at[tile(z, CAP)], cot),
                    (mixed_ref, mixed),
                    (normed_ref, normed),
                )
            )
        ]
        for copy in ins:
            copy.start()
        narrow(0, 0)
        line_own(1)
        for copy in ins:
            copy.wait()
        line_sum(0, dsec)

        scale = rms_scale(middle[...])
        wide = 512

        def gather_mean(i, total):
            at = tile(i, wide)
            n = middle[:, at] * scale
            ds = dsec[:, at]
            s_sum[3, 0:1, at] = jnp.sum(n * ds, axis=0, keepdims=True)
            return total + lane_sum(n * ds * gains_ref[1:2, at])

        mean = lax.fori_loop(0, dim // wide, gather_mean, jnp.zeros((CAP, 1), f32)) / dim

        def spread_mean(i, carry):
            at = tile(i, wide)
            n = middle[:, at] * scale
            e = dsec[:, at] * gains_ref[1:2, at]
            d_middle = cot[:, at].astype(f32) + scale * (e - n * mean)
            dmid[:, at] = d_middle
            dbr[:, at] = d_middle.astype(bf16)
            return carry

        lax.fori_loop(0, dim // wide, spread_mean, 0)
        shards = w_rows.shape[1]
        rows = shards * w_rows.shape[2]

        def w_fetch(i, slot):
            return (
                pltpu.make_async_copy(
                    w_ref.at[tile(i, shards), :, pl.ds(qkv_width, dim)],
                    w_rows.at[slot],
                    stream.at[slot],
                ),
            )

        def through_out(i, slot):
            dmix[:, tile(i, rows)] = dot_nt(dbr[...], w_rows[slot].reshape(rows, dim)).astype(bf16)

        streamed(dim // rows, w_fetch, through_out)
        narrow(1, 0)
        relay(1, 0)

        cosine, sine, bias = rope_ref[0], rope_ref[1], rope_ref[2]
        s_sum[3, 1:8] = jnp.zeros((7, dim), f32)

        def unrope(raw_v, d_rot, row):
            d_hat = d_rot * cosine - half_turn(d_rot * sine)
            r = rms_scale(raw_v)
            n = raw_v * r
            s_sum[3, row : row + 1, 0:HD] += jnp.sum(n * d_hat, axis=0, keepdims=True)
            e = d_hat * gains_ref[row + 1 : row + 2, 0:HD]
            return (r * (e - n * jnp.mean(n * e, axis=-1, keepdims=True))).astype(bf16)

        def head(g, carry):
            at = tile(g, HD)
            key, value = k[:, at], v[:, at]
            d_key = jnp.zeros((CAP, HD), f32)
            d_value = jnp.zeros((CAP, HD), f32)
            for i in range(2):
                cols = tile(2 * g + i, HD)
                query, d_mix = q[:, cols], dmix[:, cols]
                logits = dot_nt(query, key) * (HD ** (-0.5)) + bias
                exponent = jnp.exp(logits - jnp.max(logits, axis=-1, keepdims=True))
                probs = exponent / lane_sum(exponent)
                d_probs = dot_nt(d_mix, value)
                d_logits = probs * (d_probs - lane_sum(probs * d_probs))
                d_scores = (d_logits * (HD ** (-0.5))).astype(bf16)
                d_value = d_value + dot_tn(probs.astype(bf16), d_mix)
                d_key = d_key + dot_tn(d_scores, query)
                d_query = jnp.dot(d_scores, key, preferred_element_type=f32)
                dqkv[:, cols] = unrope(raw[:, cols], d_query, 1)
            cols = pl.ds(pl.multiple_of(kv0 + g * HD, HD), HD)
            dqkv[:, cols] = unrope(raw[:, cols], d_key, 2)
            dqkv[:, pl.ds(pl.multiple_of(v0 + g * HD, HD), HD)] = d_value.astype(bf16)
            return carry

        lax.fori_loop(0, KVH // 2, head, 0, unroll=2)
        narrow(2, 0)
        lax.fori_loop(KVH // 2, KVH, head, 0, unroll=2)

    order = (
        last * (1 - z // 2),
        2 - 2 * z + 5 * (z // 2),
        1 + z % 2,
        z,
    )

    def a_own(t, quad, h):
        return gu_all.at[t, 2 * quad + (core if h else 1 - core)]

    def sums(dbr, mixed, normed, cbuf, stage):
        span = dim // LINE

        def a_sibling(t, quad, h, slot):
            return remote(
                cbuf.at[slot, quad],
                c_land.at[t, h, quad],
                ac_send.at[slot, quad],
                ac_recv.at[t, h, quad],
                sibling,
            )

        def a_second(t, quad, h, slot):
            return remote(
                a_own(t, quad, h),
                s_land.at[slot, t, h],
                as_send.at[slot, t, h],
                as_recv.at[slot, t, h],
                second,
            )

        def a_first(t, h):
            return remote(
                a_own(t, fst, h), f_land.at[t, h], af_send.at[t, h], af_recv.at[t, h], first
            )

        def a_line(t, h, upward):
            src = a_own(t, mine, h)
            if upward:
                return remote(
                    src, l_land.at[1, t, h], au_send.at[t, h], au_recv.at[t, h], me + RING
                )
            return remote(src, l_land.at[0, t, h], ad_send.at[t, h], ad_recv.at[t, h], me - RING)

        def staged(lo, *landed):
            return [
                pltpu.make_async_copy(src, stage.at[lo + i], a_load.at[lo + i])
                for i, src in enumerate(landed)
            ]

        def begin(copies):
            for copy in copies:
                copy.start()

        def add_staged(own, copies, lo):
            for copy in copies:
                copy.wait()
            add_rows(own, own, *[stage.at[lo + i] for i in range(len(copies))])

        def compute(k):
            h, t, slot = k // LINE, order[k % LINE], k % 2
            if k > 1:
                for quad in (far, fst, sec, mine):
                    a_sibling(order[(k - 2) % LINE], quad, (k - 2) // LINE, slot).wait_send()
            col0 = v0 if h else 0
            own_core = core if h else 1 - core

            def columns(n, carry, left, right, at):
                grad = dot_tn(left[:, tile(t, span)], right).astype(bf16)
                grad = grad.reshape(RING // 2, 2, shard_rows, 512)
                ours = jnp.where(core == 0, grad[:, 0], grad[:, 1])
                theirs = jnp.where(core == 0, grad[:, 1], grad[:, 0])
                for quad in range(RING // 2):
                    gu_all[t, 2 * quad + own_core, :, at] = ours[quad]
                cbuf[slot, :, :, at] = theirs
                return carry

            def from_qkv(n, carry):
                at = tile(n, 512)
                right = dqkv[:, pl.ds(pl.multiple_of(col0 + n * 512, 512), 512)]
                return columns(n, carry, normed, right, at)

            def from_out(n, carry):
                at = pl.ds(pl.multiple_of(qkv_width - v0 + n * 512, 512), 512)
                return columns(n, carry, mixed, dbr[:, tile(n, 512)], at)

            if h == 0:
                lax.fori_loop(0, v0 // 512, from_qkv, 0)
            else:
                lax.fori_loop(0, (qkv_width - v0) // 512, from_qkv, 0)
                lax.fori_loop(0, dim // 512, from_out, 0)

        def share(k):
            h, t, slot = k // LINE, order[k % LINE], k % 2
            for quad in (far, fst, sec, mine):
                a_sibling(t, quad, h, slot).start()

        def spread_in(k):
            t, h = order[k % LINE], k // LINE
            return staged(0, c_land.at[t, h, far], c_land.at[t, h, sec])

        def spread_begin(k):
            h, t, slot = k // LINE, order[k % LINE], k % 2
            for quad in (far, sec):
                a_sibling(t, quad, h, slot).wait_recv()
            begin(spread_in(k))

        def spread(k):
            h, t = k // LINE, order[k % LINE]
            copies = spread_in(k)
            for i, (quad, place) in enumerate(((far, 1), (sec, 0))):
                add_staged(a_own(t, quad, h), copies[i : i + 1], i)
                a_second(t, quad, h, place).start()

        def inward_in(k):
            t, h = order[k % LINE], k // LINE
            return staged(2, c_land.at[t, h, fst], s_land.at[1, t, h])

        def inward_begin(k):
            h, t, slot = k // LINE, order[k % LINE], k % 2
            a_sibling(t, fst, h, slot).wait_recv()
            a_second(t, far, h, 1).wait_recv()
            begin(inward_in(k))

        def inward(k):
            h, t = k // LINE, order[k % LINE]
            add_staged(a_own(t, fst, h), inward_in(k), 2)
            a_first(t, h).start()

        def collect_in(k):
            t, h = order[k % LINE], k // LINE
            return staged(4, c_land.at[t, h, mine], s_land.at[0, t, h], f_land.at[t, h])

        def collect_begin(k):
            h, t, slot = k // LINE, order[k % LINE], k % 2
            a_sibling(t, mine, h, slot).wait_recv()
            a_second(t, sec, h, 0).wait_recv()
            a_first(t, h).wait_recv()
            begin(collect_in(k))

        def collect(k):
            h, t = k // LINE, order[k % LINE]
            add_staged(a_own(t, mine, h), collect_in(k), 4)

            @pl.when((t < z) & (z == last))
            def _():
                a_line(t, h, False).start()

            @pl.when((t > z) & (z == 0))
            def _():
                a_line(t, h, True).start()

        def onward(k):
            h, t = k // LINE, order[k % LINE]

            @pl.when((t < z) & (z < last))
            def _():
                a_line(t, h, False).wait_recv()
                copies = staged(7, l_land.at[0, t, h])
                begin(copies)
                add_staged(a_own(t, mine, h), copies, 7)
                a_line(t, h, False).start()

            @pl.when((t > z) & (z > 0))
            def _():
                a_line(t, h, True).wait_recv()
                copies = staged(7, l_land.at[1, t, h])
                begin(copies)
                add_staged(a_own(t, mine, h), copies, 7)
                a_line(t, h, True).start()

        def exchange(k):
            peer_z = lax.rem(z + k, LINE)
            return remote(
                gu_out.at[peer_z], ex_land.at[z], ex_s.at[k], ex_r.at[k], me % RING + RING * peer_z
            )

        def small(step, src, dst, device):
            return remote(src, dst, small_s.at[step], small_r.at[step], device)

        def first_norm(w_rows):
            shards = w_rows.shape[1]
            wide = 512
            x_scale = rms_scale(x_ref[...].astype(f32))
            w_tile = shards * w_rows.shape[2]

            def w_fetch(i, slot):
                return (
                    pltpu.make_async_copy(
                        w_ref.at[tile(i, shards), :, pl.ds(0, qkv_width)],
                        w_rows.at[slot],
                        stream.at[slot],
                    ),
                )

            def through(i, slot):
                x_out[:, tile(i, w_tile)] = dot_nt(dqkv[...], w_rows[slot].reshape(w_tile, qkv_width))

            streamed(dim // w_tile, w_fetch, through)

            def gather_mean(i, total):
                at = tile(i, wide)
                n = x_ref[:, at].astype(f32) * x_scale
                s_sum[3, 3:4, at] = jnp.sum(n * x_out[:, at], axis=0, keepdims=True)
                return total + lane_sum(n * x_out[:, at] * gains_ref[0:1, at])

            mean = lax.fori_loop(0, dim // wide, gather_mean, jnp.zeros((CAP, 1), f32)) / dim

            def spread_mean(i, carry):
                at = tile(i, wide)
                n = x_ref[:, at].astype(f32) * x_scale
                e = x_out[:, at] * gains_ref[0:1, at]
                x_out[:, at] = dmid[:, at] + x_scale * (e - n * mean)
                return carry

            lax.fori_loop(0, dim // wide, spread_mean, 0)

        def mlp_results(d_tmp, middle, y, y_half):
            middle_in = pltpu.make_async_copy(middle_ref, middle, load.at[0])
            middle_in.start()
            each(MLP_D, lambda piece, group: finish(piece, group, d_tmp))
            d_back = pltpu.make_async_copy(d_tmp, d_out, load.at[1])
            d_back.start()
            line_sum(1, y)
            middle_in.wait()

            def last_add(i, carry):
                at = tile(i, 512)
                y_half[:, at] = (middle[:, at] + y[:, at]).astype(bf16)
                return carry

            lax.fori_loop(0, dim // 512, last_add, 0)
            y_back = pltpu.make_async_copy(y_half, y_out, load.at[2])
            y_back.start()
            each(MLP_D, drain_sibling)
            each(MLP_D, drain)
            d_back.wait()
            y_back.wait()

        small_c = small(0, s_sum.at[3], s_got.at[0], sibling)
        each(MLP_GU, drain_sibling)
        compute(0)
        share(0)
        narrow(3, 0)
        compute(1)
        share(1)
        spread_begin(0)
        compute(2)
        share(2)
        spread(0)
        spread_begin(1)
        relay(1, 1)
        compute(3)
        share(3)
        spread(1)
        spread_begin(2)
        inward_begin(0)
        spread(2)
        spread_begin(3)
        inward(0)
        each(MLP_GU, finish)
        gu_back = pltpu.make_async_copy(gu_all.at[:, 2 * mine + core], gu_out, back.at[0])
        gu_back.start()
        ex_in = pltpu.make_async_copy(gu_all.at[z, 2 * mine + core], ex_land.at[z], back.at[1])
        ex_in.start()
        spread(3)
        each(MLP_GU, drain)
        gu_back.wait()
        exchange(2).start()
        exchange(1).start()
        ex_in.wait()
        compute(4)
        share(4)
        pl.run_scoped(first_norm, pltpu.VMEM((2, 4, shard_rows, qkv_width), bf16))
        small_c.start()
        inward_begin(1)
        compute(5)
        share(5)
        inward(1)
        small_c.wait()
        s_sum[0] = s_sum[3] + s_got[0]
        small_f = small(1, s_sum.at[0], s_got.at[1], first)
        small_f.start()
        spread_begin(4)
        relay(1, 2)
        compute(6)
        share(6)
        spread(4)
        spread_begin(5)
        inward_begin(2)
        compute(7)
        share(7)
        inward(2)
        spread(5)
        spread_begin(6)
        small_f.wait()
        s_sum[1] = s_sum[0] + s_got[1]
        small_s2 = small(2, s_sum.at[1], s_got.at[2], second)
        small_s2.start()
        spread(6)
        spread_begin(7)
        collect_begin(0)
        spread(7)
        collect(0)
        collect_begin(1)
        inward_begin(3)
        collect(1)
        inward(3)
        collect_begin(2)
        collect(2)
        onward(0)
        onward(2)
        collect_begin(3)
        inward_begin(4)
        collect(3)
        inward(4)
        exchange(3).start()
        onward(1)
        pl.run_scoped(
            mlp_results,
            pltpu.VMEM(gd_fst.shape, f32),
            pltpu.VMEM((CAP, dim), f32),
            pltpu.VMEM((CAP, dim), f32),
            pltpu.VMEM((CAP, dim), bf16),
        )
        inward_begin(5)
        collect_begin(4)
        inward(5)
        collect(4)
        inward_begin(6)
        collect_begin(5)
        inward(6)
        collect(5)
        onward(4)
        small_s2.wait()
        s_sum[2] = s_sum[1] + s_got[2]
        small_line = [
            small(2 + k, s_sum.at[2], s_line.at[k], me % RING + RING * lax.rem(z + k, LINE))
            for k in range(1, LINE)
        ]
        for copy in small_line:
            copy.start()
        onward(5)
        inward_begin(7)
        collect_begin(6)
        inward(7)
        collect(6)
        onward(6)
        collect_begin(7)
        collect(7)
        for copy in small_line:
            copy.wait()
        small_out[...] = (s_sum[2] + s_line[2]) + (s_line[1] + s_line[3])
        for k in (6, 7):
            for quad in (far, fst, sec, mine):
                a_sibling(order[k % LINE], quad, k // LINE, k % 2).wait_send()
        for k in range(1, LINE):
            exchange(k).wait_send()
            src_z = lax.rem(z + LINE - k, LINE)
            landed = ex_land.at[src_z]
            remote(landed, landed, ex_s.at[k], ex_r.at[k], sibling).wait_recv()
        for t in range(LINE):
            for h in range(2):
                a_second(t, far, h, 1).wait_send()
                a_second(t, sec, h, 0).wait_send()
                a_first(t, h).wait_send()

                @pl.when(t < z)
                def _(t=t, h=h):
                    a_line(t, h, False).wait_send()

                @pl.when(t > z)
                def _(t=t, h=h):
                    a_line(t, h, True).wait_send()

    slots = CAP
    kv = KVH * HD
    rows = gu_all.shape[2]

    def both(dbr, mixed, normed):
        pl.run_scoped(
            lambda *refs: attention(dbr, mixed, normed, *refs),
            pltpu.VMEM((slots, v0), f32),
            pltpu.VMEM((slots, dim), bf16),
            pltpu.VMEM((slots, kv), bf16),
            pltpu.VMEM((slots, kv), bf16),
            pltpu.VMEM((slots, dim), bf16),
            pltpu.VMEM((slots, dim), f32),
            pltpu.VMEM((slots, dim), bf16),
            pltpu.VMEM((slots, dim), f32),
            pltpu.VMEM((2, 4, rows, dim), bf16),
        )
        pl.run_scoped(
            lambda *refs: sums(dbr, mixed, normed, *refs),
            pltpu.VMEM((2, RING // 2, rows, piece_cols), bf16),
            pltpu.VMEM((8, rows, piece_cols), bf16),
        )

    pl.run_scoped(
        both,
        pltpu.VMEM((slots, dim), bf16),
        pltpu.VMEM((slots, dim), bf16),
        pltpu.VMEM((slots, dim), bf16),
    )

    def a_landed(t, h, upward):
        landing = l_land.at[1 if upward else 0, t, h]
        sems = (au_send, au_recv) if upward else (ad_send, ad_recv)
        return remote(landing, landing, sems[0].at[t, h], sems[1].at[t, h], sibling)

    def results(a_tmp, stage):
        for h in range(2):

            @pl.when(z < last)
            def _(h=h):
                a_landed(z, h, False).wait_recv()

            @pl.when(z > 0)
            def _(h=h):
                a_landed(z, h, True).wait_recv()

        def total(*sides):
            for h in range(2):
                copies = [
                    pltpu.make_async_copy(l_land.at[side, z, h], stage.at[i], stream.at[i])
                    for i, side in enumerate(sides)
                ]
                for copy in copies:
                    copy.start()
                for copy in copies:
                    copy.wait()
                add_rows(
                    a_tmp.at[:, pl.ds(h * piece_cols, piece_cols)],
                    a_own(z, mine, h),
                    *[stage.at[i] for i in range(len(sides))],
                )

        @pl.when(z == 0)
        def _():
            total(0)

        @pl.when(z == last)
        def _():
            total(1)

        @pl.when((z > 0) & (z < last))
        def _():
            total(0, 1)

        a_back = pltpu.make_async_copy(a_tmp, a_out, load.at[3])
        a_back.start()
        a_back.wait()

    pl.run_scoped(
        results,
        pltpu.VMEM((rows, 2 * piece_cols), f32),
        pltpu.VMEM((2, rows, piece_cols), bf16),
    )
    for which in range(2):
        for k in range(LINE):

            @pl.when((z > 0) & (k < z))
            def _(which=which, k=k):
                send_line(t_own.at[which, k], which, k, False).wait_send()

            @pl.when((z < last) & (k > z))
            def _(which=which, k=k):
                send_line(t_own.at[which, k], which, k, True).wait_send()


def backward(gu, wd, tok, cot, hid, pre, w, middle, normed, raw, q, k, v, mixed, x, gains, rope):
    dim = tok.shape[1]
    rows = w.shape[1]
    drows = wd.shape[0] // RING
    cols = gu.shape[1]
    quads = RING // 2
    pieces = LINE + 2
    qkv = raw.shape[1]
    S = jax.ShapeDtypeStruct
    return pl.pallas_call(
        backward_kernel,
        out_shape=(
            S((CAP, dim), f32),
            S((8, dim), f32),
            S((CAP, dim), bf16),
            S((drows, dim), f32),
            S((rows, qkv + dim), f32),
            S((LINE, rows, cols), bf16),
            S((LINE, rows, cols), bf16),
            S((LINE, 2, quads, rows, cols), bf16),
            S((2, LINE, 2, rows, cols), bf16),
            S((LINE, 2, rows, cols), bf16),
            S((2, LINE, 2, rows, cols), bf16),
        ),
        in_specs=[ANY] * 14 + [VMEM] * 3,
        out_specs=(VMEM,) * 2 + (ANY,) * 9,
        scratch_shapes=[
            pltpu.VMEM((LINE, RING, rows, cols), bf16),
            pltpu.VMEM((RING, drows, dim), bf16),
            pltpu.VMEM((quads, LINE, rows, cols), bf16),
            pltpu.VMEM((quads, drows, dim), bf16),
            pltpu.VMEM((2, LINE, rows, cols), bf16),
            pltpu.VMEM((2, drows, dim), bf16),
            pltpu.VMEM((LINE, rows, cols), bf16),
            pltpu.VMEM((drows, dim), bf16),
            pltpu.VMEM((2, LINE, CAP, dim), bf16),
            pltpu.VMEM((2, LINE + 1, CAP, dim), bf16),
            pltpu.VMEM((CAP, dim), f32),
            pltpu.VMEM((CAP, qkv), bf16),
            pltpu.VMEM((4, 8, dim), f32),
            pltpu.VMEM((3, 8, dim), f32),
            pltpu.VMEM((LINE, 8, dim), f32),
            DMA((quads, pieces)),
            DMA((quads, pieces)),
            DMA((2, pieces)),
            DMA((2, pieces)),
            DMA((pieces,)),
            DMA((pieces,)),
            DMA((2, LINE)),
            DMA((2, LINE)),
            DMA((2, LINE)),
            DMA((2, LINE)),
            DMA((8,)),
            DMA((3,)),
            DMA((2,)),
            DMA((2, quads)),
            DMA((LINE, 2, quads)),
            DMA((2, LINE, 2)),
            DMA((2, LINE, 2)),
            DMA((LINE, 2)),
            DMA((LINE, 2)),
            DMA((LINE, 2)),
            DMA((LINE, 2)),
            DMA((LINE, 2)),
            DMA((LINE, 2)),
            DMA((LINE,)),
            DMA((LINE,)),
            DMA((2 + LINE,)),
            DMA((2 + LINE,)),
            DMA((2, 3)),
            DMA((8,)),
        ],
        compiler_params=pltpu.CompilerParams(
            collective_id=2, has_side_effects=True, vmem_limit_bytes=65400 * 1024
        ),
        name="backward",
    )(gu, wd, tok, cot, hid, pre, w, middle, normed, raw, q, k, v, mixed, x, gains, rope)


def results_kernel(
    y_ref, x_ref, small_ref, d_ref, a_ref, ex_ref,
    y_out, x_out, q_out, k_out, v_out, o_out, gate_out, up_out, d_out, ga_out, gq_out, gk_out, gm_out,
    y_tmp, x_tmp, small, d_tmp, a_tmp, ex_tmp, gate_tmp, up_tmp, sem_in, sem_out,
):
    me = lax.axis_index("fsdp")
    width = ex_tmp.shape[2] // 2
    moves = ((small_ref, small), (ex_ref, ex_tmp), (a_ref, a_tmp), (d_ref, d_tmp), (x_ref, x_tmp), (y_ref, y_tmp))
    ins = [pltpu.make_async_copy(src, dst, sem_in.at[i]) for i, (src, dst) in enumerate(moves)]
    for copy in ins:
        copy.start()
    outs = []

    def leave(src, dst):
        copy = pltpu.make_async_copy(src, dst, sem_out.at[len(outs)])
        copy.start()
        outs.append(copy)

    ins[1].wait()
    for k in range(LINE):
        add_rows(gate_tmp.at[:, pl.ds(k * width, width)], ex_tmp.at[k, :, pl.ds(0, width)])
        add_rows(up_tmp.at[:, pl.ds(k * width, width)], ex_tmp.at[k, :, pl.ds(width, width)])
    leave(gate_tmp, gate_out)
    leave(up_tmp, up_out)
    ins[2].wait()
    lo = 0
    for out in (q_out, k_out, v_out, o_out):
        leave(a_tmp.at[:, pl.ds(lo, out.shape[1])], out)
        lo += out.shape[1]
    ins[3].wait()
    leave(d_tmp, d_out)
    ins[4].wait()
    leave(x_tmp, x_out)
    ins[5].wait()
    leave(y_tmp, y_out)
    ins[0].wait()
    for row, out in ((3, ga_out), (1, gq_out), (2, gk_out), (0, gm_out)):
        count = out.shape[1]
        value = jnp.zeros((1, 128), f32)
        for i in range(small.shape[1] // 128):
            held = small[row : row + 1, i * 128 : (i + 1) * 128]
            value = jnp.where((me * count) // 128 == i, held, value)
        value = pltpu.roll(value, (128 - (me * count) % 128) % 128, 1)
        out[...] = value[:, 0:count]
    for copy in outs:
        copy.wait()


def results(y, x, small, d, a, ex, widths, shares):
    rows = a.shape[0]
    wide = LINE * ex.shape[2] // 2
    S = jax.ShapeDtypeStruct
    return pl.pallas_call(
        results_kernel,
        out_shape=(
            S(y.shape, bf16),
            S(x.shape, f32),
            *[S((rows, w), f32) for w in widths],
            S((rows, wide), f32),
            S((rows, wide), f32),
            S(d.shape, f32),
            *[S((1, s), f32) for s in shares],
        ),
        in_specs=[ANY] * 6,
        out_specs=(ANY,) * 9 + (VMEM,) * 4,
        scratch_shapes=[
            pltpu.VMEM(y.shape, bf16),
            pltpu.VMEM(x.shape, f32),
            pltpu.VMEM(small.shape, f32),
            pltpu.VMEM(d.shape, f32),
            pltpu.VMEM(a.shape, f32),
            pltpu.VMEM(ex.shape, bf16),
            pltpu.VMEM((rows, wide), f32),
            pltpu.VMEM((rows, wide), f32),
            DMA((6,)),
            DMA((9,)),
        ],
        name="results",
    )(y, x, small, d, a, ex)


def layout(seq_lengths, seq_device, owner, slots):
    owned = seq_device == owner
    counts = jnp.where(owned, seq_lengths, 0)
    starts = jnp.cumsum(counts) - counts
    places = jnp.arange(slots, dtype=jnp.int32)
    inside = (
        owned[:, None]
        & (places[None, :] >= starts[:, None])
        & (places[None, :] < (starts + counts)[:, None])
    )
    labels = jnp.arange(seq_lengths.shape[0], dtype=jnp.int32)
    segment = jnp.sum(jnp.where(inside, labels[:, None] + 1, 0), axis=0) - 1
    position = jnp.sum(jnp.where(inside, places[None, :] - starts[:, None], 0), axis=0)
    return (segment, position)


def allowed_pairs(segment):
    places = jnp.arange(segment.shape[0], dtype=jnp.int32)
    earlier = places[None, :] < places[:, None]
    same_seq = (segment[:, None] == segment[None, :]) & (segment[:, None] >= 0)
    return (places[:, None] == places[None, :]) | earlier & same_seq


def rmsnorm(values, gain):
    return values * lax.rsqrt(jnp.mean(values * values, axis=-1, keepdims=True) + epsilon) * gain


def rotary(values, position):
    half_dim = values.shape[-1] // 2
    freqs = jnp.power(rope_base, -2.0 * jnp.arange(half_dim, dtype=jnp.float32) / values.shape[-1])
    angles = position.astype(jnp.float32)[:, None] * freqs[None, :]
    cosine = jnp.concatenate([jnp.cos(angles), jnp.cos(angles)], axis=-1)[:, None, :]
    sine = jnp.concatenate([jnp.sin(angles), jnp.sin(angles)], axis=-1)[:, None, :]
    rotated = jnp.concatenate([-values[..., half_dim:], values[..., :half_dim]], axis=-1)
    return values * cosine + rotated * sine


def matmul(left, right):
    return jnp.dot(left, right, preferred_element_type=jnp.float32)


def times_rows(left, right):
    return lax.dot_general(left, right, contract_rows, preferred_element_type=jnp.float32)


def times_cols(left, right):
    return lax.dot_general(left, right, contract_cols, preferred_element_type=jnp.float32)


def scatter_sum(partial):
    total = lax.psum_scatter(
        partial.astype(jnp.bfloat16), "fsdp", scatter_dimension=0, tiled=True
    )
    return total.astype(jnp.float32)


def plain(
    hidden_in,
    out_grad,
    seq_lengths,
    seq_device,
    attn_gain,
    q_gain,
    k_gain,
    w_query,
    w_key,
    w_value,
    w_out,
    mlp_gain,
    w_gate,
    w_up,
    w_down,
):
    slots = hidden_in.shape[0]
    groups = H // KVH
    score_scale = HD ** (-0.5)
    segment, position = layout(seq_lengths, seq_device, lax.axis_index("fsdp"), slots)
    allowed = allowed_pairs(segment)[None, None]

    def query_path(raw, gain):
        return rotary(rmsnorm(raw.reshape(slots, H, HD), gain), position)

    def key_path(raw, gain):
        return rotary(rmsnorm(raw.reshape(slots, KVH, HD), gain), position)

    def swiglu(gate_in, up_in):
        return jax.nn.silu(gate_in) * up_in

    attn_set = (
        lax.all_gather(attn_gain, "fsdp", axis=0, tiled=True),
        lax.all_gather(q_gain, "fsdp", axis=0, tiled=True),
        lax.all_gather(k_gain, "fsdp", axis=0, tiled=True),
        lax.all_gather(w_query, "fsdp", axis=0, tiled=True),
        lax.all_gather(w_key, "fsdp", axis=0, tiled=True),
        lax.all_gather(w_value, "fsdp", axis=0, tiled=True),
        lax.all_gather(w_out, "fsdp", axis=0, tiled=True),
    )
    gain_attn, gain_query, gain_key, query_w, key_w, value_w, out_w = attn_set
    inputs = hidden_in.astype(jnp.float32)
    normed = rmsnorm(inputs, gain_attn.astype(jnp.float32)).astype(jnp.bfloat16)
    query_raw = matmul(normed, query_w)
    key_raw = matmul(normed, key_w)
    value_raw = matmul(normed, value_w)
    queries = (
        query_path(query_raw, gain_query.astype(jnp.float32))
        .astype(jnp.bfloat16)
        .reshape(slots, KVH, groups, HD)
    )
    keys = key_path(key_raw, gain_key.astype(jnp.float32)).astype(jnp.bfloat16)
    values = value_raw.astype(jnp.bfloat16).reshape(slots, KVH, HD)

    def masked_logits():
        scores = (
            jnp.einsum("qgrd,kgd->grqk", queries, keys, preferred_element_type=jnp.float32)
            * score_scale
        )
        return jnp.where(allowed, scores, masked_score)

    logits = masked_logits()
    row_top = jnp.max(logits, axis=-1, keepdims=True)
    exponent = jnp.exp(logits - row_top)
    row_total = jnp.sum(exponent, axis=-1, keepdims=True)
    log_total = row_top + jnp.log(row_total)
    weights = (exponent / row_total).astype(jnp.bfloat16)
    mixed = jnp.einsum("grqk,kgd->qgrd", weights, values, preferred_element_type=jnp.float32)
    mixed = mixed.reshape(slots, H * HD).astype(jnp.bfloat16)
    middle = inputs + matmul(mixed, out_w)
    mlp_set = (
        lax.all_gather(mlp_gain, "fsdp", axis=0, tiled=True),
        lax.all_gather(w_gate, "fsdp", axis=0, tiled=True),
        lax.all_gather(w_up, "fsdp", axis=0, tiled=True),
        lax.all_gather(w_down, "fsdp", axis=0, tiled=True),
    )
    gain_mlp, gate_w, up_w, down_w = mlp_set
    second = rmsnorm(middle, gain_mlp.astype(jnp.float32)).astype(jnp.bfloat16)
    gate_out = matmul(second, gate_w)
    up_out = matmul(second, up_w)
    hidden = swiglu(gate_out, up_out).astype(jnp.bfloat16)
    hidden_out = (middle + matmul(hidden, down_w)).astype(jnp.bfloat16)
    gain_mlp, gate_w, up_w, down_w = (
        lax.all_gather(mlp_gain, "fsdp", axis=0, tiled=True),
        lax.all_gather(w_gate, "fsdp", axis=0, tiled=True),
        lax.all_gather(w_up, "fsdp", axis=0, tiled=True),
        lax.all_gather(w_down, "fsdp", axis=0, tiled=True),
    )
    grad_down = scatter_sum(times_rows(hidden, out_grad))
    d_hidden = times_cols(out_grad, down_w)
    unused_out, swiglu_pull = jax.vjp(swiglu, gate_out, up_out)
    d_gate, d_up = swiglu_pull(d_hidden)
    d_gate_up = jnp.concatenate([d_gate.astype(jnp.bfloat16), d_up.astype(jnp.bfloat16)], axis=1)
    grad_gate_up = scatter_sum(times_rows(second, d_gate_up))
    ff_width = gate_w.shape[1]
    d_second = times_cols(d_gate_up, jnp.concatenate([gate_w, up_w], axis=1))
    unused_norm, second_pull = jax.vjp(rmsnorm, middle, gain_mlp.astype(jnp.float32))
    d_middle_norm, grad_gain_mlp = second_pull(d_second)
    d_middle = out_grad.astype(jnp.float32) + d_middle_norm
    gain_attn, gain_query, gain_key, query_w, key_w, value_w, out_w = (
        lax.all_gather(attn_gain, "fsdp", axis=0, tiled=True),
        lax.all_gather(q_gain, "fsdp", axis=0, tiled=True),
        lax.all_gather(k_gain, "fsdp", axis=0, tiled=True),
        lax.all_gather(w_query, "fsdp", axis=0, tiled=True),
        lax.all_gather(w_key, "fsdp", axis=0, tiled=True),
        lax.all_gather(w_value, "fsdp", axis=0, tiled=True),
        lax.all_gather(w_out, "fsdp", axis=0, tiled=True),
    )
    d_branch = d_middle.astype(jnp.bfloat16)
    grad_out_w = scatter_sum(times_rows(mixed, d_branch))
    d_mixed = times_cols(d_branch, out_w).astype(jnp.bfloat16).reshape(slots, KVH, groups, HD)
    probs = jnp.exp(masked_logits() - log_total)
    weights = probs.astype(jnp.bfloat16)
    d_probs = jnp.einsum("qgrd,kgd->grqk", d_mixed, values, preferred_element_type=jnp.float32)
    d_logits = probs * (d_probs - jnp.sum(probs * d_probs, axis=-1, keepdims=True))
    d_scores = (d_logits * score_scale).astype(jnp.bfloat16)
    d_values = jnp.einsum("grqk,qgrd->kgd", weights, d_mixed, preferred_element_type=jnp.float32)
    d_values = d_values.astype(jnp.bfloat16).reshape(slots, KVH * HD)
    d_queries_rot = jnp.einsum(
        "grqk,kgd->qgrd", d_scores, keys, preferred_element_type=jnp.float32
    ).reshape(slots, H, HD)
    d_keys_rot = jnp.einsum("grqk,qgrd->kgd", d_scores, queries, preferred_element_type=jnp.float32)
    unused_query, query_pull = jax.vjp(query_path, query_raw, gain_query.astype(jnp.float32))
    d_query_raw, grad_gain_query = query_pull(d_queries_rot)
    unused_key, key_pull = jax.vjp(key_path, key_raw, gain_key.astype(jnp.float32))
    d_key_raw, grad_gain_key = key_pull(d_keys_rot)
    d_qkv = jnp.concatenate(
        [d_query_raw.astype(jnp.bfloat16), d_key_raw.astype(jnp.bfloat16), d_values], axis=1
    )
    grad_qkv = scatter_sum(times_rows(normed, d_qkv))
    d_normed = times_cols(d_qkv, jnp.concatenate([query_w, key_w, value_w], axis=1))
    unused_first, first_pull = jax.vjp(rmsnorm, inputs, gain_attn.astype(jnp.float32))
    d_input_norm, grad_gain_attn = first_pull(d_normed)
    input_grad = d_middle + d_input_norm
    gain_sums = (
        lax.psum_scatter(grad_gain_attn, "fsdp", scatter_dimension=0, tiled=True),
        lax.psum_scatter(grad_gain_query, "fsdp", scatter_dimension=0, tiled=True),
        lax.psum_scatter(grad_gain_key, "fsdp", scatter_dimension=0, tiled=True),
        lax.psum_scatter(grad_gain_mlp, "fsdp", scatter_dimension=0, tiled=True),
    )
    query_width = H * HD
    key_width = KVH * HD
    grad_query_w = grad_qkv[:, :query_width]
    grad_key_w = grad_qkv[:, query_width : query_width + key_width]
    grad_value_w = grad_qkv[:, query_width + key_width :]
    grad_gate = grad_gate_up[:, :ff_width]
    grad_up = grad_gate_up[:, ff_width:]
    return (
        hidden_out,
        input_grad,
        gain_sums[0],
        gain_sums[1],
        gain_sums[2],
        grad_query_w,
        grad_key_w,
        grad_value_w,
        grad_out_w,
        gain_sums[3],
        grad_gate,
        grad_up,
        grad_down,
    )


def layered(
    hidden_in,
    out_grad,
    seq_lengths,
    seq_device,
    attn_gain,
    q_gain,
    k_gain,
    w_query,
    w_key,
    w_value,
    w_out,
    mlp_gain,
    w_gate,
    w_up,
    w_down,
):
    (
        attn_w, gate_up_w, down_w, tokens, cotangent, hidden, gate_up,
        middle, normed, qkv_raw, queries, keys, values, mixed, gains, rope,
    ) = forward(
        hidden_in, out_grad, seq_lengths, seq_device, (attn_gain, mlp_gain, q_gain, k_gain),
        w_query, w_key, w_value, w_out, w_gate, w_up, w_down,
    )
    dim = hidden_in.shape[1]
    x, small, y, grad_down, attn_sums, exchanged, *unused = backward(
        gate_up_w.reshape(-1, gate_up_w.shape[-1]),
        down_w.reshape(-1, dim),
        tokens.reshape(-1, dim),
        cotangent.reshape(-1, dim),
        hidden, gate_up, attn_w, middle, normed, qkv_raw, queries, keys, values, mixed,
        hidden_in, gains, rope,
    )
    (
        hidden_out, input_grad, g_query, g_key, g_value, g_out, g_gate, g_up, g_down,
        g_attn_gain, g_q_gain, g_k_gain, g_mlp_gain,
    ) = results(
        y, x, small, grad_down, attn_sums, exchanged,
        [w.shape[1] for w in (w_query, w_key, w_value, w_out)],
        [g.shape[0] for g in (attn_gain, q_gain, k_gain, mlp_gain)],
    )
    return (
        hidden_out,
        input_grad,
        g_attn_gain[0],
        g_q_gain[0],
        g_k_gain[0],
        g_query,
        g_key,
        g_value,
        g_out,
        g_mlp_gain[0],
        g_gate,
        g_up,
        g_down,
    )


def solution(mesh):
    per_device = layered if mesh.shape["fsdp"] == RING * LINE else plain
    return jax.shard_map(
        per_device,
        mesh=mesh,
        in_specs=(
            P("fsdp", None),
            P("fsdp", None),
            P(),
            P(),
            P("fsdp"),
            P("fsdp"),
            P("fsdp"),
            P("fsdp", None),
            P("fsdp", None),
            P("fsdp", None),
            P("fsdp", None),
            P("fsdp"),
            P("fsdp", None),
            P("fsdp", None),
            P("fsdp", None),
        ),
        out_specs=(
            P("fsdp", None),
            P("fsdp", None),
            P("fsdp"),
            P("fsdp"),
            P("fsdp"),
            P("fsdp", None),
            P("fsdp", None),
            P("fsdp", None),
            P("fsdp", None),
            P("fsdp"),
            P("fsdp", None),
            P("fsdp", None),
            P("fsdp", None),
        ),
        check_vma=False,
    )
```

```python
import math

import jax
import jax.numpy as jnp
from jax import lax
from jax.experimental import pallas as pl
from jax.experimental.pallas import tpu as pltpu
from jax.sharding import PartitionSpec as P

H = 16
KVH = 8
HD = 128
CAP = 128
LINE = 4
RING = 8
MESH = pl.DeviceIdType.MESH
ANY = pl.BlockSpec(memory_space=pl.ANY)
VMEM = pl.BlockSpec(memory_space=pltpu.VMEM)
DMA = pltpu.SemaphoreType.DMA
bf16 = jnp.bfloat16
f32 = jnp.float32
epsilon = 1e-06
rope_base = 1000000.0
masked_score = -1e30
contract_rows = (((0,), (0,)), ((), ()))
contract_cols = (((1,), (1,)), ((), ()))


def where_am_i():
    me = lax.axis_index("fsdp")
    core = me % 2
    z = me // RING
    f_bit = 2 + 2 * core
    s_bit = 4 - 2 * core
    first = me + f_bit * (1 - 2 * ((me // f_bit) % 2))
    second = me + s_bit * (1 - 2 * ((me // s_bit) % 2))
    sibling = me + 1 - 2 * core
    return me, z, first, second, sibling


def greet(peers):
    barrier = pltpu.get_barrier_semaphore()
    for peer in peers:
        pl.semaphore_signal(barrier, inc=1, device_id=(peer,), device_id_type=MESH)
    pl.semaphore_wait(barrier, len(peers))


def remote(src, dst, send_sem, recv_sem, device):
    return pltpu.make_async_remote_copy(
        src_ref=src,
        dst_ref=dst,
        send_sem=send_sem,
        recv_sem=recv_sem,
        device_id=(device,),
        device_id_type=MESH,
    )


def line_peers(me):
    return [lax.rem(me + RING * k, RING * LINE) for k in range(1, LINE)]


def on_line(z, k, body):
    for step in ((-k, k) if k else (0,)):

        @pl.when((z + step >= 0) & (z + step < LINE))
        def _(step=step):
            body(step)


def dot_nt(left, right):
    return lax.dot_general(left, right, contract_cols, preferred_element_type=f32)


def dot_tn(left, right):
    return lax.dot_general(left, right, contract_rows, preferred_element_type=f32)


def streamed(count, fetch, body):
    for copy in fetch(0, 0):
        copy.start()

    def step(i, carry):
        slot = i % 2

        @pl.when(i + 1 < count)
        def _():
            for copy in fetch(i + 1, 1 - slot):
                copy.start()

        for copy in fetch(i, slot):
            copy.wait()
        body(i, slot)
        return carry

    lax.fori_loop(0, count, step, 0)


def tile(i, size):
    return pl.ds(pl.multiple_of(i * size, size), size)


def add_rows(out, *terms):
    rows = out.shape[0]

    def body(i, carry):
        at = pl.ds(pl.multiple_of(i * 16, 16), 16)
        total = terms[0][at, :].astype(f32)
        for term in terms[1:]:
            total = total + term[at, :].astype(f32)
        out[at, :] = total.astype(out.dtype)
        return carry

    lax.fori_loop(0, rows // 16, body, 0, unroll=2)


def lane_sum(x):
    return jnp.sum(x, axis=-1, keepdims=True)


def token_places(lengths, devices, me):
    seqs = lengths.shape[1]
    counts_row = jnp.where(devices == me, lengths, 0).astype(f32)
    up = lax.broadcasted_iota(jnp.int32, (seqs, seqs), 0)
    across = lax.broadcasted_iota(jnp.int32, (seqs, seqs), 1)
    counts_col = lane_sum(jnp.where(up == across, counts_row, 0.0))
    starts_row = jnp.sum(jnp.where(up < across, counts_col, 0.0), axis=0, keepdims=True)
    starts_col = lane_sum(jnp.where(across < up, counts_row, 0.0))

    def within(places, starts, counts):
        return (places >= starts) & (places < starts + counts)

    places = lax.broadcasted_iota(jnp.int32, (CAP, seqs), 0).astype(f32)
    labels = lax.broadcasted_iota(jnp.int32, (CAP, seqs), 1).astype(f32)
    inside = within(places, starts_row, counts_row)
    segment_col = lane_sum(jnp.where(inside, labels + 1.0, 0.0)) - 1.0
    position = lane_sum(jnp.where(inside, places - starts_row, 0.0))
    places = lax.broadcasted_iota(jnp.int32, (seqs, CAP), 1).astype(f32)
    labels = lax.broadcasted_iota(jnp.int32, (seqs, CAP), 0).astype(f32)
    inside = within(places, starts_col, counts_col)
    segment_row = jnp.sum(jnp.where(inside, labels + 1.0, 0.0), axis=0, keepdims=True) - 1.0
    return segment_col, segment_row, position


def allowed_bias(segment_col, segment_row):
    t = lax.broadcasted_iota(jnp.int32, (CAP, CAP), 0)
    u = lax.broadcasted_iota(jnp.int32, (CAP, CAP), 1)
    same = (segment_col == segment_row) & (segment_col >= 0.0)
    return jnp.where((t == u) | ((u < t) & same), 0.0, masked_score)


def half_turn(v):
    lane = lax.broadcasted_iota(jnp.int32, v.shape, v.ndim - 1)
    turned = pltpu.roll(v, HD // 2, v.ndim - 1)
    return jnp.where(lane < HD // 2, -turned, turned)


def rms_scale(v):
    return lax.rsqrt(jnp.mean(v * v, axis=-1, keepdims=True) + epsilon)


def forward_kernel(
    x_ref, len_ref, dev_ref, ga_ref, gm_ref, gq_ref, gk_ref, cot_ref,
    wq_ref, wk_ref, wv_ref, wo_ref, gate_ref, up_ref, wd_ref,
    w_out, gu_out, d_out, tok_out, cot_out, hid_out, pre_out,
    middle_out, normed_out, raw_out, q_out, k_out, v_out, mixed_out, gains_out, rope_out,
    w_tmp, p_tmp, d_tmp, cot_tmp, second_tmp, chunk, ow_all, gain_tmp, gain_own,
    tok_all, gate_up, m_chunk, hid,
    local, up_s, down_s, first_s, second_s, sib_s, recv, ex_send, ex_recv,
    m_first_s, m_second_s, m_sib_s, m_recv, line_up, line_down, line_r, w_load, o_load, g_load,
    act_out,
):
    me, z, first, second, sibling = where_am_i()
    col, fcol, scol = me % RING, first % RING, second % RING
    sfcol = (second + first - me) % RING
    width = p_tmp.shape[2] // 2
    rows = w_tmp.shape[0]
    qkv_width = raw_out.shape[1]
    attn_width = qkv_width + wo_ref.shape[1]
    last = LINE - 1
    pieces = LINE + 1

    w_in = []
    lo = 0
    for i, ref in enumerate((wq_ref, wk_ref, wv_ref, wo_ref)):
        at = pl.ds(lo, ref.shape[1])
        w_in.append(pltpu.make_async_copy(ref, w_tmp.at[:, at], local.at[i]))
        lo += ref.shape[1]
    p_in = [
        pltpu.make_async_copy(
            ref.at[:, pl.ds(pl.multiple_of(z * width, width), width)],
            p_tmp.at[z, :, pl.ds(which * width, width)],
            local.at[5 + which],
        )
        for which, ref in enumerate((gate_ref, up_ref))
    ]
    cot_in = pltpu.make_async_copy(cot_ref, cot_tmp, local.at[8])
    d_in = pltpu.make_async_copy(wd_ref, d_tmp, local.at[7])
    for copy in w_in + p_in + [d_in, cot_in]:
        copy.start()
    gain_own[...] = jnp.zeros_like(gain_own)
    for i, ref in enumerate((ga_ref, gm_ref, gq_ref, gk_ref)):
        gain_own[i : i + 1, 0 : ref.shape[1]] = ref[...].astype(f32)
    flat = gain_own[...]
    paired = jnp.where(me % 2 == 0, flat, pltpu.roll(flat, rows, 1))
    shared = pltpu.roll(flat, gq_ref.shape[1] * me, 1)
    placed = jnp.where(lax.broadcasted_iota(jnp.int32, flat.shape, 0) < 2, paired, shared)
    w_tmp[0:16, attn_width:] = placed.astype(bf16)
    w_tmp[16:, attn_width:] = jnp.zeros((rows - 16, 128), bf16)
    greet(line_peers(me) + [first, second, sibling])

    def send(src, shard, sems, device):
        return remote(src, w_out.at[shard], sems.at[shard], recv.at[shard], device)

    def arrived(shard):
        send(w_out.at[shard], shard, sib_s, sibling).wait_recv()

    def exchange(k, which):
        peer_z = lax.rem(z + k, LINE)
        src = (gate_ref, up_ref)[which].at[:, pl.ds(pl.multiple_of(peer_z * width, width), width)]
        dst = p_tmp.at[z, :, pl.ds(which * width, width)]
        return remote(src, dst, ex_send.at[k, which], ex_recv.at[k, which], col + RING * peer_z)

    token_half = second_tmp.shape[1] // 2

    def line_spot(which, shard):
        if which == 1:
            return cot_out.at[shard]
        return tok_out.at[shard, :, pl.ds(token_half * (which // 2), token_half)]

    def line_send(src, which, shard, sems, device):
        landing = line_spot(which, shard)
        return remote(src, landing, sems.at[which, shard], line_r.at[which, shard], device)

    def line_own(which, src):
        @pl.when(z < last)
        def _():
            line_send(src, which, z, line_up, me + RING).start()

        @pl.when(z > 0)
        def _():
            line_send(src, which, z, line_down, me - RING).start()

    def line_relay(which, k):
        def body(step):
            shard = z + step
            src = line_spot(which, shard)
            line_send(src, which, shard, line_up, second).wait_recv()
            if step < 0:

                @pl.when(z < last)
                def _():
                    line_send(src, which, shard, line_up, me + RING).start()
            else:

                @pl.when(z > 0)
                def _():
                    line_send(src, which, shard, line_down, me - RING).start()

        on_line(z, k, body)

    for copy in w_in:
        copy.wait()

    @pl.when(z < last)
    def _():
        send(w_tmp, me, up_s, me + RING).start()

    @pl.when(z > 0)
    def _():
        send(w_tmp, me, down_s, me - RING).start()

    send(w_tmp, me, first_s, first).start()
    send(w_tmp, me, second_s, second).start()
    send(w_tmp, me, sib_s, sibling).start()
    w_back = pltpu.make_async_copy(w_tmp, w_out.at[me], local.at[9])
    w_back.start()

    def own(k):
        def body(step):
            shard = me + RING * step
            src = w_out.at[shard]
            arrived(shard)
            if step < 0:

                @pl.when(z < last)
                def _():
                    send(src, shard, up_s, me + RING).start()
            else:

                @pl.when(z > 0)
                def _():
                    send(src, shard, down_s, me - RING).start()

            send(src, shard, first_s, first).start()
            send(src, shard, second_s, second).start()
            send(src, shard, sib_s, sibling).start()

        on_line(z, k, body)

    def other(base, k, onward):
        def body(step):
            shard = base + RING * (z + step)
            src = w_out.at[shard]
            arrived(shard)
            if onward:
                send(src, shard, second_s, second).start()
            send(src, shard, sib_s, sibling).start()

        on_line(z, k, body)

    segment_col, segment_row, position = token_places(len_ref[...], dev_ref[...], me)
    rope_out[2] = allowed_bias(segment_col, segment_row)
    lane = lax.broadcasted_iota(jnp.int32, (1, HD), 1) % (HD // 2)
    angles = position * jnp.exp(lane.astype(f32) * (-2.0 * math.log(rope_base) / HD))
    rope_out[0] = jnp.cos(angles)
    rope_out[1] = jnp.sin(angles)
    x_scale = rms_scale(x_ref[...].astype(f32))
    raw_out[...] = jnp.zeros_like(raw_out)

    def load_group(step):
        zz = z + step
        part = w_out.at[pl.ds(RING * zz, RING)]
        return (
            pltpu.make_async_copy(part.at[:, :, pl.ds(0, qkv_width)], chunk, w_load),
            pltpu.make_async_copy(
                part.at[:, :, pl.ds(qkv_width, attn_width - qkv_width)],
                ow_all.at[pl.ds(RING * zz, RING)],
                o_load.at[zz],
            ),
            pltpu.make_async_copy(
                part.at[:, pl.ds(0, 16), pl.ds(attn_width, 128)], gain_tmp.at[zz], g_load
            ),
        )

    def group(k):
        def body(step):
            zz = z + step
            for i in range(RING // 2):
                arrived(RING * zz + 2 * i + sibling % 2)
            copies = load_group(step)
            for copy in copies:
                copy.start()
            copies[2].wait()
            span = RING * rows
            for pair in range(RING // 2):
                at = pl.ds(pl.multiple_of(zz * span + pair * 128, 128), 128)
                both = gain_tmp[zz, 2 * pair].astype(f32) + gain_tmp[zz, 2 * pair + 1].astype(f32)
                gains_out[0:2, at] = both[0:2]
                piece = x_ref[:, at].astype(f32) * x_scale * both[0:1]
                normed_out[:, at] = piece.astype(bf16)
            copies[0].wait()
            left = normed_out[:, pl.ds(pl.multiple_of(zz * span, span), span)]

            def tile(i, carry):
                at = pl.ds(pl.multiple_of(i * 512, 512), 512)
                right = chunk[:, :, at].reshape(span, 512)
                raw_out[:, at] += jnp.dot(left, right, preferred_element_type=f32)
                return carry

            lax.fori_loop(0, qkv_width // 512, tile, 0)

        on_line(z, k, body)

    own(1)
    other(fcol, 0, True)
    own(2)
    other(fcol, 1, True)
    other(scol, 0, False)
    for k in range(1, LINE):
        for which in range(2):
            exchange(k, which).start()
    cot_in.wait()
    line_own(1, cot_tmp)
    cot_back = pltpu.make_async_copy(cot_tmp, cot_out.at[z], local.at[10])
    cot_back.start()
    own(3)
    other(fcol, 2, True)
    other(scol, 1, False)
    other(sfcol, 0, False)
    w_back.wait()
    line_relay(1, 1)
    group(0)
    other(fcol, 3, True)
    other(scol, 2, False)
    other(sfcol, 1, False)
    for copy in p_in + [d_in]:
        copy.wait()
    for k in range(1, LINE):
        for which in range(2):
            src_z = lax.rem(z + LINE - k, LINE)
            landed = p_tmp.at[src_z, :, pl.ds(which * width, width)]
            remote(landed, landed, ex_send.at[k, which], ex_recv.at[k, which], second).wait_recv()

    def spot(piece, shard):
        return gu_out.at[piece, shard] if piece < LINE else d_out.at[shard]

    def source(piece):
        return p_tmp.at[piece] if piece < LINE else d_tmp

    def m_send(src, piece, shard, sems, device):
        return remote(
            src, spot(piece, shard), sems.at[piece, shard], m_recv.at[piece, shard], device
        )

    def m_arrived(piece, shard):
        m_send(spot(piece, shard), piece, shard, m_sib_s, sibling).wait_recv()

    def m_own_second(piece):
        m_send(source(piece), piece, col, m_second_s, second).start()

    def m_own_first(piece):
        m_send(source(piece), piece, col, m_first_s, first).start()
        m_send(source(piece), piece, col, m_sib_s, sibling).start()

    def m_own(piece):
        m_own_second(piece)
        m_own_first(piece)

    m_own_second(0)
    m_own_second(1)
    m_own_second(LINE)
    p_back = pltpu.make_async_copy(p_tmp, gu_out.at[:, col], local.at[11])
    p_back.start()
    d_back = pltpu.make_async_copy(d_tmp, d_out.at[col], local.at[4])
    d_back.start()
    line_relay(1, 2)
    group(1)

    other(scol, 3, False)
    other(sfcol, 2, False)
    group(2)
    other(sfcol, 3, False)
    m_own_first(0)
    m_own_first(1)
    m_own_first(LINE)
    line_relay(1, 3)
    group(3)

    small = jnp.zeros((16, 128), f32)
    for zz in range(LINE):
        for i in range(RING):
            small = small + gain_tmp[zz, i].astype(f32)
    q_gain, k_gain = small[2:3], small[3:4]
    gains_out[2:4, 0:128] = small[2:4]
    cosine, sine, bias = rope_out[0], rope_out[1], rope_out[2]

    def turned(v, gain):
        v = v * rms_scale(v) * gain
        return (v * cosine + half_turn(v) * sine).astype(bf16)

    kv0 = H * HD
    v0 = kv0 + KVH * HD

    def head(g, carry):
        at = pl.ds(pl.multiple_of(g * HD, HD), HD)
        qa = pl.ds(pl.multiple_of(g * 2 * HD, 2 * HD), HD)
        qb = pl.ds(pl.multiple_of(g * 2 * HD + HD, HD), HD)
        key = turned(raw_out[:, pl.ds(pl.multiple_of(kv0 + g * HD, HD), HD)], k_gain)
        value = raw_out[:, pl.ds(pl.multiple_of(v0 + g * HD, HD), HD)].astype(bf16)
        k_out[:, at] = key
        v_out[:, at] = value
        query_a = turned(raw_out[:, qa], q_gain)
        query_b = turned(raw_out[:, qb], q_gain)
        q_out[:, qa] = query_a
        q_out[:, qb] = query_b
        for query, where in ((query_a, qa), (query_b, qb)):
            scores = lax.dot_general(query, key, contract_cols, preferred_element_type=f32)
            logits = scores * (HD ** (-0.5)) + bias
            exponent = jnp.exp(logits - jnp.max(logits, axis=-1, keepdims=True))
            weights = (exponent / lane_sum(exponent)).astype(bf16)
            mixed = jnp.dot(weights, value, preferred_element_type=f32)
            mixed_out[:, where] = mixed.astype(bf16)
        return carry

    lax.fori_loop(0, KVH, head, 0, unroll=2)
    for zz in range(LINE):
        pltpu.make_async_copy(
            w_out.at[pl.ds(RING * zz, RING), :, pl.ds(qkv_width, attn_width - qkv_width)],
            ow_all.at[pl.ds(RING * zz, RING)],
            o_load.at[zz],
        ).wait()
    mixed = mixed_out[...]

    def out_tile(i, total):
        at = pl.ds(pl.multiple_of(i * 512, 512), 512)
        right = ow_all[:, :, at].reshape(mixed.shape[1], 512)
        middle = x_ref[:, at].astype(f32) + jnp.dot(mixed, right, preferred_element_type=f32)
        middle_out[:, at] = middle
        return total + lane_sum(middle * middle)

    tiles = middle_out.shape[1] // 512
    total = lax.fori_loop(0, tiles, out_tile, jnp.zeros((CAP, 1), f32))
    scale = lax.rsqrt(total / middle_out.shape[1] + epsilon)

    def norm_tile(i, carry):
        at = pl.ds(pl.multiple_of(i * 512, 512), 512)
        second_tmp[:, at] = (middle_out[:, at] * scale * gains_out[1:2, at]).astype(bf16)
        return carry

    lax.fori_loop(0, tiles, norm_tile, 0)

    def m_other(piece, shard, onward):
        m_arrived(piece, shard)
        if onward:
            m_send(spot(piece, shard), piece, shard, m_second_s, second).start()
        m_send(spot(piece, shard), piece, shard, m_sib_s, sibling).start()

    def m_whole(piece):
        for k in range(RING // 2):
            m_arrived(piece, 2 * k + sibling % 2)

    part = width

    def gate_up_copy(piece):
        return pltpu.make_async_copy(
            gu_out.at[piece], m_chunk.at[piece % 2], act_out.at[piece % 2, 0]
        )

    def gate_up_load(piece):
        m_whole(piece)
        gate_up_copy(piece).start()

    def gate_up_rows(piece):
        gate_up_copy(piece).wait()
        span = RING * rows
        left = tok_all[:, :, pl.ds(piece * span, span)].reshape(LINE * CAP, span)

        def columns(n, carry):
            at = tile(n, 512)
            right = m_chunk[piece % 2, :, :, at].reshape(span, 512)
            term = jnp.dot(left, right, preferred_element_type=f32)
            if piece == 0:
                gate_up[:, at] = term
            else:
                gate_up[:, at] += term
            return carry

        lax.fori_loop(0, 2 * part // 512, columns, 0)

    m_own(2)
    line_own(0, second_tmp.at[:, pl.ds(0, token_half)])
    line_own(2, second_tmp.at[:, pl.ds(token_half, token_half)])
    tok_back = pltpu.make_async_copy(second_tmp, tok_out.at[z], local.at[13])
    tok_back.start()
    m_other(0, fcol, True)
    m_other(0, scol, False)
    m_own(3)
    line_relay(0, 1)
    line_relay(2, 1)
    m_other(1, fcol, True)
    m_other(1, scol, False)
    m_other(0, sfcol, False)
    line_relay(0, 2)
    line_relay(2, 2)
    m_other(2, fcol, True)
    m_other(2, scol, False)
    m_other(1, sfcol, False)
    p_back.wait()
    gate_up_load(0)
    m_other(3, fcol, True)
    m_other(3, scol, False)
    m_other(LINE, fcol, True)
    m_other(LINE, scol, False)
    line_relay(0, 3)
    tok_back.wait()
    cot_back.wait()
    tok_in = []
    for half in range(2):
        at = pl.ds(half * token_half, token_half)
        tok_in.append(
            pltpu.make_async_copy(
                tok_out.at[:, :, at], tok_all.at[:, :, at], local.at[10 if half else 12]
            )
        )
    tok_in[0].start()
    gate_up_load(1)
    tok_in[0].wait()
    gate_up_rows(0)
    m_other(2, sfcol, False)
    gate_up_load(2)
    gate_up_rows(1)
    line_relay(2, 3)
    tok_in[1].start()
    tok_in[1].wait()
    m_other(3, sfcol, False)
    gate_up_load(3)
    gate_up_rows(2)
    gate_up_rows(3)

    def hid_copy(n):
        at = tile(n, 256)
        return pltpu.make_async_copy(hid.at[:, at], hid_out.at[:, at], act_out.at[n, 0])

    def pre_copies(n):
        up_at = pl.ds(pl.multiple_of(part + n * 256, 256), 256)
        return [
            pltpu.make_async_copy(gate_up.at[:, at], pre_out.at[:, at], act_out.at[n, i])
            for i, at in ((1, tile(n, 256)), (2, up_at))
        ]

    def units(n, carry):
        at = tile(n, 256)
        up_at = pl.ds(pl.multiple_of(part + n * 256, 256), 256)
        for copy in pre_copies(n):
            copy.start()

        def act(r, inner):
            some = tile(r, 32)
            gate, up = gate_up[some, at], gate_up[some, up_at]
            hid[some, at] = (gate * jax.nn.sigmoid(gate) * up).astype(bf16)
            return inner

        lax.fori_loop(0, LINE * CAP // 32, act, 0, unroll=4)
        hid_copy(n).start()
        return carry

    lax.fori_loop(0, part // 256, units, 0)
    m_other(LINE, sfcol, False)
    d_back.wait()
    m_whole(LINE)

    for n in range(part // 256):
        for copy in [hid_copy(n)] + pre_copies(n):
            copy.wait()
    for k in range(1, LINE):
        for which in range(2):
            exchange(k, which).wait_send()
    for k in range(LINE):

        @pl.when((z < last) & (k <= z))
        def _(k=k):
            send(w_tmp, col + RING * k, up_s, me + RING).wait_send()
            for which in range(3):
                line_send(line_spot(which, k), which, k, line_up, me + RING).wait_send()

        @pl.when((z > 0) & (k >= z))
        def _(k=k):
            send(w_tmp, col + RING * k, down_s, me - RING).wait_send()
            for which in range(3):
                line_send(line_spot(which, k), which, k, line_down, me - RING).wait_send()

        send(w_tmp, col + RING * k, first_s, first).wait_send()
        send(w_tmp, col + RING * k, second_s, second).wait_send()
        send(w_tmp, fcol + RING * k, second_s, second).wait_send()
        for base in (col, fcol, scol, sfcol):
            send(w_tmp, base + RING * k, sib_s, sibling).wait_send()
    for piece in range(pieces):
        src = source(piece)
        m_send(src, piece, col, m_first_s, first).wait_send()
        m_send(src, piece, col, m_second_s, second).wait_send()
        m_send(src, piece, fcol, m_second_s, second).wait_send()
        for base in (col, fcol, scol, sfcol):
            m_send(src, piece, base, m_sib_s, sibling).wait_send()


def forward(hidden_in, out_grad, seq_lengths, seq_device, gains, wq, wk, wv, wo, gate, up, wd):
    slots, dim = hidden_in.shape
    rows = wq.shape[0]
    n = RING * LINE
    width = gate.shape[1] // LINE
    qkv_width = wq.shape[1] + wk.shape[1] + wv.shape[1]
    wide = qkv_width + wo.shape[1] + 128
    pieces = LINE + 1
    S = jax.ShapeDtypeStruct
    return pl.pallas_call(
        forward_kernel,
        out_shape=(
            S((n, rows, wide), bf16),
            S((LINE, RING, rows, 2 * width), bf16),
            S((RING,) + wd.shape, bf16),
            S((LINE, slots, dim), bf16),
            S((LINE, slots, dim), bf16),
            S((LINE * slots, width), bf16),
            S((LINE * slots, 2 * width), f32),
            S((slots, dim), f32),
            S((slots, dim), bf16),
            S((slots, qkv_width), f32),
            S((slots, H * HD), bf16),
            S((slots, KVH * HD), bf16),
            S((slots, KVH * HD), bf16),
            S((slots, H * HD), bf16),
            S((8, dim), f32),
            S((3, slots, HD), f32),
        ),
        in_specs=[VMEM] * 7 + [ANY] * 8,
        out_specs=(ANY,) * 7 + (VMEM,) * 9,
        scratch_shapes=[
            pltpu.VMEM((rows, wide), bf16),
            pltpu.VMEM((LINE, rows, 2 * width), bf16),
            pltpu.VMEM(wd.shape, bf16),
            pltpu.VMEM((slots, dim), bf16),
            pltpu.VMEM((slots, dim), bf16),
            pltpu.VMEM((RING, rows, qkv_width), bf16),
            pltpu.VMEM((n, rows, wo.shape[1]), bf16),
            pltpu.VMEM((LINE, RING, 16, 128), bf16),
            pltpu.VMEM((16, 128), f32),
            pltpu.VMEM((LINE, slots, dim), bf16),
            pltpu.VMEM((LINE * slots, 2 * width), f32),
            pltpu.VMEM((2, RING, rows, 2 * width), bf16),
            pltpu.VMEM((LINE * slots, width), bf16),
            DMA((14,)),
            DMA((n,)),
            DMA((n,)),
            DMA((n,)),
            DMA((n,)),
            DMA((n,)),
            DMA((n,)),
            DMA((LINE, 2)),
            DMA((LINE, 2)),
            DMA((pieces, RING)),
            DMA((pieces, RING)),
            DMA((pieces, RING)),
            DMA((pieces, RING)),
            DMA((3, LINE)),
            DMA((3, LINE)),
            DMA((3, LINE)),
            DMA,
            DMA((LINE,)),
            DMA,
            DMA((width // 256, 3)),
        ],
        compiler_params=pltpu.CompilerParams(
            collective_id=0, has_side_effects=True, vmem_limit_bytes=64000 * 1024
        ),
        name="forward",
    )(
        hidden_in, seq_lengths[None, :], seq_device[None, :], *[g[None, :] for g in gains],
        out_grad, wq, wk, wv, wo, gate, up, wd,
    )


def backward_kernel(
    gu_ref, wd_ref, tok_ref, cot_ref, hid_ref, pre_ref, w_ref, middle_ref, normed_ref, raw_ref,
    q_ref, k_ref, v_ref, mixed_ref, x_ref, gains_ref, rope_ref,
    x_out, small_out, y_out, d_out, a_out, ex_land, gu_out, c_land, s_land, f_land, l_land,
    gu_all, gd_all, gu_sib, gd_sib, gu_sec, gd_sec, gu_fst, gd_fst, t_own, t_land,
    dmid, dqkv, s_sum, s_got, s_line,
    c_send, c_recv, s_send, s_recv, f_send, f_recv, down_s, down_r, up_s, up_r, load, stream, back,
    ac_send, ac_recv, as_send, as_recv, af_send, af_recv, ad_send, ad_recv, au_send, au_recv,
    ex_s, ex_r, small_s, small_r, units_in,
    a_load,
):
    me, z, first, second, sibling = where_am_i()
    greet(line_peers(me) + [first, second, sibling])
    core = me % 2
    mine, fst, sec = (me % RING) // 2, (first % RING) // 2, (second % RING) // 2
    far = ((second + first - me) % RING) // 2
    half = gd_fst.shape[0] // 2
    last = LINE - 1
    tokens, dim = tok_ref.shape
    part = hid_ref.shape[1]
    quad_rows = part // LINE
    shard_rows = dim // (RING * LINE)
    piece_cols = gu_all.shape[3]
    kv0 = H * HD
    v0 = kv0 + KVH * HD
    qkv_width = v0 + KVH * HD
    MLP_GU, MLP_D = (0, 0, LINE), (1, LINE, LINE + 2)

    def block(gu, d, piece, group):
        if group == 0:
            return gu.at[piece]
        return d.at[tile(piece - LINE, half)]

    def own_block(quad, piece, group, theirs=False):
        shard = 2 * quad + (1 - core if theirs else core)
        if group == 0:
            return gu_all.at[piece, shard]
        return block(None, gd_all.at[shard], piece, group)

    def each(span, body):
        group, lo, hi = span

        def step(piece, carry):
            body(piece, group)
            return carry

        lax.fori_loop(lo, hi, step, 0)

    def to_sibling(quad, piece, group):
        return remote(
            own_block(quad, piece, group, theirs=True),
            block(gu_sib.at[quad], gd_sib.at[quad], piece, group),
            c_send.at[quad, piece],
            c_recv.at[quad, piece],
            sibling,
        )

    def to_second(quad, slot, piece, group):
        return remote(
            own_block(quad, piece, group),
            block(gu_sec.at[slot], gd_sec.at[slot], piece, group),
            s_send.at[slot, piece],
            s_recv.at[slot, piece],
            second,
        )

    def to_first(piece, group):
        return remote(
            own_block(fst, piece, group),
            block(gu_fst, gd_fst, piece, group),
            f_send.at[piece],
            f_recv.at[piece],
            first,
        )

    def pass_on(piece, group):
        for quad, slot in ((far, 1), (sec, 0)):
            to_sibling(quad, piece, group).wait_recv()
            own = own_block(quad, piece, group)
            add_rows(own, own, block(gu_sib.at[quad], gd_sib.at[quad], piece, group))
            to_second(quad, slot, piece, group).start()

    def narrow(piece, group):
        to_sibling(fst, piece, group).wait_recv()
        to_second(far, 1, piece, group).wait_recv()
        own = own_block(fst, piece, group)
        add_rows(
            own,
            own,
            block(gu_sib.at[fst], gd_sib.at[fst], piece, group),
            block(gu_sec.at[1], gd_sec.at[1], piece, group),
        )
        to_first(piece, group).start()

    def finish(piece, group, out=None):
        to_sibling(mine, piece, group).wait_recv()
        to_second(sec, 0, piece, group).wait_recv()
        to_first(piece, group).wait_recv()
        own = own_block(mine, piece, group)
        add_rows(
            own if group == 0 else block(None, out, piece, group),
            own,
            block(gu_sib.at[mine], gd_sib.at[mine], piece, group),
            block(gu_sec.at[0], gd_sec.at[0], piece, group),
            block(gu_fst, gd_fst, piece, group),
        )

    def drain_sibling(piece, group):
        for quad in (far, fst, sec, mine):
            to_sibling(quad, piece, group).wait_send()

    def drain(piece, group):
        to_second(far, 1, piece, group).wait_send()
        to_second(sec, 0, piece, group).wait_send()
        to_first(piece, group).wait_send()

    def send_line(src, which, t, up):
        return remote(
            src,
            t_land.at[which, t + 1 if up else t],
            (up_s if up else down_s).at[which, t],
            (up_r if up else down_r).at[which, t],
            me + RING if up else me - RING,
        )

    def line_own(which):
        for k in range(last):

            @pl.when(z == last)
            def _(k=k):
                send_line(t_own.at[which, k], which, k, False).start()

            @pl.when(z == 0)
            def _(k=k):
                send_line(t_own.at[which, last - k], which, last - k, True).start()

    def relay_at(which, at, t, up):
        @pl.when(z == at)
        def _():
            landing = t_land.at[which, t + 1 if up else t]
            send_line(landing, which, t, up).wait_recv()
            add_rows(landing, landing, t_own.at[which, t])
            send_line(landing, which, t, up).start()

    def relay(which, step):
        if step < 2:
            relay_at(which, 2, step, False)
            relay_at(which, 1, last - step, True)
        else:
            relay_at(which, 1, 0, False)
            relay_at(which, 2, last, True)

    def line_sum(which, out):
        own, above, below = t_own.at[which, z], t_land.at[which, z], t_land.at[which, z + 1]

        @pl.when(z < last)
        def _():
            send_line(above, which, z, False).wait_recv()

        @pl.when(z > 0)
        def _():
            send_line(below, which, z, True).wait_recv()

        @pl.when(z == 0)
        def _():
            add_rows(out, own, above)

        @pl.when(z == last)
        def _():
            add_rows(out, own, below)

        @pl.when((z > 0) & (z < last))
        def _():
            add_rows(out, own, above, below)

    def mlp(tok, cot, hid, dgu):
        ins = [
            pltpu.make_async_copy(hid_ref, hid, load.at[0]),
            pltpu.make_async_copy(cot_ref, cot, load.at[1]),
            pltpu.make_async_copy(tok_ref, tok, load.at[3]),
        ]
        for copy in ins:
            copy.start()
        wide = 256
        for copy in ins[:2]:
            copy.wait()

        previous = None
        for quad in (far, sec, fst, mine):

            def columns(n, carry, quad=quad):
                at = tile(n, 512)
                both = dot_tn(hid[:, tile(quad, quad_rows)], cot[:, at]).astype(bf16)
                gd_all[2 * quad, :, at] = both[: quad_rows // 2]
                gd_all[2 * quad + 1, :, at] = both[quad_rows // 2 :]
                return carry

            lax.fori_loop(0, dim // 512, columns, 0)
            if previous is not None:
                each(MLP_D, lambda piece, group, q=previous: to_sibling(q, piece, group).start())
            previous = quad
        each(MLP_D, lambda piece, group, q=previous: to_sibling(q, piece, group).start())
        each(MLP_D, pass_on)

        def units(gate_t, up_t, down_w, dhid_t):
            def fetch(i, slot):
                up_at = pl.ds(pl.multiple_of(part + i * wide, wide), wide)
                return (
                    pltpu.make_async_copy(
                        pre_ref.at[:, tile(i, wide)], gate_t.at[slot], units_in.at[slot, 0]
                    ),
                    pltpu.make_async_copy(pre_ref.at[:, up_at], up_t.at[slot], units_in.at[slot, 1]),
                    pltpu.make_async_copy(
                        wd_ref.at[tile(i, wide)], down_w.at[slot], units_in.at[slot, 2]
                    ),
                )

            def body(i, slot):
                dhid_t[...] = dot_nt(cot[...], down_w[slot])

                def act(r, carry):
                    at = tile(r, 32)
                    gate, up, dhid = gate_t[slot, at], up_t[slot, at], dhid_t[at]
                    sig = jax.nn.sigmoid(gate)
                    dgate = dhid * up * (sig * (1.0 + gate * (1.0 - sig)))
                    dgu[at, tile(i, wide)] = dgate.astype(bf16)
                    up_at = pl.ds(pl.multiple_of(part + i * wide, wide), wide)
                    dgu[at, up_at] = (dhid * (gate * sig)).astype(bf16)
                    return carry

                lax.fori_loop(0, tokens // 32, act, 0, unroll=4)

            streamed(part // wide, fetch, body)

        pl.run_scoped(
            units,
            pltpu.VMEM((2, tokens, wide), f32),
            pltpu.VMEM((2, tokens, wide), f32),
            pltpu.VMEM((2, wide, dim), bf16),
            pltpu.VMEM((tokens, wide), f32),
        )

        def back_through(rows_w):
            def fetch(i, slot):
                return (
                    pltpu.make_async_copy(
                        gu_ref.at[tile(i, wide)], rows_w.at[slot], stream.at[slot]
                    ),
                )

            def body(i, slot):
                out = dot_nt(dgu[...], rows_w[slot]).astype(bf16)
                t_own[0, :, :, tile(i, wide)] = out.reshape(LINE, CAP, wide)

            streamed(dim // wide, fetch, body)

        pl.run_scoped(back_through, pltpu.VMEM((2, wide, 2 * part), bf16))
        ins[2].wait()
        line_own(0)

        rows = dim // LINE
        for piece in range(LINE):

            def columns(n, carry, piece=piece):
                at = tile(n, 512)
                grad = dot_tn(tok[:, pl.ds(piece * rows, rows)], dgu[:, at]).astype(bf16)
                gu_all[piece, :, :, at] = grad.reshape(RING, rows // RING, 512)
                return carry

            lax.fori_loop(0, 2 * part // 512, columns, 0)
            if piece > 0:
                pass_on(piece - 1, 0)
            for quad in (far, fst, sec, mine):
                to_sibling(quad, piece, 0).start()
            if piece == 2:
                relay(0, 0)
        pass_on(LINE - 1, 0)
        each(MLP_D, narrow)

        def out_through(cols_w):
            def fetch(i, slot):
                return (
                    pltpu.make_async_copy(
                        wd_ref.at[:, tile(i, wide)], cols_w.at[slot], stream.at[slot]
                    ),
                )

            def body(i, slot):
                out = jnp.dot(hid[...], cols_w[slot], preferred_element_type=f32).astype(bf16)
                t_own[1, :, :, tile(i, wide)] = out.reshape(LINE, CAP, wide)

                @pl.when(i == 3)
                def _():
                    relay(0, 1)

                @pl.when(i == 5)
                def _():
                    relay(0, 2)

            streamed(dim // wide, fetch, body)

        pl.run_scoped(out_through, pltpu.VMEM((2, part, wide), bf16))

    pl.run_scoped(
        mlp,
        pltpu.VMEM((tokens, dim), bf16),
        pltpu.VMEM((tokens, dim), bf16),
        pltpu.VMEM((tokens, part), bf16),
        pltpu.VMEM((tokens, 2 * part), bf16),
    )
    def attention(dbr, mixed, normed, raw, q, k, v, cot, dsec, dmix, middle, w_rows):
        ins = [
            pltpu.make_async_copy(src, dst, load.at[i])
            for i, (src, dst) in enumerate(
                (
                    (middle_ref, middle),
                    (raw_ref.at[:, pl.ds(0, v0)], raw),
                    (q_ref, q),
                    (k_ref, k),
                    (v_ref, v),
                    (cot_ref.at[tile(z, CAP)], cot),
                    (mixed_ref, mixed),
                    (normed_ref, normed),
                )
            )
        ]
        for copy in ins:
            copy.start()
        narrow(0, 0)
        line_own(1)
        for copy in ins:
            copy.wait()
        line_sum(0, dsec)

        scale = rms_scale(middle[...])
        wide = 512

        def gather_mean(i, total):
            at = tile(i, wide)
            n = middle[:, at] * scale
            ds = dsec[:, at]
            s_sum[3, 0:1, at] = jnp.sum(n * ds, axis=0, keepdims=True)
            return total + lane_sum(n * ds * gains_ref[1:2, at])

        mean = lax.fori_loop(0, dim // wide, gather_mean, jnp.zeros((CAP, 1), f32)) / dim

        def spread_mean(i, carry):
            at = tile(i, wide)
            n = middle[:, at] * scale
            e = dsec[:, at] * gains_ref[1:2, at]
            d_middle = cot[:, at].astype(f32) + scale * (e - n * mean)
            dmid[:, at] = d_middle
            dbr[:, at] = d_middle.astype(bf16)
            return carry

        lax.fori_loop(0, dim // wide, spread_mean, 0)
        shards = w_rows.shape[1]
        rows = shards * w_rows.shape[2]

        def w_fetch(i, slot):
            return (
                pltpu.make_async_copy(
                    w_ref.at[tile(i, shards), :, pl.ds(qkv_width, dim)],
                    w_rows.at[slot],
                    stream.at[slot],
                ),
            )

        def through_out(i, slot):
            dmix[:, tile(i, rows)] = dot_nt(dbr[...], w_rows[slot].reshape(rows, dim)).astype(bf16)

        streamed(dim // rows, w_fetch, through_out)
        narrow(1, 0)
        relay(1, 0)

        cosine, sine, bias = rope_ref[0], rope_ref[1], rope_ref[2]
        s_sum[3, 1:8] = jnp.zeros((7, dim), f32)

        def unrope(raw_v, d_rot, row):
            d_hat = d_rot * cosine - half_turn(d_rot * sine)
            r = rms_scale(raw_v)
            n = raw_v * r
            s_sum[3, row : row + 1, 0:HD] += jnp.sum(n * d_hat, axis=0, keepdims=True)
            e = d_hat * gains_ref[row + 1 : row + 2, 0:HD]
            return (r * (e - n * jnp.mean(n * e, axis=-1, keepdims=True))).astype(bf16)

        def head(g, carry):
            at = tile(g, HD)
            key, value = k[:, at], v[:, at]
            d_key = jnp.zeros((CAP, HD), f32)
            d_value = jnp.zeros((CAP, HD), f32)
            for i in range(2):
                cols = tile(2 * g + i, HD)
                query, d_mix = q[:, cols], dmix[:, cols]
                logits = dot_nt(query, key) * (HD ** (-0.5)) + bias
                exponent = jnp.exp(logits - jnp.max(logits, axis=-1, keepdims=True))
                probs = exponent / lane_sum(exponent)
                d_probs = dot_nt(d_mix, value)
                d_logits = probs * (d_probs - lane_sum(probs * d_probs))
                d_scores = (d_logits * (HD ** (-0.5))).astype(bf16)
                d_value = d_value + dot_tn(probs.astype(bf16), d_mix)
                d_key = d_key + dot_tn(d_scores, query)
                d_query = jnp.dot(d_scores, key, preferred_element_type=f32)
                dqkv[:, cols] = unrope(raw[:, cols], d_query, 1)
            cols = pl.ds(pl.multiple_of(kv0 + g * HD, HD), HD)
            dqkv[:, cols] = unrope(raw[:, cols], d_key, 2)
            dqkv[:, pl.ds(pl.multiple_of(v0 + g * HD, HD), HD)] = d_value.astype(bf16)
            return carry

        lax.fori_loop(0, KVH // 2, head, 0, unroll=2)
        narrow(2, 0)
        lax.fori_loop(KVH // 2, KVH, head, 0, unroll=2)

    order = (
        last * (1 - z // 2),
        2 - 2 * z + 5 * (z // 2),
        1 + z % 2,
        z,
    )

    def a_own(t, quad, h):
        return gu_all.at[t, 2 * quad + (core if h else 1 - core)]

    def sums(dbr, mixed, normed, cbuf, stage):
        span = dim // LINE

        def a_sibling(t, quad, h, slot):
            return remote(
                cbuf.at[slot, quad],
                c_land.at[t, h, quad],
                ac_send.at[slot, quad],
                ac_recv.at[t, h, quad],
                sibling,
            )

        def a_second(t, quad, h, slot):
            return remote(
                a_own(t, quad, h),
                s_land.at[slot, t, h],
                as_send.at[slot, t, h],
                as_recv.at[slot, t, h],
                second,
            )

        def a_first(t, h):
            return remote(
                a_own(t, fst, h), f_land.at[t, h], af_send.at[t, h], af_recv.at[t, h], first
            )

        def a_line(t, h, upward):
            src = a_own(t, mine, h)
            if upward:
                return remote(
                    src, l_land.at[1, t, h], au_send.at[t, h], au_recv.at[t, h], me + RING
                )
            return remote(src, l_land.at[0, t, h], ad_send.at[t, h], ad_recv.at[t, h], me - RING)

        def staged(lo, *landed):
            return [
                pltpu.make_async_copy(src, stage.at[lo + i], a_load.at[lo + i])
                for i, src in enumerate(landed)
            ]

        def begin(copies):
            for copy in copies:
                copy.start()

        def add_staged(own, copies, lo):
            for copy in copies:
                copy.wait()
            add_rows(own, own, *[stage.at[lo + i] for i in range(len(copies))])

        def compute(k):
            h, t, slot = k // LINE, order[k % LINE], k % 2
            if k > 1:
                for quad in (far, fst, sec, mine):
                    a_sibling(order[(k - 2) % LINE], quad, (k - 2) // LINE, slot).wait_send()
            col0 = v0 if h else 0
            own_core = core if h else 1 - core

            def columns(n, carry, left, right, at):
                grad = dot_tn(left[:, tile(t, span)], right).astype(bf16)
                grad = grad.reshape(RING // 2, 2, shard_rows, 512)
                ours = jnp.where(core == 0, grad[:, 0], grad[:, 1])
                theirs = jnp.where(core == 0, grad[:, 1], grad[:, 0])
                for quad in range(RING // 2):
                    gu_all[t, 2 * quad + own_core, :, at] = ours[quad]
                cbuf[slot, :, :, at] = theirs
                return carry

            def from_qkv(n, carry):
                at = tile(n, 512)
                right = dqkv[:, pl.ds(pl.multiple_of(col0 + n * 512, 512), 512)]
                return columns(n, carry, normed, right, at)

            def from_out(n, carry):
                at = pl.ds(pl.multiple_of(qkv_width - v0 + n * 512, 512), 512)
                return columns(n, carry, mixed, dbr[:, tile(n, 512)], at)

            if h == 0:
                lax.fori_loop(0, v0 // 512, from_qkv, 0)
            else:
                lax.fori_loop(0, (qkv_width - v0) // 512, from_qkv, 0)
                lax.fori_loop(0, dim // 512, from_out, 0)

        def share(k):
            h, t, slot = k // LINE, order[k % LINE], k % 2
            for quad in (far, fst, sec, mine):
                a_sibling(t, quad, h, slot).start()

        def spread_in(k):
            t, h = order[k % LINE], k // LINE
            return staged(0, c_land.at[t, h, far], c_land.at[t, h, sec])

        def spread_begin(k):
            h, t, slot = k // LINE, order[k % LINE], k % 2
            for quad in (far, sec):
                a_sibling(t, quad, h, slot).wait_recv()
            begin(spread_in(k))

        def spread(k):
            h, t = k // LINE, order[k % LINE]
            copies = spread_in(k)
            for i, (quad, place) in enumerate(((far, 1), (sec, 0))):
                add_staged(a_own(t, quad, h), copies[i : i + 1], i)
                a_second(t, quad, h, place).start()

        def inward_in(k):
            t, h = order[k % LINE], k // LINE
            return staged(2, c_land.at[t, h, fst], s_land.at[1, t, h])

        def inward_begin(k):
            h, t, slot = k // LINE, order[k % LINE], k % 2
            a_sibling(t, fst, h, slot).wait_recv()
            a_second(t, far, h, 1).wait_recv()
            begin(inward_in(k))

        def inward(k):
            h, t = k // LINE, order[k % LINE]
            add_staged(a_own(t, fst, h), inward_in(k), 2)
            a_first(t, h).start()

        def collect_in(k):
            t, h = order[k % LINE], k // LINE
            return staged(4, c_land.at[t, h, mine], s_land.at[0, t, h], f_land.at[t, h])

        def collect_begin(k):
            h, t, slot = k // LINE, order[k % LINE], k % 2
            a_sibling(t, mine, h, slot).wait_recv()
            a_second(t, sec, h, 0).wait_recv()
            a_first(t, h).wait_recv()
            begin(collect_in(k))

        def collect(k):
            h, t = k // LINE, order[k % LINE]
            add_staged(a_own(t, mine, h), collect_in(k), 4)

            @pl.when((t < z) & (z == last))
            def _():
                a_line(t, h, False).start()

            @pl.when((t > z) & (z == 0))
            def _():
                a_line(t, h, True).start()

        def onward(k):
            h, t = k // LINE, order[k % LINE]

            @pl.when((t < z) & (z < last))
            def _():
                a_line(t, h, False).wait_recv()
                copies = staged(7, l_land.at[0, t, h])
                begin(copies)
                add_staged(a_own(t, mine, h), copies, 7)
                a_line(t, h, False).start()

            @pl.when((t > z) & (z > 0))
            def _():
                a_line(t, h, True).wait_recv()
                copies = staged(7, l_land.at[1, t, h])
                begin(copies)
                add_staged(a_own(t, mine, h), copies, 7)
                a_line(t, h, True).start()

        def exchange(k):
            peer_z = lax.rem(z + k, LINE)
            return remote(
                gu_out.at[peer_z], ex_land.at[z], ex_s.at[k], ex_r.at[k], me % RING + RING * peer_z
            )

        def small(step, src, dst, device):
            return remote(src, dst, small_s.at[step], small_r.at[step], device)

        def first_norm(w_rows):
            shards = w_rows.shape[1]
            wide = 512
            x_scale = rms_scale(x_ref[...].astype(f32))
            w_tile = shards * w_rows.shape[2]

            def w_fetch(i, slot):
                return (
                    pltpu.make_async_copy(
                        w_ref.at[tile(i, shards), :, pl.ds(0, qkv_width)],
                        w_rows.at[slot],
                        stream.at[slot],
                    ),
                )

            def through(i, slot):
                x_out[:, tile(i, w_tile)] = dot_nt(dqkv[...], w_rows[slot].reshape(w_tile, qkv_width))

            streamed(dim // w_tile, w_fetch, through)

            def gather_mean(i, total):
                at = tile(i, wide)
                n = x_ref[:, at].astype(f32) * x_scale
                s_sum[3, 3:4, at] = jnp.sum(n * x_out[:, at], axis=0, keepdims=True)
                return total + lane_sum(n * x_out[:, at] * gains_ref[0:1, at])

            mean = lax.fori_loop(0, dim // wide, gather_mean, jnp.zeros((CAP, 1), f32)) / dim

            def spread_mean(i, carry):
                at = tile(i, wide)
                n = x_ref[:, at].astype(f32) * x_scale
                e = x_out[:, at] * gains_ref[0:1, at]
                x_out[:, at] = dmid[:, at] + x_scale * (e - n * mean)
                return carry

            lax.fori_loop(0, dim // wide, spread_mean, 0)

        def mlp_results(d_tmp, middle, y, y_half):
            middle_in = pltpu.make_async_copy(middle_ref, middle, load.at[0])
            middle_in.start()
            each(MLP_D, lambda piece, group: finish(piece, group, d_tmp))
            d_back = pltpu.make_async_copy(d_tmp, d_out, load.at[1])
            d_back.start()
            line_sum(1, y)
            middle_in.wait()

            def last_add(i, carry):
                at = tile(i, 512)
                y_half[:, at] = (middle[:, at] + y[:, at]).astype(bf16)
                return carry

            lax.fori_loop(0, dim // 512, last_add, 0)
            y_back = pltpu.make_async_copy(y_half, y_out, load.at[2])
            y_back.start()
            each(MLP_D, drain_sibling)
            each(MLP_D, drain)
            d_back.wait()
            y_back.wait()

        small_c = small(0, s_sum.at[3], s_got.at[0], sibling)
        each(MLP_GU, drain_sibling)
        compute(0)
        share(0)
        narrow(3, 0)
        compute(1)
        share(1)
        spread_begin(0)
        compute(2)
        share(2)
        spread(0)
        spread_begin(1)
        relay(1, 1)
        compute(3)
        share(3)
        spread(1)
        spread_begin(2)
        inward_begin(0)
        spread(2)
        spread_begin(3)
        inward(0)
        each(MLP_GU, finish)
        gu_back = pltpu.make_async_copy(gu_all.at[:, 2 * mine + core], gu_out, back.at[0])
        gu_back.start()
        ex_in = pltpu.make_async_copy(gu_all.at[z, 2 * mine + core], ex_land.at[z], back.at[1])
        ex_in.start()
        spread(3)
        each(MLP_GU, drain)
        gu_back.wait()
        exchange(2).start()
        exchange(1).start()
        ex_in.wait()
        compute(4)
        share(4)
        pl.run_scoped(first_norm, pltpu.VMEM((2, 4, shard_rows, qkv_width), bf16))
        small_c.start()
        inward_begin(1)
        compute(5)
        share(5)
        inward(1)
        small_c.wait()
        s_sum[0] = s_sum[3] + s_got[0]
        small_f = small(1, s_sum.at[0], s_got.at[1], first)
        small_f.start()
        spread_begin(4)
        relay(1, 2)
        compute(6)
        share(6)
        spread(4)
        spread_begin(5)
        inward_begin(2)
        compute(7)
        share(7)
        inward(2)
        spread(5)
        spread_begin(6)
        small_f.wait()
        s_sum[1] = s_sum[0] + s_got[1]
        small_s2 = small(2, s_sum.at[1], s_got.at[2], second)
        small_s2.start()
        spread(6)
        spread_begin(7)
        collect_begin(0)
        spread(7)
        collect(0)
        collect_begin(1)
        inward_begin(3)
        collect(1)
        inward(3)
        collect_begin(2)
        collect(2)
        onward(0)
        onward(2)
        collect_begin(3)
        inward_begin(4)
        collect(3)
        inward(4)
        exchange(3).start()
        onward(1)
        pl.run_scoped(
            mlp_results,
            pltpu.VMEM(gd_fst.shape, f32),
            pltpu.VMEM((CAP, dim), f32),
            pltpu.VMEM((CAP, dim), f32),
            pltpu.VMEM((CAP, dim), bf16),
        )
        inward_begin(5)
        collect_begin(4)
        inward(5)
        collect(4)
        inward_begin(6)
        collect_begin(5)
        inward(6)
        collect(5)
        onward(4)
        small_s2.wait()
        s_sum[2] = s_sum[1] + s_got[2]
        small_line = [
            small(2 + k, s_sum.at[2], s_line.at[k], me % RING + RING * lax.rem(z + k, LINE))
            for k in range(1, LINE)
        ]
        for copy in small_line:
            copy.start()
        onward(5)
        inward_begin(7)
        collect_begin(6)
        inward(7)
        collect(6)
        onward(6)
        collect_begin(7)
        collect(7)
        for copy in small_line:
            copy.wait()
        small_out[...] = (s_sum[2] + s_line[2]) + (s_line[1] + s_line[3])
        for k in (6, 7):
            for quad in (far, fst, sec, mine):
                a_sibling(order[k % LINE], quad, k // LINE, k % 2).wait_send()
        for k in range(1, LINE):
            exchange(k).wait_send()
            src_z = lax.rem(z + LINE - k, LINE)
            landed = ex_land.at[src_z]
            remote(landed, landed, ex_s.at[k], ex_r.at[k], sibling).wait_recv()
        for t in range(LINE):
            for h in range(2):
                a_second(t, far, h, 1).wait_send()
                a_second(t, sec, h, 0).wait_send()
                a_first(t, h).wait_send()

                @pl.when(t < z)
                def _(t=t, h=h):
                    a_line(t, h, False).wait_send()

                @pl.when(t > z)
                def _(t=t, h=h):
                    a_line(t, h, True).wait_send()

    slots = CAP
    kv = KVH * HD
    rows = gu_all.shape[2]

    def both(dbr, mixed, normed):
        pl.run_scoped(
            lambda *refs: attention(dbr, mixed, normed, *refs),
            pltpu.VMEM((slots, v0), f32),
            pltpu.VMEM((slots, dim), bf16),
            pltpu.VMEM((slots, kv), bf16),
            pltpu.VMEM((slots, kv), bf16),
            pltpu.VMEM((slots, dim), bf16),
            pltpu.VMEM((slots, dim), f32),
            pltpu.VMEM((slots, dim), bf16),
            pltpu.VMEM((slots, dim), f32),
            pltpu.VMEM((2, 4, rows, dim), bf16),
        )
        pl.run_scoped(
            lambda *refs: sums(dbr, mixed, normed, *refs),
            pltpu.VMEM((2, RING // 2, rows, piece_cols), bf16),
            pltpu.VMEM((8, rows, piece_cols), bf16),
        )

    pl.run_scoped(
        both,
        pltpu.VMEM((slots, dim), bf16),
        pltpu.VMEM((slots, dim), bf16),
        pltpu.VMEM((slots, dim), bf16),
    )

    def a_landed(t, h, upward):
        landing = l_land.at[1 if upward else 0, t, h]
        sems = (au_send, au_recv) if upward else (ad_send, ad_recv)
        return remote(landing, landing, sems[0].at[t, h], sems[1].at[t, h], sibling)

    def results(a_tmp, stage):
        for h in range(2):

            @pl.when(z < last)
            def _(h=h):
                a_landed(z, h, False).wait_recv()

            @pl.when(z > 0)
            def _(h=h):
                a_landed(z, h, True).wait_recv()

        def total(*sides):
            for h in range(2):
                copies = [
                    pltpu.make_async_copy(l_land.at[side, z, h], stage.at[i], stream.at[i])
                    for i, side in enumerate(sides)
                ]
                for copy in copies:
                    copy.start()
                for copy in copies:
                    copy.wait()
                add_rows(
                    a_tmp.at[:, pl.ds(h * piece_cols, piece_cols)],
                    a_own(z, mine, h),
                    *[stage.at[i] for i in range(len(sides))],
                )

        @pl.when(z == 0)
        def _():
            total(0)

        @pl.when(z == last)
        def _():
            total(1)

        @pl.when((z > 0) & (z < last))
        def _():
            total(0, 1)

        a_back = pltpu.make_async_copy(a_tmp, a_out, load.at[3])
        a_back.start()
        a_back.wait()

    pl.run_scoped(
        results,
        pltpu.VMEM((rows, 2 * piece_cols), f32),
        pltpu.VMEM((2, rows, piece_cols), bf16),
    )
    for which in range(2):
        for k in range(LINE):

            @pl.when((z > 0) & (k < z))
            def _(which=which, k=k):
                send_line(t_own.at[which, k], which, k, False).wait_send()

            @pl.when((z < last) & (k > z))
            def _(which=which, k=k):
                send_line(t_own.at[which, k], which, k, True).wait_send()


def backward(gu, wd, tok, cot, hid, pre, w, middle, normed, raw, q, k, v, mixed, x, gains, rope):
    dim = tok.shape[1]
    rows = w.shape[1]
    drows = wd.shape[0] // RING
    cols = gu.shape[1]
    quads = RING // 2
    pieces = LINE + 2
    qkv = raw.shape[1]
    S = jax.ShapeDtypeStruct
    return pl.pallas_call(
        backward_kernel,
        out_shape=(
            S((CAP, dim), f32),
            S((8, dim), f32),
            S((CAP, dim), bf16),
            S((drows, dim), f32),
            S((rows, qkv + dim), f32),
            S((LINE, rows, cols), bf16),
            S((LINE, rows, cols), bf16),
            S((LINE, 2, quads, rows, cols), bf16),
            S((2, LINE, 2, rows, cols), bf16),
            S((LINE, 2, rows, cols), bf16),
            S((2, LINE, 2, rows, cols), bf16),
        ),
        in_specs=[ANY] * 14 + [VMEM] * 3,
        out_specs=(VMEM,) * 2 + (ANY,) * 9,
        scratch_shapes=[
            pltpu.VMEM((LINE, RING, rows, cols), bf16),
            pltpu.VMEM((RING, drows, dim), bf16),
            pltpu.VMEM((quads, LINE, rows, cols), bf16),
            pltpu.VMEM((quads, drows, dim), bf16),
            pltpu.VMEM((2, LINE, rows, cols), bf16),
            pltpu.VMEM((2, drows, dim), bf16),
            pltpu.VMEM((LINE, rows, cols), bf16),
            pltpu.VMEM((drows, dim), bf16),
            pltpu.VMEM((2, LINE, CAP, dim), bf16),
            pltpu.VMEM((2, LINE + 1, CAP, dim), bf16),
            pltpu.VMEM((CAP, dim), f32),
            pltpu.VMEM((CAP, qkv), bf16),
            pltpu.VMEM((4, 8, dim), f32),
            pltpu.VMEM((3, 8, dim), f32),
            pltpu.VMEM((LINE, 8, dim), f32),
            DMA((quads, pieces)),
            DMA((quads, pieces)),
            DMA((2, pieces)),
            DMA((2, pieces)),
            DMA((pieces,)),
            DMA((pieces,)),
            DMA((2, LINE)),
            DMA((2, LINE)),
            DMA((2, LINE)),
            DMA((2, LINE)),
            DMA((8,)),
            DMA((3,)),
            DMA((2,)),
            DMA((2, quads)),
            DMA((LINE, 2, quads)),
            DMA((2, LINE, 2)),
            DMA((2, LINE, 2)),
            DMA((LINE, 2)),
            DMA((LINE, 2)),
            DMA((LINE, 2)),
            DMA((LINE, 2)),
            DMA((LINE, 2)),
            DMA((LINE, 2)),
            DMA((LINE,)),
            DMA((LINE,)),
            DMA((2 + LINE,)),
            DMA((2 + LINE,)),
            DMA((2, 3)),
            DMA((8,)),
        ],
        compiler_params=pltpu.CompilerParams(
            collective_id=2, has_side_effects=True, vmem_limit_bytes=65400 * 1024
        ),
        name="backward",
    )(gu, wd, tok, cot, hid, pre, w, middle, normed, raw, q, k, v, mixed, x, gains, rope)


def results_kernel(
    y_ref, x_ref, small_ref, d_ref, a_ref, ex_ref,
    y_out, x_out, q_out, k_out, v_out, o_out, gate_out, up_out, d_out, ga_out, gq_out, gk_out, gm_out,
    y_tmp, x_tmp, small, d_tmp, a_tmp, ex_tmp, gate_tmp, up_tmp, sem_in, sem_out,
):
    me = lax.axis_index("fsdp")
    width = ex_tmp.shape[2] // 2
    moves = ((small_ref, small), (ex_ref, ex_tmp), (a_ref, a_tmp), (d_ref, d_tmp), (x_ref, x_tmp), (y_ref, y_tmp))
    ins = [pltpu.make_async_copy(src, dst, sem_in.at[i]) for i, (src, dst) in enumerate(moves)]
    for copy in ins:
        copy.start()
    outs = []

    def leave(src, dst):
        copy = pltpu.make_async_copy(src, dst, sem_out.at[len(outs)])
        copy.start()
        outs.append(copy)

    ins[1].wait()
    for k in range(LINE):
        add_rows(gate_tmp.at[:, pl.ds(k * width, width)], ex_tmp.at[k, :, pl.ds(0, width)])
        add_rows(up_tmp.at[:, pl.ds(k * width, width)], ex_tmp.at[k, :, pl.ds(width, width)])
    leave(gate_tmp, gate_out)
    leave(up_tmp, up_out)
    ins[2].wait()
    lo = 0
    for out in (q_out, k_out, v_out, o_out):
        leave(a_tmp.at[:, pl.ds(lo, out.shape[1])], out)
        lo += out.shape[1]
    ins[3].wait()
    leave(d_tmp, d_out)
    ins[4].wait()
    leave(x_tmp, x_out)
    ins[5].wait()
    leave(y_tmp, y_out)
    ins[0].wait()
    for row, out in ((3, ga_out), (1, gq_out), (2, gk_out), (0, gm_out)):
        count = out.shape[1]
        value = jnp.zeros((1, 128), f32)
        for i in range(small.shape[1] // 128):
            held = small[row : row + 1, i * 128 : (i + 1) * 128]
            value = jnp.where((me * count) // 128 == i, held, value)
        value = pltpu.roll(value, (128 - (me * count) % 128) % 128, 1)
        out[...] = value[:, 0:count]
    for copy in outs:
        copy.wait()


def results(y, x, small, d, a, ex, widths, shares):
    rows = a.shape[0]
    wide = LINE * ex.shape[2] // 2
    S = jax.ShapeDtypeStruct
    return pl.pallas_call(
        results_kernel,
        out_shape=(
            S(y.shape, bf16),
            S(x.shape, f32),
            *[S((rows, w), f32) for w in widths],
            S((rows, wide), f32),
            S((rows, wide), f32),
            S(d.shape, f32),
            *[S((1, s), f32) for s in shares],
        ),
        in_specs=[ANY] * 6,
        out_specs=(ANY,) * 9 + (VMEM,) * 4,
        scratch_shapes=[
            pltpu.VMEM(y.shape, bf16),
            pltpu.VMEM(x.shape, f32),
            pltpu.VMEM(small.shape, f32),
            pltpu.VMEM(d.shape, f32),
            pltpu.VMEM(a.shape, f32),
            pltpu.VMEM(ex.shape, bf16),
            pltpu.VMEM((rows, wide), f32),
            pltpu.VMEM((rows, wide), f32),
            DMA((6,)),
            DMA((9,)),
        ],
        name="results",
    )(y, x, small, d, a, ex)


def layout(seq_lengths, seq_device, owner, slots):
    owned = seq_device == owner
    counts = jnp.where(owned, seq_lengths, 0)
    starts = jnp.cumsum(counts) - counts
    places = jnp.arange(slots, dtype=jnp.int32)
    inside = (
        owned[:, None]
        & (places[None, :] >= starts[:, None])
        & (places[None, :] < (starts + counts)[:, None])
    )
    labels = jnp.arange(seq_lengths.shape[0], dtype=jnp.int32)
    segment = jnp.sum(jnp.where(inside, labels[:, None] + 1, 0), axis=0) - 1
    position = jnp.sum(jnp.where(inside, places[None, :] - starts[:, None], 0), axis=0)
    return (segment, position)


def allowed_pairs(segment):
    places = jnp.arange(segment.shape[0], dtype=jnp.int32)
    earlier = places[None, :] < places[:, None]
    same_seq = (segment[:, None] == segment[None, :]) & (segment[:, None] >= 0)
    return (places[:, None] == places[None, :]) | earlier & same_seq


def rmsnorm(values, gain):
    return values * lax.rsqrt(jnp.mean(values * values, axis=-1, keepdims=True) + epsilon) * gain


def rotary(values, position):
    half_dim = values.shape[-1] // 2
    freqs = jnp.power(rope_base, -2.0 * jnp.arange(half_dim, dtype=jnp.float32) / values.shape[-1])
    angles = position.astype(jnp.float32)[:, None] * freqs[None, :]
    cosine = jnp.concatenate([jnp.cos(angles), jnp.cos(angles)], axis=-1)[:, None, :]
    sine = jnp.concatenate([jnp.sin(angles), jnp.sin(angles)], axis=-1)[:, None, :]
    rotated = jnp.concatenate([-values[..., half_dim:], values[..., :half_dim]], axis=-1)
    return values * cosine + rotated * sine


def matmul(left, right):
    return jnp.dot(left, right, preferred_element_type=jnp.float32)


def times_rows(left, right):
    return lax.dot_general(left, right, contract_rows, preferred_element_type=jnp.float32)


def times_cols(left, right):
    return lax.dot_general(left, right, contract_cols, preferred_element_type=jnp.float32)


def scatter_sum(partial):
    total = lax.psum_scatter(
        partial.astype(jnp.bfloat16), "fsdp", scatter_dimension=0, tiled=True
    )
    return total.astype(jnp.float32)


def plain(
    hidden_in,
    out_grad,
    seq_lengths,
    seq_device,
    attn_gain,
    q_gain,
    k_gain,
    w_query,
    w_key,
    w_value,
    w_out,
    mlp_gain,
    w_gate,
    w_up,
    w_down,
):
    slots = hidden_in.shape[0]
    groups = H // KVH
    score_scale = HD ** (-0.5)
    segment, position = layout(seq_lengths, seq_device, lax.axis_index("fsdp"), slots)
    allowed = allowed_pairs(segment)[None, None]

    def query_path(raw, gain):
        return rotary(rmsnorm(raw.reshape(slots, H, HD), gain), position)

    def key_path(raw, gain):
        return rotary(rmsnorm(raw.reshape(slots, KVH, HD), gain), position)

    def swiglu(gate_in, up_in):
        return jax.nn.silu(gate_in) * up_in

    attn_set = (
        lax.all_gather(attn_gain, "fsdp", axis=0, tiled=True),
        lax.all_gather(q_gain, "fsdp", axis=0, tiled=True),
        lax.all_gather(k_gain, "fsdp", axis=0, tiled=True),
        lax.all_gather(w_query, "fsdp", axis=0, tiled=True),
        lax.all_gather(w_key, "fsdp", axis=0, tiled=True),
        lax.all_gather(w_value, "fsdp", axis=0, tiled=True),
        lax.all_gather(w_out, "fsdp", axis=0, tiled=True),
    )
    gain_attn, gain_query, gain_key, query_w, key_w, value_w, out_w = attn_set
    inputs = hidden_in.astype(jnp.float32)
    normed = rmsnorm(inputs, gain_attn.astype(jnp.float32)).astype(jnp.bfloat16)
    query_raw = matmul(normed, query_w)
    key_raw = matmul(normed, key_w)
    value_raw = matmul(normed, value_w)
    queries = (
        query_path(query_raw, gain_query.astype(jnp.float32))
        .astype(jnp.bfloat16)
        .reshape(slots, KVH, groups, HD)
    )
    keys = key_path(key_raw, gain_key.astype(jnp.float32)).astype(jnp.bfloat16)
    values = value_raw.astype(jnp.bfloat16).reshape(slots, KVH, HD)

    def masked_logits():
        scores = (
            jnp.einsum("qgrd,kgd->grqk", queries, keys, preferred_element_type=jnp.float32)
            * score_scale
        )
        return jnp.where(allowed, scores, masked_score)

    logits = masked_logits()
    row_top = jnp.max(logits, axis=-1, keepdims=True)
    exponent = jnp.exp(logits - row_top)
    row_total = jnp.sum(exponent, axis=-1, keepdims=True)
    log_total = row_top + jnp.log(row_total)
    weights = (exponent / row_total).astype(jnp.bfloat16)
    mixed = jnp.einsum("grqk,kgd->qgrd", weights, values, preferred_element_type=jnp.float32)
    mixed = mixed.reshape(slots, H * HD).astype(jnp.bfloat16)
    middle = inputs + matmul(mixed, out_w)
    mlp_set = (
        lax.all_gather(mlp_gain, "fsdp", axis=0, tiled=True),
        lax.all_gather(w_gate, "fsdp", axis=0, tiled=True),
        lax.all_gather(w_up, "fsdp", axis=0, tiled=True),
        lax.all_gather(w_down, "fsdp", axis=0, tiled=True),
    )
    gain_mlp, gate_w, up_w, down_w = mlp_set
    second = rmsnorm(middle, gain_mlp.astype(jnp.float32)).astype(jnp.bfloat16)
    gate_out = matmul(second, gate_w)
    up_out = matmul(second, up_w)
    hidden = swiglu(gate_out, up_out).astype(jnp.bfloat16)
    hidden_out = (middle + matmul(hidden, down_w)).astype(jnp.bfloat16)
    gain_mlp, gate_w, up_w, down_w = (
        lax.all_gather(mlp_gain, "fsdp", axis=0, tiled=True),
        lax.all_gather(w_gate, "fsdp", axis=0, tiled=True),
        lax.all_gather(w_up, "fsdp", axis=0, tiled=True),
        lax.all_gather(w_down, "fsdp", axis=0, tiled=True),
    )
    grad_down = scatter_sum(times_rows(hidden, out_grad))
    d_hidden = times_cols(out_grad, down_w)
    unused_out, swiglu_pull = jax.vjp(swiglu, gate_out, up_out)
    d_gate, d_up = swiglu_pull(d_hidden)
    d_gate_up = jnp.concatenate([d_gate.astype(jnp.bfloat16), d_up.astype(jnp.bfloat16)], axis=1)
    grad_gate_up = scatter_sum(times_rows(second, d_gate_up))
    ff_width = gate_w.shape[1]
    d_second = times_cols(d_gate_up, jnp.concatenate([gate_w, up_w], axis=1))
    unused_norm, second_pull = jax.vjp(rmsnorm, middle, gain_mlp.astype(jnp.float32))
    d_middle_norm, grad_gain_mlp = second_pull(d_second)
    d_middle = out_grad.astype(jnp.float32) + d_middle_norm
    gain_attn, gain_query, gain_key, query_w, key_w, value_w, out_w = (
        lax.all_gather(attn_gain, "fsdp", axis=0, tiled=True),
        lax.all_gather(q_gain, "fsdp", axis=0, tiled=True),
        lax.all_gather(k_gain, "fsdp", axis=0, tiled=True),
        lax.all_gather(w_query, "fsdp", axis=0, tiled=True),
        lax.all_gather(w_key, "fsdp", axis=0, tiled=True),
        lax.all_gather(w_value, "fsdp", axis=0, tiled=True),
        lax.all_gather(w_out, "fsdp", axis=0, tiled=True),
    )
    d_branch = d_middle.astype(jnp.bfloat16)
    grad_out_w = scatter_sum(times_rows(mixed, d_branch))
    d_mixed = times_cols(d_branch, out_w).astype(jnp.bfloat16).reshape(slots, KVH, groups, HD)
    probs = jnp.exp(masked_logits() - log_total)
    weights = probs.astype(jnp.bfloat16)
    d_probs = jnp.einsum("qgrd,kgd->grqk", d_mixed, values, preferred_element_type=jnp.float32)
    d_logits = probs * (d_probs - jnp.sum(probs * d_probs, axis=-1, keepdims=True))
    d_scores = (d_logits * score_scale).astype(jnp.bfloat16)
    d_values = jnp.einsum("grqk,qgrd->kgd", weights, d_mixed, preferred_element_type=jnp.float32)
    d_values = d_values.astype(jnp.bfloat16).reshape(slots, KVH * HD)
    d_queries_rot = jnp.einsum(
        "grqk,kgd->qgrd", d_scores, keys, preferred_element_type=jnp.float32
    ).reshape(slots, H, HD)
    d_keys_rot = jnp.einsum("grqk,qgrd->kgd", d_scores, queries, preferred_element_type=jnp.float32)
    unused_query, query_pull = jax.vjp(query_path, query_raw, gain_query.astype(jnp.float32))
    d_query_raw, grad_gain_query = query_pull(d_queries_rot)
    unused_key, key_pull = jax.vjp(key_path, key_raw, gain_key.astype(jnp.float32))
    d_key_raw, grad_gain_key = key_pull(d_keys_rot)
    d_qkv = jnp.concatenate(
        [d_query_raw.astype(jnp.bfloat16), d_key_raw.astype(jnp.bfloat16), d_values], axis=1
    )
    grad_qkv = scatter_sum(times_rows(normed, d_qkv))
    d_normed = times_cols(d_qkv, jnp.concatenate([query_w, key_w, value_w], axis=1))
    unused_first, first_pull = jax.vjp(rmsnorm, inputs, gain_attn.astype(jnp.float32))
    d_input_norm, grad_gain_attn = first_pull(d_normed)
    input_grad = d_middle + d_input_norm
    gain_sums = (
        lax.psum_scatter(grad_gain_attn, "fsdp", scatter_dimension=0, tiled=True),
        lax.psum_scatter(grad_gain_query, "fsdp", scatter_dimension=0, tiled=True),
        lax.psum_scatter(grad_gain_key, "fsdp", scatter_dimension=0, tiled=True),
        lax.psum_scatter(grad_gain_mlp, "fsdp", scatter_dimension=0, tiled=True),
    )
    query_width = H * HD
    key_width = KVH * HD
    grad_query_w = grad_qkv[:, :query_width]
    grad_key_w = grad_qkv[:, query_width : query_width + key_width]
    grad_value_w = grad_qkv[:, query_width + key_width :]
    grad_gate = grad_gate_up[:, :ff_width]
    grad_up = grad_gate_up[:, ff_width:]
    return (
        hidden_out,
        input_grad,
        gain_sums[0],
        gain_sums[1],
        gain_sums[2],
        grad_query_w,
        grad_key_w,
        grad_value_w,
        grad_out_w,
        gain_sums[3],
        grad_gate,
        grad_up,
        grad_down,
    )


def layered(
    hidden_in,
    out_grad,
    seq_lengths,
    seq_device,
    attn_gain,
    q_gain,
    k_gain,
    w_query,
    w_key,
    w_value,
    w_out,
    mlp_gain,
    w_gate,
    w_up,
    w_down,
):
    (
        attn_w, gate_up_w, down_w, tokens, cotangent, hidden, gate_up,
        middle, normed, qkv_raw, queries, keys, values, mixed, gains, rope,
    ) = forward(
        hidden_in, out_grad, seq_lengths, seq_device, (attn_gain, mlp_gain, q_gain, k_gain),
        w_query, w_key, w_value, w_out, w_gate, w_up, w_down,
    )
    dim = hidden_in.shape[1]
    x, small, y, grad_down, attn_sums, exchanged, *unused = backward(
        gate_up_w.reshape(-1, gate_up_w.shape[-1]),
        down_w.reshape(-1, dim),
        tokens.reshape(-1, dim),
        cotangent.reshape(-1, dim),
        hidden, gate_up, attn_w, middle, normed, qkv_raw, queries, keys, values, mixed,
        hidden_in, gains, rope,
    )
    (
        hidden_out, input_grad, g_query, g_key, g_value, g_out, g_gate, g_up, g_down,
        g_attn_gain, g_q_gain, g_k_gain, g_mlp_gain,
    ) = results(
        y, x, small, grad_down, attn_sums, exchanged,
        [w.shape[1] for w in (w_query, w_key, w_value, w_out)],
        [g.shape[0] for g in (attn_gain, q_gain, k_gain, mlp_gain)],
    )
    return (
        hidden_out,
        input_grad,
        g_attn_gain[0],
        g_q_gain[0],
        g_k_gain[0],
        g_query,
        g_key,
        g_value,
        g_out,
        g_mlp_gain[0],
        g_gate,
        g_up,
        g_down,
    )


def solution(mesh):
    per_device = layered if mesh.shape["fsdp"] == RING * LINE else plain
    return jax.shard_map(
        per_device,
        mesh=mesh,
        in_specs=(
            P("fsdp", None),
            P("fsdp", None),
            P(),
            P(),
            P("fsdp"),
            P("fsdp"),
            P("fsdp"),
            P("fsdp", None),
            P("fsdp", None),
            P("fsdp", None),
            P("fsdp", None),
            P("fsdp"),
            P("fsdp", None),
            P("fsdp", None),
            P("fsdp", None),
        ),
        out_specs=(
            P("fsdp", None),
            P("fsdp", None),
            P("fsdp"),
            P("fsdp"),
            P("fsdp"),
            P("fsdp", None),
            P("fsdp", None),
            P("fsdp", None),
            P("fsdp", None),
            P("fsdp"),
            P("fsdp", None),
            P("fsdp", None),
            P("fsdp", None),
        ),
        check_vma=False,
    )
```
